32 devices in a mesh: dp: 8 (over z, x), tp: 4 (over y, core).
Axes of the slice: x: 2, y: 2, z: 4, core: 2. Of those that a mesh axis runs over, the one named last changes fastest.
Arguments:
- main: bfloat16 [16512, 1152], P('dp', 'tp'), may hold values from -6 to 6
- long_skip: bfloat16 [16512, 1152], P('dp', 'tp'), may hold values from -6 to 6
- cotangent: bfloat16 [16512, 1152], P('dp', 'tp'), may hold values from -6 to 6
- timesteps: int32 [64], P('dp'), may hold values from 0 to 999
- loss_codes: int32 [64], P('dp'), may hold values from 0 to 7
- code_weights: float32 [8], replicated, may hold values from 0.25 to 4
- item_counts: int32 [8], P('dp'), may hold values from 4 to 8, as said below
- w_skip_main: bfloat16 [1152, 1152], P('tp'), may hold values from -0.125 to 0.125
- w_skip_long: bfloat16 [1152, 1152], P('tp'), may hold values from -0.125 to 0.125
- b_skip: float32 [1152], P('tp'), may hold values from -3 to 3
- ln1_gain: float32 [1152], P('tp'), may hold values from 0.25 to 1.75
- ln1_bias: float32 [1152], P('tp'), may hold values from -2.4 to 2.4
- w_qkv: bfloat16 [3, 1152, 1152], P(None, None, 'tp'), may hold values from -0.1875 to 0.1875
- w_proj: bfloat16 [1152, 1152], P('tp'), may hold values from -1.5 to 1.5
- b_proj: float32 [1152], P('tp'), may hold values from -3 to 3
- ln2_gain: float32 [1152], P('tp'), may hold values from 0.25 to 1.75
- ln2_bias: float32 [1152], P('tp'), may hold values from -2.4 to 2.4
- w_up: bfloat16 [1152, 4608], P(None, 'tp'), may hold values from -0.1875 to 0.1875
- b_up: float32 [4608], P('tp'), may hold values from -3 to 3
- w_down: bfloat16 [4608, 1152], P('tp'), may hold values from -0.09375 to 0.09375
- b_down: float32 [1152], P('tp'), may hold values from -3 to 3
Outputs:
- out: bfloat16 [16512, 1152], P('dp', 'tp')
- d_main: bfloat16 [16512, 1152], P('dp', 'tp')
- d_long: bfloat16 [16512, 1152], P('dp', 'tp')
- g_w_skip_main: float32 [1152, 1152], P('tp')
- g_w_skip_long: float32 [1152, 1152], P('tp')
- g_b_skip: float32 [1152], P('tp')
- g_ln1_gain: float32 [1152], P('tp')
- g_ln1_bias: float32 [1152], P('tp')
- g_w_qkv: float32 [3, 1152, 1152], P(None, None, 'tp')
- g_w_proj: float32 [1152, 1152], P('tp')
- g_b_proj: float32 [1152], P('tp')
- g_ln2_gain: float32 [1152], P('tp')
- g_ln2_bias: float32 [1152], P('tp')
- g_w_up: float32 [1152, 4608], P(None, 'tp')
- g_b_up: float32 [4608], P('tp')
- g_w_down: float32 [4608, 1152], P('tp')
- g_b_down: float32 [1152], P('tp')
The draws below stay inside these ranges and needn't reach their ends.
Inputs may be any that keep to these rules, and one draw needn't show every extreme that they name: `item_counts`: each batch group holds 4 to 8 items; some group is full and some holds exactly 4.
All inputs are finite; a program needn't handle non-finite values.
Results may differ from the reference program's by a relative error of at most 0.02.
Values may be sent and summed in bfloat16 or wider, within the bound.
A program may use at most 192 MiB of HBM per device.

```python
import math
import jax
import jax.numpy as jnp
from jax import lax

D = 1152
HEADS = 16
HEAD = 72
FF = 4608
SEQ = 258
SLOTS = 8
TSTEPS = 1000
CODES = 8
ITEMS = 64
TOKENS = 16512
N_DP = 8


def draw_item_counts(key, part):
    values = jax.random.randint(key, (N_DP,), SLOTS // 2, SLOTS + 1)
    full_spot = jax.random.randint(jax.random.fold_in(key, 7), (), 0, N_DP)
    offset = jax.random.randint(jax.random.fold_in(key, 11), (), 1, N_DP)
    half_spot = (full_spot + offset) % N_DP
    places = jnp.arange(N_DP, dtype=jnp.int32)
    values = jnp.where(places == full_spot, SLOTS, values)
    values = jnp.where(places == half_spot, SLOTS // 2, values)
    return values.astype(jnp.int32)


def touch_ends(values, rng, low, high):
    shape = values.shape
    spot = [jax.random.randint(jax.random.fold_in(rng, axis), (), 0, shape[axis]) for axis in range(len(shape))]
    values = values.at[tuple(spot)].set(low)
    longest = shape.index(max(shape))
    spot[longest] = (spot[longest] + 1) % shape[longest]
    return values.at[tuple(spot)].set(high)


def steps_of(key, dims, shards, least, top_value):
    factor_of, own = 1.0, jax.random.fold_in(key, 6)
    for axis_at, parts in shards:
        steps = jnp.exp(jax.random.uniform(jax.random.fold_in(own, axis_at), (parts,), jnp.float32, least / len(shards), top_value / len(shards)))
        factor_of = factor_of * jnp.repeat(steps, dims[axis_at] // parts).reshape([-1 if axis == axis_at else 1 for axis in range(len(dims))])
    return factor_of


def centred(own_key, dims, scale, reach, cuts=(), kind=jnp.bfloat16):
    values = jax.random.normal(own_key, dims, jnp.float32) * scale
    if len(cuts) > 0:
        values = steps_of(own_key, dims, cuts, -0.22, 0.18) * values
    return jnp.clip(values, min=-reach, max=reach).astype(kind)


def setup_inputs(seed: int = 0) -> dict:
    key_of = jax.random.split(jax.random.key(seed), 22)
    return {
        "main": centred(key_of[0], (TOKENS, D), 1.0, 6.0, ((0, 8), (1, 4))),
        "long_skip": centred(key_of[1], (TOKENS, D), 1.0, 6.0, ((0, 8), (1, 4))),
        "cotangent": centred(key_of[2], (TOKENS, D), 1.0, 6.0, ((0, 8), (1, 4))),
        "timesteps": touch_ends(jax.random.randint(key_of[3], (ITEMS,), 0, TSTEPS), jax.random.fold_in(key_of[3], 1), 0, TSTEPS - 1).astype(jnp.int32),
        "loss_codes": touch_ends(jax.random.randint(key_of[4], (ITEMS,), 0, CODES), jax.random.fold_in(key_of[4], 1), 0, CODES - 1).astype(jnp.int32),
        "code_weights": jnp.clip(jnp.exp(jax.random.uniform(key_of[5], (CODES,), jnp.float32, math.log(0.25), math.log(4.0))), 0.25, 4.0),
        "item_counts": draw_item_counts(jax.random.fold_in(key_of[21], 71), 0),
        "w_skip_main": centred(key_of[7], (D, D), (2 * D) ** -0.5, 0.125, ((0, 4),)),
        "w_skip_long": centred(key_of[8], (D, D), (2 * D) ** -0.5, 0.125, ((0, 4),)),
        "b_skip": centred(key_of[9], (D,), 0.5, 3.0, ((0, 4),), jnp.float32),
        "ln1_gain": jnp.clip(1.0 + 0.15 * jax.random.normal(key_of[10], (D,), jnp.float32), 0.25, 1.75),
        "ln1_bias": centred(key_of[11], (D,), 0.4, 2.4, ((0, 4),), jnp.float32),
        "w_qkv": centred(key_of[12], (3, D, D), D ** -0.5, 0.1875, ((2, 4),)),
        "w_proj": centred(key_of[13], (D, D), (D // 64) ** -0.5, 1.5, ((0, 4),)),
        "b_proj": centred(key_of[14], (D,), 0.5, 3.0, ((0, 4),), jnp.float32),
        "ln2_gain": jnp.clip(1.0 + 0.15 * jax.random.normal(key_of[15], (D,), jnp.float32), 0.25, 1.75),
        "ln2_bias": centred(key_of[16], (D,), 0.4, 2.4, ((0, 4),), jnp.float32),
        "w_up": centred(key_of[17], (D, FF), D ** -0.5, 0.1875, ((1, 4),)),
        "b_up": centred(key_of[18], (FF,), 0.5, 3.0, ((0, 4),), jnp.float32),
        "w_down": centred(key_of[19], (FF, D), FF ** -0.5, 0.09375, ((0, 4),)),
        "b_down": centred(key_of[20], (D,), 0.5, 3.0, ((0, 4),), jnp.float32),
    }


EPSILON = 1e-06

@jax.custom_vjp
def low(v):
    return lax.optimization_barrier(v.astype(jnp.bfloat16)).astype(jnp.float32)

@jax.custom_vjp
def low_back(v):
    return v

def low_keep(v):
    return (low(v), None)

def low_pass(kept, grad):
    return (grad,)

def back_keep(v):
    return (v, None)

def back_low(kept, grad):
    return (low(grad),)
low.defvjp(low_keep, low_pass)
low_back.defvjp(back_keep, back_low)

def matmul(left, right):
    return jnp.dot(left, right, precision=lax.Precision.HIGHEST)

def layer_norm(hidden, gain, bias):
    mean = lax.optimization_barrier(jnp.mean(hidden, axis=-1, keepdims=True))
    square = lax.optimization_barrier(jnp.mean(hidden * hidden, axis=-1, keepdims=True))
    rstd = lax.rsqrt(square - mean * mean + EPSILON)
    return (hidden - mean) * rstd * gain + bias

def attend_item(block):
    query_item, key_item, value_item = block
    scale = 1.0 / math.sqrt(HEAD)
    scores = low_back(jnp.einsum('ihd,jhd->hij', query_item, key_item, precision=lax.Precision.HIGHEST) * scale)
    probs = jax.nn.softmax(scores, axis=-1)
    return jnp.einsum('hij,jhd->ihd', low(probs), value_item, precision=lax.Precision.HIGHEST)

def forward(params, main_rows, long_rows):
    w_main, w_long, b_skip, gain_one, bias_one, w_qkv, w_proj, b_proj, gain_two, bias_two, w_up, b_up, w_down, b_down = params
    rows = main_rows.shape[0]
    hidden_h = low_back(matmul(main_rows, w_main) + matmul(long_rows, w_long) + b_skip)
    normed_one = low(layer_norm(hidden_h, gain_one, bias_one))
    query = low(low_back(matmul(normed_one, w_qkv[0])))
    key_part = low(low_back(matmul(normed_one, w_qkv[1])))
    value = low(low_back(matmul(normed_one, w_qkv[2])))
    shape = (rows // SEQ, SEQ, HEADS, HEAD)
    attended = lax.map(jax.checkpoint(attend_item), (query.reshape(shape), key_part.reshape(shape), value.reshape(shape)))
    attended = low(low_back(attended.reshape(rows, D)))
    hidden_two = low_back(hidden_h + matmul(attended, w_proj) + b_proj)
    normed_two = low(layer_norm(hidden_two, gain_two, bias_two))
    upward = low_back(matmul(normed_two, w_up) + b_up)
    activated = low(jax.nn.gelu(upward, approximate=False))
    return hidden_two + matmul(activated, w_down) + b_down

def reference(main, long_skip, cotangent, timesteps, loss_codes, code_weights, item_counts, w_skip_main, w_skip_long, b_skip, ln1_gain, ln1_bias, w_qkv, w_proj, b_proj, ln2_gain, ln2_bias, w_up, b_up, w_down, b_down):
    params = tuple((a.astype(jnp.float32) for a in (w_skip_main, w_skip_long, b_skip, ln1_gain, ln1_bias, w_qkv, w_proj, b_proj, ln2_gain, ln2_bias, w_up, b_up, w_down, b_down)))
    rows = SLOTS * SEQ
    steps_float = timesteps.astype(jnp.float32)
    phase = (steps_float / TSTEPS + 0.008) / 1.008 * (math.pi / 2.0)
    cosine = jnp.cos(phase)
    signal = cosine * cosine
    weight = jnp.minimum(1.0, 5.0 * (1.0 - signal) / signal)
    coded = code_weights[loss_codes]
    valid = (jnp.arange(SLOTS, dtype=jnp.int32)[None, :] < item_counts[:, None]).astype(jnp.float32)
    item_scale = (weight * coded).reshape(N_DP, SLOTS) * valid
    token_scale = jnp.repeat(item_scale, SEQ, axis=1)
    token_valid = jnp.repeat(valid, SEQ, axis=1)
    main_groups = main.astype(jnp.float32).reshape(N_DP, rows, D)
    long_groups = long_skip.astype(jnp.float32).reshape(N_DP, rows, D)
    cot_groups = cotangent.astype(jnp.float32).reshape(N_DP, rows, D)

    def group_step(totals, inputs):
        main_rows, long_rows, cot_rows, scale_rows, valid_rows = inputs
        result, pullback = jax.vjp(forward, params, main_rows, long_rows)
        weighted = low(cot_rows * scale_rows[:, None])
        grads, d_main_rows, d_long_rows = pullback(weighted)
        totals = jax.tree.map(lambda acc, new: acc + new, totals, grads)
        outputs = ((result * valid_rows[:, None]).astype(jnp.bfloat16), d_main_rows.astype(jnp.bfloat16), d_long_rows.astype(jnp.bfloat16))
        return (totals, outputs)
    zeros = tuple((jnp.zeros_like(p) for p in params))
    grads, (outputs, d_mains, d_longs) = lax.scan(group_step, zeros, (main_groups, long_groups, cot_groups, token_scale, token_valid))
    return (outputs.reshape(TOKENS, D), d_mains.reshape(TOKENS, D), d_longs.reshape(TOKENS, D), grads[0], grads[1], grads[2], grads[3], grads[4], grads[5], grads[6], grads[7], grads[8], grads[9], grads[10], grads[11], grads[12], grads[13])
```

```python
import math

import jax
import jax.numpy as jnp
from jax import lax
from jax.sharding import PartitionSpec as P

HEAD = 72
SEQ = 258
TSTEPS = 1000


EPSILON = 1e-06
ROOT_HALF = 0.7071067811865476
DENSITY_SCALE = 0.3989422804014327


def item_factors(timesteps, loss_codes, code_weights, group_items):
    steps_float = timesteps.astype(jnp.float32)
    phase = (steps_float / TSTEPS + 0.008) / 1.008 * (math.pi / 2.0)
    cosine = jnp.cos(phase)
    signal = cosine * cosine
    weight = jnp.minimum(1.0, 5.0 * (1.0 - signal) / signal)
    picks = (
        loss_codes[:, None] == jnp.arange(code_weights.shape[0], dtype=jnp.int32)[None, :]
    ).astype(jnp.float32)
    coded = jnp.sum(picks * code_weights[None, :], axis=1)
    valid = (jnp.arange(timesteps.shape[0], dtype=jnp.int32) < group_items).astype(jnp.float32)
    return (weight * coded * valid, valid)


def layer_norm(stream, gain, bias, width):
    totals, squares = lax.psum((jnp.sum(stream, 0), jnp.sum(stream * stream, 0)), "tp")
    mean = totals / width
    rstd = lax.rsqrt(squares / width - mean * mean + EPSILON)
    normed = (stream - mean[None, :]) * rstd[None, :]
    rounded = (normed * gain[:, None] + bias[:, None]).astype(jnp.bfloat16)
    return (normed, rstd, lax.all_gather(rounded, "tp", axis=0, tiled=True))


def norm_back(d_normed, normed, rstd, gain, width):
    g_gain = jnp.sum(d_normed * normed, 1)
    g_bias = jnp.sum(d_normed, 1)
    scaled = d_normed * gain[:, None]
    first, second = lax.psum((jnp.sum(scaled, 0), jnp.sum(scaled * normed, 0)), "tp")
    back = rstd[None, :] * (scaled - first[None, :] / width - normed * second[None, :] / width)
    return (back, g_gain, g_bias)


def reduce_back(term, local_width):
    return lax.psum_scatter(
        term(jnp.int32(0), lax.axis_size("tp") * local_width).astype(jnp.bfloat16),
        "tp",
        scatter_dimension=0,
        tiled=True,
    ).astype(jnp.float32)


def fold_back(shard, pairs):
    piece = lax.all_gather(shard, "tp", axis=0, tiled=True)
    new_acts = tuple(
        (
            jnp.einsum("fc,ct->ft", weight, piece, preferred_element_type=jnp.float32)
            for weight, acts in pairs
        )
    )
    new_weights = tuple(
        (
            jnp.einsum("ft,ct->fc", acts, piece, preferred_element_type=jnp.float32)
            for weight, acts in pairs
        )
    )
    return (new_acts, new_weights)


def split_heads(flat, heads_here):
    pair_count = flat.shape[1] // (2 * SEQ)
    shaped = flat.reshape(heads_here, HEAD, pair_count, 2, SEQ)
    return jnp.moveaxis(shaped, 2, 0)


def join_heads(blocks):
    moved = jnp.moveaxis(blocks, 0, 2)
    return moved.reshape(moved.shape[0] * moved.shape[1], -1)


def attend(block):
    query_rows, key_rows, value_rows = block
    scale = 1.0 / math.sqrt(HEAD)
    scores = (
        jnp.einsum("hdbi,hdbj->hbij", query_rows, key_rows, preferred_element_type=jnp.float32)
        * scale
    )
    peak = jnp.max(scores, axis=-1, keepdims=True)
    logsum = peak + jnp.log(jnp.sum(jnp.exp(scores - peak), axis=-1, keepdims=True))
    probs = jnp.exp(scores - logsum).astype(jnp.bfloat16)
    attended = jnp.einsum("hbij,hdbj->hdbi", probs, value_rows, preferred_element_type=jnp.float32)
    return (attended.astype(jnp.bfloat16), logsum[..., 0])


def attend_back(block):
    query_rows, key_rows, value_rows, logsum, d_attended = block
    scale = 1.0 / math.sqrt(HEAD)
    scores = (
        jnp.einsum("hdbi,hdbj->hbij", query_rows, key_rows, preferred_element_type=jnp.float32)
        * scale
    )
    probs = jnp.exp(scores - logsum[..., None])
    probs_low = probs.astype(jnp.bfloat16)
    d_probs = jnp.einsum(
        "hdbi,hdbj->hbij", d_attended, value_rows, preferred_element_type=jnp.float32
    )
    delta = jnp.sum(probs * d_probs, axis=-1, keepdims=True)
    d_scores = (probs * (d_probs - delta)).astype(jnp.bfloat16)
    d_query = (
        jnp.einsum("hbij,hdbj->hdbi", d_scores, key_rows, preferred_element_type=jnp.float32)
        * scale
    )
    d_key = (
        jnp.einsum("hbij,hdbi->hdbj", d_scores, query_rows, preferred_element_type=jnp.float32)
        * scale
    )
    d_value = jnp.einsum(
        "hbij,hdbi->hdbj", probs_low, d_attended, preferred_element_type=jnp.float32
    )
    return (d_query.astype(jnp.bfloat16), d_key.astype(jnp.bfloat16), d_value.astype(jnp.bfloat16))


def body_features(
    main,
    long_skip,
    cotangent,
    timesteps,
    loss_codes,
    code_weights,
    item_counts,
    w_skip_main,
    w_skip_long,
    b_skip,
    ln1_gain,
    ln1_bias,
    w_qkv,
    w_proj,
    b_proj,
    ln2_gain,
    ln2_bias,
    w_up,
    b_up,
    w_down,
    b_down,
):
    local_width = main.shape[1]
    width = w_skip_main.shape[1]
    heads_here = local_width // HEAD
    item_scale, valid = item_factors(timesteps, loss_codes, code_weights, item_counts[0])
    row_scale = jnp.repeat(item_scale, SEQ)
    row_valid = jnp.repeat(valid, SEQ)
    main_cols = main.T
    long_cols = long_skip.T
    stream = (
        lax.psum_scatter(
            jnp.einsum("dc,dt->ct", w_skip_main, main_cols, preferred_element_type=jnp.float32)
            + jnp.einsum("dc,dt->ct", w_skip_long, long_cols, preferred_element_type=jnp.float32),
            "tp",
            scatter_dimension=0,
            tiled=True,
        )
        + b_skip[:, None]
    )
    normed_one, rstd_one, full_one = layer_norm(stream, ln1_gain, ln1_bias, width)
    qkv = jnp.einsum("edc,dt->ect", w_qkv, full_one, preferred_element_type=jnp.float32).astype(
        jnp.bfloat16
    )
    query_blocks = split_heads(qkv[0], heads_here)
    key_blocks = split_heads(qkv[1], heads_here)
    value_blocks = split_heads(qkv[2], heads_here)
    attended_blocks, logsums = lax.map(attend, (query_blocks, key_blocks, value_blocks))
    attended = join_heads(attended_blocks)
    cols_here = w_proj
    projected = lax.psum_scatter(
        jnp.einsum("rc,rt->ct", cols_here, attended, preferred_element_type=jnp.float32).astype(
            jnp.bfloat16
        ),
        "tp",
        scatter_dimension=0,
        tiled=True,
    ).astype(jnp.float32)
    stream_two = stream + projected + b_proj[:, None]
    normed_two, rstd_two, full_two = layer_norm(stream_two, ln2_gain, ln2_bias, width)
    upward = (
        jnp.einsum("dc,dt->ct", w_up, full_two, preferred_element_type=jnp.float32) + b_up[:, None]
    )
    activated = jax.nn.gelu(upward, approximate=False).astype(jnp.bfloat16)
    cols_here = w_down
    result = (
        stream_two
        + lax.psum_scatter(
            jnp.einsum(
                "fc,ft->ct", cols_here, activated, preferred_element_type=jnp.float32
            ).astype(jnp.bfloat16),
            "tp",
            scatter_dimension=0,
            tiled=True,
        ).astype(jnp.float32)
        + b_down[:, None]
    )
    out = (result * row_valid[None, :]).T.astype(jnp.bfloat16)
    grad_low = (cotangent.T.astype(jnp.float32) * row_scale[None, :]).astype(jnp.bfloat16)
    grad_wide = grad_low.astype(jnp.float32)
    g_b_down = jnp.sum(grad_wide, 1)
    (d_activated,), (g_w_down,) = fold_back(grad_low, ((w_down, activated),))
    cumulative = 0.5 * (1.0 + lax.erf(upward * ROOT_HALF))
    density = jnp.exp(-0.5 * upward * upward) * DENSITY_SCALE
    d_upward = (d_activated * (cumulative + upward * density)).astype(jnp.bfloat16)
    g_b_up = jnp.sum(d_upward.astype(jnp.float32), 1)
    g_w_up = jnp.einsum("dt,ft->df", full_two, d_upward, preferred_element_type=jnp.float32)

    def up_term(start, count_rows):
        return jnp.einsum("cf,ft->ct", w_up, d_upward, preferred_element_type=jnp.float32)

    d_normed_two = reduce_back(up_term, local_width)
    back_two, g_ln2_gain, g_ln2_bias = norm_back(
        d_normed_two, normed_two, rstd_two, ln2_gain, width
    )
    d_stream_two = (back_two + grad_wide).astype(jnp.bfloat16)
    d_stream_wide = d_stream_two.astype(jnp.float32)
    g_b_proj = jnp.sum(d_stream_wide, 1)
    (d_attended,), (g_w_proj,) = fold_back(d_stream_two, ((w_proj, attended),))
    d_attended_blocks = split_heads(d_attended.astype(jnp.bfloat16), heads_here)
    d_queries, d_keys, d_values = lax.map(
        attend_back, (query_blocks, key_blocks, value_blocks, logsums, d_attended_blocks)
    )
    d_qkv = jnp.stack([join_heads(d_queries), join_heads(d_keys), join_heads(d_values)], axis=0)
    g_w_qkv = jnp.einsum("dt,ect->edc", full_one, d_qkv, preferred_element_type=jnp.float32)

    def qkv_term(start, count_rows):
        return jnp.einsum("ecr,ert->ct", w_qkv, d_qkv, preferred_element_type=jnp.float32)

    d_normed_one = reduce_back(qkv_term, local_width)
    back_one, g_ln1_gain, g_ln1_bias = norm_back(
        d_normed_one, normed_one, rstd_one, ln1_gain, width
    )
    d_stream = (back_one + d_stream_wide).astype(jnp.bfloat16)
    g_b_skip = jnp.sum(d_stream.astype(jnp.float32), 1)
    (d_main_cols, d_long_cols), (g_w_main, g_w_long) = fold_back(
        d_stream, ((w_skip_main, main_cols), (w_skip_long, long_cols))
    )
    (
        g_w_main,
        g_w_long,
        g_b_skip,
        g_ln1_gain,
        g_ln1_bias,
        g_w_qkv,
        g_w_proj,
        g_b_proj,
        g_ln2_gain,
        g_ln2_bias,
        g_w_up,
        g_b_up,
        g_w_down,
        g_b_down,
    ) = (
        lax.psum(g_w_main.astype(jnp.bfloat16), "dp").astype(jnp.float32),
        lax.psum(g_w_long.astype(jnp.bfloat16), "dp").astype(jnp.float32),
        lax.psum(g_b_skip.astype(jnp.bfloat16), "dp").astype(jnp.float32),
        lax.psum(g_ln1_gain.astype(jnp.bfloat16), "dp").astype(jnp.float32),
        lax.psum(g_ln1_bias.astype(jnp.bfloat16), "dp").astype(jnp.float32),
        lax.psum(g_w_qkv.astype(jnp.bfloat16), "dp").astype(jnp.float32),
        lax.psum(g_w_proj.astype(jnp.bfloat16), "dp").astype(jnp.float32),
        lax.psum(g_b_proj.astype(jnp.bfloat16), "dp").astype(jnp.float32),
        lax.psum(g_ln2_gain.astype(jnp.bfloat16), "dp").astype(jnp.float32),
        lax.psum(g_ln2_bias.astype(jnp.bfloat16), "dp").astype(jnp.float32),
        lax.psum(g_w_up.astype(jnp.bfloat16), "dp").astype(jnp.float32),
        lax.psum(g_b_up.astype(jnp.bfloat16), "dp").astype(jnp.float32),
        lax.psum(g_w_down.astype(jnp.bfloat16), "dp").astype(jnp.float32),
        lax.psum(g_b_down.astype(jnp.bfloat16), "dp").astype(jnp.float32),
    )
    d_main = d_main_cols.T.astype(jnp.bfloat16)
    d_long = d_long_cols.T.astype(jnp.bfloat16)
    return (
        out,
        d_main,
        d_long,
        g_w_main,
        g_w_long,
        g_b_skip,
        g_ln1_gain,
        g_ln1_bias,
        g_w_qkv,
        g_w_proj,
        g_b_proj,
        g_ln2_gain,
        g_ln2_bias,
        g_w_up,
        g_b_up,
        g_w_down,
        g_b_down,
    )


ITEM_ROWS = 264
CORE = ("tp", 1)
ACROSS_Y = ("tp", 2)
ACROSS_X = ("dp", 1)
ACROSS_Z = ("dp", 2)
FAR_Z = ("dp", 4)


def swap(value, link):
    axis, bit = link
    return lax.ppermute(value, axis, [(i, i ^ bit) for i in range(lax.axis_size(axis))])


def side(link):
    axis, bit = link
    return (lax.axis_index(axis) // bit) % 2


def in_order(bit, mine, theirs):
    flip = bit == 1
    return jnp.stack([jnp.where(flip, theirs, mine), jnp.where(flip, mine, theirs)])


def pick(value, index):
    return lax.dynamic_index_in_dim(value, index, 0, keepdims=False)


def gather_peer_shard(shard, first, second):
    rows, cols = shard.shape
    quarters = shard.reshape(2, 2, rows // 4, cols)
    mine = pick(pick(quarters, side(second)), side(first))
    got = swap(mine, ACROSS_Y)
    pair = in_order(side(first), got, swap(got, first))
    whole = in_order(side(second), pair, swap(pair, second))
    return whole.reshape(rows, cols)


def add_low(mine, theirs):
    return (mine.astype(jnp.float32) + theirs.astype(jnp.float32)).astype(jnp.bfloat16)


def reduce_shard(mine, other, first, second):
    rows, cols = mine.shape
    total = add_low(mine, swap(other, ACROSS_Y))
    for link in (first, second):
        bit = side(link)
        halves = total.reshape(2, -1, cols)
        total = add_low(pick(halves, bit), swap(pick(halves, 1 - bit), link))
    total = add_low(total, swap(total, FAR_Z))
    for link in (second, first):
        total = in_order(side(link), total, swap(total, link)).reshape(-1, cols)
    return total


def spread_tokens(block):
    cols = block.shape[1]
    padded = jnp.pad(block.reshape(-1, SEQ, cols), ((0, 0), (0, ITEM_ROWS - SEQ), (0, 0)))
    return padded.reshape(2, 2, -1, cols)


def exchange_in(block):
    tokens = spread_tokens(block)
    y, core = side(ACROSS_Y), side(CORE)
    near = pick(tokens, y)
    far = swap(pick(tokens, 1 - y), ACROSS_Y)
    both = jnp.concatenate([near, far], axis=2)
    mine = pick(both, core)
    theirs = pick(both, 1 - core)
    return mine, theirs, swap(theirs, CORE)


def exchange_out(own_half, partner_half):
    core, y = side(CORE), side(ACROSS_Y)
    both = in_order(core, own_half, swap(partner_half, CORE))
    width = own_half.shape[1] // 2
    near, far = both[:, :, :width], both[:, :, width:]
    tokens = in_order(y, near, swap(far, ACROSS_Y))
    return tokens.reshape(-1, ITEM_ROWS, width)[:, :SEQ].reshape(-1, width)


def natural(own_half, partner_half, width, axis):
    flip_y, flip_core = side(ACROSS_Y) == 1, side(CORE) == 1
    r0, r2 = jnp.split(own_half, 2, axis)
    r1, r3 = jnp.split(partner_half, 2, axis)
    a0, a2 = jnp.where(flip_y, r2, r0), jnp.where(flip_y, r0, r2)
    a1, a3 = jnp.where(flip_y, r3, r1), jnp.where(flip_y, r1, r3)
    b0, b1 = jnp.where(flip_core, a1, a0), jnp.where(flip_core, a0, a1)
    b2, b3 = jnp.where(flip_core, a3, a2), jnp.where(flip_core, a2, a3)
    return (b0, b1, b2, b3)


def by_distance(blocks):
    flip_y, flip_core = side(ACROSS_Y) == 1, side(CORE) == 1
    b0, b1, b2, b3 = blocks
    a0, a1 = jnp.where(flip_core, b1, b0), jnp.where(flip_core, b0, b1)
    a2, a3 = jnp.where(flip_core, b3, b2), jnp.where(flip_core, b2, b3)
    r0, r2 = jnp.where(flip_y, a2, a0), jnp.where(flip_y, a0, a2)
    r1, r3 = jnp.where(flip_y, a3, a1), jnp.where(flip_y, a1, a3)
    return r0, r1, r2, r3


def dot(spec, left, right):
    return jnp.einsum(spec, left, right, preferred_element_type=jnp.float32)


def low(value):
    return value.astype(jnp.bfloat16)


def norm_rows(stream, gain, bias):
    mean = jnp.mean(stream, 1, keepdims=True)
    square = jnp.mean(stream * stream, 1, keepdims=True)
    rstd = lax.rsqrt(square - mean * mean + EPSILON)
    normed = (stream - mean) * rstd
    return normed, rstd, low(normed * gain + bias)


def norm_rows_back(d_out, normed, rstd, gain):
    g_gain = jnp.sum(d_out * normed, 0)
    g_bias = jnp.sum(d_out, 0)
    scaled = d_out * gain
    first = jnp.mean(scaled, 1, keepdims=True)
    second = jnp.mean(scaled * normed, 1, keepdims=True)
    return rstd * (scaled - first - normed * second), g_gain, g_bias


def heads_of(rows):
    return rows.reshape(-1, ITEM_ROWS, rows.shape[1] // HEAD, HEAD)


def item_scores(query, key):
    scores = dot("bqhd,bkhd->bhqk", query, key) * (1.0 / math.sqrt(HEAD))
    present = lax.broadcasted_iota(jnp.int32, scores.shape, 3) < SEQ
    return jnp.where(present, scores, -1e30)


def item_attend(query, key, value):
    query, key, value = heads_of(query), heads_of(key), heads_of(value)
    scores = item_scores(query, key)
    peak = jnp.max(scores, axis=-1, keepdims=True)
    logsum = peak + jnp.log(jnp.sum(jnp.exp(scores - peak), axis=-1, keepdims=True))
    probs = low(jnp.exp(scores - logsum))
    out = low(dot("bhqk,bkhd->bqhd", probs, value))
    return out.reshape(-1, out.shape[2] * HEAD), logsum


def item_attend_back(query, key, value, logsum, d_out):
    query, key, value, d_out = heads_of(query), heads_of(key), heads_of(value), heads_of(d_out)
    scale = 1.0 / math.sqrt(HEAD)
    probs = jnp.exp(item_scores(query, key) - logsum)
    d_probs = dot("bqhd,bkhd->bhqk", d_out, value)
    delta = jnp.sum(probs * d_probs, axis=-1, keepdims=True)
    d_scores = low(probs * (d_probs - delta))
    d_query = low(dot("bhqk,bkhd->bqhd", d_scores, key) * scale)
    d_key = low(dot("bhqk,bqhd->bkhd", d_scores, query) * scale)
    d_value = low(dot("bhqk,bqhd->bkhd", low(probs), d_out))
    flat = lambda a: a.reshape(-1, a.shape[2] * HEAD)
    return flat(d_query), flat(d_key), flat(d_value)


def body_items(
    main,
    long_skip,
    cotangent,
    timesteps,
    loss_codes,
    code_weights,
    item_counts,
    w_skip_main,
    w_skip_long,
    b_skip,
    ln1_gain,
    ln1_bias,
    w_qkv,
    w_proj,
    b_proj,
    ln2_gain,
    ln2_bias,
    w_up,
    b_up,
    w_down,
    b_down,
):
    local = main.shape[1]
    width = 4 * local
    rank = lax.axis_index("tp")
    a_order, b_order = (ACROSS_X, ACROSS_Z), (ACROSS_Z, ACROSS_X)

    vectors = jnp.concatenate(
        [jnp.stack([b_skip, ln1_gain, ln1_bias, b_proj, ln2_gain, ln2_bias, b_down]), b_up.reshape(4, local)]
    )
    own_vectors = jnp.concatenate([vectors, swap(vectors, ACROSS_Y)], axis=1)
    partner_vectors = swap(own_vectors, CORE)
    joined = jnp.concatenate(natural(own_vectors[:7], partner_vectors[:7], local, 1), axis=1)
    b_skip_all, gain_one, bias_one, b_proj_all, gain_two, bias_two, b_down_all = (
        joined[k : k + 1] for k in range(7)
    )

    def up_vector(pair):
        near, far = jnp.split(pair[7:], 2, 1)
        return jnp.concatenate([near.reshape(1, -1), far.reshape(1, -1)], axis=1)

    b_up_own, b_up_partner = up_vector(own_vectors), up_vector(partner_vectors)

    main_own, main_pass, main_partner = exchange_in(main)
    long_own, long_pass, long_partner = exchange_in(long_skip)

    def halves(shard, order):
        own = jnp.stack([shard, gather_peer_shard(shard, *order)])
        return own, swap(own, CORE)

    wm_own, wm_partner = halves(w_skip_main, a_order)
    wl_own, wl_partner = halves(w_skip_long, b_order)
    qkv_rows = jnp.swapaxes(w_qkv, 1, 2)
    wq = halves(qkv_rows[0], a_order)
    wk = halves(qkv_rows[1], b_order)
    wv = halves(qkv_rows[2], a_order)
    wp_own, wp_partner = halves(w_proj, b_order)

    def tall(shard):
        top = gather_peer_shard(shard[: 2 * local], *a_order)
        bottom = gather_peer_shard(shard[2 * local :], *b_order)
        own = jnp.stack([shard, jnp.concatenate([top, bottom])])
        return own, swap(own, CORE)

    wu_own, wu_partner = tall(w_up)
    wd_own, wd_partner = tall(w_down)
    cot_own, cot_pass, cot_partner = exchange_in(cotangent)

    flat = lambda w: w.reshape(-1, w.shape[-1])
    stream = (
        dot("td,dc->tc", main_own, flat(wm_own))
        + dot("td,dc->tc", main_partner, flat(wm_partner))
        + dot("td,dc->tc", long_own, flat(wl_own))
        + dot("td,dc->tc", long_partner, flat(wl_partner))
        + b_skip_all
    )
    normed_one, rstd_one, full_one = norm_rows(stream, gain_one, bias_one)
    n1_other = swap(full_one, CORE)
    projected = jnp.zeros_like(stream)
    kept = []
    for side_at in (0, 1):
        query, key, value = (low(dot("td,cd->tc", full_one, flat(w[side_at]))) for w in (wq, wk, wv))
        attended, logsum = item_attend(query, key, value)
        kept.append((query, key, value, logsum, attended))
        projected = projected + dot("tc,cd->td", attended, flat((wp_own, wp_partner)[side_at]))
    attended_other = swap(kept[1][4], CORE)
    stream_two = stream + projected + b_proj_all
    normed_two, rstd_two, full_two = norm_rows(stream_two, gain_two, bias_two)
    n2_other = swap(full_two, CORE)

    def up(weight, bias):
        near = dot("td,dc->tc", full_two, weight[0])
        far = dot("td,dc->tc", full_two, weight[1])
        return jnp.concatenate([near, far], axis=1) + bias

    up_own, up_partner = up(wu_own, b_up_own), up(wu_partner, b_up_partner)
    act_own, act_partner = (low(jax.nn.gelu(u, approximate=False)) for u in (up_own, up_partner))
    act_other = swap(act_partner, CORE)

    item_scale, valid = item_factors(timesteps, loss_codes, code_weights, item_counts[0])
    my_scale = pick(item_scale.reshape(4, -1), rank)
    my_valid = pick(valid.reshape(4, -1), rank)
    row_scale = jnp.repeat(my_scale, ITEM_ROWS)[:, None]
    row_valid = jnp.repeat(my_valid, ITEM_ROWS)[:, None]
    cot_rows = jnp.concatenate(natural(cot_own, cot_partner, local, 1), axis=1)
    grad_low = low(cot_rows.astype(jnp.float32) * row_scale)
    grad_other = swap(grad_low, CORE)
    grad_wide = grad_low.astype(jnp.float32)
    g_b_down = jnp.sum(grad_wide, 0)

    both = lambda mine, other: jnp.concatenate([mine, other], axis=0)
    grad_both = both(grad_low, grad_other)

    def weight_grad(left, right):
        return low(dot("tf,tc->fc", left, right))

    down_part = weight_grad(both(act_own, act_other), grad_both).reshape(2, -1, width)

    def reduce_tall(part):
        cut = 2 * local
        return jnp.concatenate(
            [
                reduce_shard(part[0, :cut], part[1, :cut], *a_order),
                reduce_shard(part[0, cut:], part[1, cut:], *b_order),
            ]
        )

    g_w_down = reduce_tall(down_part)

    result = (
        stream_two
        + dot("tf,fc->tc", act_own, flat(wd_own))
        + dot("tf,fc->tc", act_partner, flat(wd_partner))
        + b_down_all
    )
    out_rows = low(result * row_valid)
    pieces = by_distance(jnp.split(out_rows, 4, 1))
    out = exchange_out(
        jnp.concatenate([pieces[0], pieces[2]], axis=1), jnp.concatenate([pieces[1], pieces[3]], axis=1)
    )

    def up_back(upward, weight):
        d_act = dot("tc,fc->tf", grad_low, flat(weight))
        cumulative = 0.5 * (1.0 + lax.erf(upward * ROOT_HALF))
        density = jnp.exp(-0.5 * upward * upward) * DENSITY_SCALE
        return low(d_act * (cumulative + upward * density))

    d_up_partner = up_back(up_partner, wd_partner)
    d_up_other = swap(d_up_partner, CORE)
    d_up_own = up_back(up_own, wd_own)
    g_b_up_own = jnp.sum(d_up_own.astype(jnp.float32), 0)
    g_b_up_partner = jnp.sum(d_up_partner.astype(jnp.float32), 0)
    d_up_both = both(d_up_own, d_up_other)
    n2_both = both(full_two, n2_other)
    cut = d_up_own.shape[1] // 2
    up_part = jnp.stack(
        [weight_grad(n2_both, d_up_both[:, :cut]), weight_grad(n2_both, d_up_both[:, cut:])]
    )
    g_w_up = reduce_tall(up_part)

    def up_term(d_up, weight):
        return dot("tf,cf->tc", d_up[:, :cut], weight[0]) + dot("tf,cf->tc", d_up[:, cut:], weight[1])

    d_n2 = up_term(d_up_own, wu_own) + up_term(d_up_partner, wu_partner)
    back_two, g_ln2_gain, g_ln2_bias = norm_rows_back(d_n2, normed_two, rstd_two, gain_two)
    d_stream_two = low(back_two + grad_wide)
    d_stream_two_other = swap(d_stream_two, CORE)
    d_stream_wide = d_stream_two.astype(jnp.float32)
    g_b_proj = jnp.sum(d_stream_wide, 0)
    proj_part = weight_grad(
        both(kept[0][4], attended_other), both(d_stream_two, d_stream_two_other)
    ).reshape(2, -1, width)
    g_w_proj = reduce_shard(proj_part[0], proj_part[1], *b_order)

    d_qkv = []
    for side_at in (1, 0):
        d_attended = low(dot("tc,fc->tf", d_stream_two, flat((wp_own, wp_partner)[side_at])))
        d_qkv.append(item_attend_back(*kept[side_at][:4], d_attended))
    d_partner, d_own = d_qkv
    n1_both = both(full_one, n1_other)
    g_w_qkv = []
    d_n1 = jnp.zeros_like(d_n2)
    for k, (w, order) in enumerate(((wq, a_order), (wk, a_order), (wv, a_order))):
        part = weight_grad(both(d_own[k], swap(d_partner[k], CORE)), n1_both).reshape(2, -1, width)
        g_w_qkv.append(reduce_shard(part[0], part[1], *order))
        d_n1 = d_n1 + dot("tc,cd->td", d_own[k], flat(w[0])) + dot("tc,cd->td", d_partner[k], flat(w[1]))
    back_one, g_ln1_gain, g_ln1_bias = norm_rows_back(d_n1, normed_one, rstd_one, gain_one)
    d_stream = low(back_one + d_stream_wide)
    d_stream_both = both(d_stream, swap(d_stream, CORE))
    g_b_skip = jnp.sum(d_stream.astype(jnp.float32), 0)

    core = side(CORE)

    def skip_parts(own, passed, other_rows, order):
        part = weight_grad(both(own, other_rows), d_stream_both).reshape(2, -1, width)
        return reduce_shard(part[0], part[1], *order)

    g_w_main = skip_parts(main_own, None, main_pass, a_order)
    g_w_long = skip_parts(long_own, None, long_pass, b_order)
    d_main = exchange_out(
        low(dot("tc,fc->tf", d_stream, flat(wm_own))), low(dot("tc,fc->tf", d_stream, flat(wm_partner)))
    )
    d_long = exchange_out(
        low(dot("tc,fc->tf", d_stream, flat(wl_own))), low(dot("tc,fc->tf", d_stream, flat(wl_partner)))
    )

    b_up_blocks = natural(
        g_b_up_own.reshape(2, -1), g_b_up_partner.reshape(2, -1), 0, 0
    )
    small = jnp.concatenate(
        [
            jnp.stack([g_b_skip, g_ln1_gain, g_ln1_bias, g_b_proj, g_ln2_gain, g_ln2_bias, g_b_down]),
            jnp.concatenate(b_up_blocks, axis=0),
        ]
    )
    for link in (CORE, ACROSS_X, ACROSS_Z, ACROSS_Y, FAR_Z):
        small = small + swap(small, link)
    mine = pick(jnp.stack(jnp.split(small[:7], 4, 1)), rank)
    g_b_up = pick(small[7:], rank)
    wide = lambda a: a.astype(jnp.float32)
    return (
        out,
        d_main,
        d_long,
        wide(g_w_main),
        wide(g_w_long),
        mine[0],
        mine[1],
        mine[2],
        jnp.stack([wide(g.T) for g in g_w_qkv]),
        wide(g_w_proj),
        mine[3],
        mine[4],
        mine[5],
        wide(g_w_up),
        g_b_up,
        wide(g_w_down),
        mine[6],
    )


def solution(mesh):
    by_items = mesh.shape["tp"] == 4 and mesh.shape["dp"] == 8
    return jax.shard_map(
        body_items if by_items else body_features,
        mesh=mesh,
        in_specs=(
            P("dp", "tp"),
            P("dp", "tp"),
            P("dp", "tp"),
            P("dp"),
            P("dp"),
            P(),
            P("dp"),
            P("tp", None),
            P("tp", None),
            P("tp"),
            P("tp"),
            P("tp"),
            P(None, None, "tp"),
            P("tp", None),
            P("tp"),
            P("tp"),
            P("tp"),
            P(None, "tp"),
            P("tp"),
            P("tp", None),
            P("tp"),
        ),
        out_specs=(
            P("dp", "tp"),
            P("dp", "tp"),
            P("dp", "tp"),
            P("tp", None),
            P("tp", None),
            P("tp"),
            P("tp"),
            P("tp"),
            P(None, None, "tp"),
            P("tp", None),
            P("tp"),
            P("tp"),
            P("tp"),
            P(None, "tp"),
            P("tp"),
            P("tp", None),
            P("tp"),
        ),
        check_vma=False,
    )
```

```python
import functools
import math

import jax
import jax.numpy as jnp
from jax import lax
from jax.experimental import pallas as pl
from jax.experimental.pallas import tpu as pltpu
from jax.sharding import PartitionSpec as P

HEAD = 72
SEQ = 258
TSTEPS = 1000


EPSILON = 1e-06
ROOT_HALF = 0.7071067811865476
DENSITY_SCALE = 0.3989422804014327


def item_factors(timesteps, loss_codes, code_weights, group_items):
    steps_float = timesteps.astype(jnp.float32)
    phase = (steps_float / TSTEPS + 0.008) / 1.008 * (math.pi / 2.0)
    cosine = jnp.cos(phase)
    signal = cosine * cosine
    weight = jnp.minimum(1.0, 5.0 * (1.0 - signal) / signal)
    picks = (
        loss_codes[:, None] == jnp.arange(code_weights.shape[0], dtype=jnp.int32)[None, :]
    ).astype(jnp.float32)
    coded = jnp.sum(picks * code_weights[None, :], axis=1)
    valid = (jnp.arange(timesteps.shape[0], dtype=jnp.int32) < group_items).astype(jnp.float32)
    return (weight * coded * valid, valid)


def layer_norm(stream, gain, bias, width):
    totals, squares = lax.psum((jnp.sum(stream, 0), jnp.sum(stream * stream, 0)), "tp")
    mean = totals / width
    rstd = lax.rsqrt(squares / width - mean * mean + EPSILON)
    normed = (stream - mean[None, :]) * rstd[None, :]
    rounded = (normed * gain[:, None] + bias[:, None]).astype(jnp.bfloat16)
    return (normed, rstd, lax.all_gather(rounded, "tp", axis=0, tiled=True))


def norm_back(d_normed, normed, rstd, gain, width):
    g_gain = jnp.sum(d_normed * normed, 1)
    g_bias = jnp.sum(d_normed, 1)
    scaled = d_normed * gain[:, None]
    first, second = lax.psum((jnp.sum(scaled, 0), jnp.sum(scaled * normed, 0)), "tp")
    back = rstd[None, :] * (scaled - first[None, :] / width - normed * second[None, :] / width)
    return (back, g_gain, g_bias)


def reduce_back(term, local_width):
    return lax.psum_scatter(
        term(jnp.int32(0), lax.axis_size("tp") * local_width).astype(jnp.bfloat16),
        "tp",
        scatter_dimension=0,
        tiled=True,
    ).astype(jnp.float32)


def fold_back(shard, pairs):
    piece = lax.all_gather(shard, "tp", axis=0, tiled=True)
    new_acts = tuple(
        (
            jnp.einsum("fc,ct->ft", weight, piece, preferred_element_type=jnp.float32)
            for weight, acts in pairs
        )
    )
    new_weights = tuple(
        (
            jnp.einsum("ft,ct->fc", acts, piece, preferred_element_type=jnp.float32)
            for weight, acts in pairs
        )
    )
    return (new_acts, new_weights)


def split_heads(flat, heads_here):
    pair_count = flat.shape[1] // (2 * SEQ)
    shaped = flat.reshape(heads_here, HEAD, pair_count, 2, SEQ)
    return jnp.moveaxis(shaped, 2, 0)


def join_heads(blocks):
    moved = jnp.moveaxis(blocks, 0, 2)
    return moved.reshape(moved.shape[0] * moved.shape[1], -1)


def attend(block):
    query_rows, key_rows, value_rows = block
    scale = 1.0 / math.sqrt(HEAD)
    scores = (
        jnp.einsum("hdbi,hdbj->hbij", query_rows, key_rows, preferred_element_type=jnp.float32)
        * scale
    )
    peak = jnp.max(scores, axis=-1, keepdims=True)
    logsum = peak + jnp.log(jnp.sum(jnp.exp(scores - peak), axis=-1, keepdims=True))
    probs = jnp.exp(scores - logsum).astype(jnp.bfloat16)
    attended = jnp.einsum("hbij,hdbj->hdbi", probs, value_rows, preferred_element_type=jnp.float32)
    return (attended.astype(jnp.bfloat16), logsum[..., 0])


def attend_back(block):
    query_rows, key_rows, value_rows, logsum, d_attended = block
    scale = 1.0 / math.sqrt(HEAD)
    scores = (
        jnp.einsum("hdbi,hdbj->hbij", query_rows, key_rows, preferred_element_type=jnp.float32)
        * scale
    )
    probs = jnp.exp(scores - logsum[..., None])
    probs_low = probs.astype(jnp.bfloat16)
    d_probs = jnp.einsum(
        "hdbi,hdbj->hbij", d_attended, value_rows, preferred_element_type=jnp.float32
    )
    delta = jnp.sum(probs * d_probs, axis=-1, keepdims=True)
    d_scores = (probs * (d_probs - delta)).astype(jnp.bfloat16)
    d_query = (
        jnp.einsum("hbij,hdbj->hdbi", d_scores, key_rows, preferred_element_type=jnp.float32)
        * scale
    )
    d_key = (
        jnp.einsum("hbij,hdbi->hdbj", d_scores, query_rows, preferred_element_type=jnp.float32)
        * scale
    )
    d_value = jnp.einsum(
        "hbij,hdbi->hdbj", probs_low, d_attended, preferred_element_type=jnp.float32
    )
    return (d_query.astype(jnp.bfloat16), d_key.astype(jnp.bfloat16), d_value.astype(jnp.bfloat16))


def body_features(
    main,
    long_skip,
    cotangent,
    timesteps,
    loss_codes,
    code_weights,
    item_counts,
    w_skip_main,
    w_skip_long,
    b_skip,
    ln1_gain,
    ln1_bias,
    w_qkv,
    w_proj,
    b_proj,
    ln2_gain,
    ln2_bias,
    w_up,
    b_up,
    w_down,
    b_down,
):
    local_width = main.shape[1]
    width = w_skip_main.shape[1]
    heads_here = local_width // HEAD
    item_scale, valid = item_factors(timesteps, loss_codes, code_weights, item_counts[0])
    row_scale = jnp.repeat(item_scale, SEQ)
    row_valid = jnp.repeat(valid, SEQ)
    main_cols = main.T
    long_cols = long_skip.T
    stream = (
        lax.psum_scatter(
            jnp.einsum("dc,dt->ct", w_skip_main, main_cols, preferred_element_type=jnp.float32)
            + jnp.einsum("dc,dt->ct", w_skip_long, long_cols, preferred_element_type=jnp.float32),
            "tp",
            scatter_dimension=0,
            tiled=True,
        )
        + b_skip[:, None]
    )
    normed_one, rstd_one, full_one = layer_norm(stream, ln1_gain, ln1_bias, width)
    qkv = jnp.einsum("edc,dt->ect", w_qkv, full_one, preferred_element_type=jnp.float32).astype(
        jnp.bfloat16
    )
    query_blocks = split_heads(qkv[0], heads_here)
    key_blocks = split_heads(qkv[1], heads_here)
    value_blocks = split_heads(qkv[2], heads_here)
    attended_blocks, logsums = lax.map(attend, (query_blocks, key_blocks, value_blocks))
    attended = join_heads(attended_blocks)
    cols_here = w_proj
    projected = lax.psum_scatter(
        jnp.einsum("rc,rt->ct", cols_here, attended, preferred_element_type=jnp.float32).astype(
            jnp.bfloat16
        ),
        "tp",
        scatter_dimension=0,
        tiled=True,
    ).astype(jnp.float32)
    stream_two = stream + projected + b_proj[:, None]
    normed_two, rstd_two, full_two = layer_norm(stream_two, ln2_gain, ln2_bias, width)
    upward = (
        jnp.einsum("dc,dt->ct", w_up, full_two, preferred_element_type=jnp.float32) + b_up[:, None]
    )
    activated = jax.nn.gelu(upward, approximate=False).astype(jnp.bfloat16)
    cols_here = w_down
    result = (
        stream_two
        + lax.psum_scatter(
            jnp.einsum(
                "fc,ft->ct", cols_here, activated, preferred_element_type=jnp.float32
            ).astype(jnp.bfloat16),
            "tp",
            scatter_dimension=0,
            tiled=True,
        ).astype(jnp.float32)
        + b_down[:, None]
    )
    out = (result * row_valid[None, :]).T.astype(jnp.bfloat16)
    grad_low = (cotangent.T.astype(jnp.float32) * row_scale[None, :]).astype(jnp.bfloat16)
    grad_wide = grad_low.astype(jnp.float32)
    g_b_down = jnp.sum(grad_wide, 1)
    (d_activated,), (g_w_down,) = fold_back(grad_low, ((w_down, activated),))
    cumulative = 0.5 * (1.0 + lax.erf(upward * ROOT_HALF))
    density = jnp.exp(-0.5 * upward * upward) * DENSITY_SCALE
    d_upward = (d_activated * (cumulative + upward * density)).astype(jnp.bfloat16)
    g_b_up = jnp.sum(d_upward.astype(jnp.float32), 1)
    g_w_up = jnp.einsum("dt,ft->df", full_two, d_upward, preferred_element_type=jnp.float32)

    def up_term(start, count_rows):
        return jnp.einsum("cf,ft->ct", w_up, d_upward, preferred_element_type=jnp.float32)

    d_normed_two = reduce_back(up_term, local_width)
    back_two, g_ln2_gain, g_ln2_bias = norm_back(
        d_normed_two, normed_two, rstd_two, ln2_gain, width
    )
    d_stream_two = (back_two + grad_wide).astype(jnp.bfloat16)
    d_stream_wide = d_stream_two.astype(jnp.float32)
    g_b_proj = jnp.sum(d_stream_wide, 1)
    (d_attended,), (g_w_proj,) = fold_back(d_stream_two, ((w_proj, attended),))
    d_attended_blocks = split_heads(d_attended.astype(jnp.bfloat16), heads_here)
    d_queries, d_keys, d_values = lax.map(
        attend_back, (query_blocks, key_blocks, value_blocks, logsums, d_attended_blocks)
    )
    d_qkv = jnp.stack([join_heads(d_queries), join_heads(d_keys), join_heads(d_values)], axis=0)
    g_w_qkv = jnp.einsum("dt,ect->edc", full_one, d_qkv, preferred_element_type=jnp.float32)

    def qkv_term(start, count_rows):
        return jnp.einsum("ecr,ert->ct", w_qkv, d_qkv, preferred_element_type=jnp.float32)

    d_normed_one = reduce_back(qkv_term, local_width)
    back_one, g_ln1_gain, g_ln1_bias = norm_back(
        d_normed_one, normed_one, rstd_one, ln1_gain, width
    )
    d_stream = (back_one + d_stream_wide).astype(jnp.bfloat16)
    g_b_skip = jnp.sum(d_stream.astype(jnp.float32), 1)
    (d_main_cols, d_long_cols), (g_w_main, g_w_long) = fold_back(
        d_stream, ((w_skip_main, main_cols), (w_skip_long, long_cols))
    )
    (
        g_w_main,
        g_w_long,
        g_b_skip,
        g_ln1_gain,
        g_ln1_bias,
        g_w_qkv,
        g_w_proj,
        g_b_proj,
        g_ln2_gain,
        g_ln2_bias,
        g_w_up,
        g_b_up,
        g_w_down,
        g_b_down,
    ) = (
        lax.psum(g_w_main.astype(jnp.bfloat16), "dp").astype(jnp.float32),
        lax.psum(g_w_long.astype(jnp.bfloat16), "dp").astype(jnp.float32),
        lax.psum(g_b_skip.astype(jnp.bfloat16), "dp").astype(jnp.float32),
        lax.psum(g_ln1_gain.astype(jnp.bfloat16), "dp").astype(jnp.float32),
        lax.psum(g_ln1_bias.astype(jnp.bfloat16), "dp").astype(jnp.float32),
        lax.psum(g_w_qkv.astype(jnp.bfloat16), "dp").astype(jnp.float32),
        lax.psum(g_w_proj.astype(jnp.bfloat16), "dp").astype(jnp.float32),
        lax.psum(g_b_proj.astype(jnp.bfloat16), "dp").astype(jnp.float32),
        lax.psum(g_ln2_gain.astype(jnp.bfloat16), "dp").astype(jnp.float32),
        lax.psum(g_ln2_bias.astype(jnp.bfloat16), "dp").astype(jnp.float32),
        lax.psum(g_w_up.astype(jnp.bfloat16), "dp").astype(jnp.float32),
        lax.psum(g_b_up.astype(jnp.bfloat16), "dp").astype(jnp.float32),
        lax.psum(g_w_down.astype(jnp.bfloat16), "dp").astype(jnp.float32),
        lax.psum(g_b_down.astype(jnp.bfloat16), "dp").astype(jnp.float32),
    )
    d_main = d_main_cols.T.astype(jnp.bfloat16)
    d_long = d_long_cols.T.astype(jnp.bfloat16)
    return (
        out,
        d_main,
        d_long,
        g_w_main,
        g_w_long,
        g_b_skip,
        g_ln1_gain,
        g_ln1_bias,
        g_w_qkv,
        g_w_proj,
        g_b_proj,
        g_ln2_gain,
        g_ln2_bias,
        g_w_up,
        g_b_up,
        g_w_down,
        g_b_down,
    )


ITEM_ROWS = 264
GRAD_ROWS = 24
CORE = ("tp", 1)
ACROSS_Y = ("tp", 2)
ACROSS_X = ("dp", 1)
ACROSS_Z = ("dp", 2)


def swap(value, link):
    axis, bit = link
    return lax.ppermute(value, axis, [(i, i ^ bit) for i in range(lax.axis_size(axis))])


def side(link):
    axis, bit = link
    return (lax.axis_index(axis) // bit) % 2


def in_order(bit, mine, theirs):
    flip = bit == 1
    return jnp.stack([jnp.where(flip, theirs, mine), jnp.where(flip, mine, theirs)])


def pick(value, index):
    return lax.dynamic_index_in_dim(value, index, 0, keepdims=False)


def peer(value, bit):
    return value + bit - 2 * bit * ((value // bit) % 2)


def greet(peers):
    barrier = pltpu.get_barrier_semaphore()
    for where in peers:
        pl.semaphore_signal(barrier, inc=1, device_id=where, device_id_type=pl.DeviceIdType.MESH)
    pl.semaphore_wait(barrier, len(peers))


def send(source, target, send_sem, recv_sem, where):
    return pltpu.make_async_remote_copy(
        src_ref=source,
        dst_ref=target,
        send_sem=send_sem,
        recv_sem=recv_sem,
        device_id=where,
        device_id_type=pl.DeviceIdType.MESH,
    )


def gather_kernel(pieces, orders, count, *refs):
    n = len(pieces)
    arrays, outs, held = refs[:count], refs[count : 2 * count], refs[2 * count : 3 * count]
    shards = [arrays[k].at[h] for k, h in pieces]
    fulls = [[outs[k].at[place, h] for place in range(4)] for k, h in pieces]
    stage = [held[k].at[h] for k, h in pieces]
    y_sem, one_sem, two_sem, own_sem, far_sem, local_sem = refs[3 * count :]
    dp, tp = lax.axis_index("dp"), lax.axis_index("tp")
    to_core, to_y = {"tp": peer(tp, 1)}, {"tp": peer(tp, 2)}
    to_x, to_z = {"dp": peer(dp, 1)}, {"dp": peer(dp, 2)}
    bits = {"x": dp % 2, "z": (dp // 2) % 2}
    to = {"x": to_x, "z": to_z}
    greet((to_core, to_y, to_x, to_z))

    def places(k):
        first, second = orders[k]
        return first, second, bits[first], bits[second]

    def y_copy(k):
        _, _, f, s = places(k)
        return send(shards[k].at[s, f], fulls[k][1].at[s, f], y_sem.at[0, k], y_sem.at[1, k], to_y)

    def one_copy(k):
        first, _, f, s = places(k)
        part = fulls[k][1].at[s, f]
        return send(part, part, one_sem.at[0, k], one_sem.at[1, k], to[first])

    def two_copy(k):
        _, second, f, s = places(k)
        part = fulls[k][1].at[s]
        return send(part, part, two_sem.at[0, k], two_sem.at[1, k], to[second])

    def own_copy(k):
        return send(shards[k], fulls[k][2], own_sem.at[0, k], own_sem.at[1, k], to_core)

    def far_copy(k):
        return send(fulls[k][1], fulls[k][3], far_sem.at[0, k], far_sem.at[1, k], to_core)

    def load(k):
        return pltpu.make_async_copy(shards[k], stage[k], local_sem.at[0, k])

    def store(k):
        return pltpu.make_async_copy(stage[k], fulls[k][0], local_sem.at[1, k])

    for k in range(n):
        y_copy(k).start()
        own_copy(k).start()
        load(k).start()
    for step in range(n + 3):
        if step < n:
            load(step).wait()
            store(step).start()
            y_copy(step).wait_recv()
            one_copy(step).start()
        if 0 <= step - 1 < n:
            one_copy(step - 1).wait_recv()
            two_copy(step - 1).start()
        if 0 <= step - 2 < n:
            two_copy(step - 2).wait_recv()
            far_copy(step - 2).start()
    for k in range(n):
        far_copy(k).wait()
        own_copy(k).wait()
        store(k).wait()
        for copy in (y_copy(k), one_copy(k), two_copy(k)):
            copy.wait_send()


def gather_weights(arrays):
    count = len(arrays)
    pieces = [(k, h) for k, a in enumerate(arrays) for h in range(a.shape[0])]
    orders = [(("x", "z"), ("z", "x"))[at % 2] for at in range(len(pieces))]
    sems = [pltpu.SemaphoreType.DMA((2, len(pieces)))] * 6
    return pl.pallas_call(
        functools.partial(gather_kernel, pieces, orders, count),
        out_shape=[jax.ShapeDtypeStruct((4,) + a.shape, a.dtype) for a in arrays],
        in_specs=[pl.BlockSpec(memory_space=pl.ANY)] * count,
        out_specs=[pl.BlockSpec(memory_space=pl.ANY)] * count,
        scratch_shapes=[pltpu.VMEM(a.shape, a.dtype) for a in arrays] + sems,
        compiler_params=pltpu.CompilerParams(
            collective_id=1, has_side_effects=True, vmem_limit_bytes=32 * 2**20
        ),
        name="gather_weights",
    )(*arrays)


def reduce_kernel(sizes, stacked, *refs):
    parts, at = [], 0
    for whole in stacked:
        parts.append((refs[at].at[0], refs[at].at[1]) if whole else (refs[at], refs[at + 1]))
        at += 1 if whole else 2
    m, refs = len(sizes), refs[at - len(sizes) :]
    out = refs[m]
    total, from_y, from_one, from_two, from_far, final = refs[m + 1 : m + 7]
    y_sem, one_sem, two_sem, far_sem, back_two, back_one, load_sem, out_sem = refs[m + 7 :]
    chunks = total.shape[0]
    dp, tp = lax.axis_index("dp"), lax.axis_index("tp")
    to_y, to_far = {"tp": peer(tp, 2)}, {"dp": peer(dp, 4)}
    greet((to_y, to_far, {"dp": peer(dp, 1)}, {"dp": peer(dp, 2)}))

    def plan(s):
        z_first = (s % 4) // 3
        first, second = 1 + z_first, 2 - z_first
        return (
            {"dp": peer(dp, first)},
            {"dp": peer(dp, second)},
            (dp // first) % 2,
            (dp // second) % 2,
        )

    def one_copy(s):
        to_one, _, f, _ = plan(s)
        return send(total.at[s, 1 - f], from_one.at[s], one_sem.at[0, s], one_sem.at[1, s], to_one)

    def two_copy(s):
        _, to_two, f, g = plan(s)
        return send(total.at[s, f, 1 - g], from_two.at[s], two_sem.at[0, s], two_sem.at[1, s], to_two)

    def far_copy(s):
        _, _, f, g = plan(s)
        return send(total.at[s, f, g], from_far.at[s], far_sem.at[0, s], far_sem.at[1, s], to_far)

    def back_two_copy(s):
        _, to_two, f, g = plan(s)
        part = final.at[s, f, g]
        return send(part, part, back_two.at[0, s], back_two.at[1, s], to_two)

    def back_one_copy(s):
        to_one, _, f, _ = plan(s)
        part = final.at[s, f]
        return send(part, part, back_one.at[0, s], back_one.at[1, s], to_one)

    def out_copy(s):
        return pltpu.make_async_copy(final.at[s], out.at[s], out_sem.at[s])

    loads, starts = [], []
    at = 0
    for k in range(m):
        loads.append(pltpu.make_async_copy(parts[k][0], total.at[pl.ds(at, sizes[k])], load_sem.at[k]))
        loads[-1].start()
        for s in range(sizes[k]):
            y = send(parts[k][1].at[s], from_y.at[at + s], y_sem.at[0, at + s], y_sem.at[1, at + s], to_y)
            y.start()
            starts.append(y)
        at += sizes[k]
    for copy in loads:
        copy.wait()

    def y_wait(s):
        send(total.at[s], from_y.at[s], y_sem.at[0, s], y_sem.at[1, s], to_y).wait_recv()

    def plus(left, right):
        return (left.astype(jnp.float32) + right.astype(jnp.float32)).astype(jnp.bfloat16)

    def step(t, carry):
        @pl.when(t < chunks)
        def _():
            y_wait(t)
            total[t] = plus(total[t], from_y[t])
            one_copy(t).start()

        @pl.when((t >= 1) & (t < chunks + 1))
        def _():
            s = t - 1
            _, _, f, _ = plan(s)
            one_copy(s).wait_recv()
            total[s, f] = plus(total[s, f], from_one[s])
            two_copy(s).start()

        @pl.when((t >= 2) & (t < chunks + 2))
        def _():
            s = t - 2
            _, _, f, g = plan(s)
            two_copy(s).wait_recv()
            total[s, f, g] = plus(total[s, f, g], from_two[s])
            far_copy(s).start()

        @pl.when((t >= 4) & (t < chunks + 4))
        def _():
            s = t - 4
            _, _, f, g = plan(s)
            far_copy(s).wait_recv()
            final[s, f, g] = plus(total[s, f, g], from_far[s])
            back_two_copy(s).start()

        @pl.when((t >= 5) & (t < chunks + 5))
        def _():
            back_two_copy(t - 5).wait_recv()
            back_one_copy(t - 5).start()

        @pl.when((t >= 6) & (t < chunks + 6))
        def _():
            back_one_copy(t - 6).wait_recv()
            out_copy(t - 6).start()

        return carry

    lax.fori_loop(0, chunks + 6, step, 0)

    def finish(s, carry):
        send(total.at[s], from_y.at[s], y_sem.at[0, s], y_sem.at[1, s], to_y).wait_send()
        for copy in (one_copy(s), two_copy(s), far_copy(s), back_two_copy(s), back_one_copy(s)):
            copy.wait_send()
        out_copy(s).wait()
        return carry

    lax.fori_loop(0, chunks, finish, 0)


def reduce_grads(parts):
    stacked = [not isinstance(p, tuple) for p in parts]
    arrays = [a for p in parts for a in (p if isinstance(p, tuple) else (p,))]
    sizes = tuple(p[0].shape[0] for p in parts)
    chunks = sum(sizes)
    rows, width = arrays[0].shape[-2:]
    low_type = arrays[0].dtype
    whole, half, quarter = (chunks, 2, 2, rows, width), (chunks, 2, rows, width), (chunks, rows, width)
    pair = pltpu.SemaphoreType.DMA((2, chunks))
    return pl.pallas_call(
        functools.partial(reduce_kernel, sizes, stacked),
        out_shape=jax.ShapeDtypeStruct(whole, low_type),
        in_specs=[pl.BlockSpec(memory_space=pl.ANY)] * len(arrays),
        out_specs=pl.BlockSpec(memory_space=pl.ANY),
        scratch_shapes=[
            pltpu.VMEM(whole, low_type),
            pltpu.VMEM(whole, low_type),
            pltpu.VMEM(half, low_type),
            pltpu.VMEM(quarter, low_type),
            pltpu.VMEM(quarter, low_type),
            pltpu.VMEM(whole, low_type),
            pair,
            pair,
            pair,
            pair,
            pair,
            pair,
            pltpu.SemaphoreType.DMA((len(parts),)),
            pltpu.SemaphoreType.DMA((chunks,)),
        ],
        compiler_params=pltpu.CompilerParams(
            collective_id=2, has_side_effects=True, vmem_limit_bytes=60 * 2**20
        ),
        name="reduce_grads",
    )(*arrays)


def spread_tokens(block):
    cols = block.shape[1]
    padded = jnp.pad(block.reshape(-1, SEQ, cols), ((0, 0), (0, ITEM_ROWS - SEQ), (0, 0)))
    return padded.reshape(2, 2, -1, cols)


def exchange_in(block):
    tokens = spread_tokens(block)
    y, core = side(ACROSS_Y), side(CORE)
    near = pick(tokens, y)
    far = swap(pick(tokens, 1 - y), ACROSS_Y)
    both = jnp.concatenate([near, far], axis=2)
    mine = pick(both, core)
    theirs = pick(both, 1 - core)
    return mine, theirs, swap(theirs, CORE)


def exchange_out(own_half, partner_half):
    core, y = side(CORE), side(ACROSS_Y)
    both = in_order(core, own_half, swap(partner_half, CORE))
    width = own_half.shape[1] // 2
    near, far = both[:, :, :width], both[:, :, width:]
    tokens = in_order(y, near, swap(far, ACROSS_Y))
    return tokens.reshape(-1, ITEM_ROWS, width)[:, :SEQ].reshape(-1, width)


def natural(own_half, partner_half, width, axis):
    flip_y, flip_core = side(ACROSS_Y) == 1, side(CORE) == 1
    r0, r2 = jnp.split(own_half, 2, axis)
    r1, r3 = jnp.split(partner_half, 2, axis)
    a0, a2 = jnp.where(flip_y, r2, r0), jnp.where(flip_y, r0, r2)
    a1, a3 = jnp.where(flip_y, r3, r1), jnp.where(flip_y, r1, r3)
    b0, b1 = jnp.where(flip_core, a1, a0), jnp.where(flip_core, a0, a1)
    b2, b3 = jnp.where(flip_core, a3, a2), jnp.where(flip_core, a2, a3)
    return (b0, b1, b2, b3)


def by_distance(blocks):
    flip_y, flip_core = side(ACROSS_Y) == 1, side(CORE) == 1
    b0, b1, b2, b3 = blocks
    a0, a1 = jnp.where(flip_core, b1, b0), jnp.where(flip_core, b0, b1)
    a2, a3 = jnp.where(flip_core, b3, b2), jnp.where(flip_core, b2, b3)
    r0, r2 = jnp.where(flip_y, a2, a0), jnp.where(flip_y, a0, a2)
    r1, r3 = jnp.where(flip_y, a3, a1), jnp.where(flip_y, a1, a3)
    return r0, r1, r2, r3


def dot(spec, left, right):
    return jnp.einsum(spec, left, right, preferred_element_type=jnp.float32)


def low(value):
    return value.astype(jnp.bfloat16)


def norm_rows(stream, gain, bias):
    mean = jnp.mean(stream, 1, keepdims=True)
    square = jnp.mean(stream * stream, 1, keepdims=True)
    rstd = lax.rsqrt(square - mean * mean + EPSILON)
    normed = (stream - mean) * rstd
    return normed, rstd, low(normed * gain + bias)


def norm_rows_back(d_out, normed, rstd, gain):
    g_gain = jnp.sum(d_out * normed, 0)
    g_bias = jnp.sum(d_out, 0)
    scaled = d_out * gain
    first = jnp.mean(scaled, 1, keepdims=True)
    second = jnp.mean(scaled * normed, 1, keepdims=True)
    return rstd * (scaled - first - normed * second), g_gain, g_bias


def heads_of(rows):
    return rows.reshape(-1, ITEM_ROWS, rows.shape[1] // HEAD, HEAD)


def item_scores(query, key):
    scores = dot("bqhd,bkhd->bhqk", query, key) * (1.0 / math.sqrt(HEAD))
    present = lax.broadcasted_iota(jnp.int32, scores.shape, 3) < SEQ
    return jnp.where(present, scores, -1e30)


def item_attend(query, key, value):
    query, key, value = heads_of(query), heads_of(key), heads_of(value)
    scores = item_scores(query, key)
    peak = jnp.max(scores, axis=-1, keepdims=True)
    logsum = peak + jnp.log(jnp.sum(jnp.exp(scores - peak), axis=-1, keepdims=True))
    probs = low(jnp.exp(scores - logsum))
    out = low(dot("bhqk,bkhd->bqhd", probs, value))
    return out.reshape(-1, out.shape[2] * HEAD), logsum


def item_attend_back(query, key, value, logsum, d_out):
    query, key, value, d_out = heads_of(query), heads_of(key), heads_of(value), heads_of(d_out)
    scale = 1.0 / math.sqrt(HEAD)
    probs = jnp.exp(item_scores(query, key) - logsum)
    d_probs = dot("bqhd,bkhd->bhqk", d_out, value)
    delta = jnp.sum(probs * d_probs, axis=-1, keepdims=True)
    d_scores = low(probs * (d_probs - delta))
    d_query = low(dot("bhqk,bkhd->bqhd", d_scores, key) * scale)
    d_key = low(dot("bhqk,bqhd->bkhd", d_scores, query) * scale)
    d_value = low(dot("bhqk,bqhd->bkhd", low(probs), d_out))
    flat = lambda a: a.reshape(-1, a.shape[2] * HEAD)
    return flat(d_query), flat(d_key), flat(d_value)


def body_items(
    main,
    long_skip,
    cotangent,
    timesteps,
    loss_codes,
    code_weights,
    item_counts,
    w_skip_main,
    w_skip_long,
    b_skip,
    ln1_gain,
    ln1_bias,
    w_qkv,
    w_proj,
    b_proj,
    ln2_gain,
    ln2_bias,
    w_up,
    b_up,
    w_down,
    b_down,
):
    local = main.shape[1]
    width = 4 * local
    rank = lax.axis_index("tp")

    vectors = jnp.concatenate(
        [jnp.stack([b_skip, ln1_gain, ln1_bias, b_proj, ln2_gain, ln2_bias, b_down]), b_up.reshape(4, local)]
    )
    own_vectors = jnp.concatenate([vectors, swap(vectors, ACROSS_Y)], axis=1)
    partner_vectors = swap(own_vectors, CORE)
    joined = jnp.concatenate(natural(own_vectors[:7], partner_vectors[:7], local, 1), axis=1)
    b_skip_all, gain_one, bias_one, b_proj_all, gain_two, bias_two, b_down_all = (
        joined[k : k + 1] for k in range(7)
    )

    def up_vector(pair):
        near, far = jnp.split(pair[7:], 2, 1)
        return jnp.concatenate([near.reshape(1, -1), far.reshape(1, -1)], axis=1)

    b_up_all = jnp.concatenate([up_vector(own_vectors), up_vector(partner_vectors)], axis=1)

    main_own, main_pass, main_partner = exchange_in(main)
    long_own, long_pass, long_partner = exchange_in(long_skip)

    cut = 2 * local
    quarters = lambda w: w.reshape(max(1, w.shape[0] // cut), 2, 2, -1, width)
    qkv_rows = jnp.swapaxes(w_qkv, 1, 2)
    gathered = gather_weights(
        [
            quarters(w)
            for w in (w_skip_main, w_skip_long, qkv_rows[0], qkv_rows[1], qkv_rows[2], w_proj, w_up, w_down)
        ]
    )
    wm, wl, wq, wk, wv, wp, wu, wd = (g.reshape(-1, width) for g in gathered)
    wu = wu.reshape(4, width, width)
    cot_own, cot_pass, cot_partner = exchange_in(cotangent)
    other = lambda value: swap(value, CORE)
    both = lambda mine, others: jnp.concatenate([mine, others], axis=0)
    shares = lambda value: both(value[:, : value.shape[1] // 2], other(value[:, value.shape[1] // 2 :]))

    main_rows = jnp.concatenate([main_own, main_partner], axis=1)
    long_rows = jnp.concatenate([long_own, long_partner], axis=1)
    stream = dot("td,dc->tc", main_rows, wm) + dot("td,dc->tc", long_rows, wl) + b_skip_all
    normed_one, rstd_one, full_one = norm_rows(stream, gain_one, bias_one)
    n1_both = both(full_one, other(full_one))
    query, key, value = (low(dot("td,cd->tc", full_one, w)) for w in (wq, wk, wv))
    attended, logsum = item_attend(query, key, value)
    attended_both = shares(attended)
    stream_two = stream + dot("tc,cd->td", attended, wp) + b_proj_all
    normed_two, rstd_two, full_two = norm_rows(stream_two, gain_two, bias_two)
    n2_both = both(full_two, other(full_two))
    upward = jnp.concatenate([dot("td,dc->tc", full_two, wu[r]) for r in range(4)], axis=1) + b_up_all
    activated = low(jax.nn.gelu(upward, approximate=False))
    act_both = shares(activated)

    item_scale, valid = item_factors(timesteps, loss_codes, code_weights, item_counts[0])
    row_scale = jnp.repeat(pick(item_scale.reshape(4, -1), rank), ITEM_ROWS)[:, None]
    row_valid = jnp.repeat(pick(valid.reshape(4, -1), rank), ITEM_ROWS)[:, None]
    cot_rows = jnp.concatenate(natural(cot_own, cot_partner, local, 1), axis=1)
    grad_low = low(cot_rows.astype(jnp.float32) * row_scale)
    grad_both = both(grad_low, other(grad_low))
    grad_wide = grad_low.astype(jnp.float32)
    g_b_down = jnp.sum(grad_wide, 0)

    result = stream_two + dot("tf,fc->tc", activated, wd) + b_down_all
    out_rows = low(result * row_valid)
    pieces = by_distance(jnp.split(out_rows, 4, 1))
    out = exchange_out(
        jnp.concatenate([pieces[0], pieces[2]], axis=1), jnp.concatenate([pieces[1], pieces[3]], axis=1)
    )

    def weight_grad(left, right, lead):
        return low(dot("tf,tc->fc", left, right)).reshape(lead + (-1, 2, 2, GRAD_ROWS, width))

    down_part = weight_grad(act_both, grad_both, (2,))
    d_act = dot("tc,fc->tf", grad_low, wd)
    cumulative = 0.5 * (1.0 + lax.erf(upward * ROOT_HALF))
    density = jnp.exp(-0.5 * upward * upward) * DENSITY_SCALE
    d_up = low(d_act * (cumulative + upward * density))
    g_b_up = jnp.sum(d_up.astype(jnp.float32), 0)
    d_up_both = shares(d_up)
    up_part = (
        weight_grad(n2_both, d_up_both[:, :width], ()),
        weight_grad(n2_both, d_up_both[:, width:], ()),
    )
    d_n2 = sum(dot("tf,cf->tc", d_up[:, r * width : (r + 1) * width], wu[r]) for r in range(4))
    back_two, g_ln2_gain, g_ln2_bias = norm_rows_back(d_n2, normed_two, rstd_two, gain_two)
    d_stream_two = low(back_two + grad_wide)
    d_stream_wide = d_stream_two.astype(jnp.float32)
    g_b_proj = jnp.sum(d_stream_wide, 0)
    proj_part = weight_grad(attended_both, both(d_stream_two, other(d_stream_two)), (2,))
    d_attended = low(dot("tc,fc->tf", d_stream_two, wp))
    d_qkv = item_attend_back(query, key, value, logsum, d_attended)
    qkv_parts = [weight_grad(shares(d), n1_both, (2,)) for d in d_qkv]
    d_n1 = sum(dot("tc,cd->td", d, w) for d, w in zip(d_qkv, (wq, wk, wv)))
    back_one, g_ln1_gain, g_ln1_bias = norm_rows_back(d_n1, normed_one, rstd_one, gain_one)
    d_stream = low(back_one + d_stream_wide)
    d_stream_both = both(d_stream, other(d_stream))
    g_b_skip = jnp.sum(d_stream.astype(jnp.float32), 0)
    main_part = weight_grad(both(main_own, main_pass), d_stream_both, (2,))
    long_part = weight_grad(both(long_own, long_pass), d_stream_both, (2,))
    d_main_rows = low(dot("tc,fc->tf", d_stream, wm))
    d_long_rows = low(dot("tc,fc->tf", d_stream, wl))
    d_main = exchange_out(d_main_rows[:, :cut], d_main_rows[:, cut:])
    d_long = exchange_out(d_long_rows[:, :cut], d_long_rows[:, cut:])

    small = jnp.stack([g_b_skip, g_ln1_gain, g_ln1_bias, g_b_proj, g_ln2_gain, g_ln2_bias, g_b_down])
    b_up_halves = g_b_up.reshape(2, 2, width)
    arrived = other(jnp.concatenate([small, b_up_halves[1]]))
    small = jnp.moveaxis((small + arrived[:7]).reshape(7, 4, local), 1, 0)
    b_up_sums = b_up_halves[0] + arrived[7:]

    def vector_rows(shard, row):
        flat = jnp.concatenate([pick(small, shard).reshape(-1), b_up_sums[row]])
        return jnp.pad(flat, (0, 4 * GRAD_ROWS * width - flat.size)).reshape(1, 2, 2, GRAD_ROWS, width)

    vector_part = low(jnp.stack([vector_rows(rank, 0), vector_rows(peer(rank, 2), 1)]))
    sums = reduce_grads(
        [down_part, up_part, proj_part] + qkv_parts + [vector_part, main_part, long_part]
    )
    sums = sums.reshape(-1, width).astype(jnp.float32)
    ends = [0]
    for rows in (width, width, local, 3 * local, 4 * GRAD_ROWS, local, local):
        ends.append(ends[-1] + rows)
    g_w_down, g_w_up, g_w_proj, g_qkv, vectors, g_w_main, g_w_long = (
        sums[a:b] for a, b in zip(ends[:-1], ends[1:])
    )
    vectors = vectors.reshape(-1)
    mine = vectors[: 7 * local].reshape(7, local)
    return (
        out,
        d_main,
        d_long,
        g_w_main,
        g_w_long,
        mine[0],
        mine[1],
        mine[2],
        jnp.swapaxes(g_qkv.reshape(3, local, width), 1, 2),
        g_w_proj,
        mine[3],
        mine[4],
        mine[5],
        g_w_up,
        vectors[7 * local : 7 * local + width],
        g_w_down,
        mine[6],
    )


def solution(mesh):
    by_items = mesh.shape["tp"] == 4 and mesh.shape["dp"] == 8
    return jax.shard_map(
        body_items if by_items else body_features,
        mesh=mesh,
        in_specs=(
            P("dp", "tp"),
            P("dp", "tp"),
            P("dp", "tp"),
            P("dp"),
            P("dp"),
            P(),
            P("dp"),
            P("tp", None),
            P("tp", None),
            P("tp"),
            P("tp"),
            P("tp"),
            P(None, None, "tp"),
            P("tp", None),
            P("tp"),
            P("tp"),
            P("tp"),
            P(None, "tp"),
            P("tp"),
            P("tp", None),
            P("tp"),
        ),
        out_specs=(
            P("dp", "tp"),
            P("dp", "tp"),
            P("dp", "tp"),
            P("tp", None),
            P("tp", None),
            P("tp"),
            P("tp"),
            P("tp"),
            P(None, None, "tp"),
            P("tp", None),
            P("tp"),
            P("tp"),
            P("tp"),
            P(None, "tp"),
            P("tp"),
            P("tp", None),
            P("tp"),
        ),
        check_vma=False,
    )
```

```python
import functools
import math

import jax
import jax.numpy as jnp
from jax import lax
from jax.experimental import pallas as pl
from jax.experimental.pallas import tpu as pltpu
from jax.sharding import PartitionSpec as P

HEAD = 72
SEQ = 258
TSTEPS = 1000


EPSILON = 1e-06
ROOT_HALF = 0.7071067811865476
DENSITY_SCALE = 0.3989422804014327


def item_factors(timesteps, loss_codes, code_weights, group_items):
    steps_float = timesteps.astype(jnp.float32)
    phase = (steps_float / TSTEPS + 0.008) / 1.008 * (math.pi / 2.0)
    cosine = jnp.cos(phase)
    signal = cosine * cosine
    weight = jnp.minimum(1.0, 5.0 * (1.0 - signal) / signal)
    picks = (
        loss_codes[:, None] == jnp.arange(code_weights.shape[0], dtype=jnp.int32)[None, :]
    ).astype(jnp.float32)
    coded = jnp.sum(picks * code_weights[None, :], axis=1)
    valid = (jnp.arange(timesteps.shape[0], dtype=jnp.int32) < group_items).astype(jnp.float32)
    return (weight * coded * valid, valid)


def layer_norm(stream, gain, bias, width):
    totals, squares = lax.psum((jnp.sum(stream, 0), jnp.sum(stream * stream, 0)), "tp")
    mean = totals / width
    rstd = lax.rsqrt(squares / width - mean * mean + EPSILON)
    normed = (stream - mean[None, :]) * rstd[None, :]
    rounded = (normed * gain[:, None] + bias[:, None]).astype(jnp.bfloat16)
    return (normed, rstd, lax.all_gather(rounded, "tp", axis=0, tiled=True))


def norm_back(d_normed, normed, rstd, gain, width):
    g_gain = jnp.sum(d_normed * normed, 1)
    g_bias = jnp.sum(d_normed, 1)
    scaled = d_normed * gain[:, None]
    first, second = lax.psum((jnp.sum(scaled, 0), jnp.sum(scaled * normed, 0)), "tp")
    back = rstd[None, :] * (scaled - first[None, :] / width - normed * second[None, :] / width)
    return (back, g_gain, g_bias)


def reduce_back(term, local_width):
    return lax.psum_scatter(
        term(jnp.int32(0), lax.axis_size("tp") * local_width).astype(jnp.bfloat16),
        "tp",
        scatter_dimension=0,
        tiled=True,
    ).astype(jnp.float32)


def fold_back(shard, pairs):
    piece = lax.all_gather(shard, "tp", axis=0, tiled=True)
    new_acts = tuple(
        (
            jnp.einsum("fc,ct->ft", weight, piece, preferred_element_type=jnp.float32)
            for weight, acts in pairs
        )
    )
    new_weights = tuple(
        (
            jnp.einsum("ft,ct->fc", acts, piece, preferred_element_type=jnp.float32)
            for weight, acts in pairs
        )
    )
    return (new_acts, new_weights)


def split_heads(flat, heads_here):
    pair_count = flat.shape[1] // (2 * SEQ)
    shaped = flat.reshape(heads_here, HEAD, pair_count, 2, SEQ)
    return jnp.moveaxis(shaped, 2, 0)


def join_heads(blocks):
    moved = jnp.moveaxis(blocks, 0, 2)
    return moved.reshape(moved.shape[0] * moved.shape[1], -1)


def attend(block):
    query_rows, key_rows, value_rows = block
    scale = 1.0 / math.sqrt(HEAD)
    scores = (
        jnp.einsum("hdbi,hdbj->hbij", query_rows, key_rows, preferred_element_type=jnp.float32)
        * scale
    )
    peak = jnp.max(scores, axis=-1, keepdims=True)
    logsum = peak + jnp.log(jnp.sum(jnp.exp(scores - peak), axis=-1, keepdims=True))
    probs = jnp.exp(scores - logsum).astype(jnp.bfloat16)
    attended = jnp.einsum("hbij,hdbj->hdbi", probs, value_rows, preferred_element_type=jnp.float32)
    return (attended.astype(jnp.bfloat16), logsum[..., 0])


def attend_back(block):
    query_rows, key_rows, value_rows, logsum, d_attended = block
    scale = 1.0 / math.sqrt(HEAD)
    scores = (
        jnp.einsum("hdbi,hdbj->hbij", query_rows, key_rows, preferred_element_type=jnp.float32)
        * scale
    )
    probs = jnp.exp(scores - logsum[..., None])
    probs_low = probs.astype(jnp.bfloat16)
    d_probs = jnp.einsum(
        "hdbi,hdbj->hbij", d_attended, value_rows, preferred_element_type=jnp.float32
    )
    delta = jnp.sum(probs * d_probs, axis=-1, keepdims=True)
    d_scores = (probs * (d_probs - delta)).astype(jnp.bfloat16)
    d_query = (
        jnp.einsum("hbij,hdbj->hdbi", d_scores, key_rows, preferred_element_type=jnp.float32)
        * scale
    )
    d_key = (
        jnp.einsum("hbij,hdbi->hdbj", d_scores, query_rows, preferred_element_type=jnp.float32)
        * scale
    )
    d_value = jnp.einsum(
        "hbij,hdbi->hdbj", probs_low, d_attended, preferred_element_type=jnp.float32
    )
    return (d_query.astype(jnp.bfloat16), d_key.astype(jnp.bfloat16), d_value.astype(jnp.bfloat16))


def body_features(
    main,
    long_skip,
    cotangent,
    timesteps,
    loss_codes,
    code_weights,
    item_counts,
    w_skip_main,
    w_skip_long,
    b_skip,
    ln1_gain,
    ln1_bias,
    w_qkv,
    w_proj,
    b_proj,
    ln2_gain,
    ln2_bias,
    w_up,
    b_up,
    w_down,
    b_down,
):
    local_width = main.shape[1]
    width = w_skip_main.shape[1]
    heads_here = local_width // HEAD
    item_scale, valid = item_factors(timesteps, loss_codes, code_weights, item_counts[0])
    row_scale = jnp.repeat(item_scale, SEQ)
    row_valid = jnp.repeat(valid, SEQ)
    main_cols = main.T
    long_cols = long_skip.T
    stream = (
        lax.psum_scatter(
            jnp.einsum("dc,dt->ct", w_skip_main, main_cols, preferred_element_type=jnp.float32)
            + jnp.einsum("dc,dt->ct", w_skip_long, long_cols, preferred_element_type=jnp.float32),
            "tp",
            scatter_dimension=0,
            tiled=True,
        )
        + b_skip[:, None]
    )
    normed_one, rstd_one, full_one = layer_norm(stream, ln1_gain, ln1_bias, width)
    qkv = jnp.einsum("edc,dt->ect", w_qkv, full_one, preferred_element_type=jnp.float32).astype(
        jnp.bfloat16
    )
    query_blocks = split_heads(qkv[0], heads_here)
    key_blocks = split_heads(qkv[1], heads_here)
    value_blocks = split_heads(qkv[2], heads_here)
    attended_blocks, logsums = lax.map(attend, (query_blocks, key_blocks, value_blocks))
    attended = join_heads(attended_blocks)
    cols_here = w_proj
    projected = lax.psum_scatter(
        jnp.einsum("rc,rt->ct", cols_here, attended, preferred_element_type=jnp.float32).astype(
            jnp.bfloat16
        ),
        "tp",
        scatter_dimension=0,
        tiled=True,
    ).astype(jnp.float32)
    stream_two = stream + projected + b_proj[:, None]
    normed_two, rstd_two, full_two = layer_norm(stream_two, ln2_gain, ln2_bias, width)
    upward = (
        jnp.einsum("dc,dt->ct", w_up, full_two, preferred_element_type=jnp.float32) + b_up[:, None]
    )
    activated = jax.nn.gelu(upward, approximate=False).astype(jnp.bfloat16)
    cols_here = w_down
    result = (
        stream_two
        + lax.psum_scatter(
            jnp.einsum(
                "fc,ft->ct", cols_here, activated, preferred_element_type=jnp.float32
            ).astype(jnp.bfloat16),
            "tp",
            scatter_dimension=0,
            tiled=True,
        ).astype(jnp.float32)
        + b_down[:, None]
    )
    out = (result * row_valid[None, :]).T.astype(jnp.bfloat16)
    grad_low = (cotangent.T.astype(jnp.float32) * row_scale[None, :]).astype(jnp.bfloat16)
    grad_wide = grad_low.astype(jnp.float32)
    g_b_down = jnp.sum(grad_wide, 1)
    (d_activated,), (g_w_down,) = fold_back(grad_low, ((w_down, activated),))
    cumulative = 0.5 * (1.0 + lax.erf(upward * ROOT_HALF))
    density = jnp.exp(-0.5 * upward * upward) * DENSITY_SCALE
    d_upward = (d_activated * (cumulative + upward * density)).astype(jnp.bfloat16)
    g_b_up = jnp.sum(d_upward.astype(jnp.float32), 1)
    g_w_up = jnp.einsum("dt,ft->df", full_two, d_upward, preferred_element_type=jnp.float32)

    def up_term(start, count_rows):
        return jnp.einsum("cf,ft->ct", w_up, d_upward, preferred_element_type=jnp.float32)

    d_normed_two = reduce_back(up_term, local_width)
    back_two, g_ln2_gain, g_ln2_bias = norm_back(
        d_normed_two, normed_two, rstd_two, ln2_gain, width
    )
    d_stream_two = (back_two + grad_wide).astype(jnp.bfloat16)
    d_stream_wide = d_stream_two.astype(jnp.float32)
    g_b_proj = jnp.sum(d_stream_wide, 1)
    (d_attended,), (g_w_proj,) = fold_back(d_stream_two, ((w_proj, attended),))
    d_attended_blocks = split_heads(d_attended.astype(jnp.bfloat16), heads_here)
    d_queries, d_keys, d_values = lax.map(
        attend_back, (query_blocks, key_blocks, value_blocks, logsums, d_attended_blocks)
    )
    d_qkv = jnp.stack([join_heads(d_queries), join_heads(d_keys), join_heads(d_values)], axis=0)
    g_w_qkv = jnp.einsum("dt,ect->edc", full_one, d_qkv, preferred_element_type=jnp.float32)

    def qkv_term(start, count_rows):
        return jnp.einsum("ecr,ert->ct", w_qkv, d_qkv, preferred_element_type=jnp.float32)

    d_normed_one = reduce_back(qkv_term, local_width)
    back_one, g_ln1_gain, g_ln1_bias = norm_back(
        d_normed_one, normed_one, rstd_one, ln1_gain, width
    )
    d_stream = (back_one + d_stream_wide).astype(jnp.bfloat16)
    g_b_skip = jnp.sum(d_stream.astype(jnp.float32), 1)
    (d_main_cols, d_long_cols), (g_w_main, g_w_long) = fold_back(
        d_stream, ((w_skip_main, main_cols), (w_skip_long, long_cols))
    )
    (
        g_w_main,
        g_w_long,
        g_b_skip,
        g_ln1_gain,
        g_ln1_bias,
        g_w_qkv,
        g_w_proj,
        g_b_proj,
        g_ln2_gain,
        g_ln2_bias,
        g_w_up,
        g_b_up,
        g_w_down,
        g_b_down,
    ) = (
        lax.psum(g_w_main.astype(jnp.bfloat16), "dp").astype(jnp.float32),
        lax.psum(g_w_long.astype(jnp.bfloat16), "dp").astype(jnp.float32),
        lax.psum(g_b_skip.astype(jnp.bfloat16), "dp").astype(jnp.float32),
        lax.psum(g_ln1_gain.astype(jnp.bfloat16), "dp").astype(jnp.float32),
        lax.psum(g_ln1_bias.astype(jnp.bfloat16), "dp").astype(jnp.float32),
        lax.psum(g_w_qkv.astype(jnp.bfloat16), "dp").astype(jnp.float32),
        lax.psum(g_w_proj.astype(jnp.bfloat16), "dp").astype(jnp.float32),
        lax.psum(g_b_proj.astype(jnp.bfloat16), "dp").astype(jnp.float32),
        lax.psum(g_ln2_gain.astype(jnp.bfloat16), "dp").astype(jnp.float32),
        lax.psum(g_ln2_bias.astype(jnp.bfloat16), "dp").astype(jnp.float32),
        lax.psum(g_w_up.astype(jnp.bfloat16), "dp").astype(jnp.float32),
        lax.psum(g_b_up.astype(jnp.bfloat16), "dp").astype(jnp.float32),
        lax.psum(g_w_down.astype(jnp.bfloat16), "dp").astype(jnp.float32),
        lax.psum(g_b_down.astype(jnp.bfloat16), "dp").astype(jnp.float32),
    )
    d_main = d_main_cols.T.astype(jnp.bfloat16)
    d_long = d_long_cols.T.astype(jnp.bfloat16)
    return (
        out,
        d_main,
        d_long,
        g_w_main,
        g_w_long,
        g_b_skip,
        g_ln1_gain,
        g_ln1_bias,
        g_w_qkv,
        g_w_proj,
        g_b_proj,
        g_ln2_gain,
        g_ln2_bias,
        g_w_up,
        g_b_up,
        g_w_down,
        g_b_down,
    )


ITEM_ROWS = 264
GRAD_ROWS = 24
CORE = ("tp", 1)
ACROSS_Y = ("tp", 2)
ACROSS_X = ("dp", 1)


def swap(value, link):
    axis, bit = link
    return lax.ppermute(value, axis, [(i, i ^ bit) for i in range(lax.axis_size(axis))])


def side(link):
    axis, bit = link
    return (lax.axis_index(axis) // bit) % 2


def in_order(bit, mine, theirs):
    flip = bit == 1
    return jnp.stack([jnp.where(flip, theirs, mine), jnp.where(flip, mine, theirs)])


def pick(value, index):
    return lax.dynamic_index_in_dim(value, index, 0, keepdims=False)


def peer(value, bit):
    return value + bit - 2 * bit * ((value // bit) % 2)


def greet(peers):
    barrier = pltpu.get_barrier_semaphore()
    for where in peers:
        pl.semaphore_signal(barrier, inc=1, device_id=where, device_id_type=pl.DeviceIdType.MESH)
    pl.semaphore_wait(barrier, len(peers))


def send(source, target, sems, index, where):
    return pltpu.make_async_remote_copy(
        src_ref=source,
        dst_ref=target,
        send_sem=sems.at[0, index],
        recv_sem=sems.at[1, index],
        device_id=where,
        device_id_type=pl.DeviceIdType.MESH,
    )


def gather_kernel(pieces, n_in, n_out, *refs):
    tokens, inputs = refs[0], refs[1 : 1 + n_in]
    refs = refs[1 + n_in :]
    far_tokens, core_near, core_far = refs[:3]
    outs, held = refs[3 : 3 + n_out], refs[3 + n_out : 3 + n_out + n_in]
    y_sem, one_sem, two_sem, own_sem, far_sem, local_sem, token_sem = refs[3 + n_out + n_in :]
    n = len(pieces)
    shards = [inputs[a].at[lead] if lead else inputs[a] for a, lead, _, _ in pieces]
    stage = [held[a].at[lead] if lead else held[a] for a, lead, _, _ in pieces]
    fulls = [[outs[b].at[(place,) + tail] for place in range(4)] for _, _, b, tail in pieces]
    dp, tp = lax.axis_index("dp"), lax.axis_index("tp")
    core, y = tp % 2, (tp // 2) % 2
    to_core, to_y = {"tp": peer(tp, 1)}, {"tp": peer(tp, 2)}
    links = ({"dp": peer(dp, 1)}, {"dp": peer(dp, 2)})
    bits = (dp % 2, (dp // 2) % 2)
    greet((to_core, to_y) + links)

    def places(k):
        return k % 2, 1 - k % 2, bits[k % 2], bits[1 - k % 2]

    def y_copy(k):
        _, _, f, s = places(k)
        return send(shards[k].at[s, f], fulls[k][1].at[s, f], y_sem, k, to_y)

    def one_copy(k):
        first, _, f, s = places(k)
        part = fulls[k][1].at[s, f]
        return send(part, part, one_sem, k, links[first])

    def two_copy(k):
        _, second, _, s = places(k)
        part = fulls[k][1].at[s]
        return send(part, part, two_sem, k, links[second])

    def own_copy(k):
        return send(shards[k], fulls[k][2], own_sem, k, to_core)

    def far_copy(k):
        return send(fulls[k][1], fulls[k][3], far_sem, k, to_core)

    def load(k):
        return pltpu.make_async_copy(shards[k], stage[k], local_sem.at[0, k])

    def store(k):
        return pltpu.make_async_copy(stage[k], fulls[k][0], local_sem.at[1, k])

    token_y = send(tokens.at[1 - y], far_tokens, token_sem, 0, to_y)
    token_near = send(tokens.at[y, 1 - core], core_near, token_sem, 1, to_core)
    token_far = send(far_tokens.at[1 - core], core_far, token_sem, 2, to_core)
    for k in range(n):
        y_copy(k).start()
    token_y.start()
    token_near.start()
    for k in range(n):
        load(k).start()
        own_copy(k).start()
    for step in range(n + 2):
        if step < n:
            y_copy(step).wait_recv()
            one_copy(step).start()
            load(step).wait()
            store(step).start()
        if 0 <= step - 1 < n:
            one_copy(step - 1).wait_recv()
            two_copy(step - 1).start()
        if 0 <= step - 2 < n:
            two_copy(step - 2).wait_recv()
            far_copy(step - 2).start()
    token_y.wait_recv()
    token_far.start()
    for copy in (token_near, token_far):
        copy.wait()
    token_y.wait_send()
    for k in range(n):
        far_copy(k).wait()
        own_copy(k).wait()
        store(k).wait()
        for copy in (y_copy(k), one_copy(k), two_copy(k)):
            copy.wait_send()


def gather_weights(tokens, arrays, pieces, out_shapes):
    n = len(pieces)
    shape = lambda dims, like: jax.ShapeDtypeStruct(dims, like.dtype)
    rows = tokens.shape[2:]
    outs = [shape((2,) + rows, tokens), shape(rows, tokens), shape(rows, tokens)]
    outs += [shape(dims, arrays[0]) for dims in out_shapes]
    sems = [pltpu.SemaphoreType.DMA((2, n))] * 6 + [pltpu.SemaphoreType.DMA((2, 3))]
    return pl.pallas_call(
        functools.partial(gather_kernel, pieces, len(arrays), len(out_shapes)),
        out_shape=outs,
        in_specs=[pl.BlockSpec(memory_space=pl.ANY)] * (1 + len(arrays)),
        out_specs=[pl.BlockSpec(memory_space=pl.ANY)] * len(outs),
        scratch_shapes=[pltpu.VMEM(a.shape, a.dtype) for a in arrays] + sems,
        compiler_params=pltpu.CompilerParams(
            collective_id=1, has_side_effects=True, vmem_limit_bytes=32 * 2**20
        ),
        name="gather_weights",
    )(tokens, *arrays)


LAG = 5


def reduce_kernel(n_early, whole_sizes, views, n_arrays, *refs):
    early, arrays, blocks = refs[0], refs[1 : 1 + n_arrays], refs[1 + n_arrays]
    out, from_core, y_blocks = refs[2 + n_arrays : 5 + n_arrays]
    refs = refs[5 + n_arrays :]
    total, from_y, from_one, half, from_two, from_far, final = refs[:7]
    y_sem, one_sem, two_sem, far_sem, back_two, back_one, block_sem, load_sem, out_sem = refs[7:]
    n_whole = total.shape[0]
    chunks = n_early + n_whole
    dp, tp = lax.axis_index("dp"), lax.axis_index("tp")
    f, g = dp % 2, (dp // 2) % 2
    to_core, to_y = {"tp": peer(tp, 1)}, {"tp": peer(tp, 2)}
    to_x, to_z, to_far = {"dp": peer(dp, 1)}, {"dp": peer(dp, 2)}, {"dp": peer(dp, 4)}
    greet((to_core, to_y, to_x, to_z, to_far))

    def y_copy(r, source):
        return send(source, from_y.at[r], y_sem, r, to_y)

    def one_copy(r):
        return send(total.at[r, 1 - f], from_one.at[r], one_sem, r, to_x)

    def two_copy(s):
        return send(half.at[s, 1 - g], from_two.at[s], two_sem, s, to_z)

    def far_copy(s):
        return send(half.at[s, g], from_far.at[s], far_sem, s, to_far)

    def back_two_copy(s):
        part = final.at[s, f, g]
        return send(part, part, back_two, s, to_z)

    def back_one_copy(s):
        part = final.at[s, f]
        return send(part, part, back_one, s, to_x)

    def out_copy(s):
        return pltpu.make_async_copy(final.at[s], out.at[s], out_sem.at[s])

    early_load = pltpu.make_async_copy(early, half.at[pl.ds(0, n_early)], load_sem.at[0])
    early_load.start()
    core_blocks = [send(blocks.at[2 + k], from_core.at[k], block_sem, k, to_core) for k in range(2)]
    own_block = send(blocks.at[1], y_blocks.at[0], block_sem, 2, to_y)
    core_block = send(from_core.at[1], y_blocks.at[1], block_sem, 3, to_y)
    loads, at = [], 0
    for k, (size, (a, mine, theirs)) in enumerate(zip(whole_sizes, views)):
        source = arrays[a].at[mine]
        loads.append(pltpu.make_async_copy(source, total.at[pl.ds(at, size)], load_sem.at[1 + k]))
        loads[-1].start()
        for r in range(size):
            y_copy(at + r, arrays[a].at[theirs + (r,)]).start()
        at += size
    for copy in core_blocks:
        copy.start()
    own_block.start()
    early_load.wait()
    for copy in loads:
        copy.wait()

    def plus(left, right):
        return (left.astype(jnp.float32) + right.astype(jnp.float32)).astype(jnp.bfloat16)

    def step(t, carry):
        @pl.when(t < n_early)
        def _():
            two_copy(t).start()

        @pl.when((t >= n_early) & (t < chunks))
        def _():
            one_copy(t - n_early).wait_recv()
            half[t] = plus(total[t - n_early, f], from_one[t - n_early])
            two_copy(t).start()

        @pl.when((t >= 1) & (t < chunks + 1))
        def _():
            s = t - 1
            two_copy(s).wait_recv()
            half[s, g] = plus(half[s, g], from_two[s])
            far_copy(s).start()

        @pl.when((t >= 3) & (t < chunks + 3))
        def _():
            s = t - 3
            far_copy(s).wait_recv()
            final[s, f, g] = plus(half[s, g], from_far[s])
            back_two_copy(s).start()

        @pl.when((t >= 4) & (t < chunks + 4))
        def _():
            back_two_copy(t - 4).wait_recv()
            back_one_copy(t - 4).start()

        @pl.when((t >= 5) & (t < chunks + 5))
        def _():
            back_one_copy(t - 5).wait_recv()
            out_copy(t - 5).start()

        @pl.when((t >= LAG) & (t < LAG + n_whole))
        def _():
            r = t - LAG
            y_copy(r, total.at[r]).wait_recv()
            total[r] = plus(total[r], from_y[r])
            one_copy(r).start()

        @pl.when(t == 2)
        def _():
            for copy in core_blocks:
                copy.wait_recv()
            core_block.start()

        return carry

    lax.fori_loop(0, chunks + 5, step, 0)

    def finish_whole(r, carry):
        y_copy(r, total.at[r]).wait_send()
        one_copy(r).wait_send()
        return carry

    lax.fori_loop(0, n_whole, finish_whole, 0)

    def finish(s, carry):
        for copy in (two_copy(s), far_copy(s), back_two_copy(s), back_one_copy(s)):
            copy.wait_send()
        out_copy(s).wait()
        return carry

    lax.fori_loop(0, chunks, finish, 0)
    for copy in core_blocks:
        copy.wait_send()
    own_block.wait()
    core_block.wait()


def reduce_grads(early, arrays, views, blocks):
    sizes = tuple(arrays[a].shape[len(mine)] for a, mine, _ in views)
    n_early, n_whole = early.shape[0], sum(sizes)
    assert LAG + n_whole <= n_early + n_whole
    chunks = n_early + n_whole
    rows, width = early.shape[-2:]
    kind = early.dtype
    sem = lambda n: pltpu.SemaphoreType.DMA((2, n))
    two_blocks = jax.ShapeDtypeStruct((2,) + blocks.shape[1:], blocks.dtype)
    return pl.pallas_call(
        functools.partial(reduce_kernel, n_early, sizes, views, len(arrays)),
        out_shape=[jax.ShapeDtypeStruct((chunks, 2, 2, rows, width), kind), two_blocks, two_blocks],
        in_specs=[pl.BlockSpec(memory_space=pl.ANY)] * (2 + len(arrays)),
        out_specs=[pl.BlockSpec(memory_space=pl.ANY)] * 3,
        scratch_shapes=[
            pltpu.VMEM((n_whole, 2, 2, rows, width), kind),
            pltpu.VMEM((n_whole, 2, 2, rows, width), kind),
            pltpu.VMEM((n_whole, 2, rows, width), kind),
            pltpu.VMEM((chunks, 2, rows, width), kind),
            pltpu.VMEM((chunks, rows, width), kind),
            pltpu.VMEM((chunks, rows, width), kind),
            pltpu.VMEM((chunks, 2, 2, rows, width), kind),
            sem(n_whole),
            sem(n_whole),
            sem(chunks),
            sem(chunks),
            sem(chunks),
            sem(chunks),
            sem(4),
            pltpu.SemaphoreType.DMA((1 + len(views),)),
            pltpu.SemaphoreType.DMA((chunks,)),
        ],
        compiler_params=pltpu.CompilerParams(
            collective_id=2, has_side_effects=True, vmem_limit_bytes=56 * 2**20
        ),
        name="reduce_grads",
    )(early, *arrays, blocks)


def add_low(mine, theirs):
    return (mine.astype(jnp.float32) + theirs.astype(jnp.float32)).astype(jnp.bfloat16)


def spread_tokens(block):
    cols = block.shape[1]
    padded = jnp.pad(block.reshape(-1, SEQ, cols), ((0, 0), (0, ITEM_ROWS - SEQ), (0, 0)))
    return padded.reshape(2, 2, -1, cols)


def exchange_in(block):
    tokens = spread_tokens(block)
    y, core = side(ACROSS_Y), side(CORE)
    near = pick(tokens, y)
    far = swap(pick(tokens, 1 - y), ACROSS_Y)
    both = jnp.concatenate([near, far], axis=2)
    mine = pick(both, core)
    theirs = pick(both, 1 - core)
    return mine, theirs, swap(theirs, CORE)


def exchange_out(own_half, partner_half):
    core, y = side(CORE), side(ACROSS_Y)
    both = in_order(core, own_half, swap(partner_half, CORE))
    width = own_half.shape[1] // 2
    near, far = both[:, :, :width], both[:, :, width:]
    tokens = in_order(y, near, swap(far, ACROSS_Y))
    return tokens.reshape(-1, ITEM_ROWS, width)[:, :SEQ].reshape(-1, width)


def natural(own_half, partner_half, width, axis):
    flip_y, flip_core = side(ACROSS_Y) == 1, side(CORE) == 1
    r0, r2 = jnp.split(own_half, 2, axis)
    r1, r3 = jnp.split(partner_half, 2, axis)
    a0, a2 = jnp.where(flip_y, r2, r0), jnp.where(flip_y, r0, r2)
    a1, a3 = jnp.where(flip_y, r3, r1), jnp.where(flip_y, r1, r3)
    b0, b1 = jnp.where(flip_core, a1, a0), jnp.where(flip_core, a0, a1)
    b2, b3 = jnp.where(flip_core, a3, a2), jnp.where(flip_core, a2, a3)
    return (b0, b1, b2, b3)


def by_distance(blocks):
    flip_y, flip_core = side(ACROSS_Y) == 1, side(CORE) == 1
    b0, b1, b2, b3 = blocks
    a0, a1 = jnp.where(flip_core, b1, b0), jnp.where(flip_core, b0, b1)
    a2, a3 = jnp.where(flip_core, b3, b2), jnp.where(flip_core, b2, b3)
    r0, r2 = jnp.where(flip_y, a2, a0), jnp.where(flip_y, a0, a2)
    r1, r3 = jnp.where(flip_y, a3, a1), jnp.where(flip_y, a1, a3)
    return r0, r1, r2, r3


def dot(spec, left, right):
    return jnp.einsum(spec, left, right, preferred_element_type=jnp.float32)


def low(value):
    return value.astype(jnp.bfloat16)


def norm_rows(stream, gain, bias):
    mean = jnp.mean(stream, 1, keepdims=True)
    square = jnp.mean(stream * stream, 1, keepdims=True)
    rstd = lax.rsqrt(square - mean * mean + EPSILON)
    normed = (stream - mean) * rstd
    return normed, rstd, low(normed * gain + bias)


def norm_rows_back(d_out, normed, rstd, gain):
    g_gain = jnp.sum(d_out * normed, 0)
    g_bias = jnp.sum(d_out, 0)
    scaled = d_out * gain
    first = jnp.mean(scaled, 1, keepdims=True)
    second = jnp.mean(scaled * normed, 1, keepdims=True)
    return rstd * (scaled - first - normed * second), g_gain, g_bias


LAST = (((1,), (1,)), ((), ()))
LEAD = (((0,), (0,)), ((), ()))


def item_scores(key, query):
    scores = lax.dot_general(key, query, LAST, preferred_element_type=jnp.float32)
    present = lax.broadcasted_iota(jnp.int32, scores.shape, 0) < SEQ
    return jnp.where(present, scores * (1.0 / math.sqrt(HEAD)), -1e30)


def attend_kernel(q_ref, k_ref, v_ref, out_ref, lse_ref):
    for h in range(q_ref.shape[1] // HEAD):
        at = slice(h * HEAD, (h + 1) * HEAD)
        scores = item_scores(k_ref[:, at], q_ref[:, at])
        peak = jnp.max(scores, axis=0, keepdims=True)
        weights = jnp.exp(scores - peak)
        total = jnp.sum(weights, axis=0, keepdims=True)
        probs = (weights * (1.0 / total)).astype(jnp.bfloat16)
        out = lax.dot_general(probs, v_ref[:, at], LEAD, preferred_element_type=jnp.float32)
        out_ref[:, at] = out.astype(jnp.bfloat16)
        lse_ref[0, h : h + 1, :] = peak + jnp.log(total)


def attend_back_kernel(q_ref, k_ref, v_ref, lse_ref, d_ref, dq_ref, dk_ref, dv_ref):
    scale = 1.0 / math.sqrt(HEAD)
    for h in range(q_ref.shape[1] // HEAD):
        at = slice(h * HEAD, (h + 1) * HEAD)
        query, key, d_out = q_ref[:, at], k_ref[:, at], d_ref[:, at]
        probs = jnp.exp(item_scores(key, query) - lse_ref[0, h : h + 1, :])
        d_probs = lax.dot_general(v_ref[:, at], d_out, LAST, preferred_element_type=jnp.float32)
        delta = jnp.sum(probs * d_probs, axis=0, keepdims=True)
        d_scores = (probs * (d_probs - delta)).astype(jnp.bfloat16)
        dq = lax.dot_general(d_scores, key, LEAD, preferred_element_type=jnp.float32)
        dk = jnp.dot(d_scores, query, preferred_element_type=jnp.float32)
        dv = jnp.dot(probs.astype(jnp.bfloat16), d_out, preferred_element_type=jnp.float32)
        dq_ref[:, at] = (dq * scale).astype(jnp.bfloat16)
        dk_ref[:, at] = (dk * scale).astype(jnp.bfloat16)
        dv_ref[:, at] = dv.astype(jnp.bfloat16)


def attention(query, key, value):
    rows, cols = query.shape
    heads, items = cols // HEAD, rows // ITEM_ROWS
    block = pl.BlockSpec((ITEM_ROWS, cols), lambda i: (i, 0))
    return pl.pallas_call(
        attend_kernel,
        grid=(items,),
        out_shape=[
            jax.ShapeDtypeStruct((rows, cols), jnp.bfloat16),
            jax.ShapeDtypeStruct((items, heads, ITEM_ROWS), jnp.float32),
        ],
        in_specs=[block] * 3,
        out_specs=[block, pl.BlockSpec((1, heads, ITEM_ROWS), lambda i: (i, 0, 0))],
        cost_estimate=pl.CostEstimate(
            flops=4 * rows * ITEM_ROWS * cols, bytes_accessed=8 * rows * cols, transcendentals=rows * ITEM_ROWS * heads
        ),
        name="attend",
    )(query, key, value)


def attention_back(query, key, value, lse, d_out):
    rows, cols = query.shape
    heads, items = cols // HEAD, rows // ITEM_ROWS
    block = pl.BlockSpec((ITEM_ROWS, cols), lambda i: (i, 0))
    return pl.pallas_call(
        attend_back_kernel,
        grid=(items,),
        out_shape=[jax.ShapeDtypeStruct((rows, cols), jnp.bfloat16)] * 3,
        in_specs=[block, block, block, pl.BlockSpec((1, heads, ITEM_ROWS), lambda i: (i, 0, 0)), block],
        out_specs=[block] * 3,
        cost_estimate=pl.CostEstimate(
            flops=10 * rows * ITEM_ROWS * cols, bytes_accessed=14 * rows * cols, transcendentals=rows * ITEM_ROWS * heads
        ),
        name="attend_back",
    )(query, key, value, lse, d_out)


def body_items(
    main,
    long_skip,
    cotangent,
    timesteps,
    loss_codes,
    code_weights,
    item_counts,
    w_skip_main,
    w_skip_long,
    b_skip,
    ln1_gain,
    ln1_bias,
    w_qkv,
    w_proj,
    b_proj,
    ln2_gain,
    ln2_bias,
    w_up,
    b_up,
    w_down,
    b_down,
):
    local = main.shape[1]
    width = 4 * local
    rank = lax.axis_index("tp")

    vectors = jnp.concatenate(
        [jnp.stack([b_skip, ln1_gain, ln1_bias, b_proj, ln2_gain, ln2_bias, b_down]), b_up.reshape(4, local)]
    )
    own_vectors = jnp.concatenate([vectors, swap(vectors, ACROSS_Y)], axis=1)
    partner_vectors = swap(own_vectors, CORE)
    joined = jnp.concatenate(natural(own_vectors[:7], partner_vectors[:7], local, 1), axis=1)
    b_skip_all, gain_one, bias_one, b_proj_all, gain_two, bias_two, b_down_all = (
        joined[k : k + 1] for k in range(7)
    )

    def up_vector(pair):
        near, far = jnp.split(pair[7:], 2, 1)
        return jnp.concatenate([near.reshape(1, -1), far.reshape(1, -1)], axis=1)

    b_up_all = jnp.concatenate([up_vector(own_vectors), up_vector(partner_vectors)], axis=1)

    y, core, x = side(ACROSS_Y), side(CORE), side(ACROSS_X)
    cut = 2 * local
    quarters = lambda w: w.reshape(2, 2, -1, width)
    tokens = spread_tokens(jnp.concatenate([main, long_skip], axis=1))
    qkv_rows = jnp.swapaxes(w_qkv, 1, 2).reshape(3, 2, 2, local // 4, width)
    one = (4, 2, 2, local // 4, width)
    far_tokens, core_near, core_far, wskip, wq, wk, wv, wp = gather_weights(
        tokens,
        [quarters(w_skip_main), quarters(w_skip_long), qkv_rows, quarters(w_proj)],
        [
            (0, (), 0, (0,)),
            (1, (), 0, (1,)),
            (2, (0,), 1, ()),
            (2, (1,), 2, ()),
            (2, (2,), 3, ()),
            (3, (), 4, ()),
        ],
        [(4, 2) + one[1:], one, one, one, one],
    )
    wskip, wq, wk, wv, wp = (g.reshape(-1, width) for g in (wskip, wq, wk, wv, wp))
    near_tokens = pick(tokens, y)
    skip_rows = jnp.concatenate([pick(near_tokens, core), pick(far_tokens, core), core_near, core_far], axis=1)
    other = lambda value: swap(value, CORE)
    both = lambda mine, others: jnp.concatenate([mine, others], axis=0)
    shares = lambda value: both(value[:, : value.shape[1] // 2], other(value[:, value.shape[1] // 2 :]))
    after = lambda value, event: lax.optimization_barrier((value, event))[0]

    def four_places(shard):
        along_y = swap(shard, ACROSS_Y)
        return [shard, along_y, other(shard), other(along_y)]

    wu = four_places(after(w_up, wskip))
    cot_own, cot_pass, cot_partner = exchange_in(after(cotangent, wskip))

    stream = dot("td,dc->tc", skip_rows, wskip) + b_skip_all
    normed_one, rstd_one, full_one = norm_rows(stream, gain_one, bias_one)
    wd = four_places(after(w_down, full_one))
    n1_both = both(full_one, other(full_one))
    query, key, value = (low(dot("td,cd->tc", full_one, w)) for w in (wq, wk, wv))
    attended, logsum = attention(query, key, value)
    attended_both = shares(attended)
    stream_two = stream + dot("tc,cd->td", attended, wp) + b_proj_all
    normed_two, rstd_two, full_two = norm_rows(stream_two, gain_two, bias_two)
    n2_both = both(full_two, other(full_two))
    acts, slopes = [], []
    for r in range(4):
        upward = dot("td,dc->tc", full_two, wu[r]) + b_up_all[:, r * width : (r + 1) * width]
        cumulative = 0.5 * (1.0 + lax.erf(upward * ROOT_HALF))
        density = jnp.exp(-0.5 * upward * upward) * DENSITY_SCALE
        acts.append(low(upward * cumulative))
        slopes.append(low(cumulative + upward * density))

    item_scale, valid = item_factors(timesteps, loss_codes, code_weights, item_counts[0])
    row_scale = jnp.repeat(pick(item_scale.reshape(4, -1), rank), ITEM_ROWS)[:, None]
    row_valid = jnp.repeat(pick(valid.reshape(4, -1), rank), ITEM_ROWS)[:, None]
    cot_rows = jnp.concatenate(natural(cot_own, cot_partner, local, 1), axis=1)
    grad_low = low(cot_rows.astype(jnp.float32) * row_scale)
    grad_both = both(grad_low, other(grad_low))
    grad_wide = grad_low.astype(jnp.float32)
    g_b_down = jnp.sum(grad_wide, 0)

    def weight_grad(left, right):
        return low(dot("tf,tc->fc", left, right))

    def early_sum(mine, theirs):
        total = add_low(mine, swap(theirs, ACROSS_Y)).reshape(2, -1, width)
        return add_low(pick(total, x), swap(pick(total, 1 - x), ACROSS_X))

    down_parts = [weight_grad(both(acts[p], other(acts[2 + p])), grad_both) for p in (1, 0)]
    grad_then = after(grad_low, down_parts[0])
    down_half = early_sum(down_parts[1], down_parts[0])

    result = stream_two + sum(dot("tf,fc->tc", acts[r], wd[r]) for r in range(4)) + b_down_all
    out_rows = low(result * row_valid)
    outs = by_distance(jnp.split(out_rows, 4, 1))
    out = exchange_out(
        jnp.concatenate([outs[0], outs[2]], axis=1), jnp.concatenate([outs[1], outs[3]], axis=1)
    )

    d_up = [low(dot("tc,fc->tf", grad_then, wd[r]) * slopes[r].astype(jnp.float32)) for r in range(4)]
    g_b_up = jnp.stack([jnp.sum(d.astype(jnp.float32), 0) for d in d_up])
    up_parts = [weight_grad(n2_both, both(d_up[p], other(d_up[2 + p]))) for p in (1, 0)]
    d_up = [after(d, up_parts[0]) for d in d_up]
    up_half = early_sum(up_parts[1], up_parts[0])
    d_n2 = sum(dot("tf,cf->tc", d_up[r], wu[r]) for r in range(4))
    back_two, g_ln2_gain, g_ln2_bias = norm_rows_back(d_n2, normed_two, rstd_two, gain_two)
    d_stream_two = low(back_two + grad_wide)
    d_stream_wide = d_stream_two.astype(jnp.float32)
    g_b_proj = jnp.sum(d_stream_wide, 0)
    chunked = lambda g, lead: g.reshape(lead + (-1, 2, 2, GRAD_ROWS, width))
    proj_part = chunked(weight_grad(attended_both, both(d_stream_two, other(d_stream_two))), (2,))
    d_attended = low(dot("tc,fc->tf", d_stream_two, wp))
    d_qkv = attention_back(query, key, value, logsum, d_attended)
    d_own = jnp.concatenate([d[:, :cut] for d in d_qkv], axis=1)
    d_partner = jnp.concatenate([d[:, cut:] for d in d_qkv], axis=1)
    qkv_part = chunked(weight_grad(both(d_own, other(d_partner)), n1_both), (3, 2))
    d_n1 = sum(dot("tc,cd->td", d, w) for d, w in zip(d_qkv, (wq, wk, wv)))
    back_one, g_ln1_gain, g_ln1_bias = norm_rows_back(d_n1, normed_one, rstd_one, gain_one)
    d_stream = low(back_one + d_stream_wide)
    d_stream_both = both(d_stream, other(d_stream))
    g_b_skip = jnp.sum(d_stream.astype(jnp.float32), 0)
    passed = jnp.concatenate([pick(near_tokens, 1 - core), pick(far_tokens, 1 - core)], axis=1)
    skip_part = chunked(weight_grad(both(skip_rows[:, : 2 * cut], passed), d_stream_both), (2,))
    d_skip = low(dot("tc,fc->tf", d_stream, wskip))
    d_blocks = jnp.stack(jnp.split(d_skip, 4, 1))

    small = jnp.stack([g_b_skip, g_ln1_gain, g_ln1_bias, g_b_proj, g_ln2_gain, g_ln2_bias, g_b_down])
    arrived = other(jnp.concatenate([small, g_b_up[2:]]))
    small = jnp.moveaxis((small + arrived[:7]).reshape(7, 4, local), 1, 0)
    b_up_sums = g_b_up[:2] + arrived[7:]

    def vector_rows(shard, row):
        flat = jnp.concatenate([pick(small, shard).reshape(-1), b_up_sums[row]])
        return jnp.pad(flat, (0, 4 * GRAD_ROWS * width - flat.size)).reshape(1, 2, 2, GRAD_ROWS, width)

    vector_part = low(jnp.stack([vector_rows(rank, 0), vector_rows(peer(rank, 2), 1)]))
    early = jnp.stack([down_half, up_half]).reshape(-1, 2, GRAD_ROWS, width)
    sums, from_core, y_blocks = reduce_grads(
        early,
        [proj_part, qkv_part, vector_part, skip_part],
        [(0, (0,), (1,)), (1, (0, 0), (0, 1)), (1, (1, 0), (1, 1)), (1, (2, 0), (2, 1)), (2, (0,), (1,)), (3, (0,), (1,))],
        d_blocks,
    )
    wide = lambda value: value.astype(jnp.float32)
    n_early = early.shape[0]
    halves = sums[:n_early].reshape(2, n_early // 2, 2, 2 * GRAD_ROWS, width)
    g_w_down, g_w_up = (wide(jnp.swapaxes(h, 0, 1)).reshape(width, width) for h in halves)
    rest = sums[n_early:].reshape(-1, width)
    ends = [0]
    for rows in (local, 3 * local, 4 * GRAD_ROWS, local, local):
        ends.append(ends[-1] + rows)
    g_w_proj, g_qkv, vectors, g_w_main, g_w_long = (wide(rest[a:b]) for a, b in zip(ends[:-1], ends[1:]))
    vectors = vectors.reshape(-1)
    mine = vectors[: 7 * local].reshape(7, local)

    d_tokens = in_order(y, in_order(core, d_blocks[0], from_core[0]), in_order(core, y_blocks[0], y_blocks[1]))
    d_tokens = d_tokens.reshape(-1, ITEM_ROWS, cut)[:, :SEQ].reshape(-1, cut)
    return (
        out,
        d_tokens[:, :local],
        d_tokens[:, local:],
        g_w_main,
        g_w_long,
        mine[0],
        mine[1],
        mine[2],
        jnp.swapaxes(g_qkv.reshape(3, local, width), 1, 2),
        g_w_proj,
        mine[3],
        mine[4],
        mine[5],
        g_w_up,
        vectors[7 * local : 7 * local + width],
        g_w_down,
        mine[6],
    )


def solution(mesh):
    by_items = mesh.shape["tp"] == 4 and mesh.shape["dp"] == 8
    return jax.shard_map(
        body_items if by_items else body_features,
        mesh=mesh,
        in_specs=(
            P("dp", "tp"),
            P("dp", "tp"),
            P("dp", "tp"),
            P("dp"),
            P("dp"),
            P(),
            P("dp"),
            P("tp", None),
            P("tp", None),
            P("tp"),
            P("tp"),
            P("tp"),
            P(None, None, "tp"),
            P("tp", None),
            P("tp"),
            P("tp"),
            P("tp"),
            P(None, "tp"),
            P("tp"),
            P("tp", None),
            P("tp"),
        ),
        out_specs=(
            P("dp", "tp"),
            P("dp", "tp"),
            P("dp", "tp"),
            P("tp", None),
            P("tp", None),
            P("tp"),
            P("tp"),
            P("tp"),
            P(None, None, "tp"),
            P("tp", None),
            P("tp"),
            P("tp"),
            P("tp"),
            P(None, "tp"),
            P("tp"),
            P("tp", None),
            P("tp"),
        ),
        check_vma=False,
    )
```

```python
import functools
import math

import jax
import jax.numpy as jnp
from jax import lax
from jax.experimental import pallas as pl
from jax.experimental.pallas import tpu as pltpu
from jax.sharding import PartitionSpec as P

HEAD = 72
SEQ = 258
TSTEPS = 1000


EPSILON = 1e-06
ROOT_HALF = 0.7071067811865476
DENSITY_SCALE = 0.3989422804014327


def item_factors(timesteps, loss_codes, code_weights, group_items):
    steps_float = timesteps.astype(jnp.float32)
    phase = (steps_float / TSTEPS + 0.008) / 1.008 * (math.pi / 2.0)
    cosine = jnp.cos(phase)
    signal = cosine * cosine
    weight = jnp.minimum(1.0, 5.0 * (1.0 - signal) / signal)
    picks = (
        loss_codes[:, None] == jnp.arange(code_weights.shape[0], dtype=jnp.int32)[None, :]
    ).astype(jnp.float32)
    coded = jnp.sum(picks * code_weights[None, :], axis=1)
    valid = (jnp.arange(timesteps.shape[0], dtype=jnp.int32) < group_items).astype(jnp.float32)
    return (weight * coded * valid, valid)


def layer_norm(stream, gain, bias, width):
    totals, squares = lax.psum((jnp.sum(stream, 0), jnp.sum(stream * stream, 0)), "tp")
    mean = totals / width
    rstd = lax.rsqrt(squares / width - mean * mean + EPSILON)
    normed = (stream - mean[None, :]) * rstd[None, :]
    rounded = (normed * gain[:, None] + bias[:, None]).astype(jnp.bfloat16)
    return (normed, rstd, lax.all_gather(rounded, "tp", axis=0, tiled=True))


def norm_back(d_normed, normed, rstd, gain, width):
    g_gain = jnp.sum(d_normed * normed, 1)
    g_bias = jnp.sum(d_normed, 1)
    scaled = d_normed * gain[:, None]
    first, second = lax.psum((jnp.sum(scaled, 0), jnp.sum(scaled * normed, 0)), "tp")
    back = rstd[None, :] * (scaled - first[None, :] / width - normed * second[None, :] / width)
    return (back, g_gain, g_bias)


def reduce_back(term, local_width):
    return lax.psum_scatter(
        term(jnp.int32(0), lax.axis_size("tp") * local_width).astype(jnp.bfloat16),
        "tp",
        scatter_dimension=0,
        tiled=True,
    ).astype(jnp.float32)


def fold_back(shard, pairs):
    piece = lax.all_gather(shard, "tp", axis=0, tiled=True)
    new_acts = tuple(
        (
            jnp.einsum("fc,ct->ft", weight, piece, preferred_element_type=jnp.float32)
            for weight, acts in pairs
        )
    )
    new_weights = tuple(
        (
            jnp.einsum("ft,ct->fc", acts, piece, preferred_element_type=jnp.float32)
            for weight, acts in pairs
        )
    )
    return (new_acts, new_weights)


def split_heads(flat, heads_here):
    pair_count = flat.shape[1] // (2 * SEQ)
    shaped = flat.reshape(heads_here, HEAD, pair_count, 2, SEQ)
    return jnp.moveaxis(shaped, 2, 0)


def join_heads(blocks):
    moved = jnp.moveaxis(blocks, 0, 2)
    return moved.reshape(moved.shape[0] * moved.shape[1], -1)


def attend(block):
    query_rows, key_rows, value_rows = block
    scale = 1.0 / math.sqrt(HEAD)
    scores = (
        jnp.einsum("hdbi,hdbj->hbij", query_rows, key_rows, preferred_element_type=jnp.float32)
        * scale
    )
    peak = jnp.max(scores, axis=-1, keepdims=True)
    logsum = peak + jnp.log(jnp.sum(jnp.exp(scores - peak), axis=-1, keepdims=True))
    probs = jnp.exp(scores - logsum).astype(jnp.bfloat16)
    attended = jnp.einsum("hbij,hdbj->hdbi", probs, value_rows, preferred_element_type=jnp.float32)
    return (attended.astype(jnp.bfloat16), logsum[..., 0])


def attend_back(block):
    query_rows, key_rows, value_rows, logsum, d_attended = block
    scale = 1.0 / math.sqrt(HEAD)
    scores = (
        jnp.einsum("hdbi,hdbj->hbij", query_rows, key_rows, preferred_element_type=jnp.float32)
        * scale
    )
    probs = jnp.exp(scores - logsum[..., None])
    probs_low = probs.astype(jnp.bfloat16)
    d_probs = jnp.einsum(
        "hdbi,hdbj->hbij", d_attended, value_rows, preferred_element_type=jnp.float32
    )
    delta = jnp.sum(probs * d_probs, axis=-1, keepdims=True)
    d_scores = (probs * (d_probs - delta)).astype(jnp.bfloat16)
    d_query = (
        jnp.einsum("hbij,hdbj->hdbi", d_scores, key_rows, preferred_element_type=jnp.float32)
        * scale
    )
    d_key = (
        jnp.einsum("hbij,hdbi->hdbj", d_scores, query_rows, preferred_element_type=jnp.float32)
        * scale
    )
    d_value = jnp.einsum(
        "hbij,hdbi->hdbj", probs_low, d_attended, preferred_element_type=jnp.float32
    )
    return (d_query.astype(jnp.bfloat16), d_key.astype(jnp.bfloat16), d_value.astype(jnp.bfloat16))


def body_features(
    main,
    long_skip,
    cotangent,
    timesteps,
    loss_codes,
    code_weights,
    item_counts,
    w_skip_main,
    w_skip_long,
    b_skip,
    ln1_gain,
    ln1_bias,
    w_qkv,
    w_proj,
    b_proj,
    ln2_gain,
    ln2_bias,
    w_up,
    b_up,
    w_down,
    b_down,
):
    local_width = main.shape[1]
    width = w_skip_main.shape[1]
    heads_here = local_width // HEAD
    item_scale, valid = item_factors(timesteps, loss_codes, code_weights, item_counts[0])
    row_scale = jnp.repeat(item_scale, SEQ)
    row_valid = jnp.repeat(valid, SEQ)
    main_cols = main.T
    long_cols = long_skip.T
    stream = (
        lax.psum_scatter(
            jnp.einsum("dc,dt->ct", w_skip_main, main_cols, preferred_element_type=jnp.float32)
            + jnp.einsum("dc,dt->ct", w_skip_long, long_cols, preferred_element_type=jnp.float32),
            "tp",
            scatter_dimension=0,
            tiled=True,
        )
        + b_skip[:, None]
    )
    normed_one, rstd_one, full_one = layer_norm(stream, ln1_gain, ln1_bias, width)
    qkv = jnp.einsum("edc,dt->ect", w_qkv, full_one, preferred_element_type=jnp.float32).astype(
        jnp.bfloat16
    )
    query_blocks = split_heads(qkv[0], heads_here)
    key_blocks = split_heads(qkv[1], heads_here)
    value_blocks = split_heads(qkv[2], heads_here)
    attended_blocks, logsums = lax.map(attend, (query_blocks, key_blocks, value_blocks))
    attended = join_heads(attended_blocks)
    cols_here = w_proj
    projected = lax.psum_scatter(
        jnp.einsum("rc,rt->ct", cols_here, attended, preferred_element_type=jnp.float32).astype(
            jnp.bfloat16
        ),
        "tp",
        scatter_dimension=0,
        tiled=True,
    ).astype(jnp.float32)
    stream_two = stream + projected + b_proj[:, None]
    normed_two, rstd_two, full_two = layer_norm(stream_two, ln2_gain, ln2_bias, width)
    upward = (
        jnp.einsum("dc,dt->ct", w_up, full_two, preferred_element_type=jnp.float32) + b_up[:, None]
    )
    activated = jax.nn.gelu(upward, approximate=False).astype(jnp.bfloat16)
    cols_here = w_down
    result = (
        stream_two
        + lax.psum_scatter(
            jnp.einsum(
                "fc,ft->ct", cols_here, activated, preferred_element_type=jnp.float32
            ).astype(jnp.bfloat16),
            "tp",
            scatter_dimension=0,
            tiled=True,
        ).astype(jnp.float32)
        + b_down[:, None]
    )
    out = (result * row_valid[None, :]).T.astype(jnp.bfloat16)
    grad_low = (cotangent.T.astype(jnp.float32) * row_scale[None, :]).astype(jnp.bfloat16)
    grad_wide = grad_low.astype(jnp.float32)
    g_b_down = jnp.sum(grad_wide, 1)
    (d_activated,), (g_w_down,) = fold_back(grad_low, ((w_down, activated),))
    cumulative = 0.5 * (1.0 + lax.erf(upward * ROOT_HALF))
    density = jnp.exp(-0.5 * upward * upward) * DENSITY_SCALE
    d_upward = (d_activated * (cumulative + upward * density)).astype(jnp.bfloat16)
    g_b_up = jnp.sum(d_upward.astype(jnp.float32), 1)
    g_w_up = jnp.einsum("dt,ft->df", full_two, d_upward, preferred_element_type=jnp.float32)

    def up_term(start, count_rows):
        return jnp.einsum("cf,ft->ct", w_up, d_upward, preferred_element_type=jnp.float32)

    d_normed_two = reduce_back(up_term, local_width)
    back_two, g_ln2_gain, g_ln2_bias = norm_back(
        d_normed_two, normed_two, rstd_two, ln2_gain, width
    )
    d_stream_two = (back_two + grad_wide).astype(jnp.bfloat16)
    d_stream_wide = d_stream_two.astype(jnp.float32)
    g_b_proj = jnp.sum(d_stream_wide, 1)
    (d_attended,), (g_w_proj,) = fold_back(d_stream_two, ((w_proj, attended),))
    d_attended_blocks = split_heads(d_attended.astype(jnp.bfloat16), heads_here)
    d_queries, d_keys, d_values = lax.map(
        attend_back, (query_blocks, key_blocks, value_blocks, logsums, d_attended_blocks)
    )
    d_qkv = jnp.stack([join_heads(d_queries), join_heads(d_keys), join_heads(d_values)], axis=0)
    g_w_qkv = jnp.einsum("dt,ect->edc", full_one, d_qkv, preferred_element_type=jnp.float32)

    def qkv_term(start, count_rows):
        return jnp.einsum("ecr,ert->ct", w_qkv, d_qkv, preferred_element_type=jnp.float32)

    d_normed_one = reduce_back(qkv_term, local_width)
    back_one, g_ln1_gain, g_ln1_bias = norm_back(
        d_normed_one, normed_one, rstd_one, ln1_gain, width
    )
    d_stream = (back_one + d_stream_wide).astype(jnp.bfloat16)
    g_b_skip = jnp.sum(d_stream.astype(jnp.float32), 1)
    (d_main_cols, d_long_cols), (g_w_main, g_w_long) = fold_back(
        d_stream, ((w_skip_main, main_cols), (w_skip_long, long_cols))
    )
    (
        g_w_main,
        g_w_long,
        g_b_skip,
        g_ln1_gain,
        g_ln1_bias,
        g_w_qkv,
        g_w_proj,
        g_b_proj,
        g_ln2_gain,
        g_ln2_bias,
        g_w_up,
        g_b_up,
        g_w_down,
        g_b_down,
    ) = (
        lax.psum(g_w_main.astype(jnp.bfloat16), "dp").astype(jnp.float32),
        lax.psum(g_w_long.astype(jnp.bfloat16), "dp").astype(jnp.float32),
        lax.psum(g_b_skip.astype(jnp.bfloat16), "dp").astype(jnp.float32),
        lax.psum(g_ln1_gain.astype(jnp.bfloat16), "dp").astype(jnp.float32),
        lax.psum(g_ln1_bias.astype(jnp.bfloat16), "dp").astype(jnp.float32),
        lax.psum(g_w_qkv.astype(jnp.bfloat16), "dp").astype(jnp.float32),
        lax.psum(g_w_proj.astype(jnp.bfloat16), "dp").astype(jnp.float32),
        lax.psum(g_b_proj.astype(jnp.bfloat16), "dp").astype(jnp.float32),
        lax.psum(g_ln2_gain.astype(jnp.bfloat16), "dp").astype(jnp.float32),
        lax.psum(g_ln2_bias.astype(jnp.bfloat16), "dp").astype(jnp.float32),
        lax.psum(g_w_up.astype(jnp.bfloat16), "dp").astype(jnp.float32),
        lax.psum(g_b_up.astype(jnp.bfloat16), "dp").astype(jnp.float32),
        lax.psum(g_w_down.astype(jnp.bfloat16), "dp").astype(jnp.float32),
        lax.psum(g_b_down.astype(jnp.bfloat16), "dp").astype(jnp.float32),
    )
    d_main = d_main_cols.T.astype(jnp.bfloat16)
    d_long = d_long_cols.T.astype(jnp.bfloat16)
    return (
        out,
        d_main,
        d_long,
        g_w_main,
        g_w_long,
        g_b_skip,
        g_ln1_gain,
        g_ln1_bias,
        g_w_qkv,
        g_w_proj,
        g_b_proj,
        g_ln2_gain,
        g_ln2_bias,
        g_w_up,
        g_b_up,
        g_w_down,
        g_b_down,
    )


ITEM_ROWS = 264
GRAD_ROWS = 24
CORE = ("tp", 1)
ACROSS_Y = ("tp", 2)
ACROSS_X = ("dp", 1)
ACROSS_Z = ("dp", 2)
FAR_Z = ("dp", 4)


def swap(value, link):
    axis, bit = link
    return lax.ppermute(value, axis, [(i, i ^ bit) for i in range(lax.axis_size(axis))])


def side(link):
    axis, bit = link
    return (lax.axis_index(axis) // bit) % 2


def in_order(bit, mine, theirs):
    flip = bit == 1
    return jnp.stack([jnp.where(flip, theirs, mine), jnp.where(flip, mine, theirs)])


def pick(value, index):
    return lax.dynamic_index_in_dim(value, index, 0, keepdims=False)


def peer(value, bit):
    return value + bit - 2 * bit * ((value // bit) % 2)


def greet(peers):
    barrier = pltpu.get_barrier_semaphore()
    for where in peers:
        pl.semaphore_signal(barrier, inc=1, device_id=where, device_id_type=pl.DeviceIdType.MESH)
    pl.semaphore_wait(barrier, len(peers))


def send(source, target, sems, index, where):
    return pltpu.make_async_remote_copy(
        src_ref=source,
        dst_ref=target,
        send_sem=sems.at[0, index],
        recv_sem=sems.at[1, index],
        device_id=where,
        device_id_type=pl.DeviceIdType.MESH,
    )


def gather_kernel(pieces, n_in, n_out, *refs):
    tokens, inputs = refs[0], refs[1 : 1 + n_in]
    refs = refs[1 + n_in :]
    far_tokens, core_near, core_far = refs[:3]
    outs, held = refs[3 : 3 + n_out], refs[3 + n_out : 3 + n_out + n_in]
    y_sem, one_sem, two_sem, own_sem, far_sem, local_sem, token_sem = refs[3 + n_out + n_in :]
    n = len(pieces)
    shards = [inputs[a].at[lead] if lead else inputs[a] for a, lead, _, _ in pieces]
    stage = [held[a].at[lead] if lead else held[a] for a, lead, _, _ in pieces]
    fulls = [[outs[b].at[(place,) + tail] for place in range(4)] for _, _, b, tail in pieces]
    dp, tp = lax.axis_index("dp"), lax.axis_index("tp")
    core, y = tp % 2, (tp // 2) % 2
    to_core, to_y = {"tp": peer(tp, 1)}, {"tp": peer(tp, 2)}
    links = ({"dp": peer(dp, 1)}, {"dp": peer(dp, 2)})
    bits = (dp % 2, (dp // 2) % 2)
    greet((to_core, to_y) + links)

    def places(k):
        return k % 2, 1 - k % 2, bits[k % 2], bits[1 - k % 2]

    def y_copy(k):
        _, _, f, s = places(k)
        return send(shards[k].at[s, f], fulls[k][1].at[s, f], y_sem, k, to_y)

    def one_copy(k):
        first, _, f, s = places(k)
        part = fulls[k][1].at[s, f]
        return send(part, part, one_sem, k, links[first])

    def two_copy(k):
        _, second, _, s = places(k)
        part = fulls[k][1].at[s]
        return send(part, part, two_sem, k, links[second])

    def own_copy(k):
        return send(shards[k], fulls[k][2], own_sem, k, to_core)

    def far_copy(k):
        return send(fulls[k][1], fulls[k][3], far_sem, k, to_core)

    def load(k):
        return pltpu.make_async_copy(shards[k], stage[k], local_sem.at[0, k])

    def store(k):
        return pltpu.make_async_copy(stage[k], fulls[k][0], local_sem.at[1, k])

    token_y = send(tokens.at[1 - y], far_tokens, token_sem, 0, to_y)
    token_near = send(tokens.at[y, 1 - core], core_near, token_sem, 1, to_core)
    token_far = send(far_tokens.at[1 - core], core_far, token_sem, 2, to_core)
    for k in range(n):
        y_copy(k).start()
    token_y.start()
    token_near.start()
    for k in range(n):
        load(k).start()
        own_copy(k).start()
    for step in range(n + 2):
        if step < n:
            y_copy(step).wait_recv()
            one_copy(step).start()
            load(step).wait()
            store(step).start()
        if 0 <= step - 1 < n:
            one_copy(step - 1).wait_recv()
            two_copy(step - 1).start()
        if 0 <= step - 2 < n:
            two_copy(step - 2).wait_recv()
            far_copy(step - 2).start()
    token_y.wait_recv()
    token_far.start()
    for copy in (token_near, token_far):
        copy.wait()
    token_y.wait_send()
    for k in range(n):
        far_copy(k).wait()
        own_copy(k).wait()
        store(k).wait()
        for copy in (y_copy(k), one_copy(k), two_copy(k)):
            copy.wait_send()


def gather_weights(tokens, arrays, pieces, out_shapes):
    n = len(pieces)
    shape = lambda dims, like: jax.ShapeDtypeStruct(dims, like.dtype)
    rows = tokens.shape[2:]
    outs = [shape((2,) + rows, tokens), shape(rows, tokens), shape(rows, tokens)]
    outs += [shape(dims, arrays[0]) for dims in out_shapes]
    sems = [pltpu.SemaphoreType.DMA((2, n))] * 6 + [pltpu.SemaphoreType.DMA((2, 3))]
    return pl.pallas_call(
        functools.partial(gather_kernel, pieces, len(arrays), len(out_shapes)),
        out_shape=outs,
        in_specs=[pl.BlockSpec(memory_space=pl.ANY)] * (1 + len(arrays)),
        out_specs=[pl.BlockSpec(memory_space=pl.ANY)] * len(outs),
        scratch_shapes=[pltpu.VMEM(a.shape, a.dtype) for a in arrays] + sems,
        compiler_params=pltpu.CompilerParams(
            collective_id=1, has_side_effects=True, vmem_limit_bytes=32 * 2**20
        ),
        name="gather_weights",
    )(tokens, *arrays)


LAG = 7


def reduce_kernel(n_early, whole_sizes, views, n_arrays, *refs):
    early, arrays, blocks = refs[0], refs[1 : 1 + n_arrays], refs[1 + n_arrays]
    refs = refs[2 + n_arrays :]
    early_out, outs, refs = refs[0], refs[1 : 1 + len(views)], refs[1 + len(views) :]
    from_core, y_blocks = refs[:2]
    refs = refs[2:]
    total, from_y, from_one, half, from_two, from_far, final = refs[:7]
    y_sem, one_sem, two_sem, far_sem, back_two, back_one, block_sem, load_sem, out_sem = refs[7:]
    n_whole = total.shape[0]
    chunks = n_early + n_whole
    dp, tp = lax.axis_index("dp"), lax.axis_index("tp")
    f, g = dp % 2, (dp // 2) % 2
    to_core, to_y = {"tp": peer(tp, 1)}, {"tp": peer(tp, 2)}
    to_x, to_z, to_far = {"dp": peer(dp, 1)}, {"dp": peer(dp, 2)}, {"dp": peer(dp, 4)}
    greet((to_core, to_y, to_x, to_z, to_far))

    def y_copy(r, source):
        return send(source, from_y.at[r], y_sem, r, to_y)

    def one_copy(r):
        return send(total.at[r, 1 - f], from_one.at[r], one_sem, r, to_x)

    def two_copy(s):
        return send(half.at[s, 1 - g], from_two.at[s], two_sem, s, to_z)

    def far_copy(s):
        return send(half.at[s, g], from_far.at[s], far_sem, s, to_far)

    def back_two_copy(s):
        part = final.at[s, f, g]
        return send(part, part, back_two, s, to_z)

    def back_one_copy(s):
        part = final.at[s, f]
        return send(part, part, back_one, s, to_x)

    def out_copies(s, act):
        @pl.when(s < n_early)
        def _():
            for p in range(2):
                act(pltpu.make_async_copy(final.at[s, p], early_out.at[p, s], out_sem.at[p, s]))

        at = n_early
        for k, size in enumerate(whole_sizes):

            @pl.when((s >= at) & (s < at + size))
            def _(k=k, at=at):
                act(pltpu.make_async_copy(final.at[s], outs[k].at[s - at], out_sem.at[0, s]))

            at += size

    early_load = pltpu.make_async_copy(early, half.at[pl.ds(0, n_early)], load_sem.at[0])
    early_load.start()
    core_blocks = [send(blocks.at[2 + k], from_core.at[k], block_sem, k, to_core) for k in range(2)]
    own_block = send(blocks.at[1], y_blocks.at[0], block_sem, 2, to_y)
    core_block = send(from_core.at[1], y_blocks.at[1], block_sem, 3, to_y)
    loads, at = [], 0
    for k, (size, (a, mine, theirs)) in enumerate(zip(whole_sizes, views)):
        source = arrays[a].at[mine]
        loads.append(pltpu.make_async_copy(source, total.at[pl.ds(at, size)], load_sem.at[1 + k]))
        loads[-1].start()
        for r in range(size):
            y_copy(at + r, arrays[a].at[theirs + (r,)]).start()
        at += size
    for copy in core_blocks:
        copy.start()
    own_block.start()
    early_load.wait()
    for copy in loads:
        copy.wait()

    def plus(left, right):
        return (left.astype(jnp.float32) + right.astype(jnp.float32)).astype(jnp.bfloat16)

    def step(t, carry):
        @pl.when(t < n_early)
        def _():
            two_copy(t).start()

        @pl.when((t >= n_early) & (t < chunks))
        def _():
            one_copy(t - n_early).wait_recv()
            half[t] = plus(total[t - n_early, f], from_one[t - n_early])
            two_copy(t).start()

        @pl.when((t >= 1) & (t < chunks + 1))
        def _():
            s = t - 1
            two_copy(s).wait_recv()
            half[s, g] = plus(half[s, g], from_two[s])
            far_copy(s).start()

        @pl.when((t >= 3) & (t < chunks + 3))
        def _():
            s = t - 3
            far_copy(s).wait_recv()
            final[s, f, g] = plus(half[s, g], from_far[s])
            back_two_copy(s).start()

        @pl.when((t >= 4) & (t < chunks + 4))
        def _():
            back_two_copy(t - 4).wait_recv()
            back_one_copy(t - 4).start()

        @pl.when((t >= 5) & (t < chunks + 5))
        def _():
            back_one_copy(t - 5).wait_recv()
            out_copies(t - 5, lambda copy: copy.start())

        @pl.when((t >= LAG) & (t < LAG + n_whole))
        def _():
            r = t - LAG
            y_copy(r, total.at[r]).wait_recv()
            total[r] = plus(total[r], from_y[r])
            one_copy(r).start()

        @pl.when(t == 2)
        def _():
            for copy in core_blocks:
                copy.wait_recv()
            core_block.start()

        return carry

    lax.fori_loop(0, chunks + 5, step, 0)

    def finish_whole(r, carry):
        y_copy(r, total.at[r]).wait_send()
        one_copy(r).wait_send()
        return carry

    lax.fori_loop(0, n_whole, finish_whole, 0)

    def finish(s, carry):
        for copy in (two_copy(s), far_copy(s), back_two_copy(s), back_one_copy(s)):
            copy.wait_send()
        out_copies(s, lambda copy: copy.wait())
        return carry

    lax.fori_loop(0, chunks, finish, 0)
    for copy in core_blocks:
        copy.wait_send()
    own_block.wait()
    core_block.wait()


def reduce_grads(early, arrays, views, blocks):
    sizes = tuple(arrays[a].shape[len(mine)] for a, mine, _ in views)
    n_early, n_whole = early.shape[0], sum(sizes)
    chunks = n_early + n_whole
    rows, width = early.shape[-2:]
    kind = early.dtype
    sem = lambda n: pltpu.SemaphoreType.DMA((2, n))
    two_blocks = jax.ShapeDtypeStruct((2,) + blocks.shape[1:], blocks.dtype)
    return pl.pallas_call(
        functools.partial(reduce_kernel, n_early, sizes, views, len(arrays)),
        out_shape=[jax.ShapeDtypeStruct((2, n_early, 2, rows, width), kind)]
        + [jax.ShapeDtypeStruct((n, 2, 2, rows, width), kind) for n in sizes]
        + [two_blocks, two_blocks],
        in_specs=[pl.BlockSpec(memory_space=pl.ANY)] * (2 + len(arrays)),
        out_specs=[pl.BlockSpec(memory_space=pl.ANY)] * (3 + len(views)),
        scratch_shapes=[
            pltpu.VMEM((n_whole, 2, 2, rows, width), kind),
            pltpu.VMEM((n_whole, 2, 2, rows, width), kind),
            pltpu.VMEM((n_whole, 2, rows, width), kind),
            pltpu.VMEM((chunks, 2, rows, width), kind),
            pltpu.VMEM((chunks, rows, width), kind),
            pltpu.VMEM((chunks, rows, width), kind),
            pltpu.VMEM((chunks, 2, 2, rows, width), kind),
            sem(n_whole),
            sem(n_whole),
            sem(chunks),
            sem(chunks),
            sem(chunks),
            sem(chunks),
            sem(4),
            pltpu.SemaphoreType.DMA((1 + len(views),)),
            sem(chunks),
        ],
        compiler_params=pltpu.CompilerParams(
            collective_id=2, has_side_effects=True, vmem_limit_bytes=56 * 2**20
        ),
        name="reduce_grads",
    )(early, *arrays, blocks)


def add_low(mine, theirs):
    return (mine.astype(jnp.float32) + theirs.astype(jnp.float32)).astype(jnp.bfloat16)


def place_of(index):
    rank = lax.axis_index("tp")
    core, y = rank % 2, (rank // 2) % 2
    there_core, there_y = index % 2, index // 2
    apart = lambda a, b: a + b - 2 * a * b
    return apart(y, there_y) + 2 * apart(core, there_core)


def spread_kernel(main_ref, long_ref, cot_ref, tokens_ref, cot_tokens_ref):
    cols = main_ref.shape[1]
    items = tokens_ref.shape[1] // ITEM_ROWS
    for p in range(4):
        for i in range(items):
            source = slice((p * items + i) * SEQ, (p * items + i + 1) * SEQ)
            target = slice(i * ITEM_ROWS, i * ITEM_ROWS + SEQ)
            blank = slice(i * ITEM_ROWS + SEQ, (i + 1) * ITEM_ROWS)
            tokens_ref[p, target, :cols] = main_ref[source, :]
            tokens_ref[p, target, cols:] = long_ref[source, :]
            cot_tokens_ref[p, target, :] = cot_ref[source, :]
            tokens_ref[p, blank, :] = jnp.zeros((ITEM_ROWS - SEQ, 2 * cols), tokens_ref.dtype)
            cot_tokens_ref[p, blank, :] = jnp.zeros((ITEM_ROWS - SEQ, cols), tokens_ref.dtype)


def spread(main, long_skip, cotangent):
    rows, cols = main.shape
    padded = rows // SEQ // 4 * ITEM_ROWS
    return pl.pallas_call(
        spread_kernel,
        out_shape=[
            jax.ShapeDtypeStruct((4, padded, 2 * cols), main.dtype),
            jax.ShapeDtypeStruct((4, padded, cols), main.dtype),
        ],
        compiler_params=pltpu.CompilerParams(vmem_limit_bytes=40 * 2**20),
        name="spread",
    )(main, long_skip, cotangent)


def arrange_kernel(own_ref, y_ref, partner_ref, scale_ref, out_ref, held):
    cols = own_ref.shape[1]
    held[0] = own_ref[...]
    held[1] = y_ref[...]
    held[2] = partner_ref[0]
    held[3] = partner_ref[1]
    for j in range(4):
        block = held[place_of(j)].astype(jnp.float32) * scale_ref[...]
        out_ref[:, j * cols : (j + 1) * cols] = block.astype(out_ref.dtype)


def arrange(own, along_y, partner, scale):
    rows, cols = own.shape
    return pl.pallas_call(
        arrange_kernel,
        out_shape=jax.ShapeDtypeStruct((rows, 4 * cols), own.dtype),
        scratch_shapes=[pltpu.VMEM((4, rows, cols), own.dtype)],
        compiler_params=pltpu.CompilerParams(vmem_limit_bytes=24 * 2**20),
        name="arrange",
    )(own, along_y, partner, scale)


def disperse_kernel(rows_ref, valid_ref, out_ref):
    cols = out_ref.shape[2]
    for j in range(4):
        block = rows_ref[:, j * cols : (j + 1) * cols] * valid_ref[...]
        out_ref[place_of(j)] = block.astype(out_ref.dtype)


def disperse(rows, valid):
    count, width = rows.shape
    return pl.pallas_call(
        disperse_kernel,
        out_shape=jax.ShapeDtypeStruct((4, count, width // 4), jnp.bfloat16),
        compiler_params=pltpu.CompilerParams(vmem_limit_bytes=24 * 2**20),
        name="disperse",
    )(rows, valid)


def unspread_kernel(parts, own_ref, core_ref, y_ref, *refs):
    outs, held = refs[:parts], refs[parts]
    cols = outs[0].shape[1]
    items = own_ref.shape[0] // ITEM_ROWS
    held[0] = own_ref[...]
    held[1] = y_ref[0]
    held[2] = core_ref[...]
    held[3] = y_ref[1]
    for p in range(4):
        rows = held[place_of(p)]
        for i in range(items):
            target = slice((p * items + i) * SEQ, (p * items + i + 1) * SEQ)
            source = slice(i * ITEM_ROWS, i * ITEM_ROWS + SEQ)
            for k in range(parts):
                outs[k][target, :] = rows[source, k * cols : (k + 1) * cols]


def unspread(own, core_tokens, y_tokens, parts):
    rows, width = own.shape
    out = jax.ShapeDtypeStruct((4 * rows // ITEM_ROWS * SEQ, width // parts), own.dtype)
    return pl.pallas_call(
        functools.partial(unspread_kernel, parts),
        out_shape=[out] * parts,
        scratch_shapes=[pltpu.VMEM((4, rows, width), own.dtype)],
        compiler_params=pltpu.CompilerParams(vmem_limit_bytes=40 * 2**20),
        name="unspread",
    )(own, core_tokens, y_tokens)


def natural(own_half, partner_half, width, axis):
    flip_y, flip_core = side(ACROSS_Y) == 1, side(CORE) == 1
    r0, r2 = jnp.split(own_half, 2, axis)
    r1, r3 = jnp.split(partner_half, 2, axis)
    a0, a2 = jnp.where(flip_y, r2, r0), jnp.where(flip_y, r0, r2)
    a1, a3 = jnp.where(flip_y, r3, r1), jnp.where(flip_y, r1, r3)
    b0, b1 = jnp.where(flip_core, a1, a0), jnp.where(flip_core, a0, a1)
    b2, b3 = jnp.where(flip_core, a3, a2), jnp.where(flip_core, a2, a3)
    return (b0, b1, b2, b3)


def dot(spec, left, right):
    return jnp.einsum(spec, left, right, preferred_element_type=jnp.float32)


def low(value):
    return value.astype(jnp.bfloat16)


def norm_rows(stream, gain, bias):
    mean = jnp.mean(stream, 1, keepdims=True)
    square = jnp.mean(stream * stream, 1, keepdims=True)
    rstd = lax.rsqrt(square - mean * mean + EPSILON)
    normed = (stream - mean) * rstd
    return normed, rstd, low(normed * gain + bias)


def norm_rows_back(d_out, normed, rstd, gain):
    g_gain = jnp.sum(d_out * normed, 0)
    g_bias = jnp.sum(d_out, 0)
    scaled = d_out * gain
    first = jnp.mean(scaled, 1, keepdims=True)
    second = jnp.mean(scaled * normed, 1, keepdims=True)
    return rstd * (scaled - first - normed * second), g_gain, g_bias


LAST = (((1,), (1,)), ((), ()))
LEAD = (((0,), (0,)), ((), ()))


def item_scores(key, query):
    scores = lax.dot_general(key, query, LAST, preferred_element_type=jnp.float32)
    present = lax.broadcasted_iota(jnp.int32, scores.shape, 0) < SEQ
    return jnp.where(present, scores * (1.0 / math.sqrt(HEAD)), -1e30)


def attend_kernel(q_ref, k_ref, v_ref, out_ref, lse_ref):
    for h in range(q_ref.shape[1] // HEAD):
        at = slice(h * HEAD, (h + 1) * HEAD)
        scores = item_scores(k_ref[:, at], q_ref[:, at])
        peak = jnp.max(scores, axis=0, keepdims=True)
        weights = jnp.exp(scores - peak)
        total = jnp.sum(weights, axis=0, keepdims=True)
        probs = (weights * (1.0 / total)).astype(jnp.bfloat16)
        out = lax.dot_general(probs, v_ref[:, at], LEAD, preferred_element_type=jnp.float32)
        out_ref[:, at] = out.astype(jnp.bfloat16)
        lse_ref[0, h : h + 1, :] = peak + jnp.log(total)


def attend_back_kernel(q_ref, k_ref, v_ref, lse_ref, d_ref, dq_ref, dk_ref, dv_ref):
    scale = 1.0 / math.sqrt(HEAD)
    for h in range(q_ref.shape[1] // HEAD):
        at = slice(h * HEAD, (h + 1) * HEAD)
        query, key, d_out = q_ref[:, at], k_ref[:, at], d_ref[:, at]
        probs = jnp.exp(item_scores(key, query) - lse_ref[0, h : h + 1, :])
        d_probs = lax.dot_general(v_ref[:, at], d_out, LAST, preferred_element_type=jnp.float32)
        delta = jnp.sum(probs * d_probs, axis=0, keepdims=True)
        d_scores = (probs * (d_probs - delta)).astype(jnp.bfloat16)
        dq = lax.dot_general(d_scores, key, LEAD, preferred_element_type=jnp.float32)
        dk = jnp.dot(d_scores, query, preferred_element_type=jnp.float32)
        dv = jnp.dot(probs.astype(jnp.bfloat16), d_out, preferred_element_type=jnp.float32)
        dq_ref[:, at] = (dq * scale).astype(jnp.bfloat16)
        dk_ref[:, at] = (dk * scale).astype(jnp.bfloat16)
        dv_ref[:, at] = dv.astype(jnp.bfloat16)


def attention(query, key, value):
    rows, cols = query.shape
    heads, items = cols // HEAD, rows // ITEM_ROWS
    block = pl.BlockSpec((ITEM_ROWS, cols), lambda i: (i, 0))
    return pl.pallas_call(
        attend_kernel,
        grid=(items,),
        out_shape=[
            jax.ShapeDtypeStruct((rows, cols), jnp.bfloat16),
            jax.ShapeDtypeStruct((items, heads, ITEM_ROWS), jnp.float32),
        ],
        in_specs=[block] * 3,
        out_specs=[block, pl.BlockSpec((1, heads, ITEM_ROWS), lambda i: (i, 0, 0))],
        cost_estimate=pl.CostEstimate(
            flops=4 * rows * ITEM_ROWS * cols, bytes_accessed=8 * rows * cols, transcendentals=rows * ITEM_ROWS * heads
        ),
        name="attend",
    )(query, key, value)


def attention_back(query, key, value, lse, d_out):
    rows, cols = query.shape
    heads, items = cols // HEAD, rows // ITEM_ROWS
    block = pl.BlockSpec((ITEM_ROWS, cols), lambda i: (i, 0))
    return pl.pallas_call(
        attend_back_kernel,
        grid=(items,),
        out_shape=[jax.ShapeDtypeStruct((rows, cols), jnp.bfloat16)] * 3,
        in_specs=[block, block, block, pl.BlockSpec((1, heads, ITEM_ROWS), lambda i: (i, 0, 0)), block],
        out_specs=[block] * 3,
        cost_estimate=pl.CostEstimate(
            flops=10 * rows * ITEM_ROWS * cols, bytes_accessed=14 * rows * cols, transcendentals=rows * ITEM_ROWS * heads
        ),
        name="attend_back",
    )(query, key, value, lse, d_out)


def body_items(
    main,
    long_skip,
    cotangent,
    timesteps,
    loss_codes,
    code_weights,
    item_counts,
    w_skip_main,
    w_skip_long,
    b_skip,
    ln1_gain,
    ln1_bias,
    w_qkv,
    w_proj,
    b_proj,
    ln2_gain,
    ln2_bias,
    w_up,
    b_up,
    w_down,
    b_down,
):
    local = main.shape[1]
    width = 4 * local
    rank = lax.axis_index("tp")

    vectors = jnp.concatenate(
        [jnp.stack([b_skip, ln1_gain, ln1_bias, b_proj, ln2_gain, ln2_bias, b_down]), b_up.reshape(4, local)]
    )
    own_vectors = jnp.concatenate([vectors, swap(vectors, ACROSS_Y)], axis=1)
    partner_vectors = swap(own_vectors, CORE)
    joined = jnp.concatenate(natural(own_vectors[:7], partner_vectors[:7], local, 1), axis=1)
    b_skip_all, gain_one, bias_one, b_proj_all, gain_two, bias_two, b_down_all = (
        joined[k : k + 1] for k in range(7)
    )

    def up_vector(pair):
        near, far = jnp.split(pair[7:], 2, 1)
        return jnp.concatenate([near.reshape(1, -1), far.reshape(1, -1)], axis=1)

    b_up_all = jnp.concatenate([up_vector(own_vectors), up_vector(partner_vectors)], axis=1)

    y, core, x, z = side(ACROSS_Y), side(CORE), side(ACROSS_X), side(ACROSS_Z)
    cut = 2 * local
    tokens, cot_tokens = spread(main, long_skip, cotangent)
    tokens = tokens.reshape((2, 2) + tokens.shape[1:])
    cot_tokens = cot_tokens.reshape((2, 2) + cot_tokens.shape[1:])
    quarters = lambda w: w.reshape(2, 2, -1, width)
    qkv_rows = jnp.swapaxes(w_qkv, 1, 2).reshape(3, 2, 2, local // 4, width)
    one = (4, 2, 2, local // 4, width)
    far_tokens, core_near, core_far, wskip, wq, wk, wv, wp, wu = gather_weights(
        tokens,
        [
            quarters(w_skip_main),
            quarters(w_skip_long),
            qkv_rows,
            quarters(w_proj),
            w_up.reshape(2, 2, 2, width // 8, width),
        ],
        [
            (0, (), 0, (0,)),
            (1, (), 0, (1,)),
            (2, (0,), 1, ()),
            (2, (1,), 2, ()),
            (2, (2,), 3, ()),
            (3, (), 4, ()),
            (4, (0,), 5, (0,)),
            (4, (1,), 5, (1,)),
        ],
        [(4, 2) + one[1:], one, one, one, one, (4, 2, 2, 2, width // 8, width)],
    )
    wskip, wq, wk, wv, wp = (g.reshape(-1, width) for g in (wskip, wq, wk, wv, wp))
    wu = wu.reshape(4, width, width)
    near_tokens = pick(tokens, y)
    skip_rows = jnp.concatenate([pick(near_tokens, core), pick(far_tokens, core), core_near, core_far], axis=1)
    other = lambda value: swap(value, CORE)
    both = lambda mine, others: jnp.concatenate([mine, others], axis=0)
    shares = lambda value: both(value[:, : value.shape[1] // 2], other(value[:, value.shape[1] // 2 :]))

    def after(value, *events):
        return lax.optimization_barrier((value,) + events)[0]

    w_down_then = after(w_down, wskip)
    wd_core = other(w_down_then)
    wd_y = swap(w_down_then, ACROSS_Y)
    cot_near = pick(cot_tokens, y)
    cot_far = swap(after(pick(cot_tokens, 1 - y), wskip), ACROSS_Y)

    stream = dot("td,dc->tc", skip_rows, wskip) + b_skip_all
    normed_one, rstd_one, full_one = norm_rows(stream, gain_one, bias_one)
    n1_both = both(full_one, other(full_one))
    query, key, value = (low(dot("td,cd->tc", full_one, w)) for w in (wq, wk, wv))
    attended, logsum = attention(query, key, value)
    attended_both = shares(attended)
    stream_two = stream + dot("tc,cd->td", attended, wp) + b_proj_all
    cot_far = after(cot_far, stream_two)
    cot_partner = other(jnp.stack([pick(cot_near, 1 - core), pick(cot_far, 1 - core)]))
    normed_two, rstd_two, full_two = norm_rows(stream_two, gain_two, bias_two)
    n2_both = both(full_two, other(full_two))
    acts, slopes = [], []
    for r in range(4):
        upward = dot("td,dc->tc", full_two, wu[r]) + b_up_all[:, r * width : (r + 1) * width]
        cumulative = 0.5 * (1.0 + lax.erf(upward * ROOT_HALF))
        density = jnp.exp(-0.5 * upward * upward) * DENSITY_SCALE
        acts.append(low(upward * cumulative))
        slopes.append(low(cumulative + upward * density))

    item_scale, valid = item_factors(timesteps, loss_codes, code_weights, item_counts[0])
    row_scale = jnp.repeat(pick(item_scale.reshape(4, -1), rank), ITEM_ROWS)[:, None]
    row_valid = jnp.repeat(pick(valid.reshape(4, -1), rank), ITEM_ROWS)[:, None]
    grad_low = arrange(pick(cot_near, core), pick(cot_far, core), cot_partner, row_scale)
    wd_y = after(wd_y, acts[1])
    wd = [w_down, wd_y, wd_core, other(wd_y)]
    grad_both = both(grad_low, other(grad_low))
    grad_wide = grad_low.astype(jnp.float32)
    g_b_down = jnp.sum(grad_wide, 0)

    def weight_grad(left, right):
        return low(dot("tf,tc->fc", left, right))

    def half_sum(value, bit, link):
        halves = value.reshape(2, -1, width)
        return add_low(pick(halves, bit), swap(pick(halves, 1 - bit), link))

    down_mine, down_theirs = (weight_grad(both(acts[p], other(acts[2 + p])), grad_both) for p in (0, 1))
    grad_then = after(grad_low, down_theirs)
    down_sum = add_low(down_mine, swap(down_theirs, ACROSS_Y))

    result = stream_two + sum(dot("tf,fc->tc", acts[r], wd[r]) for r in range(4)) + b_down_all
    outs = disperse(result, row_valid)
    out_core = other(outs[2:])
    out_y = swap(jnp.stack([outs[1], out_core[1]]), ACROSS_Y)
    (out,) = unspread(outs[0], out_core[0], out_y, 1)

    d_up = [low(dot("tc,fc->tf", grad_then, wd[r]) * slopes[r].astype(jnp.float32)) for r in range(4)]
    g_b_up = jnp.stack([jnp.sum(d.astype(jnp.float32), 0) for d in d_up])
    up_mine, up_theirs = (weight_grad(n2_both, both(d_up[p], other(d_up[2 + p]))) for p in (0, 1))
    d_up = [after(d, up_theirs) for d in d_up]
    up_sum = add_low(up_mine, swap(up_theirs, ACROSS_Y))
    d_n2 = sum(dot("tf,cf->tc", d_up[r], wu[r]) for r in range(4))
    back_two, g_ln2_gain, g_ln2_bias = norm_rows_back(d_n2, normed_two, rstd_two, gain_two)
    d_stream_two = low(back_two + grad_wide)
    d_stream_wide = d_stream_two.astype(jnp.float32)
    g_b_proj = jnp.sum(d_stream_wide, 0)
    chunked = lambda g, lead: g.reshape(lead + (-1, 2, 2, GRAD_ROWS, width))
    proj_part = chunked(weight_grad(attended_both, both(d_stream_two, other(d_stream_two))), (2,))
    d_attended = low(dot("tc,fc->tf", d_stream_two, wp))
    d_attended = after(d_attended, down_sum)
    down_half = half_sum(down_sum, x, ACROSS_X)
    d_qkv = attention_back(query, key, value, logsum, d_attended)
    d_qkv = lax.optimization_barrier((*d_qkv, down_half))[:3]
    down_quarter = half_sum(down_half, z, ACROSS_Z)
    d_own = jnp.concatenate([d[:, :cut] for d in d_qkv], axis=1)
    d_partner = jnp.concatenate([d[:, cut:] for d in d_qkv], axis=1)
    qkv_part = chunked(weight_grad(both(d_own, other(d_partner)), n1_both), (3, 2))
    d_n1 = sum(dot("tc,cd->td", d, w) for d, w in zip(d_qkv, (wq, wk, wv)))
    back_one, g_ln1_gain, g_ln1_bias = norm_rows_back(d_n1, normed_one, rstd_one, gain_one)
    d_stream = low(back_one + d_stream_wide)
    d_stream = after(d_stream, down_quarter)
    down_far = swap(down_quarter, FAR_Z)
    d_stream_both = both(d_stream, other(d_stream))
    g_b_skip = jnp.sum(d_stream.astype(jnp.float32), 0)
    passed = jnp.concatenate([pick(near_tokens, 1 - core), pick(far_tokens, 1 - core)], axis=1)
    skip_part = chunked(weight_grad(both(skip_rows[:, : 2 * cut], passed), d_stream_both), (2,))
    d_skip = low(dot("tc,fc->tf", d_stream, wskip))
    d_blocks = jnp.stack(jnp.split(d_skip, 4, 1))

    small = jnp.stack([g_b_skip, g_ln1_gain, g_ln1_bias, g_b_proj, g_ln2_gain, g_ln2_bias, g_b_down])
    arrived = other(jnp.concatenate([small, g_b_up[2:]]))
    small = jnp.moveaxis((small + arrived[:7]).reshape(7, 4, local), 1, 0)
    b_up_sums = g_b_up[:2] + arrived[7:]

    def vector_rows(shard, row):
        flat = jnp.concatenate([pick(small, shard).reshape(-1), b_up_sums[row]])
        return jnp.pad(flat, (0, 4 * GRAD_ROWS * width - flat.size)).reshape(1, 2, 2, GRAD_ROWS, width)

    vector_part = low(jnp.stack([vector_rows(rank, 0), vector_rows(peer(rank, 2), 1)]))
    down_quarter = add_low(down_quarter, down_far)
    down_half = in_order(z, down_quarter, swap(down_quarter, ACROSS_Z)).reshape(-1, width)
    down_back = swap(down_half, ACROSS_X)
    early = half_sum(up_sum, x, ACROSS_X).reshape(-1, 2, GRAD_ROWS, width)
    g_w_up, *sums = reduce_grads(
        early,
        [proj_part, qkv_part, vector_part, skip_part],
        [(0, (0,), (1,)), (1, (0, 0), (0, 1)), (1, (1, 0), (1, 1)), (1, (2, 0), (2, 1)), (2, (0,), (1,)), (3, (0,), (1,))],
        d_blocks,
    )
    from_core, y_blocks = sums[-2:]
    wide = lambda value: value.reshape(-1, width).astype(jnp.float32)
    g_w_down = wide(in_order(x, down_half, down_back))
    g_w_proj, g_q, g_k, g_v, vectors, g_skip = (wide(g) for g in sums[:-2])
    g_w_qkv = jnp.stack([g.T for g in (g_q, g_k, g_v)])
    vectors = vectors.reshape(-1)
    mine = vectors[: 7 * local].reshape(7, local)

    d_main, d_long = unspread(d_blocks[0], from_core[0], y_blocks, 2)
    return (
        out,
        d_main,
        d_long,
        g_skip[:local],
        g_skip[local:],
        mine[0],
        mine[1],
        mine[2],
        g_w_qkv,
        g_w_proj,
        mine[3],
        mine[4],
        mine[5],
        wide(g_w_up),
        vectors[7 * local : 7 * local + width],
        g_w_down,
        mine[6],
    )


def solution(mesh):
    by_items = mesh.shape["tp"] == 4 and mesh.shape["dp"] == 8
    return jax.shard_map(
        body_items if by_items else body_features,
        mesh=mesh,
        in_specs=(
            P("dp", "tp"),
            P("dp", "tp"),
            P("dp", "tp"),
            P("dp"),
            P("dp"),
            P(),
            P("dp"),
            P("tp", None),
            P("tp", None),
            P("tp"),
            P("tp"),
            P("tp"),
            P(None, None, "tp"),
            P("tp", None),
            P("tp"),
            P("tp"),
            P("tp"),
            P(None, "tp"),
            P("tp"),
            P("tp", None),
            P("tp"),
        ),
        out_specs=(
            P("dp", "tp"),
            P("dp", "tp"),
            P("dp", "tp"),
            P("tp", None),
            P("tp", None),
            P("tp"),
            P("tp"),
            P("tp"),
            P(None, None, "tp"),
            P("tp", None),
            P("tp"),
            P("tp"),
            P("tp"),
            P(None, "tp"),
            P("tp"),
            P("tp", None),
            P("tp"),
        ),
        check_vma=False,
    )
```

```python
import functools
import math

import jax
import jax.numpy as jnp
from jax import lax
from jax.experimental import pallas as pl
from jax.experimental.pallas import tpu as pltpu
from jax.sharding import PartitionSpec as P

HEAD = 72
SEQ = 258
TSTEPS = 1000


EPSILON = 1e-06
ROOT_HALF = 0.7071067811865476
DENSITY_SCALE = 0.3989422804014327


def item_factors(timesteps, loss_codes, code_weights, group_items):
    steps_float = timesteps.astype(jnp.float32)
    phase = (steps_float / TSTEPS + 0.008) / 1.008 * (math.pi / 2.0)
    cosine = jnp.cos(phase)
    signal = cosine * cosine
    weight = jnp.minimum(1.0, 5.0 * (1.0 - signal) / signal)
    picks = (
        loss_codes[:, None] == jnp.arange(code_weights.shape[0], dtype=jnp.int32)[None, :]
    ).astype(jnp.float32)
    coded = jnp.sum(picks * code_weights[None, :], axis=1)
    valid = (jnp.arange(timesteps.shape[0], dtype=jnp.int32) < group_items).astype(jnp.float32)
    return (weight * coded * valid, valid)


def layer_norm(stream, gain, bias, width):
    totals, squares = lax.psum((jnp.sum(stream, 0), jnp.sum(stream * stream, 0)), "tp")
    mean = totals / width
    rstd = lax.rsqrt(squares / width - mean * mean + EPSILON)
    normed = (stream - mean[None, :]) * rstd[None, :]
    rounded = (normed * gain[:, None] + bias[:, None]).astype(jnp.bfloat16)
    return (normed, rstd, lax.all_gather(rounded, "tp", axis=0, tiled=True))


def norm_back(d_normed, normed, rstd, gain, width):
    g_gain = jnp.sum(d_normed * normed, 1)
    g_bias = jnp.sum(d_normed, 1)
    scaled = d_normed * gain[:, None]
    first, second = lax.psum((jnp.sum(scaled, 0), jnp.sum(scaled * normed, 0)), "tp")
    back = rstd[None, :] * (scaled - first[None, :] / width - normed * second[None, :] / width)
    return (back, g_gain, g_bias)


def reduce_back(term, local_width):
    return lax.psum_scatter(
        term(jnp.int32(0), lax.axis_size("tp") * local_width).astype(jnp.bfloat16),
        "tp",
        scatter_dimension=0,
        tiled=True,
    ).astype(jnp.float32)


def fold_back(shard, pairs):
    piece = lax.all_gather(shard, "tp", axis=0, tiled=True)
    new_acts = tuple(
        (
            jnp.einsum("fc,ct->ft", weight, piece, preferred_element_type=jnp.float32)
            for weight, acts in pairs
        )
    )
    new_weights = tuple(
        (
            jnp.einsum("ft,ct->fc", acts, piece, preferred_element_type=jnp.float32)
            for weight, acts in pairs
        )
    )
    return (new_acts, new_weights)


def split_heads(flat, heads_here):
    pair_count = flat.shape[1] // (2 * SEQ)
    shaped = flat.reshape(heads_here, HEAD, pair_count, 2, SEQ)
    return jnp.moveaxis(shaped, 2, 0)


def join_heads(blocks):
    moved = jnp.moveaxis(blocks, 0, 2)
    return moved.reshape(moved.shape[0] * moved.shape[1], -1)


def attend(block):
    query_rows, key_rows, value_rows = block
    scale = 1.0 / math.sqrt(HEAD)
    scores = (
        jnp.einsum("hdbi,hdbj->hbij", query_rows, key_rows, preferred_element_type=jnp.float32)
        * scale
    )
    peak = jnp.max(scores, axis=-1, keepdims=True)
    logsum = peak + jnp.log(jnp.sum(jnp.exp(scores - peak), axis=-1, keepdims=True))
    probs = jnp.exp(scores - logsum).astype(jnp.bfloat16)
    attended = jnp.einsum("hbij,hdbj->hdbi", probs, value_rows, preferred_element_type=jnp.float32)
    return (attended.astype(jnp.bfloat16), logsum[..., 0])


def attend_back(block):
    query_rows, key_rows, value_rows, logsum, d_attended = block
    scale = 1.0 / math.sqrt(HEAD)
    scores = (
        jnp.einsum("hdbi,hdbj->hbij", query_rows, key_rows, preferred_element_type=jnp.float32)
        * scale
    )
    probs = jnp.exp(scores - logsum[..., None])
    probs_low = probs.astype(jnp.bfloat16)
    d_probs = jnp.einsum(
        "hdbi,hdbj->hbij", d_attended, value_rows, preferred_element_type=jnp.float32
    )
    delta = jnp.sum(probs * d_probs, axis=-1, keepdims=True)
    d_scores = (probs * (d_probs - delta)).astype(jnp.bfloat16)
    d_query = (
        jnp.einsum("hbij,hdbj->hdbi", d_scores, key_rows, preferred_element_type=jnp.float32)
        * scale
    )
    d_key = (
        jnp.einsum("hbij,hdbi->hdbj", d_scores, query_rows, preferred_element_type=jnp.float32)
        * scale
    )
    d_value = jnp.einsum(
        "hbij,hdbi->hdbj", probs_low, d_attended, preferred_element_type=jnp.float32
    )
    return (d_query.astype(jnp.bfloat16), d_key.astype(jnp.bfloat16), d_value.astype(jnp.bfloat16))


def body_features(
    main,
    long_skip,
    cotangent,
    timesteps,
    loss_codes,
    code_weights,
    item_counts,
    w_skip_main,
    w_skip_long,
    b_skip,
    ln1_gain,
    ln1_bias,
    w_qkv,
    w_proj,
    b_proj,
    ln2_gain,
    ln2_bias,
    w_up,
    b_up,
    w_down,
    b_down,
):
    local_width = main.shape[1]
    width = w_skip_main.shape[1]
    heads_here = local_width // HEAD
    item_scale, valid = item_factors(timesteps, loss_codes, code_weights, item_counts[0])
    row_scale = jnp.repeat(item_scale, SEQ)
    row_valid = jnp.repeat(valid, SEQ)
    main_cols = main.T
    long_cols = long_skip.T
    stream = (
        lax.psum_scatter(
            jnp.einsum("dc,dt->ct", w_skip_main, main_cols, preferred_element_type=jnp.float32)
            + jnp.einsum("dc,dt->ct", w_skip_long, long_cols, preferred_element_type=jnp.float32),
            "tp",
            scatter_dimension=0,
            tiled=True,
        )
        + b_skip[:, None]
    )
    normed_one, rstd_one, full_one = layer_norm(stream, ln1_gain, ln1_bias, width)
    qkv = jnp.einsum("edc,dt->ect", w_qkv, full_one, preferred_element_type=jnp.float32).astype(
        jnp.bfloat16
    )
    query_blocks = split_heads(qkv[0], heads_here)
    key_blocks = split_heads(qkv[1], heads_here)
    value_blocks = split_heads(qkv[2], heads_here)
    attended_blocks, logsums = lax.map(attend, (query_blocks, key_blocks, value_blocks))
    attended = join_heads(attended_blocks)
    cols_here = w_proj
    projected = lax.psum_scatter(
        jnp.einsum("rc,rt->ct", cols_here, attended, preferred_element_type=jnp.float32).astype(
            jnp.bfloat16
        ),
        "tp",
        scatter_dimension=0,
        tiled=True,
    ).astype(jnp.float32)
    stream_two = stream + projected + b_proj[:, None]
    normed_two, rstd_two, full_two = layer_norm(stream_two, ln2_gain, ln2_bias, width)
    upward = (
        jnp.einsum("dc,dt->ct", w_up, full_two, preferred_element_type=jnp.float32) + b_up[:, None]
    )
    activated = jax.nn.gelu(upward, approximate=False).astype(jnp.bfloat16)
    cols_here = w_down
    result = (
        stream_two
        + lax.psum_scatter(
            jnp.einsum(
                "fc,ft->ct", cols_here, activated, preferred_element_type=jnp.float32
            ).astype(jnp.bfloat16),
            "tp",
            scatter_dimension=0,
            tiled=True,
        ).astype(jnp.float32)
        + b_down[:, None]
    )
    out = (result * row_valid[None, :]).T.astype(jnp.bfloat16)
    grad_low = (cotangent.T.astype(jnp.float32) * row_scale[None, :]).astype(jnp.bfloat16)
    grad_wide = grad_low.astype(jnp.float32)
    g_b_down = jnp.sum(grad_wide, 1)
    (d_activated,), (g_w_down,) = fold_back(grad_low, ((w_down, activated),))
    cumulative = 0.5 * (1.0 + lax.erf(upward * ROOT_HALF))
    density = jnp.exp(-0.5 * upward * upward) * DENSITY_SCALE
    d_upward = (d_activated * (cumulative + upward * density)).astype(jnp.bfloat16)
    g_b_up = jnp.sum(d_upward.astype(jnp.float32), 1)
    g_w_up = jnp.einsum("dt,ft->df", full_two, d_upward, preferred_element_type=jnp.float32)

    def up_term(start, count_rows):
        return jnp.einsum("cf,ft->ct", w_up, d_upward, preferred_element_type=jnp.float32)

    d_normed_two = reduce_back(up_term, local_width)
    back_two, g_ln2_gain, g_ln2_bias = norm_back(
        d_normed_two, normed_two, rstd_two, ln2_gain, width
    )
    d_stream_two = (back_two + grad_wide).astype(jnp.bfloat16)
    d_stream_wide = d_stream_two.astype(jnp.float32)
    g_b_proj = jnp.sum(d_stream_wide, 1)
    (d_attended,), (g_w_proj,) = fold_back(d_stream_two, ((w_proj, attended),))
    d_attended_blocks = split_heads(d_attended.astype(jnp.bfloat16), heads_here)
    d_queries, d_keys, d_values = lax.map(
        attend_back, (query_blocks, key_blocks, value_blocks, logsums, d_attended_blocks)
    )
    d_qkv = jnp.stack([join_heads(d_queries), join_heads(d_keys), join_heads(d_values)], axis=0)
    g_w_qkv = jnp.einsum("dt,ect->edc", full_one, d_qkv, preferred_element_type=jnp.float32)

    def qkv_term(start, count_rows):
        return jnp.einsum("ecr,ert->ct", w_qkv, d_qkv, preferred_element_type=jnp.float32)

    d_normed_one = reduce_back(qkv_term, local_width)
    back_one, g_ln1_gain, g_ln1_bias = norm_back(
        d_normed_one, normed_one, rstd_one, ln1_gain, width
    )
    d_stream = (back_one + d_stream_wide).astype(jnp.bfloat16)
    g_b_skip = jnp.sum(d_stream.astype(jnp.float32), 1)
    (d_main_cols, d_long_cols), (g_w_main, g_w_long) = fold_back(
        d_stream, ((w_skip_main, main_cols), (w_skip_long, long_cols))
    )
    (
        g_w_main,
        g_w_long,
        g_b_skip,
        g_ln1_gain,
        g_ln1_bias,
        g_w_qkv,
        g_w_proj,
        g_b_proj,
        g_ln2_gain,
        g_ln2_bias,
        g_w_up,
        g_b_up,
        g_w_down,
        g_b_down,
    ) = (
        lax.psum(g_w_main.astype(jnp.bfloat16), "dp").astype(jnp.float32),
        lax.psum(g_w_long.astype(jnp.bfloat16), "dp").astype(jnp.float32),
        lax.psum(g_b_skip.astype(jnp.bfloat16), "dp").astype(jnp.float32),
        lax.psum(g_ln1_gain.astype(jnp.bfloat16), "dp").astype(jnp.float32),
        lax.psum(g_ln1_bias.astype(jnp.bfloat16), "dp").astype(jnp.float32),
        lax.psum(g_w_qkv.astype(jnp.bfloat16), "dp").astype(jnp.float32),
        lax.psum(g_w_proj.astype(jnp.bfloat16), "dp").astype(jnp.float32),
        lax.psum(g_b_proj.astype(jnp.bfloat16), "dp").astype(jnp.float32),
        lax.psum(g_ln2_gain.astype(jnp.bfloat16), "dp").astype(jnp.float32),
        lax.psum(g_ln2_bias.astype(jnp.bfloat16), "dp").astype(jnp.float32),
        lax.psum(g_w_up.astype(jnp.bfloat16), "dp").astype(jnp.float32),
        lax.psum(g_b_up.astype(jnp.bfloat16), "dp").astype(jnp.float32),
        lax.psum(g_w_down.astype(jnp.bfloat16), "dp").astype(jnp.float32),
        lax.psum(g_b_down.astype(jnp.bfloat16), "dp").astype(jnp.float32),
    )
    d_main = d_main_cols.T.astype(jnp.bfloat16)
    d_long = d_long_cols.T.astype(jnp.bfloat16)
    return (
        out,
        d_main,
        d_long,
        g_w_main,
        g_w_long,
        g_b_skip,
        g_ln1_gain,
        g_ln1_bias,
        g_w_qkv,
        g_w_proj,
        g_b_proj,
        g_ln2_gain,
        g_ln2_bias,
        g_w_up,
        g_b_up,
        g_w_down,
        g_b_down,
    )


ITEM_ROWS = 264
GRAD_ROWS = 24
CORE = ("tp", 1)
ACROSS_Y = ("tp", 2)
ACROSS_X = ("dp", 1)
ACROSS_Z = ("dp", 2)
FAR_Z = ("dp", 4)


def swap(value, link):
    axis, bit = link
    return lax.ppermute(value, axis, [(i, i ^ bit) for i in range(lax.axis_size(axis))])


def side(link):
    axis, bit = link
    return (lax.axis_index(axis) // bit) % 2


def in_order(bit, mine, theirs):
    flip = bit == 1
    return jnp.stack([jnp.where(flip, theirs, mine), jnp.where(flip, mine, theirs)])


def pick(value, index):
    return lax.dynamic_index_in_dim(value, index, 0, keepdims=False)


def peer(value, bit):
    return value + bit - 2 * bit * ((value // bit) % 2)


def greet(peers):
    barrier = pltpu.get_barrier_semaphore()
    for where in peers:
        pl.semaphore_signal(barrier, inc=1, device_id=where, device_id_type=pl.DeviceIdType.MESH)
    pl.semaphore_wait(barrier, len(peers))


def send(source, target, sems, index, where):
    return pltpu.make_async_remote_copy(
        src_ref=source,
        dst_ref=target,
        send_sem=sems.at[0, index],
        recv_sem=sems.at[1, index],
        device_id=where,
        device_id_type=pl.DeviceIdType.MESH,
    )


def gather_kernel(pieces, n_in, n_out, *refs):
    tokens, vectors, inputs = refs[0], refs[1], refs[2 : 2 + n_in]
    refs = refs[2 + n_in :]
    far_tokens, core_near, core_far, far_vectors, core_vectors = refs[:5]
    outs, held = refs[5 : 5 + n_out], refs[5 + n_out : 5 + n_out + n_in]
    y_sem, one_sem, two_sem, own_sem, far_sem, local_sem, token_sem = refs[5 + n_out + n_in :]
    n = len(pieces)
    shards = [inputs[a].at[lead] if lead else inputs[a] for a, lead, _, _ in pieces]
    stage = [held[a].at[lead] if lead else held[a] for a, lead, _, _ in pieces]
    fulls = [
        [outs[b[place]].at[tail] if isinstance(b, tuple) else outs[b].at[(place,) + tail] for place in range(4)]
        for _, _, b, tail in pieces
    ]
    dp, tp = lax.axis_index("dp"), lax.axis_index("tp")
    core, y = tp % 2, (tp // 2) % 2
    to_core, to_y = {"tp": peer(tp, 1)}, {"tp": peer(tp, 2)}
    links = ({"dp": peer(dp, 1)}, {"dp": peer(dp, 2)})
    bits = (dp % 2, (dp // 2) % 2)
    greet((to_core, to_y) + links)

    def places(k):
        return k % 2, 1 - k % 2, bits[k % 2], bits[1 - k % 2]

    def y_copy(k):
        _, _, f, s = places(k)
        return send(shards[k].at[s, f], fulls[k][1].at[s, f], y_sem, k, to_y)

    def one_copy(k):
        first, _, f, s = places(k)
        part = fulls[k][1].at[s, f]
        return send(part, part, one_sem, k, links[first])

    def two_copy(k):
        _, second, _, s = places(k)
        part = fulls[k][1].at[s]
        return send(part, part, two_sem, k, links[second])

    def own_copy(k):
        return send(shards[k], fulls[k][2], own_sem, k, to_core)

    def far_copy(k):
        return send(fulls[k][1], fulls[k][3], far_sem, k, to_core)

    def load(k):
        return pltpu.make_async_copy(shards[k], stage[k], local_sem.at[0, k])

    def store(k):
        return pltpu.make_async_copy(stage[k], fulls[k][0], local_sem.at[1, k])

    token_y = send(tokens.at[1 - y], far_tokens, token_sem, 0, to_y)
    token_near = send(tokens.at[y, 1 - core], core_near, token_sem, 1, to_core)
    token_far = send(far_tokens.at[1 - core], core_far, token_sem, 2, to_core)
    vectors_y = send(vectors, far_vectors, token_sem, 3, to_y)
    vectors_near = send(vectors, core_vectors.at[0], token_sem, 4, to_core)
    vectors_far = send(far_vectors, core_vectors.at[1], token_sem, 5, to_core)
    vectors_y.start()
    vectors_near.start()
    for k in range(n):
        y_copy(k).start()
    token_y.start()
    token_near.start()
    for k in range(n):
        load(k).start()
        own_copy(k).start()
    for step in range(n + 2):
        if step < n:
            y_copy(step).wait_recv()
            one_copy(step).start()
            load(step).wait()
            store(step).start()
        if 0 <= step - 1 < n:
            one_copy(step - 1).wait_recv()
            two_copy(step - 1).start()
        if 0 <= step - 2 < n:
            two_copy(step - 2).wait_recv()
            far_copy(step - 2).start()
    vectors_y.wait_recv()
    vectors_far.start()
    token_y.wait_recv()
    token_far.start()
    for copy in (token_near, token_far, vectors_near, vectors_far):
        copy.wait()
    token_y.wait_send()
    vectors_y.wait_send()
    for k in range(n):
        far_copy(k).wait()
        own_copy(k).wait()
        store(k).wait()
        for copy in (y_copy(k), one_copy(k), two_copy(k)):
            copy.wait_send()


def gather_weights(tokens, vectors, arrays, pieces, out_shapes):
    n = len(pieces)
    shape = lambda dims, like: jax.ShapeDtypeStruct(dims, like.dtype)
    rows = tokens.shape[2:]
    outs = [shape((2,) + rows, tokens), shape(rows, tokens), shape(rows, tokens)]
    outs += [shape(vectors.shape, vectors), shape((2,) + vectors.shape, vectors)]
    outs += [shape(dims, arrays[0]) for dims in out_shapes]
    sems = [pltpu.SemaphoreType.DMA((2, n))] * 6 + [pltpu.SemaphoreType.DMA((2, 6))]
    return pl.pallas_call(
        functools.partial(gather_kernel, pieces, len(arrays), len(out_shapes)),
        out_shape=outs,
        in_specs=[pl.BlockSpec(memory_space=pl.ANY)] * (2 + len(arrays)),
        out_specs=[pl.BlockSpec(memory_space=pl.ANY)] * len(outs),
        scratch_shapes=[pltpu.VMEM(a.shape, a.dtype) for a in arrays] + sems,
        compiler_params=pltpu.CompilerParams(
            collective_id=1, has_side_effects=True, vmem_limit_bytes=32 * 2**20
        ),
        name="gather_weights",
    )(tokens, vectors, *arrays)


LAG = 7


def reduce_kernel(n_early, whole_sizes, views, n_arrays, *refs):
    early, arrays, blocks = refs[0], refs[1 : 1 + n_arrays], refs[1 + n_arrays]
    refs = refs[2 + n_arrays :]
    early_out, outs, refs = refs[0], refs[1 : 1 + len(views)], refs[1 + len(views) :]
    from_core, y_blocks = refs[:2]
    refs = refs[2:]
    total, from_y, from_one, half, from_two, from_far, final = refs[:7]
    y_sem, one_sem, two_sem, far_sem, back_two, back_one, block_sem, load_sem, out_sem = refs[7:]
    n_whole = total.shape[0]
    chunks = n_early + n_whole
    dp, tp = lax.axis_index("dp"), lax.axis_index("tp")
    to_core, to_y, to_far = {"tp": peer(tp, 1)}, {"tp": peer(tp, 2)}, {"dp": peer(dp, 4)}
    greet((to_core, to_y, {"dp": peer(dp, 1)}, {"dp": peer(dp, 2)}, to_far))

    def plan(s):
        z_first = jnp.where(s >= n_early, ((s + 5 - n_early % 5) % 5) // 3, 0)
        first, second = 1 + z_first, 2 - z_first
        places = (dp // first) % 2, (dp // second) % 2
        return ({"dp": peer(dp, first)}, {"dp": peer(dp, second)}) + places

    def y_copy(r, source):
        return send(source, from_y.at[r], y_sem, r, to_y)

    def one_copy(r):
        to_one, _, f, _ = plan(r + n_early)
        return send(total.at[r, 1 - f], from_one.at[r], one_sem, r, to_one)

    def two_copy(s):
        _, to_two, _, g = plan(s)
        return send(half.at[s, 1 - g], from_two.at[s], two_sem, s, to_two)

    def far_copy(s):
        _, _, _, g = plan(s)
        return send(half.at[s, g], from_far.at[s], far_sem, s, to_far)

    def back_two_copy(s):
        _, to_two, f, g = plan(s)
        part = final.at[s, f, g]
        return send(part, part, back_two, s, to_two)

    def back_one_copy(s):
        to_one, _, f, _ = plan(s)
        part = final.at[s, f]
        return send(part, part, back_one, s, to_one)

    def out_copies(s, act):
        @pl.when(s < n_early)
        def _():
            for p in range(2):
                act(pltpu.make_async_copy(final.at[s, p], early_out.at[p, s], out_sem.at[p, s]))

        at = n_early
        for k, size in enumerate(whole_sizes):

            @pl.when((s >= at) & (s < at + size))
            def _(k=k, at=at):
                act(pltpu.make_async_copy(final.at[s], outs[k].at[s - at], out_sem.at[0, s]))

            at += size

    early_load = pltpu.make_async_copy(early, half.at[pl.ds(0, n_early)], load_sem.at[0])
    early_load.start()
    core_blocks = [send(blocks.at[2 + k], from_core.at[k], block_sem, k, to_core) for k in range(2)]
    own_block = send(blocks.at[1], y_blocks.at[0], block_sem, 2, to_y)
    core_block = send(from_core.at[1], y_blocks.at[1], block_sem, 3, to_y)
    loads, at = [], 0
    for k, (size, (a, mine, theirs)) in enumerate(zip(whole_sizes, views)):
        source = arrays[a].at[mine]
        loads.append(pltpu.make_async_copy(source, total.at[pl.ds(at, size)], load_sem.at[1 + k]))
        loads[-1].start()
        for r in range(size):
            y_copy(at + r, arrays[a].at[theirs + (r,)]).start()
        at += size
    for copy in core_blocks:
        copy.start()
    own_block.start()
    early_load.wait()
    for copy in loads:
        copy.wait()

    def plus(left, right):
        return (left.astype(jnp.float32) + right.astype(jnp.float32)).astype(jnp.bfloat16)

    def step(t, carry):
        @pl.when(t < n_early)
        def _():
            two_copy(t).start()

        @pl.when((t >= n_early) & (t < chunks))
        def _():
            _, _, f, _ = plan(t)
            one_copy(t - n_early).wait_recv()
            half[t] = plus(total[t - n_early, f], from_one[t - n_early])
            two_copy(t).start()

        @pl.when((t >= 1) & (t < chunks + 1))
        def _():
            s = t - 1
            _, _, _, g = plan(s)
            two_copy(s).wait_recv()
            half[s, g] = plus(half[s, g], from_two[s])
            far_copy(s).start()

        @pl.when((t >= 3) & (t < chunks + 3))
        def _():
            s = t - 3
            _, _, f, g = plan(s)
            far_copy(s).wait_recv()
            final[s, f, g] = plus(half[s, g], from_far[s])
            back_two_copy(s).start()

        @pl.when((t >= 4) & (t < chunks + 4))
        def _():
            back_two_copy(t - 4).wait_recv()
            back_one_copy(t - 4).start()

        @pl.when((t >= 5) & (t < chunks + 5))
        def _():
            back_one_copy(t - 5).wait_recv()
            out_copies(t - 5, lambda copy: copy.start())

        @pl.when((t >= LAG) & (t < LAG + n_whole))
        def _():
            r = t - LAG
            y_copy(r, total.at[r]).wait_recv()
            total[r] = plus(total[r], from_y[r])
            one_copy(r).start()

        @pl.when(t == 2)
        def _():
            for copy in core_blocks:
                copy.wait_recv()
            core_block.start()

        return carry

    lax.fori_loop(0, chunks + 5, step, 0)

    def finish_whole(r, carry):
        y_copy(r, total.at[r]).wait_send()
        one_copy(r).wait_send()
        return carry

    lax.fori_loop(0, n_whole, finish_whole, 0)

    def finish(s, carry):
        for copy in (two_copy(s), far_copy(s), back_two_copy(s), back_one_copy(s)):
            copy.wait_send()
        out_copies(s, lambda copy: copy.wait())
        return carry

    lax.fori_loop(0, chunks, finish, 0)
    for copy in core_blocks:
        copy.wait_send()
    own_block.wait()
    core_block.wait()


def reduce_grads(early, arrays, views, blocks):
    sizes = tuple(arrays[a].shape[len(mine)] for a, mine, _ in views)
    n_early, n_whole = early.shape[0], sum(sizes)
    chunks = n_early + n_whole
    rows, width = early.shape[-2:]
    kind = early.dtype
    sem = lambda n: pltpu.SemaphoreType.DMA((2, n))
    two_blocks = jax.ShapeDtypeStruct((2,) + blocks.shape[1:], blocks.dtype)
    return pl.pallas_call(
        functools.partial(reduce_kernel, n_early, sizes, views, len(arrays)),
        out_shape=[jax.ShapeDtypeStruct((2, n_early, 2, rows, width), kind)]
        + [jax.ShapeDtypeStruct((n, 2, 2, rows, width), kind) for n in sizes]
        + [two_blocks, two_blocks],
        in_specs=[pl.BlockSpec(memory_space=pl.ANY)] * (2 + len(arrays)),
        out_specs=[pl.BlockSpec(memory_space=pl.ANY)] * (3 + len(views)),
        scratch_shapes=[
            pltpu.VMEM((n_whole, 2, 2, rows, width), kind),
            pltpu.VMEM((n_whole, 2, 2, rows, width), kind),
            pltpu.VMEM((n_whole, 2, rows, width), kind),
            pltpu.VMEM((chunks, 2, rows, width), kind),
            pltpu.VMEM((chunks, rows, width), kind),
            pltpu.VMEM((chunks, rows, width), kind),
            pltpu.VMEM((chunks, 2, 2, rows, width), kind),
            sem(n_whole),
            sem(n_whole),
            sem(chunks),
            sem(chunks),
            sem(chunks),
            sem(chunks),
            sem(4),
            pltpu.SemaphoreType.DMA((1 + len(views),)),
            sem(chunks),
        ],
        compiler_params=pltpu.CompilerParams(
            collective_id=2, has_side_effects=True, vmem_limit_bytes=56 * 2**20
        ),
        name="reduce_grads",
    )(early, *arrays, blocks)


def add_low(mine, theirs):
    return (mine.astype(jnp.float32) + theirs.astype(jnp.float32)).astype(jnp.bfloat16)


def place_of(index):
    rank = lax.axis_index("tp")
    core, y = rank % 2, (rank // 2) % 2
    there_core, there_y = index % 2, index // 2
    apart = lambda a, b: a + b - 2 * a * b
    return apart(y, there_y) + 2 * apart(core, there_core)


def spread_kernel(main_ref, long_ref, cot_ref, tokens_ref, cot_tokens_ref):
    cols = main_ref.shape[1]
    items = tokens_ref.shape[1] // ITEM_ROWS
    for p in range(4):
        for i in range(items):
            source = slice((p * items + i) * SEQ, (p * items + i + 1) * SEQ)
            target = slice(i * ITEM_ROWS, i * ITEM_ROWS + SEQ)
            blank = slice(i * ITEM_ROWS + SEQ, (i + 1) * ITEM_ROWS)
            tokens_ref[p, target, :cols] = main_ref[source, :]
            tokens_ref[p, target, cols:] = long_ref[source, :]
            cot_tokens_ref[p, target, :] = cot_ref[source, :]
            tokens_ref[p, blank, :] = jnp.zeros((ITEM_ROWS - SEQ, 2 * cols), tokens_ref.dtype)
            cot_tokens_ref[p, blank, :] = jnp.zeros((ITEM_ROWS - SEQ, cols), tokens_ref.dtype)


def spread(main, long_skip, cotangent):
    rows, cols = main.shape
    padded = rows // SEQ // 4 * ITEM_ROWS
    return pl.pallas_call(
        spread_kernel,
        out_shape=[
            jax.ShapeDtypeStruct((4, padded, 2 * cols), main.dtype),
            jax.ShapeDtypeStruct((4, padded, cols), main.dtype),
        ],
        compiler_params=pltpu.CompilerParams(vmem_limit_bytes=40 * 2**20),
        name="spread",
    )(main, long_skip, cotangent)


def arrange_kernel(own_ref, y_ref, partner_ref, scale_ref, out_ref, held):
    cols = own_ref.shape[1]
    held[0] = own_ref[...]
    held[1] = y_ref[...]
    held[2] = partner_ref[0]
    held[3] = partner_ref[1]
    for j in range(4):
        block = held[place_of(j)].astype(jnp.float32) * scale_ref[...]
        out_ref[:, j * cols : (j + 1) * cols] = block.astype(out_ref.dtype)


def arrange(own, along_y, partner, scale):
    rows, cols = own.shape
    return pl.pallas_call(
        arrange_kernel,
        out_shape=jax.ShapeDtypeStruct((rows, 4 * cols), own.dtype),
        scratch_shapes=[pltpu.VMEM((4, rows, cols), own.dtype)],
        compiler_params=pltpu.CompilerParams(vmem_limit_bytes=24 * 2**20),
        name="arrange",
    )(own, along_y, partner, scale)


def disperse_kernel(rows_ref, valid_ref, out_ref):
    cols = out_ref.shape[2]
    for j in range(4):
        block = rows_ref[:, j * cols : (j + 1) * cols] * valid_ref[...]
        out_ref[place_of(j)] = block.astype(out_ref.dtype)


def disperse(rows, valid):
    count, width = rows.shape
    return pl.pallas_call(
        disperse_kernel,
        out_shape=jax.ShapeDtypeStruct((4, count, width // 4), jnp.bfloat16),
        compiler_params=pltpu.CompilerParams(vmem_limit_bytes=24 * 2**20),
        name="disperse",
    )(rows, valid)


def unspread_kernel(parts, own_ref, core_ref, y_ref, *refs):
    outs, held = refs[:parts], refs[parts]
    cols = outs[0].shape[1]
    items = own_ref.shape[0] // ITEM_ROWS
    held[0] = own_ref[...]
    held[1] = y_ref[0]
    held[2] = core_ref[...]
    held[3] = y_ref[1]
    for p in range(4):
        rows = held[place_of(p)]
        for i in range(items):
            target = slice((p * items + i) * SEQ, (p * items + i + 1) * SEQ)
            source = slice(i * ITEM_ROWS, i * ITEM_ROWS + SEQ)
            for k in range(parts):
                outs[k][target, :] = rows[source, k * cols : (k + 1) * cols]


def unspread(own, core_tokens, y_tokens, parts):
    rows, width = own.shape
    out = jax.ShapeDtypeStruct((4 * rows // ITEM_ROWS * SEQ, width // parts), own.dtype)
    return pl.pallas_call(
        functools.partial(unspread_kernel, parts),
        out_shape=[out] * parts,
        scratch_shapes=[pltpu.VMEM((4, rows, width), own.dtype)],
        compiler_params=pltpu.CompilerParams(vmem_limit_bytes=40 * 2**20),
        name="unspread",
    )(own, core_tokens, y_tokens)


def natural(own_half, partner_half, width, axis):
    flip_y, flip_core = side(ACROSS_Y) == 1, side(CORE) == 1
    r0, r2 = jnp.split(own_half, 2, axis)
    r1, r3 = jnp.split(partner_half, 2, axis)
    a0, a2 = jnp.where(flip_y, r2, r0), jnp.where(flip_y, r0, r2)
    a1, a3 = jnp.where(flip_y, r3, r1), jnp.where(flip_y, r1, r3)
    b0, b1 = jnp.where(flip_core, a1, a0), jnp.where(flip_core, a0, a1)
    b2, b3 = jnp.where(flip_core, a3, a2), jnp.where(flip_core, a2, a3)
    return (b0, b1, b2, b3)


def dot(spec, left, right):
    return jnp.einsum(spec, left, right, preferred_element_type=jnp.float32)


def low(value):
    return value.astype(jnp.bfloat16)


def norm_rows(stream, gain, bias):
    mean = jnp.mean(stream, 1, keepdims=True)
    square = jnp.mean(stream * stream, 1, keepdims=True)
    rstd = lax.rsqrt(square - mean * mean + EPSILON)
    normed = (stream - mean) * rstd
    return normed, rstd, low(normed * gain + bias)


def norm_rows_back(d_out, normed, rstd, gain):
    g_gain = jnp.sum(d_out * normed, 0)
    g_bias = jnp.sum(d_out, 0)
    scaled = d_out * gain
    first = jnp.mean(scaled, 1, keepdims=True)
    second = jnp.mean(scaled * normed, 1, keepdims=True)
    return rstd * (scaled - first - normed * second), g_gain, g_bias


LAST = (((1,), (1,)), ((), ()))
LEAD = (((0,), (0,)), ((), ()))


def item_scores(key, query):
    scores = lax.dot_general(key, query, LAST, preferred_element_type=jnp.float32)
    present = lax.broadcasted_iota(jnp.int32, scores.shape, 0) < SEQ
    return jnp.where(present, scores * (1.0 / math.sqrt(HEAD)), -1e30)


def attend_kernel(q_ref, k_ref, v_ref, out_ref, lse_ref):
    for h in range(q_ref.shape[1] // HEAD):
        at = slice(h * HEAD, (h + 1) * HEAD)
        scores = item_scores(k_ref[:, at], q_ref[:, at])
        peak = jnp.max(scores, axis=0, keepdims=True)
        weights = jnp.exp(scores - peak)
        total = jnp.sum(weights, axis=0, keepdims=True)
        probs = (weights * (1.0 / total)).astype(jnp.bfloat16)
        out = lax.dot_general(probs, v_ref[:, at], LEAD, preferred_element_type=jnp.float32)
        out_ref[:, at] = out.astype(jnp.bfloat16)
        lse_ref[0, h : h + 1, :] = peak + jnp.log(total)


def attend_back_kernel(q_ref, k_ref, v_ref, lse_ref, d_ref, dq_ref, dk_ref, dv_ref):
    scale = 1.0 / math.sqrt(HEAD)
    for h in range(q_ref.shape[1] // HEAD):
        at = slice(h * HEAD, (h + 1) * HEAD)
        query, key, d_out = q_ref[:, at], k_ref[:, at], d_ref[:, at]
        probs = jnp.exp(item_scores(key, query) - lse_ref[0, h : h + 1, :])
        d_probs = lax.dot_general(v_ref[:, at], d_out, LAST, preferred_element_type=jnp.float32)
        delta = jnp.sum(probs * d_probs, axis=0, keepdims=True)
        d_scores = (probs * (d_probs - delta)).astype(jnp.bfloat16)
        dq = lax.dot_general(d_scores, key, LEAD, preferred_element_type=jnp.float32)
        dk = jnp.dot(d_scores, query, preferred_element_type=jnp.float32)
        dv = jnp.dot(probs.astype(jnp.bfloat16), d_out, preferred_element_type=jnp.float32)
        dq_ref[:, at] = (dq * scale).astype(jnp.bfloat16)
        dk_ref[:, at] = (dk * scale).astype(jnp.bfloat16)
        dv_ref[:, at] = dv.astype(jnp.bfloat16)


def attention(query, key, value):
    rows, cols = query.shape
    heads, items = cols // HEAD, rows // ITEM_ROWS
    block = pl.BlockSpec((ITEM_ROWS, cols), lambda i: (i, 0))
    return pl.pallas_call(
        attend_kernel,
        grid=(items,),
        out_shape=[
            jax.ShapeDtypeStruct((rows, cols), jnp.bfloat16),
            jax.ShapeDtypeStruct((items, heads, ITEM_ROWS), jnp.float32),
        ],
        in_specs=[block] * 3,
        out_specs=[block, pl.BlockSpec((1, heads, ITEM_ROWS), lambda i: (i, 0, 0))],
        cost_estimate=pl.CostEstimate(
            flops=4 * rows * ITEM_ROWS * cols, bytes_accessed=8 * rows * cols, transcendentals=rows * ITEM_ROWS * heads
        ),
        name="attend",
    )(query, key, value)


def attention_back(query, key, value, lse, d_out):
    rows, cols = query.shape
    heads, items = cols // HEAD, rows // ITEM_ROWS
    block = pl.BlockSpec((ITEM_ROWS, cols), lambda i: (i, 0))
    return pl.pallas_call(
        attend_back_kernel,
        grid=(items,),
        out_shape=[jax.ShapeDtypeStruct((rows, cols), jnp.bfloat16)] * 3,
        in_specs=[block, block, block, pl.BlockSpec((1, heads, ITEM_ROWS), lambda i: (i, 0, 0)), block],
        out_specs=[block] * 3,
        cost_estimate=pl.CostEstimate(
            flops=10 * rows * ITEM_ROWS * cols, bytes_accessed=14 * rows * cols, transcendentals=rows * ITEM_ROWS * heads
        ),
        name="attend_back",
    )(query, key, value, lse, d_out)


def body_items(
    main,
    long_skip,
    cotangent,
    timesteps,
    loss_codes,
    code_weights,
    item_counts,
    w_skip_main,
    w_skip_long,
    b_skip,
    ln1_gain,
    ln1_bias,
    w_qkv,
    w_proj,
    b_proj,
    ln2_gain,
    ln2_bias,
    w_up,
    b_up,
    w_down,
    b_down,
):
    local = main.shape[1]
    width = 4 * local
    rank = lax.axis_index("tp")

    vectors = jnp.concatenate(
        [jnp.stack([b_skip, ln1_gain, ln1_bias, b_proj, ln2_gain, ln2_bias, b_down]), b_up.reshape(4, local)]
    )
    y, core, x, z = side(ACROSS_Y), side(CORE), side(ACROSS_X), side(ACROSS_Z)
    cut = 2 * local
    tokens, cot_tokens = spread(main, long_skip, cotangent)
    tokens = tokens.reshape((2, 2) + tokens.shape[1:])
    cot_tokens = cot_tokens.reshape((2, 2) + cot_tokens.shape[1:])
    quarters = lambda w: w.reshape(2, 2, -1, width)
    qkv_rows = jnp.swapaxes(w_qkv, 1, 2).reshape(3, 2, 2, local // 4, width)
    one = (4, 2, 2, local // 4, width)
    far_tokens, core_near, core_far, far_vectors, core_vectors, wskip, wq, wk, wv, wp, *wu = gather_weights(
        tokens,
        vectors,
        [
            quarters(w_skip_main),
            quarters(w_skip_long),
            qkv_rows,
            quarters(w_proj),
            w_up.reshape(2, 2, 2, width // 8, width),
        ],
        [
            (0, (), 0, (0,)),
            (1, (), 0, (1,)),
            (2, (0,), 1, ()),
            (2, (1,), 2, ()),
            (2, (2,), 3, ()),
            (3, (), 4, ()),
            (4, (0,), (5, 6, 7, 8), (0,)),
            (4, (1,), (5, 6, 7, 8), (1,)),
        ],
        [(4, 2) + one[1:], one, one, one, one] + [(2, 2, 2, width // 8, width)] * 4,
    )
    own_vectors = jnp.concatenate([vectors, far_vectors], axis=1)
    partner_vectors = jnp.concatenate([core_vectors[0], core_vectors[1]], axis=1)
    joined = jnp.concatenate(natural(own_vectors[:7], partner_vectors[:7], local, 1), axis=1)
    b_skip_all, gain_one, bias_one, b_proj_all, gain_two, bias_two, b_down_all = (
        joined[k : k + 1] for k in range(7)
    )

    def up_vector(pair):
        near, far = jnp.split(pair[7:], 2, 1)
        return jnp.concatenate([near.reshape(1, -1), far.reshape(1, -1)], axis=1)

    b_up_all = jnp.concatenate([up_vector(own_vectors), up_vector(partner_vectors)], axis=1)

    wskip, wq, wk, wv, wp = (g.reshape(-1, width) for g in (wskip, wq, wk, wv, wp))
    wu = [w.reshape(width, width) for w in wu]
    near_tokens = pick(tokens, y)
    skip_rows = jnp.concatenate([pick(near_tokens, core), pick(far_tokens, core), core_near, core_far], axis=1)
    other = lambda value: swap(value, CORE)
    both = lambda mine, others: jnp.concatenate([mine, others], axis=0)
    shares = lambda value: both(value[:, : value.shape[1] // 2], other(value[:, value.shape[1] // 2 :]))

    def after(value, *events):
        return lax.optimization_barrier((value,) + events)[0]

    meet = lambda *values: lax.optimization_barrier(values)

    w_down_then = after(w_down, wskip)
    wd_core = other(w_down_then)
    wd_y = swap(w_down_then, ACROSS_Y)
    cot_near = pick(cot_tokens, y)
    cot_far = swap(after(pick(cot_tokens, 1 - y), wskip), ACROSS_Y)

    stream = dot("td,dc->tc", skip_rows, wskip) + b_skip_all
    normed_one, rstd_one, full_one = norm_rows(stream, gain_one, bias_one)
    skip_both = jnp.concatenate([pick(near_tokens, 1 - core), pick(far_tokens, 1 - core)], axis=1)
    skip_both = both(skip_rows[:, : 2 * cut], skip_both)
    n1_both = both(full_one, other(full_one))
    query, key, value = (low(dot("td,cd->tc", full_one, w)) for w in (wq, wk, wv))
    attended, logsum = attention(query, key, value)
    attended_both = shares(attended)
    stream_two = stream + dot("tc,cd->td", attended, wp) + b_proj_all
    cot_far, stream_two, skip_both, n1_both = meet(cot_far, stream_two, skip_both, n1_both)
    cot_partner = other(jnp.stack([pick(cot_near, 1 - core), pick(cot_far, 1 - core)]))
    normed_two, rstd_two, full_two = norm_rows(stream_two, gain_two, bias_two)
    n2_both = both(full_two, other(full_two))
    acts, slopes = [], []
    for r in range(4):
        upward = dot("td,dc->tc", full_two, wu[r]) + b_up_all[:, r * width : (r + 1) * width]
        cumulative = 0.5 * (1.0 + lax.erf(upward * ROOT_HALF))
        density = jnp.exp(-0.5 * upward * upward) * DENSITY_SCALE
        acts.append(low(upward * cumulative))
        slopes.append(low(cumulative + upward * density))

    item_scale, valid = item_factors(timesteps, loss_codes, code_weights, item_counts[0])
    row_scale = jnp.repeat(pick(item_scale.reshape(4, -1), rank), ITEM_ROWS)[:, None]
    row_valid = jnp.repeat(pick(valid.reshape(4, -1), rank), ITEM_ROWS)[:, None]
    grad_low = arrange(pick(cot_near, core), pick(cot_far, core), cot_partner, row_scale)
    wd_y = after(wd_y, acts[1])
    wd = [w_down, wd_y, wd_core, other(wd_y)]
    grad_both = both(grad_low, other(grad_low))
    grad_wide = grad_low.astype(jnp.float32)
    g_b_down = jnp.sum(grad_wide, 0)

    def weight_grad(left, right):
        return low(dot("tf,tc->fc", left, right))

    def split(value, bit):
        halves = value.reshape(2, -1, width)
        return pick(halves, bit), pick(halves, 1 - bit)

    down_mine, down_theirs = (weight_grad(both(acts[p], other(acts[2 + p])), grad_both) for p in (0, 1))
    grad_then = after(grad_low, down_theirs)
    down_come = swap(down_theirs, ACROSS_Y)
    down_mine, grad_then = meet(down_mine, grad_then)

    result = stream_two + sum(dot("tf,fc->tc", acts[r], wd[r]) for r in range(4)) + b_down_all
    outs = disperse(result, row_valid)
    out_core = other(outs[2:])
    out_y = swap(jnp.stack([outs[1], out_core[1]]), ACROSS_Y)
    (out,) = unspread(outs[0], out_core[0], out_y, 1)

    d_up = [low(dot("tc,fc->tf", grad_then, wd[r]) * slopes[r].astype(jnp.float32)) for r in range(4)]
    g_b_up = jnp.stack([jnp.sum(d.astype(jnp.float32), 0) for d in d_up])
    up_mine, up_theirs = (weight_grad(n2_both, both(d_up[p], other(d_up[2 + p]))) for p in (0, 1))
    d_up[0] = after(d_up[0], up_theirs)
    up_come = swap(up_theirs, ACROSS_Y)
    up_mine = after(up_mine, d_up[0])
    d_n2 = sum(dot("tf,cf->tc", d_up[r], wu[r]) for r in range(4))
    back_two, g_ln2_gain, g_ln2_bias = norm_rows_back(d_n2, normed_two, rstd_two, gain_two)
    d_stream_two = low(back_two + grad_wide)
    d_stream_wide = d_stream_two.astype(jnp.float32)
    g_b_proj = jnp.sum(d_stream_wide, 0)
    chunked = lambda g, lead: g.reshape(lead + (-1, 2, 2, GRAD_ROWS, width))
    proj_part = chunked(weight_grad(attended_both, both(d_stream_two, other(d_stream_two))), (2,))
    d_attended = low(dot("tc,fc->tf", d_stream_two, wp))
    down_come, d_attended = meet(down_come, d_attended)
    down_keep, down_send = split(add_low(down_mine, down_come), x)
    down_come = swap(down_send, ACROSS_X)
    d_qkv = attention_back(query, key, value, logsum, d_attended)
    down_come, *d_qkv = meet(down_come, *d_qkv)
    down_keep, down_send = split(add_low(down_keep, down_come), z)
    down_come = swap(down_send, ACROSS_Z)
    d_own = jnp.concatenate([d[:, :cut] for d in d_qkv], axis=1)
    d_partner = jnp.concatenate([d[:, cut:] for d in d_qkv], axis=1)
    qkv_part = chunked(weight_grad(both(d_own, other(d_partner)), n1_both), (3, 2))
    d_n1 = sum(dot("tc,cd->td", d, w) for d, w in zip(d_qkv, (wq, wk, wv)))
    back_one, g_ln1_gain, g_ln1_bias = norm_rows_back(d_n1, normed_one, rstd_one, gain_one)
    d_stream = low(back_one + d_stream_wide)
    down_come, up_come, d_stream = meet(down_come, up_come, d_stream)
    down_quarter = add_low(down_keep, down_come)
    down_come = swap(down_quarter, FAR_Z)
    up_keep, up_send = split(add_low(up_mine, up_come), x)
    up_come = swap(up_send, ACROSS_X)
    d_stream_both = both(d_stream, other(d_stream))
    g_b_skip = jnp.sum(d_stream.astype(jnp.float32), 0)
    d_skip = low(dot("tc,fc->tf", d_stream, wskip))
    d_blocks = jnp.stack(jnp.split(d_skip, 4, 1))
    down_come, d_stream_both, d_blocks, proj_part, qkv_part = meet(
        down_come, d_stream_both, d_blocks, proj_part, qkv_part
    )
    down_quarter = add_low(down_quarter, down_come)
    down_come = swap(down_quarter, ACROSS_Z)
    skip_part = chunked(weight_grad(skip_both, d_stream_both), (2,))
    down_come, up_come, skip_part = meet(down_come, up_come, skip_part)
    down_half = in_order(z, down_quarter, down_come).reshape(-1, width)
    down_back = swap(down_half, ACROSS_X)

    small = jnp.stack([g_b_skip, g_ln1_gain, g_ln1_bias, g_b_proj, g_ln2_gain, g_ln2_bias, g_b_down])
    arrived = other(jnp.concatenate([small, g_b_up[2:]]))
    small = jnp.moveaxis((small + arrived[:7]).reshape(7, 4, local), 1, 0)
    b_up_sums = g_b_up[:2] + arrived[7:]

    def vector_rows(shard, row):
        flat = jnp.concatenate([pick(small, shard).reshape(-1), b_up_sums[row]])
        return jnp.pad(flat, (0, 4 * GRAD_ROWS * width - flat.size)).reshape(1, 2, 2, GRAD_ROWS, width)

    vector_part = low(jnp.stack([vector_rows(rank, 0), vector_rows(peer(rank, 2), 1)]))
    early = add_low(up_keep, up_come).reshape(-1, 2, GRAD_ROWS, width)
    g_w_up, *sums = reduce_grads(
        early,
        [proj_part, qkv_part, vector_part, skip_part],
        [(0, (0,), (1,)), (1, (0, 0), (0, 1)), (1, (1, 0), (1, 1)), (1, (2, 0), (2, 1)), (2, (0,), (1,)), (3, (0,), (1,))],
        d_blocks,
    )
    from_core, y_blocks = sums[-2:]
    down_back, y_blocks = meet(down_back, y_blocks)
    wide = lambda value: value.reshape(-1, width).astype(jnp.float32)
    g_w_down = wide(in_order(x, down_half, down_back))
    g_w_proj, g_q, g_k, g_v, vectors, g_skip = (wide(g) for g in sums[:-2])
    g_w_qkv = jnp.stack([g.T for g in (g_q, g_k, g_v)])
    vectors = vectors.reshape(-1)
    mine = vectors[: 7 * local].reshape(7, local)

    d_main, d_long = unspread(d_blocks[0], from_core[0], y_blocks, 2)
    return (
        out,
        d_main,
        d_long,
        g_skip[:local],
        g_skip[local:],
        mine[0],
        mine[1],
        mine[2],
        g_w_qkv,
        g_w_proj,
        mine[3],
        mine[4],
        mine[5],
        wide(g_w_up),
        vectors[7 * local : 7 * local + width],
        g_w_down,
        mine[6],
    )


def solution(mesh):
    by_items = mesh.shape["tp"] == 4 and mesh.shape["dp"] == 8
    return jax.shard_map(
        body_items if by_items else body_features,
        mesh=mesh,
        in_specs=(
            P("dp", "tp"),
            P("dp", "tp"),
            P("dp", "tp"),
            P("dp"),
            P("dp"),
            P(),
            P("dp"),
            P("tp", None),
            P("tp", None),
            P("tp"),
            P("tp"),
            P("tp"),
            P(None, None, "tp"),
            P("tp", None),
            P("tp"),
            P("tp"),
            P("tp"),
            P(None, "tp"),
            P("tp"),
            P("tp", None),
            P("tp"),
        ),
        out_specs=(
            P("dp", "tp"),
            P("dp", "tp"),
            P("dp", "tp"),
            P("tp", None),
            P("tp", None),
            P("tp"),
            P("tp"),
            P("tp"),
            P(None, None, "tp"),
            P("tp", None),
            P("tp"),
            P("tp"),
            P("tp"),
            P(None, "tp"),
            P("tp"),
            P("tp", None),
            P("tp"),
        ),
        check_vma=False,
    )
```

```python
import functools
import math

import jax
import jax.numpy as jnp
from jax import lax
from jax.experimental import pallas as pl
from jax.experimental.pallas import tpu as pltpu
from jax.sharding import PartitionSpec as P

HEAD = 72
SEQ = 258
TSTEPS = 1000


EPSILON = 1e-06
ROOT_HALF = 0.7071067811865476
DENSITY_SCALE = 0.3989422804014327


def item_factors(timesteps, loss_codes, code_weights, group_items):
    steps_float = timesteps.astype(jnp.float32)
    phase = (steps_float / TSTEPS + 0.008) / 1.008 * (math.pi / 2.0)
    cosine = jnp.cos(phase)
    signal = cosine * cosine
    weight = jnp.minimum(1.0, 5.0 * (1.0 - signal) / signal)
    picks = (
        loss_codes[:, None] == jnp.arange(code_weights.shape[0], dtype=jnp.int32)[None, :]
    ).astype(jnp.float32)
    coded = jnp.sum(picks * code_weights[None, :], axis=1)
    valid = (jnp.arange(timesteps.shape[0], dtype=jnp.int32) < group_items).astype(jnp.float32)
    return (weight * coded * valid, valid)


def layer_norm(stream, gain, bias, width):
    totals, squares = lax.psum((jnp.sum(stream, 0), jnp.sum(stream * stream, 0)), "tp")
    mean = totals / width
    rstd = lax.rsqrt(squares / width - mean * mean + EPSILON)
    normed = (stream - mean[None, :]) * rstd[None, :]
    rounded = (normed * gain[:, None] + bias[:, None]).astype(jnp.bfloat16)
    return (normed, rstd, lax.all_gather(rounded, "tp", axis=0, tiled=True))


def norm_back(d_normed, normed, rstd, gain, width):
    g_gain = jnp.sum(d_normed * normed, 1)
    g_bias = jnp.sum(d_normed, 1)
    scaled = d_normed * gain[:, None]
    first, second = lax.psum((jnp.sum(scaled, 0), jnp.sum(scaled * normed, 0)), "tp")
    back = rstd[None, :] * (scaled - first[None, :] / width - normed * second[None, :] / width)
    return (back, g_gain, g_bias)


def reduce_back(term, local_width):
    return lax.psum_scatter(
        term(jnp.int32(0), lax.axis_size("tp") * local_width).astype(jnp.bfloat16),
        "tp",
        scatter_dimension=0,
        tiled=True,
    ).astype(jnp.float32)


def fold_back(shard, pairs):
    piece = lax.all_gather(shard, "tp", axis=0, tiled=True)
    new_acts = tuple(
        (
            jnp.einsum("fc,ct->ft", weight, piece, preferred_element_type=jnp.float32)
            for weight, acts in pairs
        )
    )
    new_weights = tuple(
        (
            jnp.einsum("ft,ct->fc", acts, piece, preferred_element_type=jnp.float32)
            for weight, acts in pairs
        )
    )
    return (new_acts, new_weights)


def split_heads(flat, heads_here):
    pair_count = flat.shape[1] // (2 * SEQ)
    shaped = flat.reshape(heads_here, HEAD, pair_count, 2, SEQ)
    return jnp.moveaxis(shaped, 2, 0)


def join_heads(blocks):
    moved = jnp.moveaxis(blocks, 0, 2)
    return moved.reshape(moved.shape[0] * moved.shape[1], -1)


def attend(block):
    query_rows, key_rows, value_rows = block
    scale = 1.0 / math.sqrt(HEAD)
    scores = (
        jnp.einsum("hdbi,hdbj->hbij", query_rows, key_rows, preferred_element_type=jnp.float32)
        * scale
    )
    peak = jnp.max(scores, axis=-1, keepdims=True)
    logsum = peak + jnp.log(jnp.sum(jnp.exp(scores - peak), axis=-1, keepdims=True))
    probs = jnp.exp(scores - logsum).astype(jnp.bfloat16)
    attended = jnp.einsum("hbij,hdbj->hdbi", probs, value_rows, preferred_element_type=jnp.float32)
    return (attended.astype(jnp.bfloat16), logsum[..., 0])


def attend_back(block):
    query_rows, key_rows, value_rows, logsum, d_attended = block
    scale = 1.0 / math.sqrt(HEAD)
    scores = (
        jnp.einsum("hdbi,hdbj->hbij", query_rows, key_rows, preferred_element_type=jnp.float32)
        * scale
    )
    probs = jnp.exp(scores - logsum[..., None])
    probs_low = probs.astype(jnp.bfloat16)
    d_probs = jnp.einsum(
        "hdbi,hdbj->hbij", d_attended, value_rows, preferred_element_type=jnp.float32
    )
    delta = jnp.sum(probs * d_probs, axis=-1, keepdims=True)
    d_scores = (probs * (d_probs - delta)).astype(jnp.bfloat16)
    d_query = (
        jnp.einsum("hbij,hdbj->hdbi", d_scores, key_rows, preferred_element_type=jnp.float32)
        * scale
    )
    d_key = (
        jnp.einsum("hbij,hdbi->hdbj", d_scores, query_rows, preferred_element_type=jnp.float32)
        * scale
    )
    d_value = jnp.einsum(
        "hbij,hdbi->hdbj", probs_low, d_attended, preferred_element_type=jnp.float32
    )
    return (d_query.astype(jnp.bfloat16), d_key.astype(jnp.bfloat16), d_value.astype(jnp.bfloat16))


def body_features(
    main,
    long_skip,
    cotangent,
    timesteps,
    loss_codes,
    code_weights,
    item_counts,
    w_skip_main,
    w_skip_long,
    b_skip,
    ln1_gain,
    ln1_bias,
    w_qkv,
    w_proj,
    b_proj,
    ln2_gain,
    ln2_bias,
    w_up,
    b_up,
    w_down,
    b_down,
):
    local_width = main.shape[1]
    width = w_skip_main.shape[1]
    heads_here = local_width // HEAD
    item_scale, valid = item_factors(timesteps, loss_codes, code_weights, item_counts[0])
    row_scale = jnp.repeat(item_scale, SEQ)
    row_valid = jnp.repeat(valid, SEQ)
    main_cols = main.T
    long_cols = long_skip.T
    stream = (
        lax.psum_scatter(
            jnp.einsum("dc,dt->ct", w_skip_main, main_cols, preferred_element_type=jnp.float32)
            + jnp.einsum("dc,dt->ct", w_skip_long, long_cols, preferred_element_type=jnp.float32),
            "tp",
            scatter_dimension=0,
            tiled=True,
        )
        + b_skip[:, None]
    )
    normed_one, rstd_one, full_one = layer_norm(stream, ln1_gain, ln1_bias, width)
    qkv = jnp.einsum("edc,dt->ect", w_qkv, full_one, preferred_element_type=jnp.float32).astype(
        jnp.bfloat16
    )
    query_blocks = split_heads(qkv[0], heads_here)
    key_blocks = split_heads(qkv[1], heads_here)
    value_blocks = split_heads(qkv[2], heads_here)
    attended_blocks, logsums = lax.map(attend, (query_blocks, key_blocks, value_blocks))
    attended = join_heads(attended_blocks)
    cols_here = w_proj
    projected = lax.psum_scatter(
        jnp.einsum("rc,rt->ct", cols_here, attended, preferred_element_type=jnp.float32).astype(
            jnp.bfloat16
        ),
        "tp",
        scatter_dimension=0,
        tiled=True,
    ).astype(jnp.float32)
    stream_two = stream + projected + b_proj[:, None]
    normed_two, rstd_two, full_two = layer_norm(stream_two, ln2_gain, ln2_bias, width)
    upward = (
        jnp.einsum("dc,dt->ct", w_up, full_two, preferred_element_type=jnp.float32) + b_up[:, None]
    )
    activated = jax.nn.gelu(upward, approximate=False).astype(jnp.bfloat16)
    cols_here = w_down
    result = (
        stream_two
        + lax.psum_scatter(
            jnp.einsum(
                "fc,ft->ct", cols_here, activated, preferred_element_type=jnp.float32
            ).astype(jnp.bfloat16),
            "tp",
            scatter_dimension=0,
            tiled=True,
        ).astype(jnp.float32)
        + b_down[:, None]
    )
    out = (result * row_valid[None, :]).T.astype(jnp.bfloat16)
    grad_low = (cotangent.T.astype(jnp.float32) * row_scale[None, :]).astype(jnp.bfloat16)
    grad_wide = grad_low.astype(jnp.float32)
    g_b_down = jnp.sum(grad_wide, 1)
    (d_activated,), (g_w_down,) = fold_back(grad_low, ((w_down, activated),))
    cumulative = 0.5 * (1.0 + lax.erf(upward * ROOT_HALF))
    density = jnp.exp(-0.5 * upward * upward) * DENSITY_SCALE
    d_upward = (d_activated * (cumulative + upward * density)).astype(jnp.bfloat16)
    g_b_up = jnp.sum(d_upward.astype(jnp.float32), 1)
    g_w_up = jnp.einsum("dt,ft->df", full_two, d_upward, preferred_element_type=jnp.float32)

    def up_term(start, count_rows):
        return jnp.einsum("cf,ft->ct", w_up, d_upward, preferred_element_type=jnp.float32)

    d_normed_two = reduce_back(up_term, local_width)
    back_two, g_ln2_gain, g_ln2_bias = norm_back(
        d_normed_two, normed_two, rstd_two, ln2_gain, width
    )
    d_stream_two = (back_two + grad_wide).astype(jnp.bfloat16)
    d_stream_wide = d_stream_two.astype(jnp.float32)
    g_b_proj = jnp.sum(d_stream_wide, 1)
    (d_attended,), (g_w_proj,) = fold_back(d_stream_two, ((w_proj, attended),))
    d_attended_blocks = split_heads(d_attended.astype(jnp.bfloat16), heads_here)
    d_queries, d_keys, d_values = lax.map(
        attend_back, (query_blocks, key_blocks, value_blocks, logsums, d_attended_blocks)
    )
    d_qkv = jnp.stack([join_heads(d_queries), join_heads(d_keys), join_heads(d_values)], axis=0)
    g_w_qkv = jnp.einsum("dt,ect->edc", full_one, d_qkv, preferred_element_type=jnp.float32)

    def qkv_term(start, count_rows):
        return jnp.einsum("ecr,ert->ct", w_qkv, d_qkv, preferred_element_type=jnp.float32)

    d_normed_one = reduce_back(qkv_term, local_width)
    back_one, g_ln1_gain, g_ln1_bias = norm_back(
        d_normed_one, normed_one, rstd_one, ln1_gain, width
    )
    d_stream = (back_one + d_stream_wide).astype(jnp.bfloat16)
    g_b_skip = jnp.sum(d_stream.astype(jnp.float32), 1)
    (d_main_cols, d_long_cols), (g_w_main, g_w_long) = fold_back(
        d_stream, ((w_skip_main, main_cols), (w_skip_long, long_cols))
    )
    (
        g_w_main,
        g_w_long,
        g_b_skip,
        g_ln1_gain,
        g_ln1_bias,
        g_w_qkv,
        g_w_proj,
        g_b_proj,
        g_ln2_gain,
        g_ln2_bias,
        g_w_up,
        g_b_up,
        g_w_down,
        g_b_down,
    ) = (
        lax.psum(g_w_main.astype(jnp.bfloat16), "dp").astype(jnp.float32),
        lax.psum(g_w_long.astype(jnp.bfloat16), "dp").astype(jnp.float32),
        lax.psum(g_b_skip.astype(jnp.bfloat16), "dp").astype(jnp.float32),
        lax.psum(g_ln1_gain.astype(jnp.bfloat16), "dp").astype(jnp.float32),
        lax.psum(g_ln1_bias.astype(jnp.bfloat16), "dp").astype(jnp.float32),
        lax.psum(g_w_qkv.astype(jnp.bfloat16), "dp").astype(jnp.float32),
        lax.psum(g_w_proj.astype(jnp.bfloat16), "dp").astype(jnp.float32),
        lax.psum(g_b_proj.astype(jnp.bfloat16), "dp").astype(jnp.float32),
        lax.psum(g_ln2_gain.astype(jnp.bfloat16), "dp").astype(jnp.float32),
        lax.psum(g_ln2_bias.astype(jnp.bfloat16), "dp").astype(jnp.float32),
        lax.psum(g_w_up.astype(jnp.bfloat16), "dp").astype(jnp.float32),
        lax.psum(g_b_up.astype(jnp.bfloat16), "dp").astype(jnp.float32),
        lax.psum(g_w_down.astype(jnp.bfloat16), "dp").astype(jnp.float32),
        lax.psum(g_b_down.astype(jnp.bfloat16), "dp").astype(jnp.float32),
    )
    d_main = d_main_cols.T.astype(jnp.bfloat16)
    d_long = d_long_cols.T.astype(jnp.bfloat16)
    return (
        out,
        d_main,
        d_long,
        g_w_main,
        g_w_long,
        g_b_skip,
        g_ln1_gain,
        g_ln1_bias,
        g_w_qkv,
        g_w_proj,
        g_b_proj,
        g_ln2_gain,
        g_ln2_bias,
        g_w_up,
        g_b_up,
        g_w_down,
        g_b_down,
    )


ITEM_ROWS = 264
GRAD_ROWS = 24
CORE = ("tp", 1)
ACROSS_Y = ("tp", 2)
ACROSS_X = ("dp", 1)
ACROSS_Z = ("dp", 2)
FAR_Z = ("dp", 4)


def swap(value, link):
    axis, bit = link
    return lax.ppermute(value, axis, [(i, i ^ bit) for i in range(lax.axis_size(axis))])


def side(link):
    axis, bit = link
    return (lax.axis_index(axis) // bit) % 2


def in_order(bit, mine, theirs):
    flip = bit == 1
    return jnp.stack([jnp.where(flip, theirs, mine), jnp.where(flip, mine, theirs)])


def pick(value, index):
    return lax.dynamic_index_in_dim(value, index, 0, keepdims=False)


def peer(value, bit):
    return value + bit - 2 * bit * ((value // bit) % 2)


def greet(peers):
    barrier = pltpu.get_barrier_semaphore()
    for where in peers:
        pl.semaphore_signal(barrier, inc=1, device_id=where, device_id_type=pl.DeviceIdType.MESH)
    pl.semaphore_wait(barrier, len(peers))


def send(source, target, sems, index, where):
    return pltpu.make_async_remote_copy(
        src_ref=source,
        dst_ref=target,
        send_sem=sems.at[0, index],
        recv_sem=sems.at[1, index],
        device_id=where,
        device_id_type=pl.DeviceIdType.MESH,
    )


def gather_kernel(pieces, n_in, n_out, *refs):
    tokens, vectors, inputs = refs[0], refs[1], refs[2 : 2 + n_in]
    refs = refs[2 + n_in :]
    far_tokens, core_near, core_far, far_vectors, core_vectors = refs[:5]
    outs, held = refs[5 : 5 + n_out], refs[5 + n_out : 5 + n_out + n_in]
    y_sem, one_sem, two_sem, own_sem, far_sem, local_sem, token_sem = refs[5 + n_out + n_in :]
    n = len(pieces)
    shards = [inputs[a].at[lead] if lead else inputs[a] for a, lead, _, _ in pieces]
    stage = [held[a].at[lead] if lead else held[a] for a, lead, _, _ in pieces]
    fulls = [
        [outs[b[place]].at[tail] if isinstance(b, tuple) else outs[b].at[(place,) + tail] for place in range(4)]
        for _, _, b, tail in pieces
    ]
    dp, tp = lax.axis_index("dp"), lax.axis_index("tp")
    core, y = tp % 2, (tp // 2) % 2
    to_core, to_y = {"tp": peer(tp, 1)}, {"tp": peer(tp, 2)}
    links = ({"dp": peer(dp, 1)}, {"dp": peer(dp, 2)})
    bits = (dp % 2, (dp // 2) % 2)
    greet((to_core, to_y) + links)

    def places(k):
        return k % 2, 1 - k % 2, bits[k % 2], bits[1 - k % 2]

    def y_copy(k):
        _, _, f, s = places(k)
        return send(shards[k].at[s, f], fulls[k][1].at[s, f], y_sem, k, to_y)

    def one_copy(k):
        first, _, f, s = places(k)
        part = fulls[k][1].at[s, f]
        return send(part, part, one_sem, k, links[first])

    def two_copy(k):
        _, second, _, s = places(k)
        part = fulls[k][1].at[s]
        return send(part, part, two_sem, k, links[second])

    def own_copy(k):
        return send(shards[k], fulls[k][2], own_sem, k, to_core)

    def far_copy(k):
        return send(fulls[k][1], fulls[k][3], far_sem, k, to_core)

    def load(k):
        return pltpu.make_async_copy(shards[k], stage[k], local_sem.at[0, k])

    def store(k):
        return pltpu.make_async_copy(stage[k], fulls[k][0], local_sem.at[1, k])

    token_y = send(tokens.at[1 - y], far_tokens, token_sem, 0, to_y)
    token_near = send(tokens.at[y, 1 - core], core_near, token_sem, 1, to_core)
    token_far = send(far_tokens.at[1 - core], core_far, token_sem, 2, to_core)
    vectors_y = send(vectors, far_vectors, token_sem, 3, to_y)
    vectors_near = send(vectors, core_vectors.at[0], token_sem, 4, to_core)
    vectors_far = send(far_vectors, core_vectors.at[1], token_sem, 5, to_core)
    vectors_y.start()
    vectors_near.start()
    for k in range(n):
        y_copy(k).start()
    token_y.start()
    token_near.start()
    for k in range(n):
        load(k).start()
        own_copy(k).start()
    for step in range(n + 2):
        if step < n:
            y_copy(step).wait_recv()
            one_copy(step).start()
            load(step).wait()
            store(step).start()
        if 0 <= step - 1 < n:
            one_copy(step - 1).wait_recv()
            two_copy(step - 1).start()
        if 0 <= step - 2 < n:
            two_copy(step - 2).wait_recv()
            far_copy(step - 2).start()
    vectors_y.wait_recv()
    vectors_far.start()
    token_y.wait_recv()
    token_far.start()
    for copy in (token_near, token_far, vectors_near, vectors_far):
        copy.wait()
    token_y.wait_send()
    vectors_y.wait_send()
    for k in range(n):
        far_copy(k).wait()
        own_copy(k).wait()
        store(k).wait()
        for copy in (y_copy(k), one_copy(k), two_copy(k)):
            copy.wait_send()


def gather_weights(tokens, vectors, arrays, pieces, out_shapes):
    n = len(pieces)
    shape = lambda dims, like: jax.ShapeDtypeStruct(dims, like.dtype)
    rows = tokens.shape[2:]
    outs = [shape((2,) + rows, tokens), shape(rows, tokens), shape(rows, tokens)]
    outs += [shape(vectors.shape, vectors), shape((2,) + vectors.shape, vectors)]
    outs += [shape(dims, arrays[0]) for dims in out_shapes]
    sems = [pltpu.SemaphoreType.DMA((2, n))] * 6 + [pltpu.SemaphoreType.DMA((2, 6))]
    return pl.pallas_call(
        functools.partial(gather_kernel, pieces, len(arrays), len(out_shapes)),
        out_shape=outs,
        in_specs=[pl.BlockSpec(memory_space=pltpu.MemorySpace.HBM)] * (2 + len(arrays)),
        out_specs=[pl.BlockSpec(memory_space=pltpu.MemorySpace.HBM)] * len(outs),
        scratch_shapes=[pltpu.VMEM(a.shape, a.dtype) for a in arrays] + sems,
        compiler_params=pltpu.CompilerParams(
            collective_id=1, has_side_effects=True, vmem_limit_bytes=32 * 2**20
        ),
        name="gather_weights",
    )(tokens, vectors, *arrays)


LAG = 7


def reduce_kernel(n_early, whole_sizes, views, n_arrays, *refs):
    early, arrays, blocks, quarter = refs[0], refs[1 : 1 + n_arrays], refs[1 + n_arrays], refs[2 + n_arrays]
    refs = refs[3 + n_arrays :]
    early_out, outs, refs = refs[0], refs[1 : 1 + len(views)], refs[1 + len(views) :]
    from_core, y_blocks, z_quarter, x_quarters = refs[:4]
    refs = refs[4:]
    total, from_y, from_one, half, from_two, from_far, final = refs[:7]
    y_sem, one_sem, two_sem, far_sem, back_two, back_one, block_sem, load_sem, out_sem = refs[7:]
    n_whole = total.shape[0]
    chunks = n_early + n_whole
    dp, tp = lax.axis_index("dp"), lax.axis_index("tp")
    to_core, to_y, to_far = {"tp": peer(tp, 1)}, {"tp": peer(tp, 2)}, {"dp": peer(dp, 4)}
    greet((to_core, to_y, {"dp": peer(dp, 1)}, {"dp": peer(dp, 2)}, to_far))

    def plan(s):
        z_first = jnp.where(s >= n_early, ((s + 5 - n_early % 5) % 5) // 4, 0)
        first, second = 1 + z_first, 2 - z_first
        places = (dp // first) % 2, (dp // second) % 2
        return ({"dp": peer(dp, first)}, {"dp": peer(dp, second)}) + places

    def y_copy(r, source):
        return send(source, from_y.at[r], y_sem, r, to_y)

    def one_copy(r):
        to_one, _, f, _ = plan(r + n_early)
        return send(total.at[r, 1 - f], from_one.at[r], one_sem, r, to_one)

    def two_copy(s):
        _, to_two, _, g = plan(s)
        return send(half.at[s, 1 - g], from_two.at[s], two_sem, s, to_two)

    def far_copy(s):
        _, _, _, g = plan(s)
        return send(half.at[s, g], from_far.at[s], far_sem, s, to_far)

    def back_two_copy(s):
        _, to_two, f, g = plan(s)
        part = final.at[s, f, g]
        return send(part, part, back_two, s, to_two)

    def back_one_copy(s):
        to_one, _, f, _ = plan(s)
        part = final.at[s, f]
        return send(part, part, back_one, s, to_one)

    def out_copies(s, act):
        @pl.when(s < n_early)
        def _():
            for p in range(2):
                act(pltpu.make_async_copy(final.at[s, p], early_out.at[p, s], out_sem.at[p, s]))

        at = n_early
        for k, size in enumerate(whole_sizes):

            @pl.when((s >= at) & (s < at + size))
            def _(k=k, at=at):
                act(pltpu.make_async_copy(final.at[s], outs[k].at[s - at], out_sem.at[0, s]))

            at += size

    early_load = pltpu.make_async_copy(early, half.at[pl.ds(0, n_early)], load_sem.at[0])
    early_load.start()
    core_blocks = [send(blocks.at[2 + k], from_core.at[k], block_sem, k, to_core) for k in range(2)]
    own_block = send(blocks.at[1], y_blocks.at[0], block_sem, 2, to_y)
    core_block = send(from_core.at[1], y_blocks.at[1], block_sem, 3, to_y)
    to_x, to_z = {"dp": peer(dp, 1)}, {"dp": peer(dp, 2)}
    quarter_z = send(quarter, z_quarter, block_sem, 4, to_z)
    quarter_x = send(quarter, x_quarters.at[0], block_sem, 5, to_x)
    quarter_zx = send(z_quarter, x_quarters.at[1], block_sem, 6, to_x)
    loads, at = [], 0
    for k, (size, (a, mine, theirs)) in enumerate(zip(whole_sizes, views)):
        source = arrays[a].at[mine]
        loads.append(pltpu.make_async_copy(source, total.at[pl.ds(at, size)], load_sem.at[1 + k]))
        loads[-1].start()
        for r in range(size):
            y_copy(at + r, arrays[a].at[theirs + (r,)]).start()
        at += size
    for copy in core_blocks:
        copy.start()
    own_block.start()
    early_load.wait()
    for copy in loads:
        copy.wait()

    def plus(left, right):
        return (left.astype(jnp.float32) + right.astype(jnp.float32)).astype(jnp.bfloat16)

    def step(t, carry):
        @pl.when(t < n_early)
        def _():
            two_copy(t).start()

        @pl.when((t >= n_early) & (t < chunks))
        def _():
            _, _, f, _ = plan(t)
            one_copy(t - n_early).wait_recv()
            half[t] = plus(total[t - n_early, f], from_one[t - n_early])
            two_copy(t).start()

        @pl.when((t >= 1) & (t < chunks + 1))
        def _():
            s = t - 1
            _, _, _, g = plan(s)
            two_copy(s).wait_recv()
            half[s, g] = plus(half[s, g], from_two[s])
            far_copy(s).start()

        @pl.when((t >= 3) & (t < chunks + 3))
        def _():
            s = t - 3
            _, _, f, g = plan(s)
            far_copy(s).wait_recv()
            final[s, f, g] = plus(half[s, g], from_far[s])
            back_two_copy(s).start()

        @pl.when((t >= 4) & (t < chunks + 4))
        def _():
            back_two_copy(t - 4).wait_recv()
            back_one_copy(t - 4).start()

        @pl.when((t >= 5) & (t < chunks + 5))
        def _():
            back_one_copy(t - 5).wait_recv()
            out_copies(t - 5, lambda copy: copy.start())

        @pl.when((t >= LAG) & (t < LAG + n_whole))
        def _():
            r = t - LAG
            y_copy(r, total.at[r]).wait_recv()
            total[r] = plus(total[r], from_y[r])
            one_copy(r).start()

        @pl.when(t == 2)
        def _():
            for copy in core_blocks:
                copy.wait_recv()
            core_block.start()

        @pl.when(t == 10)
        def _():
            quarter_z.start()
            quarter_x.start()

        @pl.when(t == 18)
        def _():
            quarter_z.wait_recv()
            quarter_zx.start()

        return carry

    lax.fori_loop(0, chunks + 5, step, 0)

    def finish_whole(r, carry):
        y_copy(r, total.at[r]).wait_send()
        one_copy(r).wait_send()
        return carry

    lax.fori_loop(0, n_whole, finish_whole, 0)

    def finish(s, carry):
        for copy in (two_copy(s), far_copy(s), back_two_copy(s), back_one_copy(s)):
            copy.wait_send()
        out_copies(s, lambda copy: copy.wait())
        return carry

    lax.fori_loop(0, chunks, finish, 0)
    for copy in core_blocks:
        copy.wait_send()
    own_block.wait()
    core_block.wait()
    quarter_z.wait_send()
    quarter_x.wait()
    quarter_zx.wait()


def reduce_grads(early, arrays, views, blocks, quarter):
    sizes = tuple(arrays[a].shape[len(mine)] for a, mine, _ in views)
    n_early, n_whole = early.shape[0], sum(sizes)
    chunks = n_early + n_whole
    rows, width = early.shape[-2:]
    kind = early.dtype
    sem = lambda n: pltpu.SemaphoreType.DMA((2, n))
    two_blocks = jax.ShapeDtypeStruct((2,) + blocks.shape[1:], blocks.dtype)
    return pl.pallas_call(
        functools.partial(reduce_kernel, n_early, sizes, views, len(arrays)),
        out_shape=[jax.ShapeDtypeStruct((2, n_early, 2, rows, width), kind)]
        + [jax.ShapeDtypeStruct((n, 2, 2, rows, width), kind) for n in sizes]
        + [two_blocks, two_blocks]
        + [jax.ShapeDtypeStruct(lead + quarter.shape, kind) for lead in ((), (2,))],
        in_specs=[pl.BlockSpec(memory_space=pltpu.MemorySpace.HBM)] * (3 + len(arrays)),
        out_specs=[pl.BlockSpec(memory_space=pltpu.MemorySpace.HBM)] * (5 + len(views)),
        scratch_shapes=[
            pltpu.VMEM((n_whole, 2, 2, rows, width), kind),
            pltpu.VMEM((n_whole, 2, 2, rows, width), kind),
            pltpu.VMEM((n_whole, 2, rows, width), kind),
            pltpu.VMEM((chunks, 2, rows, width), kind),
            pltpu.VMEM((chunks, rows, width), kind),
            pltpu.VMEM((chunks, rows, width), kind),
            pltpu.VMEM((chunks, 2, 2, rows, width), kind),
            sem(n_whole),
            sem(n_whole),
            sem(chunks),
            sem(chunks),
            sem(chunks),
            sem(chunks),
            sem(7),
            pltpu.SemaphoreType.DMA((1 + len(views),)),
            sem(chunks),
        ],
        compiler_params=pltpu.CompilerParams(
            collective_id=2, has_side_effects=True, vmem_limit_bytes=56 * 2**20
        ),
        name="reduce_grads",
    )(early, *arrays, blocks, quarter)


def add_low(mine, theirs):
    return (mine.astype(jnp.float32) + theirs.astype(jnp.float32)).astype(jnp.bfloat16)


def place_of(index):
    rank = lax.axis_index("tp")
    core, y = rank % 2, (rank // 2) % 2
    there_core, there_y = index % 2, index // 2
    apart = lambda a, b: a + b - 2 * a * b
    return apart(y, there_y) + 2 * apart(core, there_core)


def spread_kernel(main_ref, long_ref, cot_ref, tokens_ref, cot_tokens_ref):
    cols = main_ref.shape[1]
    items = tokens_ref.shape[1] // ITEM_ROWS
    for p in range(4):
        for i in range(items):
            source = slice((p * items + i) * SEQ, (p * items + i + 1) * SEQ)
            target = slice(i * ITEM_ROWS, i * ITEM_ROWS + SEQ)
            blank = slice(i * ITEM_ROWS + SEQ, (i + 1) * ITEM_ROWS)
            tokens_ref[p, target, :cols] = main_ref[source, :]
            tokens_ref[p, target, cols:] = long_ref[source, :]
            cot_tokens_ref[p, target, :] = cot_ref[source, :]
            tokens_ref[p, blank, :] = jnp.zeros((ITEM_ROWS - SEQ, 2 * cols), tokens_ref.dtype)
            cot_tokens_ref[p, blank, :] = jnp.zeros((ITEM_ROWS - SEQ, cols), tokens_ref.dtype)


def spread(main, long_skip, cotangent):
    rows, cols = main.shape
    padded = rows // SEQ // 4 * ITEM_ROWS
    return pl.pallas_call(
        spread_kernel,
        out_shape=[
            jax.ShapeDtypeStruct((4, padded, 2 * cols), main.dtype),
            jax.ShapeDtypeStruct((4, padded, cols), main.dtype),
        ],
        compiler_params=pltpu.CompilerParams(vmem_limit_bytes=40 * 2**20),
        name="spread",
    )(main, long_skip, cotangent)


def arrange_kernel(own_ref, y_ref, partner_ref, scale_ref, out_ref, held):
    cols = own_ref.shape[1]
    held[0] = own_ref[...]
    held[1] = y_ref[...]
    held[2] = partner_ref[0]
    held[3] = partner_ref[1]
    for j in range(4):
        block = held[place_of(j)].astype(jnp.float32) * scale_ref[...]
        out_ref[:, j * cols : (j + 1) * cols] = block.astype(out_ref.dtype)


def arrange(own, along_y, partner, scale):
    rows, cols = own.shape
    return pl.pallas_call(
        arrange_kernel,
        out_shape=jax.ShapeDtypeStruct((rows, 4 * cols), own.dtype),
        scratch_shapes=[pltpu.VMEM((4, rows, cols), own.dtype)],
        compiler_params=pltpu.CompilerParams(vmem_limit_bytes=24 * 2**20),
        name="arrange",
    )(own, along_y, partner, scale)


def disperse_kernel(rows_ref, valid_ref, out_ref):
    cols = out_ref.shape[2]
    for j in range(4):
        block = rows_ref[:, j * cols : (j + 1) * cols] * valid_ref[...]
        out_ref[place_of(j)] = block.astype(out_ref.dtype)


def disperse(rows, valid):
    count, width = rows.shape
    return pl.pallas_call(
        disperse_kernel,
        out_shape=jax.ShapeDtypeStruct((4, count, width // 4), jnp.bfloat16),
        compiler_params=pltpu.CompilerParams(vmem_limit_bytes=24 * 2**20),
        name="disperse",
    )(rows, valid)


def unspread_kernel(parts, own_ref, core_ref, y_ref, *refs):
    outs, held = refs[:parts], refs[parts]
    cols = outs[0].shape[1]
    items = own_ref.shape[0] // ITEM_ROWS
    held[0] = own_ref[...]
    held[1] = y_ref[0]
    held[2] = core_ref[...]
    held[3] = y_ref[1]
    for p in range(4):
        rows = held[place_of(p)]
        for i in range(items):
            target = slice((p * items + i) * SEQ, (p * items + i + 1) * SEQ)
            source = slice(i * ITEM_ROWS, i * ITEM_ROWS + SEQ)
            for k in range(parts):
                outs[k][target, :] = rows[source, k * cols : (k + 1) * cols]


def unspread(own, core_tokens, y_tokens, parts):
    rows, width = own.shape
    out = jax.ShapeDtypeStruct((4 * rows // ITEM_ROWS * SEQ, width // parts), own.dtype)
    return pl.pallas_call(
        functools.partial(unspread_kernel, parts),
        out_shape=[out] * parts,
        scratch_shapes=[pltpu.VMEM((4, rows, width), own.dtype)],
        compiler_params=pltpu.CompilerParams(vmem_limit_bytes=40 * 2**20),
        name="unspread",
    )(own, core_tokens, y_tokens)


def natural(own_half, partner_half, width, axis):
    flip_y, flip_core = side(ACROSS_Y) == 1, side(CORE) == 1
    r0, r2 = jnp.split(own_half, 2, axis)
    r1, r3 = jnp.split(partner_half, 2, axis)
    a0, a2 = jnp.where(flip_y, r2, r0), jnp.where(flip_y, r0, r2)
    a1, a3 = jnp.where(flip_y, r3, r1), jnp.where(flip_y, r1, r3)
    b0, b1 = jnp.where(flip_core, a1, a0), jnp.where(flip_core, a0, a1)
    b2, b3 = jnp.where(flip_core, a3, a2), jnp.where(flip_core, a2, a3)
    return (b0, b1, b2, b3)


def dot(spec, left, right):
    return jnp.einsum(spec, left, right, preferred_element_type=jnp.float32)


def low(value):
    return value.astype(jnp.bfloat16)


def norm_rows(stream, gain, bias):
    mean = jnp.mean(stream, 1, keepdims=True)
    square = jnp.mean(stream * stream, 1, keepdims=True)
    rstd = lax.rsqrt(square - mean * mean + EPSILON)
    normed = (stream - mean) * rstd
    return normed, rstd, low(normed * gain + bias)


def norm_rows_back(d_out, normed, rstd, gain):
    g_gain = jnp.sum(d_out * normed, 0)
    g_bias = jnp.sum(d_out, 0)
    scaled = d_out * gain
    first = jnp.mean(scaled, 1, keepdims=True)
    second = jnp.mean(scaled * normed, 1, keepdims=True)
    return rstd * (scaled - first - normed * second), g_gain, g_bias


LAST = (((1,), (1,)), ((), ()))
LEAD = (((0,), (0,)), ((), ()))


def item_scores(key, query):
    scores = lax.dot_general(key, query, LAST, preferred_element_type=jnp.float32)
    present = lax.broadcasted_iota(jnp.int32, scores.shape, 0) < SEQ
    return jnp.where(present, scores * (1.0 / math.sqrt(HEAD)), -1e30)


def attend_kernel(q_ref, k_ref, v_ref, out_ref, lse_ref):
    for h in range(q_ref.shape[1] // HEAD):
        at = slice(h * HEAD, (h + 1) * HEAD)
        scores = item_scores(k_ref[:, at], q_ref[:, at])
        peak = jnp.max(scores, axis=0, keepdims=True)
        weights = jnp.exp(scores - peak)
        total = jnp.sum(weights, axis=0, keepdims=True)
        probs = (weights * (1.0 / total)).astype(jnp.bfloat16)
        out = lax.dot_general(probs, v_ref[:, at], LEAD, preferred_element_type=jnp.float32)
        out_ref[:, at] = out.astype(jnp.bfloat16)
        lse_ref[0, h : h + 1, :] = peak + jnp.log(total)


def attend_back_kernel(q_ref, k_ref, v_ref, lse_ref, d_ref, dq_ref, dk_ref, dv_ref, own_ref, partner_ref):
    scale = 1.0 / math.sqrt(HEAD)
    for h in range(q_ref.shape[1] // HEAD):
        at = slice(h * HEAD, (h + 1) * HEAD)
        query, key, d_out = q_ref[:, at], k_ref[:, at], d_ref[:, at]
        probs = jnp.exp(item_scores(key, query) - lse_ref[0, h : h + 1, :])
        d_probs = lax.dot_general(v_ref[:, at], d_out, LAST, preferred_element_type=jnp.float32)
        delta = jnp.sum(probs * d_probs, axis=0, keepdims=True)
        d_scores = (probs * (d_probs - delta)).astype(jnp.bfloat16)
        dq = lax.dot_general(d_scores, key, LEAD, preferred_element_type=jnp.float32)
        dk = jnp.dot(d_scores, query, preferred_element_type=jnp.float32)
        dv = jnp.dot(probs.astype(jnp.bfloat16), d_out, preferred_element_type=jnp.float32)
        cols = q_ref.shape[1] // 2
        side_ref, start = (own_ref, h * HEAD) if h * HEAD < cols else (partner_ref, h * HEAD - cols)
        for e, (ref, d) in enumerate(((dq_ref, dq * scale), (dk_ref, dk * scale), (dv_ref, dv))):
            d = d.astype(jnp.bfloat16)
            ref[:, at] = d
            side_ref[:, e * cols + start : e * cols + start + HEAD] = d


def attention(query, key, value):
    rows, cols = query.shape
    heads, items = cols // HEAD, rows // ITEM_ROWS
    block = pl.BlockSpec((ITEM_ROWS, cols), lambda i: (i, 0))
    return pl.pallas_call(
        attend_kernel,
        grid=(items,),
        out_shape=[
            jax.ShapeDtypeStruct((rows, cols), jnp.bfloat16),
            jax.ShapeDtypeStruct((items, heads, ITEM_ROWS), jnp.float32),
        ],
        in_specs=[block] * 3,
        out_specs=[block, pl.BlockSpec((1, heads, ITEM_ROWS), lambda i: (i, 0, 0))],
        cost_estimate=pl.CostEstimate(
            flops=4 * rows * ITEM_ROWS * cols, bytes_accessed=8 * rows * cols, transcendentals=rows * ITEM_ROWS * heads
        ),
        name="attend",
    )(query, key, value)


def attention_back(query, key, value, lse, d_out):
    rows, cols = query.shape
    heads, items = cols // HEAD, rows // ITEM_ROWS
    block = pl.BlockSpec((ITEM_ROWS, cols), lambda i: (i, 0))
    return pl.pallas_call(
        attend_back_kernel,
        grid=(items,),
        out_shape=[jax.ShapeDtypeStruct((rows, cols), jnp.bfloat16)] * 3
        + [jax.ShapeDtypeStruct((rows, 3 * cols // 2), jnp.bfloat16)] * 2,
        in_specs=[block, block, block, pl.BlockSpec((1, heads, ITEM_ROWS), lambda i: (i, 0, 0)), block],
        out_specs=[block] * 3 + [pl.BlockSpec((ITEM_ROWS, 3 * cols // 2), lambda i: (i, 0))] * 2,
        cost_estimate=pl.CostEstimate(
            flops=10 * rows * ITEM_ROWS * cols, bytes_accessed=14 * rows * cols, transcendentals=rows * ITEM_ROWS * heads
        ),
        name="attend_back",
    )(query, key, value, lse, d_out)


def body_items(
    main,
    long_skip,
    cotangent,
    timesteps,
    loss_codes,
    code_weights,
    item_counts,
    w_skip_main,
    w_skip_long,
    b_skip,
    ln1_gain,
    ln1_bias,
    w_qkv,
    w_proj,
    b_proj,
    ln2_gain,
    ln2_bias,
    w_up,
    b_up,
    w_down,
    b_down,
):
    local = main.shape[1]
    width = 4 * local
    rank = lax.axis_index("tp")

    vectors = jnp.concatenate(
        [jnp.stack([b_skip, ln1_gain, ln1_bias, b_proj, ln2_gain, ln2_bias, b_down]), b_up.reshape(4, local)]
    )
    y, core, x, z = side(ACROSS_Y), side(CORE), side(ACROSS_X), side(ACROSS_Z)
    cut = 2 * local
    tokens, cot_tokens = spread(main, long_skip, cotangent)
    tokens = tokens.reshape((2, 2) + tokens.shape[1:])
    cot_tokens = cot_tokens.reshape((2, 2) + cot_tokens.shape[1:])
    quarters = lambda w: w.reshape(2, 2, -1, width)
    qkv_rows = jnp.swapaxes(w_qkv, 1, 2).reshape(3, 2, 2, local // 4, width)
    one = (4, 2, 2, local // 4, width)
    far_tokens, core_near, core_far, far_vectors, core_vectors, wskip, wq, wk, wv, wp, *wu = gather_weights(
        tokens,
        vectors,
        [
            quarters(w_skip_main),
            quarters(w_skip_long),
            qkv_rows,
            quarters(w_proj),
            w_up.reshape(2, 2, 2, width // 8, width),
        ],
        [
            (0, (), 0, (0,)),
            (1, (), 0, (1,)),
            (2, (0,), 1, ()),
            (2, (1,), 2, ()),
            (2, (2,), 3, ()),
            (3, (), 4, ()),
            (4, (0,), (5, 6, 7, 8), (0,)),
            (4, (1,), (5, 6, 7, 8), (1,)),
        ],
        [(4, 2) + one[1:], one, one, one, one] + [(2, 2, 2, width // 8, width)] * 4,
    )
    own_vectors = jnp.concatenate([vectors, far_vectors], axis=1)
    partner_vectors = jnp.concatenate([core_vectors[0], core_vectors[1]], axis=1)
    joined = jnp.concatenate(natural(own_vectors[:7], partner_vectors[:7], local, 1), axis=1)
    b_skip_all, gain_one, bias_one, b_proj_all, gain_two, bias_two, b_down_all = (
        joined[k : k + 1] for k in range(7)
    )

    def up_vector(pair):
        near, far = jnp.split(pair[7:], 2, 1)
        return jnp.concatenate([near.reshape(1, -1), far.reshape(1, -1)], axis=1)

    b_up_all = jnp.concatenate([up_vector(own_vectors), up_vector(partner_vectors)], axis=1)

    wskip, wq, wk, wv, wp = (g.reshape(-1, width) for g in (wskip, wq, wk, wv, wp))
    wu = [w.reshape(width, width) for w in wu]
    near_tokens = pick(tokens, y)
    skip_rows = jnp.concatenate([pick(near_tokens, core), pick(far_tokens, core), core_near, core_far], axis=1)
    other = lambda value: swap(value, CORE)
    both = lambda mine, others: jnp.concatenate([mine, others], axis=0)
    shares = lambda value: both(value[:, : value.shape[1] // 2], other(value[:, value.shape[1] // 2 :]))

    def after(value, *events):
        return lax.optimization_barrier((value,) + events)[0]

    meet = lambda *values: lax.optimization_barrier(values)

    w_down_then = after(w_down, wskip)
    wd_core = other(w_down_then)
    wd_y = swap(w_down_then, ACROSS_Y)
    cot_near = pick(cot_tokens, y)
    cot_far = swap(after(pick(cot_tokens, 1 - y), wskip), ACROSS_Y)

    stream = dot("td,dc->tc", skip_rows, wskip) + b_skip_all
    normed_one, rstd_one, full_one = norm_rows(stream, gain_one, bias_one)
    skip_both = jnp.concatenate([pick(near_tokens, 1 - core), pick(far_tokens, 1 - core)], axis=1)
    skip_both = both(skip_rows[:, : 2 * cut], skip_both)
    n1_both = both(full_one, other(full_one))
    query, key, value = (low(dot("td,cd->tc", full_one, w)) for w in (wq, wk, wv))
    attended, logsum = attention(query, key, value)
    attended_both = shares(attended)
    stream_two = stream + dot("tc,cd->td", attended, wp) + b_proj_all
    wd_y, stream_two, skip_both, n1_both = meet(wd_y, stream_two, skip_both, n1_both)
    wd_both = other(wd_y)
    normed_two, rstd_two, full_two = norm_rows(stream_two, gain_two, bias_two)
    n2_both = both(full_two, other(full_two))
    acts, slopes = [], []
    for r in range(4):
        upward = dot("td,dc->tc", full_two, wu[r]) + b_up_all[:, r * width : (r + 1) * width]
        cumulative = 0.5 * (1.0 + lax.erf(upward * ROOT_HALF))
        density = jnp.exp(-0.5 * upward * upward) * DENSITY_SCALE
        acts.append(low(upward * cumulative))
        slopes.append(low(cumulative + upward * density))

    cot_far, acts[0] = meet(cot_far, acts[0])
    cot_partner = other(jnp.stack([pick(cot_near, 1 - core), pick(cot_far, 1 - core)]))
    item_scale, valid = item_factors(timesteps, loss_codes, code_weights, item_counts[0])
    row_scale = jnp.repeat(pick(item_scale.reshape(4, -1), rank), ITEM_ROWS)[:, None]
    row_valid = jnp.repeat(pick(valid.reshape(4, -1), rank), ITEM_ROWS)[:, None]
    grad_low = arrange(pick(cot_near, core), pick(cot_far, core), cot_partner, row_scale)
    wd = [w_down, wd_y, wd_core, wd_both]
    grad_both = both(grad_low, other(grad_low))
    grad_wide = grad_low.astype(jnp.float32)
    g_b_down = jnp.sum(grad_wide, 0)

    def weight_grad(left, right):
        return low(dot("tf,tc->fc", left, right))

    def split(value, bit):
        halves = value.reshape(2, -1, width)
        return pick(halves, bit), pick(halves, 1 - bit)

    down_mine, down_theirs = (weight_grad(both(acts[p], other(acts[2 + p])), grad_both) for p in (0, 1))
    grad_then = after(grad_low, down_theirs)
    down_come = swap(down_theirs, ACROSS_Y)
    down_mine, grad_then = meet(down_mine, grad_then)

    result = stream_two + sum(dot("tf,fc->tc", acts[r], wd[r]) for r in range(4)) + b_down_all
    outs = disperse(result, row_valid)
    out_core = other(outs[2:])
    out_y = swap(jnp.stack([outs[1], out_core[1]]), ACROSS_Y)
    (out,) = unspread(outs[0], out_core[0], out_y, 1)

    d_up = [low(dot("tc,fc->tf", grad_then, wd[r]) * slopes[r].astype(jnp.float32)) for r in range(4)]
    g_b_up = jnp.stack([jnp.sum(d.astype(jnp.float32), 0) for d in d_up])
    up_mine, up_theirs = (weight_grad(n2_both, both(d_up[p], other(d_up[2 + p]))) for p in (0, 1))
    d_up[0] = after(d_up[0], up_theirs)
    up_come = swap(up_theirs, ACROSS_Y)
    up_mine = after(up_mine, d_up[0])
    d_n2 = sum(dot("tf,cf->tc", d_up[r], wu[r]) for r in range(4))
    back_two, g_ln2_gain, g_ln2_bias = norm_rows_back(d_n2, normed_two, rstd_two, gain_two)
    d_stream_two = low(back_two + grad_wide)
    d_stream_wide = d_stream_two.astype(jnp.float32)
    g_b_proj = jnp.sum(d_stream_wide, 0)
    chunked = lambda g, lead: g.reshape(lead + (-1, 2, 2, GRAD_ROWS, width))
    proj_part = chunked(weight_grad(attended_both, both(d_stream_two, other(d_stream_two))), (2,))
    d_attended = low(dot("tc,fc->tf", d_stream_two, wp))
    down_come, d_attended = meet(down_come, d_attended)
    down_keep, down_send = split(add_low(down_mine, down_come), x)
    down_come = swap(down_send, ACROSS_X)
    d_qkv = attention_back(query, key, value, logsum, d_attended)
    down_come, *d_qkv = meet(down_come, *d_qkv)
    down_keep, down_send = split(add_low(down_keep, down_come), z)
    down_come = swap(down_send, ACROSS_Z)
    *d_qkv, d_own, d_partner = d_qkv
    qkv_part = chunked(weight_grad(both(d_own, other(d_partner)), n1_both), (3, 2))
    d_n1 = sum(dot("tc,cd->td", d, w) for d, w in zip(d_qkv, (wq, wk, wv)))
    back_one, g_ln1_gain, g_ln1_bias = norm_rows_back(d_n1, normed_one, rstd_one, gain_one)
    d_stream = low(back_one + d_stream_wide)
    down_come, up_come, d_stream = meet(down_come, up_come, d_stream)
    down_quarter = add_low(down_keep, down_come)
    down_come = swap(down_quarter, FAR_Z)
    up_keep, up_send = split(add_low(up_mine, up_come), x)
    up_come = swap(up_send, ACROSS_X)
    d_stream_both = both(d_stream, other(d_stream))
    g_b_skip = jnp.sum(d_stream.astype(jnp.float32), 0)
    d_skip = low(dot("tc,fc->tf", d_stream, wskip))
    d_blocks = jnp.stack(jnp.split(d_skip, 4, 1))
    down_come, d_stream_both, d_blocks, proj_part, qkv_part = meet(
        down_come, d_stream_both, d_blocks, proj_part, qkv_part
    )
    down_quarter = add_low(down_quarter, down_come)
    skip_part = chunked(weight_grad(skip_both, d_stream_both), (2,))
    up_come, skip_part = meet(up_come, skip_part)

    small = jnp.stack([g_b_skip, g_ln1_gain, g_ln1_bias, g_b_proj, g_ln2_gain, g_ln2_bias, g_b_down])
    arrived = other(jnp.concatenate([small, g_b_up[2:]]))
    small = jnp.moveaxis((small + arrived[:7]).reshape(7, 4, local), 1, 0)
    b_up_sums = g_b_up[:2] + arrived[7:]

    def vector_rows(shard, row):
        flat = jnp.concatenate([pick(small, shard).reshape(-1), b_up_sums[row]])
        return jnp.pad(flat, (0, 4 * GRAD_ROWS * width - flat.size)).reshape(1, 2, 2, GRAD_ROWS, width)

    vector_part = low(jnp.stack([vector_rows(rank, 0), vector_rows(peer(rank, 2), 1)]))
    early = add_low(up_keep, up_come).reshape(-1, 2, GRAD_ROWS, width)
    g_w_up, *sums = reduce_grads(
        early,
        [proj_part, qkv_part, vector_part, skip_part],
        [(0, (0,), (1,)), (1, (0, 0), (0, 1)), (1, (1, 0), (1, 1)), (1, (2, 0), (2, 1)), (2, (0,), (1,)), (3, (0,), (1,))],
        d_blocks,
        down_quarter,
    )
    *sums, from_core, y_blocks, z_quarter, x_quarters = sums
    wide = lambda value: value.reshape(-1, width).astype(jnp.float32)
    g_w_down = wide(in_order(x, in_order(z, down_quarter, z_quarter), in_order(z, x_quarters[0], x_quarters[1])))
    g_w_proj, g_q, g_k, g_v, vectors, g_skip = (wide(g) for g in sums)
    g_w_qkv = jnp.stack([g.T for g in (g_q, g_k, g_v)])
    vectors = vectors.reshape(-1)
    mine = vectors[: 7 * local].reshape(7, local)

    d_main, d_long = unspread(d_blocks[0], from_core[0], y_blocks, 2)
    return (
        out,
        d_main,
        d_long,
        g_skip[:local],
        g_skip[local:],
        mine[0],
        mine[1],
        mine[2],
        g_w_qkv,
        g_w_proj,
        mine[3],
        mine[4],
        mine[5],
        wide(g_w_up),
        vectors[7 * local : 7 * local + width],
        g_w_down,
        mine[6],
    )


def solution(mesh):
    by_items = mesh.shape["tp"] == 4 and mesh.shape["dp"] == 8
    return jax.shard_map(
        body_items if by_items else body_features,
        mesh=mesh,
        in_specs=(
            P("dp", "tp"),
            P("dp", "tp"),
            P("dp", "tp"),
            P("dp"),
            P("dp"),
            P(),
            P("dp"),
            P("tp", None),
            P("tp", None),
            P("tp"),
            P("tp"),
            P("tp"),
            P(None, None, "tp"),
            P("tp", None),
            P("tp"),
            P("tp"),
            P("tp"),
            P(None, "tp"),
            P("tp"),
            P("tp", None),
            P("tp"),
        ),
        out_specs=(
            P("dp", "tp"),
            P("dp", "tp"),
            P("dp", "tp"),
            P("tp", None),
            P("tp", None),
            P("tp"),
            P("tp"),
            P("tp"),
            P(None, None, "tp"),
            P("tp", None),
            P("tp"),
            P("tp"),
            P("tp"),
            P(None, "tp"),
            P("tp"),
            P("tp", None),
            P("tp"),
        ),
        check_vma=False,
    )
```

```python
import functools
import math

import jax
import jax.numpy as jnp
from jax import lax
from jax.experimental import pallas as pl
from jax.experimental.pallas import tpu as pltpu
from jax.sharding import PartitionSpec as P

HEAD = 72
SEQ = 258
TSTEPS = 1000


EPSILON = 1e-06
ROOT_HALF = 0.7071067811865476
DENSITY_SCALE = 0.3989422804014327


def item_factors(timesteps, loss_codes, code_weights, group_items):
    steps_float = timesteps.astype(jnp.float32)
    phase = (steps_float / TSTEPS + 0.008) / 1.008 * (math.pi / 2.0)
    cosine = jnp.cos(phase)
    signal = cosine * cosine
    weight = jnp.minimum(1.0, 5.0 * (1.0 - signal) / signal)
    picks = (
        loss_codes[:, None] == jnp.arange(code_weights.shape[0], dtype=jnp.int32)[None, :]
    ).astype(jnp.float32)
    coded = jnp.sum(picks * code_weights[None, :], axis=1)
    valid = (jnp.arange(timesteps.shape[0], dtype=jnp.int32) < group_items).astype(jnp.float32)
    return (weight * coded * valid, valid)


def layer_norm(stream, gain, bias, width):
    totals, squares = lax.psum((jnp.sum(stream, 0), jnp.sum(stream * stream, 0)), "tp")
    mean = totals / width
    rstd = lax.rsqrt(squares / width - mean * mean + EPSILON)
    normed = (stream - mean[None, :]) * rstd[None, :]
    rounded = (normed * gain[:, None] + bias[:, None]).astype(jnp.bfloat16)
    return (normed, rstd, lax.all_gather(rounded, "tp", axis=0, tiled=True))


def norm_back(d_normed, normed, rstd, gain, width):
    g_gain = jnp.sum(d_normed * normed, 1)
    g_bias = jnp.sum(d_normed, 1)
    scaled = d_normed * gain[:, None]
    first, second = lax.psum((jnp.sum(scaled, 0), jnp.sum(scaled * normed, 0)), "tp")
    back = rstd[None, :] * (scaled - first[None, :] / width - normed * second[None, :] / width)
    return (back, g_gain, g_bias)


def reduce_back(term, local_width):
    return lax.psum_scatter(
        term(jnp.int32(0), lax.axis_size("tp") * local_width).astype(jnp.bfloat16),
        "tp",
        scatter_dimension=0,
        tiled=True,
    ).astype(jnp.float32)


def fold_back(shard, pairs):
    piece = lax.all_gather(shard, "tp", axis=0, tiled=True)
    new_acts = tuple(
        (
            jnp.einsum("fc,ct->ft", weight, piece, preferred_element_type=jnp.float32)
            for weight, acts in pairs
        )
    )
    new_weights = tuple(
        (
            jnp.einsum("ft,ct->fc", acts, piece, preferred_element_type=jnp.float32)
            for weight, acts in pairs
        )
    )
    return (new_acts, new_weights)


def split_heads(flat, heads_here):
    pair_count = flat.shape[1] // (2 * SEQ)
    shaped = flat.reshape(heads_here, HEAD, pair_count, 2, SEQ)
    return jnp.moveaxis(shaped, 2, 0)


def join_heads(blocks):
    moved = jnp.moveaxis(blocks, 0, 2)
    return moved.reshape(moved.shape[0] * moved.shape[1], -1)


def attend(block):
    query_rows, key_rows, value_rows = block
    scale = 1.0 / math.sqrt(HEAD)
    scores = (
        jnp.einsum("hdbi,hdbj->hbij", query_rows, key_rows, preferred_element_type=jnp.float32)
        * scale
    )
    peak = jnp.max(scores, axis=-1, keepdims=True)
    logsum = peak + jnp.log(jnp.sum(jnp.exp(scores - peak), axis=-1, keepdims=True))
    probs = jnp.exp(scores - logsum).astype(jnp.bfloat16)
    attended = jnp.einsum("hbij,hdbj->hdbi", probs, value_rows, preferred_element_type=jnp.float32)
    return (attended.astype(jnp.bfloat16), logsum[..., 0])


def attend_back(block):
    query_rows, key_rows, value_rows, logsum, d_attended = block
    scale = 1.0 / math.sqrt(HEAD)
    scores = (
        jnp.einsum("hdbi,hdbj->hbij", query_rows, key_rows, preferred_element_type=jnp.float32)
        * scale
    )
    probs = jnp.exp(scores - logsum[..., None])
    probs_low = probs.astype(jnp.bfloat16)
    d_probs = jnp.einsum(
        "hdbi,hdbj->hbij", d_attended, value_rows, preferred_element_type=jnp.float32
    )
    delta = jnp.sum(probs * d_probs, axis=-1, keepdims=True)
    d_scores = (probs * (d_probs - delta)).astype(jnp.bfloat16)
    d_query = (
        jnp.einsum("hbij,hdbj->hdbi", d_scores, key_rows, preferred_element_type=jnp.float32)
        * scale
    )
    d_key = (
        jnp.einsum("hbij,hdbi->hdbj", d_scores, query_rows, preferred_element_type=jnp.float32)
        * scale
    )
    d_value = jnp.einsum(
        "hbij,hdbi->hdbj", probs_low, d_attended, preferred_element_type=jnp.float32
    )
    return (d_query.astype(jnp.bfloat16), d_key.astype(jnp.bfloat16), d_value.astype(jnp.bfloat16))


def body_features(
    main,
    long_skip,
    cotangent,
    timesteps,
    loss_codes,
    code_weights,
    item_counts,
    w_skip_main,
    w_skip_long,
    b_skip,
    ln1_gain,
    ln1_bias,
    w_qkv,
    w_proj,
    b_proj,
    ln2_gain,
    ln2_bias,
    w_up,
    b_up,
    w_down,
    b_down,
):
    local_width = main.shape[1]
    width = w_skip_main.shape[1]
    heads_here = local_width // HEAD
    item_scale, valid = item_factors(timesteps, loss_codes, code_weights, item_counts[0])
    row_scale = jnp.repeat(item_scale, SEQ)
    row_valid = jnp.repeat(valid, SEQ)
    main_cols = main.T
    long_cols = long_skip.T
    stream = (
        lax.psum_scatter(
            jnp.einsum("dc,dt->ct", w_skip_main, main_cols, preferred_element_type=jnp.float32)
            + jnp.einsum("dc,dt->ct", w_skip_long, long_cols, preferred_element_type=jnp.float32),
            "tp",
            scatter_dimension=0,
            tiled=True,
        )
        + b_skip[:, None]
    )
    normed_one, rstd_one, full_one = layer_norm(stream, ln1_gain, ln1_bias, width)
    qkv = jnp.einsum("edc,dt->ect", w_qkv, full_one, preferred_element_type=jnp.float32).astype(
        jnp.bfloat16
    )
    query_blocks = split_heads(qkv[0], heads_here)
    key_blocks = split_heads(qkv[1], heads_here)
    value_blocks = split_heads(qkv[2], heads_here)
    attended_blocks, logsums = lax.map(attend, (query_blocks, key_blocks, value_blocks))
    attended = join_heads(attended_blocks)
    cols_here = w_proj
    projected = lax.psum_scatter(
        jnp.einsum("rc,rt->ct", cols_here, attended, preferred_element_type=jnp.float32).astype(
            jnp.bfloat16
        ),
        "tp",
        scatter_dimension=0,
        tiled=True,
    ).astype(jnp.float32)
    stream_two = stream + projected + b_proj[:, None]
    normed_two, rstd_two, full_two = layer_norm(stream_two, ln2_gain, ln2_bias, width)
    upward = (
        jnp.einsum("dc,dt->ct", w_up, full_two, preferred_element_type=jnp.float32) + b_up[:, None]
    )
    activated = jax.nn.gelu(upward, approximate=False).astype(jnp.bfloat16)
    cols_here = w_down
    result = (
        stream_two
        + lax.psum_scatter(
            jnp.einsum(
                "fc,ft->ct", cols_here, activated, preferred_element_type=jnp.float32
            ).astype(jnp.bfloat16),
            "tp",
            scatter_dimension=0,
            tiled=True,
        ).astype(jnp.float32)
        + b_down[:, None]
    )
    out = (result * row_valid[None, :]).T.astype(jnp.bfloat16)
    grad_low = (cotangent.T.astype(jnp.float32) * row_scale[None, :]).astype(jnp.bfloat16)
    grad_wide = grad_low.astype(jnp.float32)
    g_b_down = jnp.sum(grad_wide, 1)
    (d_activated,), (g_w_down,) = fold_back(grad_low, ((w_down, activated),))
    cumulative = 0.5 * (1.0 + lax.erf(upward * ROOT_HALF))
    density = jnp.exp(-0.5 * upward * upward) * DENSITY_SCALE
    d_upward = (d_activated * (cumulative + upward * density)).astype(jnp.bfloat16)
    g_b_up = jnp.sum(d_upward.astype(jnp.float32), 1)
    g_w_up = jnp.einsum("dt,ft->df", full_two, d_upward, preferred_element_type=jnp.float32)

    def up_term(start, count_rows):
        return jnp.einsum("cf,ft->ct", w_up, d_upward, preferred_element_type=jnp.float32)

    d_normed_two = reduce_back(up_term, local_width)
    back_two, g_ln2_gain, g_ln2_bias = norm_back(
        d_normed_two, normed_two, rstd_two, ln2_gain, width
    )
    d_stream_two = (back_two + grad_wide).astype(jnp.bfloat16)
    d_stream_wide = d_stream_two.astype(jnp.float32)
    g_b_proj = jnp.sum(d_stream_wide, 1)
    (d_attended,), (g_w_proj,) = fold_back(d_stream_two, ((w_proj, attended),))
    d_attended_blocks = split_heads(d_attended.astype(jnp.bfloat16), heads_here)
    d_queries, d_keys, d_values = lax.map(
        attend_back, (query_blocks, key_blocks, value_blocks, logsums, d_attended_blocks)
    )
    d_qkv = jnp.stack([join_heads(d_queries), join_heads(d_keys), join_heads(d_values)], axis=0)
    g_w_qkv = jnp.einsum("dt,ect->edc", full_one, d_qkv, preferred_element_type=jnp.float32)

    def qkv_term(start, count_rows):
        return jnp.einsum("ecr,ert->ct", w_qkv, d_qkv, preferred_element_type=jnp.float32)

    d_normed_one = reduce_back(qkv_term, local_width)
    back_one, g_ln1_gain, g_ln1_bias = norm_back(
        d_normed_one, normed_one, rstd_one, ln1_gain, width
    )
    d_stream = (back_one + d_stream_wide).astype(jnp.bfloat16)
    g_b_skip = jnp.sum(d_stream.astype(jnp.float32), 1)
    (d_main_cols, d_long_cols), (g_w_main, g_w_long) = fold_back(
        d_stream, ((w_skip_main, main_cols), (w_skip_long, long_cols))
    )
    (
        g_w_main,
        g_w_long,
        g_b_skip,
        g_ln1_gain,
        g_ln1_bias,
        g_w_qkv,
        g_w_proj,
        g_b_proj,
        g_ln2_gain,
        g_ln2_bias,
        g_w_up,
        g_b_up,
        g_w_down,
        g_b_down,
    ) = (
        lax.psum(g_w_main.astype(jnp.bfloat16), "dp").astype(jnp.float32),
        lax.psum(g_w_long.astype(jnp.bfloat16), "dp").astype(jnp.float32),
        lax.psum(g_b_skip.astype(jnp.bfloat16), "dp").astype(jnp.float32),
        lax.psum(g_ln1_gain.astype(jnp.bfloat16), "dp").astype(jnp.float32),
        lax.psum(g_ln1_bias.astype(jnp.bfloat16), "dp").astype(jnp.float32),
        lax.psum(g_w_qkv.astype(jnp.bfloat16), "dp").astype(jnp.float32),
        lax.psum(g_w_proj.astype(jnp.bfloat16), "dp").astype(jnp.float32),
        lax.psum(g_b_proj.astype(jnp.bfloat16), "dp").astype(jnp.float32),
        lax.psum(g_ln2_gain.astype(jnp.bfloat16), "dp").astype(jnp.float32),
        lax.psum(g_ln2_bias.astype(jnp.bfloat16), "dp").astype(jnp.float32),
        lax.psum(g_w_up.astype(jnp.bfloat16), "dp").astype(jnp.float32),
        lax.psum(g_b_up.astype(jnp.bfloat16), "dp").astype(jnp.float32),
        lax.psum(g_w_down.astype(jnp.bfloat16), "dp").astype(jnp.float32),
        lax.psum(g_b_down.astype(jnp.bfloat16), "dp").astype(jnp.float32),
    )
    d_main = d_main_cols.T.astype(jnp.bfloat16)
    d_long = d_long_cols.T.astype(jnp.bfloat16)
    return (
        out,
        d_main,
        d_long,
        g_w_main,
        g_w_long,
        g_b_skip,
        g_ln1_gain,
        g_ln1_bias,
        g_w_qkv,
        g_w_proj,
        g_b_proj,
        g_ln2_gain,
        g_ln2_bias,
        g_w_up,
        g_b_up,
        g_w_down,
        g_b_down,
    )


ITEM_ROWS = 264
GRAD_ROWS = 24
CORE = ("tp", 1)
ACROSS_Y = ("tp", 2)
ACROSS_X = ("dp", 1)
ACROSS_Z = ("dp", 2)
FAR_Z = ("dp", 4)


def swap(value, link):
    axis, bit = link
    return lax.ppermute(value, axis, [(i, i ^ bit) for i in range(lax.axis_size(axis))])


def side(link):
    axis, bit = link
    return (lax.axis_index(axis) // bit) % 2


def in_order(bit, mine, theirs):
    flip = bit == 1
    return jnp.stack([jnp.where(flip, theirs, mine), jnp.where(flip, mine, theirs)])


def pick(value, index):
    return lax.dynamic_index_in_dim(value, index, 0, keepdims=False)


def peer(value, bit):
    return value + bit - 2 * bit * ((value // bit) % 2)


def greet(peers):
    barrier = pltpu.get_barrier_semaphore()
    for where in peers:
        pl.semaphore_signal(barrier, inc=1, device_id=where, device_id_type=pl.DeviceIdType.MESH)
    pl.semaphore_wait(barrier, len(peers))


def send(source, target, sems, index, where):
    return pltpu.make_async_remote_copy(
        src_ref=source,
        dst_ref=target,
        send_sem=sems.at[0, index],
        recv_sem=sems.at[1, index],
        device_id=where,
        device_id_type=pl.DeviceIdType.MESH,
    )


def gather_kernel(pieces, n_in, n_out, *refs):
    tokens, vectors, inputs = refs[0], refs[1], refs[2 : 2 + n_in]
    refs = refs[2 + n_in :]
    far_tokens, core_near, core_far, far_vectors, core_vectors = refs[:5]
    outs, held = refs[5 : 5 + n_out], refs[5 + n_out : 5 + n_out + n_in]
    y_sem, one_sem, two_sem, own_sem, far_sem, local_sem, token_sem = refs[5 + n_out + n_in :]
    n = len(pieces)
    shards = [inputs[a].at[lead] if lead else inputs[a] for a, lead, _, _ in pieces]
    stage = [held[a].at[lead] if lead else held[a] for a, lead, _, _ in pieces]
    fulls = [
        [outs[b[place]].at[tail] if isinstance(b, tuple) else outs[b].at[(place,) + tail] for place in range(4)]
        for _, _, b, tail in pieces
    ]
    dp, tp = lax.axis_index("dp"), lax.axis_index("tp")
    core, y = tp % 2, (tp // 2) % 2
    to_core, to_y = {"tp": peer(tp, 1)}, {"tp": peer(tp, 2)}
    links = ({"dp": peer(dp, 1)}, {"dp": peer(dp, 2)})
    bits = (dp % 2, (dp // 2) % 2)
    greet((to_core, to_y) + links)

    def places(k):
        return k % 2, 1 - k % 2, bits[k % 2], bits[1 - k % 2]

    def y_copy(k):
        _, _, f, s = places(k)
        return send(shards[k].at[s, f], fulls[k][1].at[s, f], y_sem, k, to_y)

    def one_copy(k):
        first, _, f, s = places(k)
        part = fulls[k][1].at[s, f]
        return send(part, part, one_sem, k, links[first])

    def two_copy(k):
        _, second, _, s = places(k)
        part = fulls[k][1].at[s]
        return send(part, part, two_sem, k, links[second])

    def own_copy(k):
        return send(shards[k], fulls[k][2], own_sem, k, to_core)

    def far_copy(k):
        return send(fulls[k][1], fulls[k][3], far_sem, k, to_core)

    def load(k):
        return pltpu.make_async_copy(shards[k], stage[k], local_sem.at[0, k])

    def store(k):
        return pltpu.make_async_copy(stage[k], fulls[k][0], local_sem.at[1, k])

    token_y = send(tokens.at[1 - y], far_tokens, token_sem, 0, to_y)
    token_near = send(tokens.at[y, 1 - core], core_near, token_sem, 1, to_core)
    token_far = send(far_tokens.at[1 - core], core_far, token_sem, 2, to_core)
    vectors_y = send(vectors, far_vectors, token_sem, 3, to_y)
    vectors_near = send(vectors, core_vectors.at[0], token_sem, 4, to_core)
    vectors_far = send(far_vectors, core_vectors.at[1], token_sem, 5, to_core)
    vectors_y.start()
    vectors_near.start()
    for k in range(n):
        y_copy(k).start()
    token_y.start()
    token_near.start()
    for k in range(n):
        load(k).start()
        own_copy(k).start()
    for step in range(n + 2):
        if step < n:
            y_copy(step).wait_recv()
            one_copy(step).start()
            load(step).wait()
            store(step).start()
        if 0 <= step - 1 < n:
            one_copy(step - 1).wait_recv()
            two_copy(step - 1).start()
        if 0 <= step - 2 < n:
            two_copy(step - 2).wait_recv()
            far_copy(step - 2).start()
    vectors_y.wait_recv()
    vectors_far.start()
    token_y.wait_recv()
    token_far.start()
    for copy in (token_near, token_far, vectors_near, vectors_far):
        copy.wait()
    token_y.wait_send()
    vectors_y.wait_send()
    for k in range(n):
        far_copy(k).wait()
        own_copy(k).wait()
        store(k).wait()
        for copy in (y_copy(k), one_copy(k), two_copy(k)):
            copy.wait_send()


def gather_weights(tokens, vectors, arrays, pieces, out_shapes):
    n = len(pieces)
    shape = lambda dims, like: jax.ShapeDtypeStruct(dims, like.dtype)
    rows = tokens.shape[2:]
    outs = [shape((2,) + rows, tokens), shape(rows, tokens), shape(rows, tokens)]
    outs += [shape(vectors.shape, vectors), shape((2,) + vectors.shape, vectors)]
    outs += [shape(dims, arrays[0]) for dims in out_shapes]
    sems = [pltpu.SemaphoreType.DMA((2, n))] * 6 + [pltpu.SemaphoreType.DMA((2, 6))]
    return pl.pallas_call(
        functools.partial(gather_kernel, pieces, len(arrays), len(out_shapes)),
        out_shape=outs,
        in_specs=[pl.BlockSpec(memory_space=pltpu.MemorySpace.HBM)] * (2 + len(arrays)),
        out_specs=[pl.BlockSpec(memory_space=pltpu.MemorySpace.HBM)] * len(outs),
        scratch_shapes=[pltpu.VMEM(a.shape, a.dtype) for a in arrays] + sems,
        compiler_params=pltpu.CompilerParams(
            collective_id=1, has_side_effects=True, vmem_limit_bytes=32 * 2**20
        ),
        name="gather_weights",
    )(tokens, vectors, *arrays)


LAG = 7


def reduce_kernel(n_early, whole_sizes, views, n_arrays, *refs):
    early, arrays, blocks, quarter = refs[0], refs[1 : 1 + n_arrays], refs[1 + n_arrays], refs[2 + n_arrays]
    refs = refs[3 + n_arrays :]
    early_out, outs, refs = refs[0], refs[1 : 1 + len(views)], refs[1 + len(views) :]
    from_core, y_blocks, z_quarter, x_quarters = refs[:4]
    refs = refs[4:]
    total, from_y, from_one, half, from_two, from_far, final = refs[:7]
    y_sem, one_sem, two_sem, far_sem, back_two, back_one, block_sem, load_sem, out_sem = refs[7:]
    n_whole = total.shape[0]
    chunks = n_early + n_whole
    dp, tp = lax.axis_index("dp"), lax.axis_index("tp")
    to_core, to_y, to_far = {"tp": peer(tp, 1)}, {"tp": peer(tp, 2)}, {"dp": peer(dp, 4)}
    greet((to_core, to_y, {"dp": peer(dp, 1)}, {"dp": peer(dp, 2)}, to_far))

    def plan(s):
        z_first = jnp.where(s >= n_early, ((s + 5 - n_early % 5) % 5) // 4, 0)
        first, second = 1 + z_first, 2 - z_first
        places = (dp // first) % 2, (dp // second) % 2
        return ({"dp": peer(dp, first)}, {"dp": peer(dp, second)}) + places

    def y_copy(r, source):
        return send(source, from_y.at[r], y_sem, r, to_y)

    def one_copy(r):
        to_one, _, f, _ = plan(r + n_early)
        return send(total.at[r, 1 - f], from_one.at[r], one_sem, r, to_one)

    def two_copy(s):
        _, to_two, _, g = plan(s)
        return send(half.at[s, 1 - g], from_two.at[s], two_sem, s, to_two)

    def far_copy(s):
        _, _, _, g = plan(s)
        return send(half.at[s, g], from_far.at[s], far_sem, s, to_far)

    def back_two_copy(s):
        _, to_two, f, g = plan(s)
        part = final.at[s, f, g]
        return send(part, part, back_two, s, to_two)

    def back_one_copy(s):
        to_one, _, f, _ = plan(s)
        part = final.at[s, f]
        return send(part, part, back_one, s, to_one)

    def out_copies(s, act):
        @pl.when(s < n_early)
        def _():
            for p in range(2):
                act(pltpu.make_async_copy(final.at[s, p], early_out.at[p, s], out_sem.at[p, s]))

        at = n_early
        for k, size in enumerate(whole_sizes):

            @pl.when((s >= at) & (s < at + size))
            def _(k=k, at=at):
                act(pltpu.make_async_copy(final.at[s], outs[k].at[s - at], out_sem.at[0, s]))

            at += size

    early_load = pltpu.make_async_copy(early, half.at[pl.ds(0, n_early)], load_sem.at[0])
    early_load.start()
    core_blocks = [send(blocks.at[2 + k], from_core.at[k], block_sem, k, to_core) for k in range(2)]
    own_block = send(blocks.at[1], y_blocks.at[0], block_sem, 2, to_y)
    core_block = send(from_core.at[1], y_blocks.at[1], block_sem, 3, to_y)
    to_x, to_z = {"dp": peer(dp, 1)}, {"dp": peer(dp, 2)}
    quarter_z = send(quarter, z_quarter, block_sem, 4, to_z)
    quarter_x = send(quarter, x_quarters.at[0], block_sem, 5, to_x)
    quarter_zx = send(z_quarter, x_quarters.at[1], block_sem, 6, to_x)
    loads, at = [], 0
    for k, (size, (a, mine, theirs)) in enumerate(zip(whole_sizes, views)):
        source = arrays[a].at[mine]
        loads.append(pltpu.make_async_copy(source, total.at[pl.ds(at, size)], load_sem.at[1 + k]))
        loads[-1].start()
        for r in range(size):
            y_copy(at + r, arrays[a].at[theirs + (r,)]).start()
        at += size
    for copy in core_blocks:
        copy.start()
    own_block.start()
    early_load.wait()
    for copy in loads:
        copy.wait()

    def plus(left, right):
        return (left.astype(jnp.float32) + right.astype(jnp.float32)).astype(jnp.bfloat16)

    def step(t, carry):
        @pl.when(t < n_early)
        def _():
            two_copy(t).start()

        @pl.when((t >= n_early) & (t < chunks))
        def _():
            _, _, f, _ = plan(t)
            one_copy(t - n_early).wait_recv()
            half[t] = plus(total[t - n_early, f], from_one[t - n_early])
            two_copy(t).start()

        @pl.when((t >= 1) & (t < chunks + 1))
        def _():
            s = t - 1
            _, _, _, g = plan(s)
            two_copy(s).wait_recv()
            half[s, g] = plus(half[s, g], from_two[s])
            far_copy(s).start()

        @pl.when((t >= 3) & (t < chunks + 3))
        def _():
            s = t - 3
            _, _, f, g = plan(s)
            far_copy(s).wait_recv()
            final[s, f, g] = plus(half[s, g], from_far[s])
            back_two_copy(s).start()

        @pl.when((t >= 4) & (t < chunks + 4))
        def _():
            back_two_copy(t - 4).wait_recv()
            back_one_copy(t - 4).start()

        @pl.when((t >= 5) & (t < chunks + 5))
        def _():
            back_one_copy(t - 5).wait_recv()
            out_copies(t - 5, lambda copy: copy.start())

        @pl.when((t >= LAG) & (t < LAG + n_whole))
        def _():
            r = t - LAG
            y_copy(r, total.at[r]).wait_recv()
            total[r] = plus(total[r], from_y[r])
            one_copy(r).start()

        @pl.when(t == 2)
        def _():
            for copy in core_blocks:
                copy.wait_recv()
            core_block.start()

        @pl.when(t == 10)
        def _():
            quarter_z.start()
            quarter_x.start()

        @pl.when(t == 18)
        def _():
            quarter_z.wait_recv()
            quarter_zx.start()

        return carry

    lax.fori_loop(0, chunks + 5, step, 0)

    def finish_whole(r, carry):
        y_copy(r, total.at[r]).wait_send()
        one_copy(r).wait_send()
        return carry

    lax.fori_loop(0, n_whole, finish_whole, 0)

    def finish(s, carry):
        for copy in (two_copy(s), far_copy(s), back_two_copy(s), back_one_copy(s)):
            copy.wait_send()
        out_copies(s, lambda copy: copy.wait())
        return carry

    lax.fori_loop(0, chunks, finish, 0)
    for copy in core_blocks:
        copy.wait_send()
    own_block.wait()
    core_block.wait()
    quarter_z.wait_send()
    quarter_x.wait()
    quarter_zx.wait()


def reduce_grads(early, arrays, views, blocks, quarter):
    sizes = tuple(arrays[a].shape[len(mine)] for a, mine, _ in views)
    n_early, n_whole = early.shape[0], sum(sizes)
    chunks = n_early + n_whole
    rows, width = early.shape[-2:]
    kind = early.dtype
    sem = lambda n: pltpu.SemaphoreType.DMA((2, n))
    two_blocks = jax.ShapeDtypeStruct((2,) + blocks.shape[1:], blocks.dtype)
    return pl.pallas_call(
        functools.partial(reduce_kernel, n_early, sizes, views, len(arrays)),
        out_shape=[jax.ShapeDtypeStruct((2, n_early, 2, rows, width), kind)]
        + [jax.ShapeDtypeStruct((n, 2, 2, rows, width), kind) for n in sizes]
        + [two_blocks, two_blocks]
        + [jax.ShapeDtypeStruct(lead + quarter.shape, kind) for lead in ((), (2,))],
        in_specs=[pl.BlockSpec(memory_space=pltpu.MemorySpace.HBM)] * (3 + len(arrays)),
        out_specs=[pl.BlockSpec(memory_space=pltpu.MemorySpace.HBM)] * (5 + len(views)),
        scratch_shapes=[
            pltpu.VMEM((n_whole, 2, 2, rows, width), kind),
            pltpu.VMEM((n_whole, 2, 2, rows, width), kind),
            pltpu.VMEM((n_whole, 2, rows, width), kind),
            pltpu.VMEM((chunks, 2, rows, width), kind),
            pltpu.VMEM((chunks, rows, width), kind),
            pltpu.VMEM((chunks, rows, width), kind),
            pltpu.VMEM((chunks, 2, 2, rows, width), kind),
            sem(n_whole),
            sem(n_whole),
            sem(chunks),
            sem(chunks),
            sem(chunks),
            sem(chunks),
            sem(7),
            pltpu.SemaphoreType.DMA((1 + len(views),)),
            sem(chunks),
        ],
        compiler_params=pltpu.CompilerParams(
            collective_id=2, has_side_effects=True, vmem_limit_bytes=56 * 2**20
        ),
        name="reduce_grads",
    )(early, *arrays, blocks, quarter)


def add_low(mine, theirs):
    return (mine.astype(jnp.float32) + theirs.astype(jnp.float32)).astype(jnp.bfloat16)


def place_of(index):
    rank = lax.axis_index("tp")
    core, y = rank % 2, (rank // 2) % 2
    there_core, there_y = index % 2, index // 2
    apart = lambda a, b: a + b - 2 * a * b
    return apart(y, there_y) + 2 * apart(core, there_core)


def spread_kernel(main_ref, long_ref, cot_ref, tokens_ref, cot_tokens_ref):
    cols = main_ref.shape[1]
    items = tokens_ref.shape[1] // ITEM_ROWS
    for p in range(4):
        for i in range(items):
            source = slice((p * items + i) * SEQ, (p * items + i + 1) * SEQ)
            target = slice(i * ITEM_ROWS, i * ITEM_ROWS + SEQ)
            blank = slice(i * ITEM_ROWS + SEQ, (i + 1) * ITEM_ROWS)
            tokens_ref[p, target, :cols] = main_ref[source, :]
            tokens_ref[p, target, cols:] = long_ref[source, :]
            cot_tokens_ref[p, target, :] = cot_ref[source, :]
            tokens_ref[p, blank, :] = jnp.zeros((ITEM_ROWS - SEQ, 2 * cols), tokens_ref.dtype)
            cot_tokens_ref[p, blank, :] = jnp.zeros((ITEM_ROWS - SEQ, cols), tokens_ref.dtype)


def spread(main, long_skip, cotangent):
    rows, cols = main.shape
    padded = rows // SEQ // 4 * ITEM_ROWS
    return pl.pallas_call(
        spread_kernel,
        out_shape=[
            jax.ShapeDtypeStruct((4, padded, 2 * cols), main.dtype),
            jax.ShapeDtypeStruct((4, padded, cols), main.dtype),
        ],
        compiler_params=pltpu.CompilerParams(vmem_limit_bytes=40 * 2**20),
        name="spread",
    )(main, long_skip, cotangent)


def arrange_kernel(own_ref, y_ref, partner_ref, scale_ref, out_ref, held):
    cols = own_ref.shape[1]
    held[0] = own_ref[...]
    held[1] = y_ref[...]
    held[2] = partner_ref[0]
    held[3] = partner_ref[1]
    for j in range(4):
        block = held[place_of(j)].astype(jnp.float32) * scale_ref[...]
        out_ref[:, j * cols : (j + 1) * cols] = block.astype(out_ref.dtype)


def arrange(own, along_y, partner, scale):
    rows, cols = own.shape
    return pl.pallas_call(
        arrange_kernel,
        out_shape=jax.ShapeDtypeStruct((rows, 4 * cols), own.dtype),
        scratch_shapes=[pltpu.VMEM((4, rows, cols), own.dtype)],
        compiler_params=pltpu.CompilerParams(vmem_limit_bytes=24 * 2**20),
        name="arrange",
    )(own, along_y, partner, scale)


def disperse_kernel(rows_ref, valid_ref, out_ref):
    cols = out_ref.shape[2]
    for j in range(4):
        block = rows_ref[:, j * cols : (j + 1) * cols] * valid_ref[...]
        out_ref[place_of(j)] = block.astype(out_ref.dtype)


def disperse(rows, valid):
    count, width = rows.shape
    return pl.pallas_call(
        disperse_kernel,
        out_shape=jax.ShapeDtypeStruct((4, count, width // 4), jnp.bfloat16),
        compiler_params=pltpu.CompilerParams(vmem_limit_bytes=24 * 2**20),
        name="disperse",
    )(rows, valid)


def unspread_kernel(parts, own_ref, core_ref, y_ref, *refs):
    outs, held = refs[:parts], refs[parts]
    cols = outs[0].shape[1]
    items = own_ref.shape[0] // ITEM_ROWS
    held[0] = own_ref[...]
    held[1] = y_ref[0]
    held[2] = core_ref[...]
    held[3] = y_ref[1]
    for p in range(4):
        rows = held[place_of(p)]
        for i in range(items):
            target = slice((p * items + i) * SEQ, (p * items + i + 1) * SEQ)
            source = slice(i * ITEM_ROWS, i * ITEM_ROWS + SEQ)
            for k in range(parts):
                outs[k][target, :] = rows[source, k * cols : (k + 1) * cols]


def unspread(own, core_tokens, y_tokens, parts):
    rows, width = own.shape
    out = jax.ShapeDtypeStruct((4 * rows // ITEM_ROWS * SEQ, width // parts), own.dtype)
    return pl.pallas_call(
        functools.partial(unspread_kernel, parts),
        out_shape=[out] * parts,
        scratch_shapes=[pltpu.VMEM((4, rows, width), own.dtype)],
        compiler_params=pltpu.CompilerParams(vmem_limit_bytes=40 * 2**20),
        name="unspread",
    )(own, core_tokens, y_tokens)


def natural(own_half, partner_half, width, axis):
    flip_y, flip_core = side(ACROSS_Y) == 1, side(CORE) == 1
    r0, r2 = jnp.split(own_half, 2, axis)
    r1, r3 = jnp.split(partner_half, 2, axis)
    a0, a2 = jnp.where(flip_y, r2, r0), jnp.where(flip_y, r0, r2)
    a1, a3 = jnp.where(flip_y, r3, r1), jnp.where(flip_y, r1, r3)
    b0, b1 = jnp.where(flip_core, a1, a0), jnp.where(flip_core, a0, a1)
    b2, b3 = jnp.where(flip_core, a3, a2), jnp.where(flip_core, a2, a3)
    return (b0, b1, b2, b3)


def dot(spec, left, right):
    return jnp.einsum(spec, left, right, preferred_element_type=jnp.float32)


def low(value):
    return value.astype(jnp.bfloat16)


def norm_rows(stream, gain, bias):
    mean = jnp.mean(stream, 1, keepdims=True)
    square = jnp.mean(stream * stream, 1, keepdims=True)
    rstd = lax.rsqrt(square - mean * mean + EPSILON)
    normed = (stream - mean) * rstd
    return normed, rstd, low(normed * gain + bias)


def norm_rows_back(d_out, normed, rstd, gain):
    g_gain = jnp.sum(d_out * normed, 0)
    g_bias = jnp.sum(d_out, 0)
    scaled = d_out * gain
    first = jnp.mean(scaled, 1, keepdims=True)
    second = jnp.mean(scaled * normed, 1, keepdims=True)
    return rstd * (scaled - first - normed * second), g_gain, g_bias


LAST = (((1,), (1,)), ((), ()))
LEAD = (((0,), (0,)), ((), ()))


def item_scores(key, query):
    scores = lax.dot_general(key, query, LAST, preferred_element_type=jnp.float32)
    present = lax.broadcasted_iota(jnp.int32, scores.shape, 0) < SEQ
    return jnp.where(present, scores * (1.0 / math.sqrt(HEAD)), -1e30)


def attend_kernel(*refs):
    def item(i, carry):
        attend_item(*(ref.at[i] for ref in refs))
        return carry

    lax.fori_loop(0, refs[0].shape[0], item, 0)


def attend_item(q_ref, k_ref, v_ref, out_ref, lse_ref):
    for h in range(q_ref.shape[1] // HEAD):
        at = slice(h * HEAD, (h + 1) * HEAD)
        scores = item_scores(k_ref[:, at], q_ref[:, at])
        peak = jnp.max(scores, axis=0, keepdims=True)
        weights = jnp.exp(scores - peak)
        total = jnp.sum(weights, axis=0, keepdims=True)
        probs = (weights * (1.0 / total)).astype(jnp.bfloat16)
        out = lax.dot_general(probs, v_ref[:, at], LEAD, preferred_element_type=jnp.float32)
        out_ref[:, at] = out.astype(jnp.bfloat16)
        lse_ref[h : h + 1, :] = peak + jnp.log(total)


def attend_back_kernel(*refs):
    def item(i, carry):
        attend_back_item(*(ref.at[i] for ref in refs))
        return carry

    lax.fori_loop(0, refs[0].shape[0], item, 0)


def attend_back_item(q_ref, k_ref, v_ref, lse_ref, d_ref, dq_ref, dk_ref, dv_ref, own_ref, partner_ref):
    scale = 1.0 / math.sqrt(HEAD)
    for h in range(q_ref.shape[1] // HEAD):
        at = slice(h * HEAD, (h + 1) * HEAD)
        query, key, d_out = q_ref[:, at], k_ref[:, at], d_ref[:, at]
        probs = jnp.exp(item_scores(key, query) - lse_ref[h : h + 1, :])
        d_probs = lax.dot_general(v_ref[:, at], d_out, LAST, preferred_element_type=jnp.float32)
        delta = jnp.sum(probs * d_probs, axis=0, keepdims=True)
        d_scores = (probs * (d_probs - delta)).astype(jnp.bfloat16)
        dq = lax.dot_general(d_scores, key, LEAD, preferred_element_type=jnp.float32)
        dk = jnp.dot(d_scores, query, preferred_element_type=jnp.float32)
        dv = jnp.dot(probs.astype(jnp.bfloat16), d_out, preferred_element_type=jnp.float32)
        cols = q_ref.shape[1] // 2
        side_ref, start = (own_ref, h * HEAD) if h * HEAD < cols else (partner_ref, h * HEAD - cols)
        for e, (ref, d) in enumerate(((dq_ref, dq * scale), (dk_ref, dk * scale), (dv_ref, dv))):
            d = d.astype(jnp.bfloat16)
            ref[:, at] = d
            side_ref[:, e * cols + start : e * cols + start + HEAD] = d


def by_item(value):
    return value.reshape(-1, ITEM_ROWS, value.shape[1])


def attention(query, key, value):
    rows, cols = query.shape
    heads, items = cols // HEAD, rows // ITEM_ROWS
    out, lse = pl.pallas_call(
        attend_kernel,
        out_shape=[
            jax.ShapeDtypeStruct((items, ITEM_ROWS, cols), jnp.bfloat16),
            jax.ShapeDtypeStruct((items, heads, ITEM_ROWS), jnp.float32),
        ],
        cost_estimate=pl.CostEstimate(
            flops=4 * rows * ITEM_ROWS * cols, bytes_accessed=8 * rows * cols, transcendentals=rows * ITEM_ROWS * heads
        ),
        compiler_params=pltpu.CompilerParams(vmem_limit_bytes=24 * 2**20),
        name="attend",
    )(by_item(query), by_item(key), by_item(value))
    return out.reshape(rows, cols), lse


def attention_back(query, key, value, lse, d_out):
    rows, cols = query.shape
    heads, items = cols // HEAD, rows // ITEM_ROWS
    shape = lambda width: jax.ShapeDtypeStruct((items, ITEM_ROWS, width), jnp.bfloat16)
    outs = pl.pallas_call(
        attend_back_kernel,
        out_shape=[shape(cols)] * 3 + [shape(3 * cols // 2)] * 2,
        cost_estimate=pl.CostEstimate(
            flops=10 * rows * ITEM_ROWS * cols, bytes_accessed=14 * rows * cols, transcendentals=rows * ITEM_ROWS * heads
        ),
        compiler_params=pltpu.CompilerParams(vmem_limit_bytes=32 * 2**20),
        name="attend_back",
    )(by_item(query), by_item(key), by_item(value), lse, by_item(d_out))
    return [o.reshape(rows, -1) for o in outs]


HIDDEN_BLOCK = 384


def feed_kernel(first, n_ref, g_ref, up_ref, bias_ref, down_ref, *refs):
    sums, (act_ref, d_up_ref, g_bias_ref, result_ref, d_n_ref) = refs[:-5], refs[-5:]
    wide = jnp.float32

    @pl.when(pl.program_id(0) == 0)
    def _():
        result_ref[...] = sums[0][...]
        d_n_ref[...] = jnp.zeros_like(d_n_ref) if first else sums[1][...]

    up = jnp.dot(n_ref[...], up_ref[...], preferred_element_type=wide) + bias_ref[...]
    d_act = lax.dot_general(g_ref[...], down_ref[...], LAST, preferred_element_type=wide)
    cumulative = 0.5 * (1.0 + lax.erf(up * ROOT_HALF))
    density = jnp.exp(-0.5 * up * up) * DENSITY_SCALE
    act = (up * cumulative).astype(jnp.bfloat16)
    d_up = (d_act * (cumulative + up * density)).astype(jnp.bfloat16)
    act_ref[...] = act
    d_up_ref[...] = d_up
    g_bias_ref[...] = jnp.sum(d_up.astype(wide), axis=0, keepdims=True)
    result_ref[...] += jnp.dot(act, down_ref[...], preferred_element_type=wide)
    d_n_ref[...] += lax.dot_general(d_up, up_ref[...], LAST, preferred_element_type=wide)


def feed(n, g, up, bias, down, result, d_n):
    rows, width = n.shape
    hidden = up.shape[1]
    whole = pl.BlockSpec((rows, width), lambda i: (0, 0))
    across = pl.BlockSpec((rows, HIDDEN_BLOCK), lambda i: (0, i))
    line = pl.BlockSpec((1, HIDDEN_BLOCK), lambda i: (0, i))
    sums = (result,) if d_n is None else (result, d_n)
    shape = jax.ShapeDtypeStruct
    return pl.pallas_call(
        functools.partial(feed_kernel, d_n is None),
        grid=(hidden // HIDDEN_BLOCK,),
        out_shape=[
            shape((rows, hidden), jnp.bfloat16),
            shape((rows, hidden), jnp.bfloat16),
            shape((1, hidden), jnp.float32),
            shape((rows, width), jnp.float32),
            shape((rows, width), jnp.float32),
        ],
        in_specs=[
            whole,
            whole,
            pl.BlockSpec((width, HIDDEN_BLOCK), lambda i: (0, i)),
            line,
            pl.BlockSpec((HIDDEN_BLOCK, width), lambda i: (i, 0)),
        ]
        + [whole] * len(sums),
        out_specs=[across, across, line, whole, whole],
        compiler_params=pltpu.CompilerParams(vmem_limit_bytes=40 * 2**20),
        cost_estimate=pl.CostEstimate(
            flops=10 * rows * width * hidden, bytes_accessed=4 * width * hidden, transcendentals=2 * rows * hidden
        ),
        name="feed",
    )(n, g, up, bias, down, *sums)


def body_items(
    main,
    long_skip,
    cotangent,
    timesteps,
    loss_codes,
    code_weights,
    item_counts,
    w_skip_main,
    w_skip_long,
    b_skip,
    ln1_gain,
    ln1_bias,
    w_qkv,
    w_proj,
    b_proj,
    ln2_gain,
    ln2_bias,
    w_up,
    b_up,
    w_down,
    b_down,
):
    local = main.shape[1]
    width = 4 * local
    rank = lax.axis_index("tp")

    vectors = jnp.concatenate(
        [jnp.stack([b_skip, ln1_gain, ln1_bias, b_proj, ln2_gain, ln2_bias, b_down]), b_up.reshape(4, local)]
    )
    y, core, x, z = side(ACROSS_Y), side(CORE), side(ACROSS_X), side(ACROSS_Z)
    cut = 2 * local
    tokens, cot_tokens = spread(main, long_skip, cotangent)
    tokens = tokens.reshape((2, 2) + tokens.shape[1:])
    cot_tokens = cot_tokens.reshape((2, 2) + cot_tokens.shape[1:])
    quarters = lambda w: w.reshape(2, 2, -1, width)
    qkv_rows = jnp.swapaxes(w_qkv, 1, 2).reshape(3, 2, 2, local // 4, width)
    one = (4, 2, 2, local // 4, width)
    far_tokens, core_near, core_far, far_vectors, core_vectors, wskip, wq, wk, wv, wp, *wu = gather_weights(
        tokens,
        vectors,
        [
            quarters(w_skip_main),
            quarters(w_skip_long),
            qkv_rows,
            quarters(w_proj),
            w_up.reshape(2, 2, 2, width // 8, width),
        ],
        [
            (0, (), 0, (0,)),
            (1, (), 0, (1,)),
            (2, (0,), 1, ()),
            (2, (1,), 2, ()),
            (2, (2,), 3, ()),
            (3, (), 4, ()),
            (4, (0,), (5, 6, 7, 8), (0,)),
            (4, (1,), (5, 6, 7, 8), (1,)),
        ],
        [(4, 2) + one[1:], one, one, one, one] + [(2, 2, 2, width // 8, width)] * 4,
    )
    own_vectors = jnp.concatenate([vectors, far_vectors], axis=1)
    partner_vectors = jnp.concatenate([core_vectors[0], core_vectors[1]], axis=1)
    joined = jnp.concatenate(natural(own_vectors[:7], partner_vectors[:7], local, 1), axis=1)
    b_skip_all, gain_one, bias_one, b_proj_all, gain_two, bias_two, b_down_all = (
        joined[k : k + 1] for k in range(7)
    )

    def up_vector(pair):
        near, far = jnp.split(pair[7:], 2, 1)
        return jnp.concatenate([near.reshape(1, -1), far.reshape(1, -1)], axis=1)

    b_up_all = jnp.concatenate([up_vector(own_vectors), up_vector(partner_vectors)], axis=1)

    wskip, wq, wk, wv, wp = (g.reshape(-1, width) for g in (wskip, wq, wk, wv, wp))
    wu = [w.reshape(width, width) for w in wu]
    near_tokens = pick(tokens, y)
    skip_rows = jnp.concatenate([pick(near_tokens, core), pick(far_tokens, core), core_near, core_far], axis=1)
    other = lambda value: swap(value, CORE)
    both = lambda mine, others: jnp.concatenate([mine, others], axis=0)
    shares = lambda value: both(value[:, : value.shape[1] // 2], other(value[:, value.shape[1] // 2 :]))

    def after(value, *events):
        return lax.optimization_barrier((value,) + events)[0]

    meet = lambda *values: lax.optimization_barrier(values)

    w_down_then = after(w_down, wskip)
    wd_core = other(w_down_then)
    wd_y = swap(w_down_then, ACROSS_Y)
    cot_near = pick(cot_tokens, y)
    cot_far = swap(after(pick(cot_tokens, 1 - y), wskip), ACROSS_Y)

    stream = dot("td,dc->tc", skip_rows, wskip) + b_skip_all
    normed_one, rstd_one, full_one = norm_rows(stream, gain_one, bias_one)
    skip_both = jnp.concatenate([pick(near_tokens, 1 - core), pick(far_tokens, 1 - core)], axis=1)
    skip_both = both(skip_rows[:, : 2 * cut], skip_both)
    n1_both = both(full_one, other(full_one))
    query, key, value = (low(dot("td,cd->tc", full_one, w)) for w in (wq, wk, wv))
    attended, logsum = attention(query, key, value)
    attended_both = shares(attended)
    stream_two = stream + dot("tc,cd->td", attended, wp) + b_proj_all
    wd_y, stream_two, skip_both, n1_both = meet(wd_y, stream_two, skip_both, n1_both)
    wd_both = other(wd_y)
    normed_two, rstd_two, full_two = norm_rows(stream_two, gain_two, bias_two)
    n2_both = both(full_two, other(full_two))
    cot_far, full_two = meet(cot_far, full_two)
    cot_partner = other(jnp.stack([pick(cot_near, 1 - core), pick(cot_far, 1 - core)]))
    item_scale, valid = item_factors(timesteps, loss_codes, code_weights, item_counts[0])
    row_scale = jnp.repeat(pick(item_scale.reshape(4, -1), rank), ITEM_ROWS)[:, None]
    row_valid = jnp.repeat(pick(valid.reshape(4, -1), rank), ITEM_ROWS)[:, None]
    grad_low = arrange(pick(cot_near, core), pick(cot_far, core), cot_partner, row_scale)
    wd = [w_down, wd_y, wd_core, wd_both]
    grad_both = both(grad_low, other(grad_low))
    grad_wide = grad_low.astype(jnp.float32)
    g_b_down = jnp.sum(grad_wide, 0)

    def weight_grad(left, right):
        return low(dot("tf,tc->fc", left, right))

    def split(value, bit):
        halves = value.reshape(2, -1, width)
        return pick(halves, bit), pick(halves, 1 - bit)

    result, d_n2 = stream_two + b_down_all, None
    acts, d_up, g_b_up = [None] * 4, [None] * 4, [None] * 4
    for r in (1, 3, 0, 2):
        bias = b_up_all[:, r * width : (r + 1) * width]
        acts[r], d_up[r], g_b_up[r], result, d_n2 = feed(full_two, grad_low, wu[r], bias, wd[r], result, d_n2)
    g_b_up = jnp.concatenate(g_b_up)
    down_mine, down_theirs = (weight_grad(both(acts[p], other(acts[2 + p])), grad_both) for p in (0, 1))
    down_come = swap(down_theirs, ACROSS_Y)
    up_mine, up_theirs = (weight_grad(n2_both, both(d_up[p], other(d_up[2 + p]))) for p in (0, 1))
    d_n2, up_theirs = meet(after(d_n2, down_theirs), up_theirs)
    up_come = swap(up_theirs, ACROSS_Y)

    outs = disperse(result, row_valid)
    out_core = other(outs[2:])
    out_y = swap(jnp.stack([outs[1], out_core[1]]), ACROSS_Y)
    back_two, g_ln2_gain, g_ln2_bias = norm_rows_back(d_n2, normed_two, rstd_two, gain_two)
    d_stream_two = low(back_two + grad_wide)
    d_stream_wide = d_stream_two.astype(jnp.float32)
    g_b_proj = jnp.sum(d_stream_wide, 0)
    chunked = lambda g, lead: g.reshape(lead + (-1, 2, 2, GRAD_ROWS, width))
    proj_part = chunked(weight_grad(attended_both, both(d_stream_two, other(d_stream_two))), (2,))
    d_attended = low(dot("tc,fc->tf", d_stream_two, wp))
    down_come, d_attended = meet(down_come, d_attended)
    down_keep, down_send = split(add_low(down_mine, down_come), x)
    down_come = swap(down_send, ACROSS_X)
    d_qkv = attention_back(query, key, value, logsum, d_attended)
    down_come, *d_qkv = meet(down_come, *d_qkv)
    down_keep, down_send = split(add_low(down_keep, down_come), z)
    down_come = swap(down_send, ACROSS_Z)
    *d_qkv, d_own, d_partner = d_qkv
    qkv_part = chunked(weight_grad(both(d_own, other(d_partner)), n1_both), (3, 2))
    d_n1 = sum(dot("tc,cd->td", d, w) for d, w in zip(d_qkv, (wq, wk, wv)))
    back_one, g_ln1_gain, g_ln1_bias = norm_rows_back(d_n1, normed_one, rstd_one, gain_one)
    d_stream = low(back_one + d_stream_wide)
    down_come, up_come, d_stream = meet(down_come, up_come, d_stream)
    down_quarter = add_low(down_keep, down_come)
    down_come = swap(down_quarter, FAR_Z)
    up_keep, up_send = split(add_low(up_mine, up_come), x)
    up_come = swap(up_send, ACROSS_X)
    d_stream_both = both(d_stream, other(d_stream))
    g_b_skip = jnp.sum(d_stream.astype(jnp.float32), 0)
    d_skip = low(dot("tc,fc->tf", d_stream, wskip))
    d_blocks = jnp.stack(jnp.split(d_skip, 4, 1))
    down_come, d_stream_both, d_blocks, proj_part, qkv_part = meet(
        down_come, d_stream_both, d_blocks, proj_part, qkv_part
    )
    down_quarter = add_low(down_quarter, down_come)
    skip_part = chunked(weight_grad(skip_both, d_stream_both), (2,))
    up_come, out_y, skip_part = meet(up_come, out_y, skip_part)
    (out,) = unspread(outs[0], out_core[0], out_y, 1)

    small = jnp.stack([g_b_skip, g_ln1_gain, g_ln1_bias, g_b_proj, g_ln2_gain, g_ln2_bias, g_b_down])
    arrived = other(jnp.concatenate([small, g_b_up[2:]]))
    small = jnp.moveaxis((small + arrived[:7]).reshape(7, 4, local), 1, 0)
    b_up_sums = g_b_up[:2] + arrived[7:]

    def vector_rows(shard, row):
        flat = jnp.concatenate([pick(small, shard).reshape(-1), b_up_sums[row]])
        return jnp.pad(flat, (0, 4 * GRAD_ROWS * width - flat.size)).reshape(1, 2, 2, GRAD_ROWS, width)

    vector_part = low(jnp.stack([vector_rows(rank, 0), vector_rows(peer(rank, 2), 1)]))
    early = add_low(up_keep, up_come).reshape(-1, 2, GRAD_ROWS, width)
    g_w_up, *sums = reduce_grads(
        early,
        [proj_part, qkv_part, vector_part, skip_part],
        [(0, (0,), (1,)), (1, (0, 0), (0, 1)), (1, (1, 0), (1, 1)), (1, (2, 0), (2, 1)), (2, (0,), (1,)), (3, (0,), (1,))],
        d_blocks,
        down_quarter,
    )
    *sums, from_core, y_blocks, z_quarter, x_quarters = sums
    wide = lambda value: value.reshape(-1, width).astype(jnp.float32)
    g_w_down = wide(in_order(x, in_order(z, down_quarter, z_quarter), in_order(z, x_quarters[0], x_quarters[1])))
    g_w_proj, g_q, g_k, g_v, vectors, g_skip = (wide(g) for g in sums)
    g_w_qkv = jnp.stack([g.T for g in (g_q, g_k, g_v)])
    vectors = vectors.reshape(-1)
    mine = vectors[: 7 * local].reshape(7, local)

    d_main, d_long = unspread(d_blocks[0], from_core[0], y_blocks, 2)
    return (
        out,
        d_main,
        d_long,
        g_skip[:local],
        g_skip[local:],
        mine[0],
        mine[1],
        mine[2],
        g_w_qkv,
        g_w_proj,
        mine[3],
        mine[4],
        mine[5],
        wide(g_w_up),
        vectors[7 * local : 7 * local + width],
        g_w_down,
        mine[6],
    )


def solution(mesh):
    by_items = mesh.shape["tp"] == 4 and mesh.shape["dp"] == 8
    return jax.shard_map(
        body_items if by_items else body_features,
        mesh=mesh,
        in_specs=(
            P("dp", "tp"),
            P("dp", "tp"),
            P("dp", "tp"),
            P("dp"),
            P("dp"),
            P(),
            P("dp"),
            P("tp", None),
            P("tp", None),
            P("tp"),
            P("tp"),
            P("tp"),
            P(None, None, "tp"),
            P("tp", None),
            P("tp"),
            P("tp"),
            P("tp"),
            P(None, "tp"),
            P("tp"),
            P("tp", None),
            P("tp"),
        ),
        out_specs=(
            P("dp", "tp"),
            P("dp", "tp"),
            P("dp", "tp"),
            P("tp", None),
            P("tp", None),
            P("tp"),
            P("tp"),
            P("tp"),
            P(None, None, "tp"),
            P("tp", None),
            P("tp"),
            P("tp"),
            P("tp"),
            P(None, "tp"),
            P("tp"),
            P("tp", None),
            P("tp"),
        ),
        check_vma=False,
    )
```

```python
import functools
import math

import jax
import jax.numpy as jnp
from jax import lax
from jax.experimental import pallas as pl
from jax.experimental.pallas import tpu as pltpu
from jax.sharding import PartitionSpec as P

HEAD = 72
SEQ = 258
TSTEPS = 1000


EPSILON = 1e-06
ROOT_HALF = 0.7071067811865476
DENSITY_SCALE = 0.3989422804014327


def item_factors(timesteps, loss_codes, code_weights, group_items):
    steps_float = timesteps.astype(jnp.float32)
    phase = (steps_float / TSTEPS + 0.008) / 1.008 * (math.pi / 2.0)
    cosine = jnp.cos(phase)
    signal = cosine * cosine
    weight = jnp.minimum(1.0, 5.0 * (1.0 - signal) / signal)
    picks = (
        loss_codes[:, None] == jnp.arange(code_weights.shape[0], dtype=jnp.int32)[None, :]
    ).astype(jnp.float32)
    coded = jnp.sum(picks * code_weights[None, :], axis=1)
    valid = (jnp.arange(timesteps.shape[0], dtype=jnp.int32) < group_items).astype(jnp.float32)
    return (weight * coded * valid, valid)


def layer_norm(stream, gain, bias, width):
    totals, squares = lax.psum((jnp.sum(stream, 0), jnp.sum(stream * stream, 0)), "tp")
    mean = totals / width
    rstd = lax.rsqrt(squares / width - mean * mean + EPSILON)
    normed = (stream - mean[None, :]) * rstd[None, :]
    rounded = (normed * gain[:, None] + bias[:, None]).astype(jnp.bfloat16)
    return (normed, rstd, lax.all_gather(rounded, "tp", axis=0, tiled=True))


def norm_back(d_normed, normed, rstd, gain, width):
    g_gain = jnp.sum(d_normed * normed, 1)
    g_bias = jnp.sum(d_normed, 1)
    scaled = d_normed * gain[:, None]
    first, second = lax.psum((jnp.sum(scaled, 0), jnp.sum(scaled * normed, 0)), "tp")
    back = rstd[None, :] * (scaled - first[None, :] / width - normed * second[None, :] / width)
    return (back, g_gain, g_bias)


def reduce_back(term, local_width):
    return lax.psum_scatter(
        term(jnp.int32(0), lax.axis_size("tp") * local_width).astype(jnp.bfloat16),
        "tp",
        scatter_dimension=0,
        tiled=True,
    ).astype(jnp.float32)


def fold_back(shard, pairs):
    piece = lax.all_gather(shard, "tp", axis=0, tiled=True)
    new_acts = tuple(
        (
            jnp.einsum("fc,ct->ft", weight, piece, preferred_element_type=jnp.float32)
            for weight, acts in pairs
        )
    )
    new_weights = tuple(
        (
            jnp.einsum("ft,ct->fc", acts, piece, preferred_element_type=jnp.float32)
            for weight, acts in pairs
        )
    )
    return (new_acts, new_weights)


def split_heads(flat, heads_here):
    pair_count = flat.shape[1] // (2 * SEQ)
    shaped = flat.reshape(heads_here, HEAD, pair_count, 2, SEQ)
    return jnp.moveaxis(shaped, 2, 0)


def join_heads(blocks):
    moved = jnp.moveaxis(blocks, 0, 2)
    return moved.reshape(moved.shape[0] * moved.shape[1], -1)


def attend(block):
    query_rows, key_rows, value_rows = block
    scale = 1.0 / math.sqrt(HEAD)
    scores = (
        jnp.einsum("hdbi,hdbj->hbij", query_rows, key_rows, preferred_element_type=jnp.float32)
        * scale
    )
    peak = jnp.max(scores, axis=-1, keepdims=True)
    logsum = peak + jnp.log(jnp.sum(jnp.exp(scores - peak), axis=-1, keepdims=True))
    probs = jnp.exp(scores - logsum).astype(jnp.bfloat16)
    attended = jnp.einsum("hbij,hdbj->hdbi", probs, value_rows, preferred_element_type=jnp.float32)
    return (attended.astype(jnp.bfloat16), logsum[..., 0])


def attend_back(block):
    query_rows, key_rows, value_rows, logsum, d_attended = block
    scale = 1.0 / math.sqrt(HEAD)
    scores = (
        jnp.einsum("hdbi,hdbj->hbij", query_rows, key_rows, preferred_element_type=jnp.float32)
        * scale
    )
    probs = jnp.exp(scores - logsum[..., None])
    probs_low = probs.astype(jnp.bfloat16)
    d_probs = jnp.einsum(
        "hdbi,hdbj->hbij", d_attended, value_rows, preferred_element_type=jnp.float32
    )
    delta = jnp.sum(probs * d_probs, axis=-1, keepdims=True)
    d_scores = (probs * (d_probs - delta)).astype(jnp.bfloat16)
    d_query = (
        jnp.einsum("hbij,hdbj->hdbi", d_scores, key_rows, preferred_element_type=jnp.float32)
        * scale
    )
    d_key = (
        jnp.einsum("hbij,hdbi->hdbj", d_scores, query_rows, preferred_element_type=jnp.float32)
        * scale
    )
    d_value = jnp.einsum(
        "hbij,hdbi->hdbj", probs_low, d_attended, preferred_element_type=jnp.float32
    )
    return (d_query.astype(jnp.bfloat16), d_key.astype(jnp.bfloat16), d_value.astype(jnp.bfloat16))


def body_features(
    main,
    long_skip,
    cotangent,
    timesteps,
    loss_codes,
    code_weights,
    item_counts,
    w_skip_main,
    w_skip_long,
    b_skip,
    ln1_gain,
    ln1_bias,
    w_qkv,
    w_proj,
    b_proj,
    ln2_gain,
    ln2_bias,
    w_up,
    b_up,
    w_down,
    b_down,
):
    local_width = main.shape[1]
    width = w_skip_main.shape[1]
    heads_here = local_width // HEAD
    item_scale, valid = item_factors(timesteps, loss_codes, code_weights, item_counts[0])
    row_scale = jnp.repeat(item_scale, SEQ)
    row_valid = jnp.repeat(valid, SEQ)
    main_cols = main.T
    long_cols = long_skip.T
    stream = (
        lax.psum_scatter(
            jnp.einsum("dc,dt->ct", w_skip_main, main_cols, preferred_element_type=jnp.float32)
            + jnp.einsum("dc,dt->ct", w_skip_long, long_cols, preferred_element_type=jnp.float32),
            "tp",
            scatter_dimension=0,
            tiled=True,
        )
        + b_skip[:, None]
    )
    normed_one, rstd_one, full_one = layer_norm(stream, ln1_gain, ln1_bias, width)
    qkv = jnp.einsum("edc,dt->ect", w_qkv, full_one, preferred_element_type=jnp.float32).astype(
        jnp.bfloat16
    )
    query_blocks = split_heads(qkv[0], heads_here)
    key_blocks = split_heads(qkv[1], heads_here)
    value_blocks = split_heads(qkv[2], heads_here)
    attended_blocks, logsums = lax.map(attend, (query_blocks, key_blocks, value_blocks))
    attended = join_heads(attended_blocks)
    cols_here = w_proj
    projected = lax.psum_scatter(
        jnp.einsum("rc,rt->ct", cols_here, attended, preferred_element_type=jnp.float32).astype(
            jnp.bfloat16
        ),
        "tp",
        scatter_dimension=0,
        tiled=True,
    ).astype(jnp.float32)
    stream_two = stream + projected + b_proj[:, None]
    normed_two, rstd_two, full_two = layer_norm(stream_two, ln2_gain, ln2_bias, width)
    upward = (
        jnp.einsum("dc,dt->ct", w_up, full_two, preferred_element_type=jnp.float32) + b_up[:, None]
    )
    activated = jax.nn.gelu(upward, approximate=False).astype(jnp.bfloat16)
    cols_here = w_down
    result = (
        stream_two
        + lax.psum_scatter(
            jnp.einsum(
                "fc,ft->ct", cols_here, activated, preferred_element_type=jnp.float32
            ).astype(jnp.bfloat16),
            "tp",
            scatter_dimension=0,
            tiled=True,
        ).astype(jnp.float32)
        + b_down[:, None]
    )
    out = (result * row_valid[None, :]).T.astype(jnp.bfloat16)
    grad_low = (cotangent.T.astype(jnp.float32) * row_scale[None, :]).astype(jnp.bfloat16)
    grad_wide = grad_low.astype(jnp.float32)
    g_b_down = jnp.sum(grad_wide, 1)
    (d_activated,), (g_w_down,) = fold_back(grad_low, ((w_down, activated),))
    cumulative = 0.5 * (1.0 + lax.erf(upward * ROOT_HALF))
    density = jnp.exp(-0.5 * upward * upward) * DENSITY_SCALE
    d_upward = (d_activated * (cumulative + upward * density)).astype(jnp.bfloat16)
    g_b_up = jnp.sum(d_upward.astype(jnp.float32), 1)
    g_w_up = jnp.einsum("dt,ft->df", full_two, d_upward, preferred_element_type=jnp.float32)

    def up_term(start, count_rows):
        return jnp.einsum("cf,ft->ct", w_up, d_upward, preferred_element_type=jnp.float32)

    d_normed_two = reduce_back(up_term, local_width)
    back_two, g_ln2_gain, g_ln2_bias = norm_back(
        d_normed_two, normed_two, rstd_two, ln2_gain, width
    )
    d_stream_two = (back_two + grad_wide).astype(jnp.bfloat16)
    d_stream_wide = d_stream_two.astype(jnp.float32)
    g_b_proj = jnp.sum(d_stream_wide, 1)
    (d_attended,), (g_w_proj,) = fold_back(d_stream_two, ((w_proj, attended),))
    d_attended_blocks = split_heads(d_attended.astype(jnp.bfloat16), heads_here)
    d_queries, d_keys, d_values = lax.map(
        attend_back, (query_blocks, key_blocks, value_blocks, logsums, d_attended_blocks)
    )
    d_qkv = jnp.stack([join_heads(d_queries), join_heads(d_keys), join_heads(d_values)], axis=0)
    g_w_qkv = jnp.einsum("dt,ect->edc", full_one, d_qkv, preferred_element_type=jnp.float32)

    def qkv_term(start, count_rows):
        return jnp.einsum("ecr,ert->ct", w_qkv, d_qkv, preferred_element_type=jnp.float32)

    d_normed_one = reduce_back(qkv_term, local_width)
    back_one, g_ln1_gain, g_ln1_bias = norm_back(
        d_normed_one, normed_one, rstd_one, ln1_gain, width
    )
    d_stream = (back_one + d_stream_wide).astype(jnp.bfloat16)
    g_b_skip = jnp.sum(d_stream.astype(jnp.float32), 1)
    (d_main_cols, d_long_cols), (g_w_main, g_w_long) = fold_back(
        d_stream, ((w_skip_main, main_cols), (w_skip_long, long_cols))
    )
    (
        g_w_main,
        g_w_long,
        g_b_skip,
        g_ln1_gain,
        g_ln1_bias,
        g_w_qkv,
        g_w_proj,
        g_b_proj,
        g_ln2_gain,
        g_ln2_bias,
        g_w_up,
        g_b_up,
        g_w_down,
        g_b_down,
    ) = (
        lax.psum(g_w_main.astype(jnp.bfloat16), "dp").astype(jnp.float32),
        lax.psum(g_w_long.astype(jnp.bfloat16), "dp").astype(jnp.float32),
        lax.psum(g_b_skip.astype(jnp.bfloat16), "dp").astype(jnp.float32),
        lax.psum(g_ln1_gain.astype(jnp.bfloat16), "dp").astype(jnp.float32),
        lax.psum(g_ln1_bias.astype(jnp.bfloat16), "dp").astype(jnp.float32),
        lax.psum(g_w_qkv.astype(jnp.bfloat16), "dp").astype(jnp.float32),
        lax.psum(g_w_proj.astype(jnp.bfloat16), "dp").astype(jnp.float32),
        lax.psum(g_b_proj.astype(jnp.bfloat16), "dp").astype(jnp.float32),
        lax.psum(g_ln2_gain.astype(jnp.bfloat16), "dp").astype(jnp.float32),
        lax.psum(g_ln2_bias.astype(jnp.bfloat16), "dp").astype(jnp.float32),
        lax.psum(g_w_up.astype(jnp.bfloat16), "dp").astype(jnp.float32),
        lax.psum(g_b_up.astype(jnp.bfloat16), "dp").astype(jnp.float32),
        lax.psum(g_w_down.astype(jnp.bfloat16), "dp").astype(jnp.float32),
        lax.psum(g_b_down.astype(jnp.bfloat16), "dp").astype(jnp.float32),
    )
    d_main = d_main_cols.T.astype(jnp.bfloat16)
    d_long = d_long_cols.T.astype(jnp.bfloat16)
    return (
        out,
        d_main,
        d_long,
        g_w_main,
        g_w_long,
        g_b_skip,
        g_ln1_gain,
        g_ln1_bias,
        g_w_qkv,
        g_w_proj,
        g_b_proj,
        g_ln2_gain,
        g_ln2_bias,
        g_w_up,
        g_b_up,
        g_w_down,
        g_b_down,
    )


ITEM_ROWS = 264
GRAD_ROWS = 24
CORE = ("tp", 1)
ACROSS_Y = ("tp", 2)
ACROSS_X = ("dp", 1)
ACROSS_Z = ("dp", 2)


def swap(value, link):
    axis, bit = link
    return lax.ppermute(value, axis, [(i, i ^ bit) for i in range(lax.axis_size(axis))])


def side(link):
    axis, bit = link
    return (lax.axis_index(axis) // bit) % 2


def in_order(bit, mine, theirs):
    flip = bit == 1
    return jnp.stack([jnp.where(flip, theirs, mine), jnp.where(flip, mine, theirs)])


def pick(value, index):
    return lax.dynamic_index_in_dim(value, index, 0, keepdims=False)


def peer(value, bit):
    return value + bit - 2 * bit * ((value // bit) % 2)


def greet(peers):
    barrier = pltpu.get_barrier_semaphore()
    for where in peers:
        pl.semaphore_signal(barrier, inc=1, device_id=where, device_id_type=pl.DeviceIdType.MESH)
    pl.semaphore_wait(barrier, len(peers))


def send(source, target, sems, index, where):
    return pltpu.make_async_remote_copy(
        src_ref=source,
        dst_ref=target,
        send_sem=sems.at[0, index],
        recv_sem=sems.at[1, index],
        device_id=where,
        device_id_type=pl.DeviceIdType.MESH,
    )


def gather_kernel(pieces, n_in, n_out, *refs):
    tokens, vectors, inputs = refs[0], refs[1], refs[2 : 2 + n_in]
    refs = refs[2 + n_in :]
    far_tokens, core_near, core_far, far_vectors, core_vectors = refs[:5]
    outs, held = refs[5 : 5 + n_out], refs[5 + n_out : 5 + n_out + n_in]
    y_sem, one_sem, two_sem, own_sem, far_sem, local_sem, token_sem = refs[5 + n_out + n_in :]
    n = len(pieces)
    shards = [inputs[a].at[lead] if lead else inputs[a] for a, lead, _, _ in pieces]
    stage = [held[a].at[lead] if lead else held[a] for a, lead, _, _ in pieces]
    fulls = [
        [outs[b[place]].at[tail] if isinstance(b, tuple) else outs[b].at[(place,) + tail] for place in range(4)]
        for _, _, b, tail in pieces
    ]
    dp, tp = lax.axis_index("dp"), lax.axis_index("tp")
    core, y = tp % 2, (tp // 2) % 2
    to_core, to_y = {"tp": peer(tp, 1)}, {"tp": peer(tp, 2)}
    links = ({"dp": peer(dp, 1)}, {"dp": peer(dp, 2)})
    bits = (dp % 2, (dp // 2) % 2)
    greet((to_core, to_y) + links)

    def places(k):
        return k % 2, 1 - k % 2, bits[k % 2], bits[1 - k % 2]

    def y_copy(k):
        _, _, f, s = places(k)
        return send(shards[k].at[s, f], fulls[k][1].at[s, f], y_sem, k, to_y)

    def one_copy(k):
        first, _, f, s = places(k)
        part = fulls[k][1].at[s, f]
        return send(part, part, one_sem, k, links[first])

    def two_copy(k):
        _, second, _, s = places(k)
        part = fulls[k][1].at[s]
        return send(part, part, two_sem, k, links[second])

    def own_copy(k):
        return send(shards[k], fulls[k][2], own_sem, k, to_core)

    def far_copy(k):
        return send(fulls[k][1], fulls[k][3], far_sem, k, to_core)

    def load(k):
        return pltpu.make_async_copy(shards[k], stage[k], local_sem.at[0, k])

    def store(k):
        return pltpu.make_async_copy(stage[k], fulls[k][0], local_sem.at[1, k])

    token_y = send(tokens.at[1 - y], far_tokens, token_sem, 0, to_y)
    token_near = send(tokens.at[y, 1 - core], core_near, token_sem, 1, to_core)
    token_far = send(far_tokens.at[1 - core], core_far, token_sem, 2, to_core)
    vectors_y = send(vectors, far_vectors, token_sem, 3, to_y)
    vectors_near = send(vectors, core_vectors.at[0], token_sem, 4, to_core)
    vectors_far = send(far_vectors, core_vectors.at[1], token_sem, 5, to_core)
    vectors_y.start()
    vectors_near.start()
    for k in range(n):
        y_copy(k).start()
    token_y.start()
    token_near.start()
    for k in range(n):
        load(k).start()
        own_copy(k).start()
    for step in range(n + 2):
        if step < n:
            y_copy(step).wait_recv()
            one_copy(step).start()
            load(step).wait()
            store(step).start()
        if 0 <= step - 1 < n:
            one_copy(step - 1).wait_recv()
            two_copy(step - 1).start()
        if 0 <= step - 2 < n:
            two_copy(step - 2).wait_recv()
            far_copy(step - 2).start()
    vectors_y.wait_recv()
    vectors_far.start()
    token_y.wait_recv()
    token_far.start()
    for copy in (token_near, token_far, vectors_near, vectors_far):
        copy.wait()
    token_y.wait_send()
    vectors_y.wait_send()
    for k in range(n):
        far_copy(k).wait()
        own_copy(k).wait()
        store(k).wait()
        for copy in (y_copy(k), one_copy(k), two_copy(k)):
            copy.wait_send()


def gather_weights(tokens, vectors, arrays, pieces, out_shapes):
    n = len(pieces)
    shape = lambda dims, like: jax.ShapeDtypeStruct(dims, like.dtype)
    rows = tokens.shape[2:]
    outs = [shape((2,) + rows, tokens), shape(rows, tokens), shape(rows, tokens)]
    outs += [shape(vectors.shape, vectors), shape((2,) + vectors.shape, vectors)]
    outs += [shape(dims, arrays[0]) for dims in out_shapes]
    sems = [pltpu.SemaphoreType.DMA((2, n))] * 6 + [pltpu.SemaphoreType.DMA((2, 6))]
    return pl.pallas_call(
        functools.partial(gather_kernel, pieces, len(arrays), len(out_shapes)),
        out_shape=outs,
        in_specs=[pl.BlockSpec(memory_space=pltpu.MemorySpace.HBM)] * (2 + len(arrays)),
        out_specs=[pl.BlockSpec(memory_space=pltpu.MemorySpace.HBM)] * len(outs),
        scratch_shapes=[pltpu.VMEM(a.shape, a.dtype) for a in arrays] + sems,
        compiler_params=pltpu.CompilerParams(
            collective_id=1, has_side_effects=True, vmem_limit_bytes=32 * 2**20
        ),
        name="gather_weights",
    )(tokens, vectors, *arrays)


def reduce_kernel(sizes, views, n_arrays, *refs):
    ready, arrays, blocks, quarter = refs[0], refs[1 : 1 + n_arrays], refs[1 + n_arrays], refs[2 + n_arrays]
    refs = refs[3 + n_arrays :]
    outs, refs = refs[: 1 + len(views)], refs[1 + len(views) :]
    from_core, y_blocks, own_quarter, z_quarter, x_quarters = refs[:5]
    total, from_y, from_one, half, from_two, from_far, final, part, far_part = refs[5:14]
    y_sem, one_sem, two_sem, far_sem, back_two, back_one, block_sem, load_sem, out_sem = refs[14:]
    chunks, n_ready = total.shape[0], sizes[0]
    dp, tp = lax.axis_index("dp"), lax.axis_index("tp")
    to_core, to_y, to_far = {"tp": peer(tp, 1)}, {"tp": peer(tp, 2)}, {"dp": peer(dp, 4)}
    to_x, to_z = {"dp": peer(dp, 1)}, {"dp": peer(dp, 2)}
    greet((to_core, to_y, to_x, to_z, to_far))

    def plan(s):
        z_first = (s % 4) // 3
        first, second = 1 + z_first, 2 - z_first
        places = (dp // first) % 2, (dp // second) % 2
        return ({"dp": peer(dp, first)}, {"dp": peer(dp, second)}) + places

    def y_copy(s, source):
        return send(source, from_y.at[s - n_ready], y_sem, s - n_ready, to_y)

    def one_copy(s):
        to_one, _, f, _ = plan(s)
        return send(total.at[s, 1 - f], from_one.at[s], one_sem, s, to_one)

    def two_copy(s):
        _, to_two, _, g = plan(s)
        return send(half.at[s, 1 - g], from_two.at[s], two_sem, s, to_two)

    def far_copy(s):
        _, _, _, g = plan(s)
        return send(half.at[s, g], from_far.at[s], far_sem, s, to_far)

    def back_two_copy(s):
        _, to_two, f, g = plan(s)
        part = final.at[s, f, g]
        return send(part, part, back_two, s, to_two)

    def back_one_copy(s):
        to_one, _, f, _ = plan(s)
        part = final.at[s, f]
        return send(part, part, back_one, s, to_one)

    def out_copies(s, act):
        at = 0
        for k, size in enumerate(sizes):

            @pl.when((s >= at) & (s < at + size))
            def _(k=k, at=at):
                act(pltpu.make_async_copy(final.at[s], outs[k].at[s - at], out_sem.at[s]))

            at += size

    quarter_load = pltpu.make_async_copy(quarter, part, load_sem.at[0])
    ready_load = pltpu.make_async_copy(ready, total.at[pl.ds(0, n_ready)], load_sem.at[1])
    ready_load.start()
    quarter_load.start()
    core_blocks = [send(blocks.at[2 + k], from_core.at[k], block_sem, k, to_core) for k in range(2)]
    own_block = send(blocks.at[1], y_blocks.at[0], block_sem, 2, to_y)
    core_block = send(from_core.at[1], y_blocks.at[1], block_sem, 3, to_y)
    quarter_far = send(quarter, far_part, block_sem, 4, to_far)
    quarter_z = send(own_quarter, z_quarter, block_sem, 5, to_z)
    quarter_x = send(own_quarter, x_quarters.at[0], block_sem, 6, to_x)
    quarter_zx = send(z_quarter, x_quarters.at[1], block_sem, 7, to_x)
    quarter_out = pltpu.make_async_copy(part, own_quarter, out_sem.at[chunks])
    loads, at = [], n_ready
    for k, (size, (a, mine, theirs)) in enumerate(zip(sizes[1:], views)):
        source = arrays[a].at[mine]
        loads.append(pltpu.make_async_copy(source, total.at[pl.ds(at, size)], load_sem.at[2 + k]))
        loads[-1].start()
        for r in range(size):
            y_copy(at + r, arrays[a].at[theirs + (r,)]).start()
        at += size
    for copy in core_blocks:
        copy.start()
    own_block.start()
    quarter_far.start()
    for copy in [ready_load, quarter_load] + loads:
        copy.wait()

    def plus(left, right):
        return (left.astype(jnp.float32) + right.astype(jnp.float32)).astype(jnp.bfloat16)

    def step(t, carry):
        @pl.when((t >= n_ready) & (t < chunks))
        def _():
            y_copy(t, total.at[t]).wait_recv()
            total[t] = plus(total[t], from_y[t - n_ready])

        @pl.when(t < chunks)
        def _():
            one_copy(t).start()

        @pl.when((t >= 2) & (t < chunks + 2))
        def _():
            s = t - 2
            _, _, f, _ = plan(s)
            one_copy(s).wait_recv()
            half[s] = plus(total[s, f], from_one[s])
            two_copy(s).start()

        @pl.when((t >= 3) & (t < chunks + 3))
        def _():
            s = t - 3
            _, _, _, g = plan(s)
            two_copy(s).wait_recv()
            half[s, g] = plus(half[s, g], from_two[s])
            far_copy(s).start()

        @pl.when((t >= 5) & (t < chunks + 5))
        def _():
            s = t - 5
            _, _, f, g = plan(s)
            far_copy(s).wait_recv()
            final[s, f, g] = plus(half[s, g], from_far[s])
            back_two_copy(s).start()

        @pl.when((t >= 6) & (t < chunks + 6))
        def _():
            back_two_copy(t - 6).wait_recv()
            back_one_copy(t - 6).start()

        @pl.when((t >= 7) & (t < chunks + 7))
        def _():
            back_one_copy(t - 7).wait_recv()
            out_copies(t - 7, lambda copy: copy.start())

        @pl.when(t == 2)
        def _():
            for copy in core_blocks:
                copy.wait_recv()
            core_block.start()

        @pl.when(t == 8)
        def _():
            quarter_far.wait()
            part[...] = plus(part[...], far_part[...])
            quarter_out.start()

        @pl.when(t == 9)
        def _():
            quarter_out.wait()
            quarter_z.start()
            quarter_x.start()

        @pl.when(t == 18)
        def _():
            quarter_z.wait_recv()
            quarter_zx.start()

        return carry

    lax.fori_loop(0, chunks + 7, step, 0)

    def finish_y(s, carry):
        y_copy(s, total.at[s]).wait_send()
        return carry

    lax.fori_loop(n_ready, chunks, finish_y, 0)

    def finish(s, carry):
        for copy in (one_copy(s), two_copy(s), far_copy(s), back_two_copy(s), back_one_copy(s)):
            copy.wait_send()
        out_copies(s, lambda copy: copy.wait())
        return carry

    lax.fori_loop(0, chunks, finish, 0)
    for copy in core_blocks:
        copy.wait_send()
    own_block.wait()
    core_block.wait()
    quarter_z.wait_send()
    quarter_x.wait()
    quarter_zx.wait()


def reduce_grads(ready, arrays, views, blocks, quarter):
    sizes = (ready.shape[0],) + tuple(arrays[a].shape[len(mine)] for a, mine, _ in views)
    chunks = sum(sizes)
    rows, width = ready.shape[-2:]
    kind = ready.dtype
    sem = lambda n: pltpu.SemaphoreType.DMA((2, n))
    two_blocks = jax.ShapeDtypeStruct((2,) + blocks.shape[1:], blocks.dtype)
    hbm = pl.BlockSpec(memory_space=pltpu.MemorySpace.HBM)
    vmem = lambda *lead: pltpu.VMEM(lead + (rows, width), kind)
    n_in, n_out = 3 + len(arrays), 6 + len(views)
    return pl.pallas_call(
        functools.partial(reduce_kernel, sizes, views, len(arrays)),
        out_shape=[jax.ShapeDtypeStruct((n, 2, 2, rows, width), kind) for n in sizes]
        + [two_blocks, two_blocks]
        + [jax.ShapeDtypeStruct(lead + quarter.shape, kind) for lead in ((), (), (2,))],
        in_specs=[hbm] * n_in,
        out_specs=[hbm] * n_out,
        scratch_shapes=[
            vmem(chunks, 2, 2),
            vmem(chunks - sizes[0], 2, 2),
            vmem(chunks, 2),
            vmem(chunks, 2),
            vmem(chunks),
            vmem(chunks),
            vmem(chunks, 2, 2),
            pltpu.VMEM(quarter.shape, kind),
            pltpu.VMEM(quarter.shape, kind),
            sem(chunks - sizes[0]),
            sem(chunks),
            sem(chunks),
            sem(chunks),
            sem(chunks),
            sem(chunks),
            sem(8),
            pltpu.SemaphoreType.DMA((2 + len(views),)),
            pltpu.SemaphoreType.DMA((chunks + 1,)),
        ],
        compiler_params=pltpu.CompilerParams(
            collective_id=2, has_side_effects=True, vmem_limit_bytes=56 * 2**20
        ),
        name="reduce_grads",
    )(ready, *arrays, blocks, quarter)


def add_low(mine, theirs):
    return (mine.astype(jnp.float32) + theirs.astype(jnp.float32)).astype(jnp.bfloat16)


def place_of(index):
    rank = lax.axis_index("tp")
    core, y = rank % 2, (rank // 2) % 2
    there_core, there_y = index % 2, index // 2
    apart = lambda a, b: a + b - 2 * a * b
    return apart(y, there_y) + 2 * apart(core, there_core)


def spread_kernel(main_ref, long_ref, cot_ref, tokens_ref, cot_tokens_ref):
    cols = main_ref.shape[1]
    items = tokens_ref.shape[1] // ITEM_ROWS
    for p in range(4):
        for i in range(items):
            source = slice((p * items + i) * SEQ, (p * items + i + 1) * SEQ)
            target = slice(i * ITEM_ROWS, i * ITEM_ROWS + SEQ)
            blank = slice(i * ITEM_ROWS + SEQ, (i + 1) * ITEM_ROWS)
            tokens_ref[p, target, :cols] = main_ref[source, :]
            tokens_ref[p, target, cols:] = long_ref[source, :]
            cot_tokens_ref[p, target, :] = cot_ref[source, :]
            tokens_ref[p, blank, :] = jnp.zeros((ITEM_ROWS - SEQ, 2 * cols), tokens_ref.dtype)
            cot_tokens_ref[p, blank, :] = jnp.zeros((ITEM_ROWS - SEQ, cols), tokens_ref.dtype)


def spread(main, long_skip, cotangent):
    rows, cols = main.shape
    padded = rows // SEQ // 4 * ITEM_ROWS
    return pl.pallas_call(
        spread_kernel,
        out_shape=[
            jax.ShapeDtypeStruct((4, padded, 2 * cols), main.dtype),
            jax.ShapeDtypeStruct((4, padded, cols), main.dtype),
        ],
        compiler_params=pltpu.CompilerParams(vmem_limit_bytes=40 * 2**20),
        name="spread",
    )(main, long_skip, cotangent)


def arrange_kernel(own_ref, y_ref, partner_ref, scale_ref, out_ref, held):
    cols = own_ref.shape[1]
    held[0] = own_ref[...]
    held[1] = y_ref[...]
    held[2] = partner_ref[0]
    held[3] = partner_ref[1]
    for j in range(4):
        block = held[place_of(j)].astype(jnp.float32) * scale_ref[...]
        out_ref[:, j * cols : (j + 1) * cols] = block.astype(out_ref.dtype)


def arrange(own, along_y, partner, scale):
    rows, cols = own.shape
    return pl.pallas_call(
        arrange_kernel,
        out_shape=jax.ShapeDtypeStruct((rows, 4 * cols), own.dtype),
        scratch_shapes=[pltpu.VMEM((4, rows, cols), own.dtype)],
        compiler_params=pltpu.CompilerParams(vmem_limit_bytes=24 * 2**20),
        name="arrange",
    )(own, along_y, partner, scale)


def disperse_kernel(rows_ref, valid_ref, out_ref):
    cols = out_ref.shape[2]
    for j in range(4):
        block = rows_ref[:, j * cols : (j + 1) * cols] * valid_ref[...]
        out_ref[place_of(j)] = block.astype(out_ref.dtype)


def disperse(rows, valid):
    count, width = rows.shape
    return pl.pallas_call(
        disperse_kernel,
        out_shape=jax.ShapeDtypeStruct((4, count, width // 4), jnp.bfloat16),
        compiler_params=pltpu.CompilerParams(vmem_limit_bytes=24 * 2**20),
        name="disperse",
    )(rows, valid)


def unspread_kernel(parts, own_ref, core_ref, y_ref, *refs):
    outs, held = refs[:parts], refs[parts]
    cols = outs[0].shape[1]
    items = own_ref.shape[0] // ITEM_ROWS
    held[0] = own_ref[...]
    held[1] = y_ref[0]
    held[2] = core_ref[...]
    held[3] = y_ref[1]
    for p in range(4):
        rows = held[place_of(p)]
        for i in range(items):
            target = slice((p * items + i) * SEQ, (p * items + i + 1) * SEQ)
            source = slice(i * ITEM_ROWS, i * ITEM_ROWS + SEQ)
            for k in range(parts):
                outs[k][target, :] = rows[source, k * cols : (k + 1) * cols]


def unspread(own, core_tokens, y_tokens, parts):
    rows, width = own.shape
    out = jax.ShapeDtypeStruct((4 * rows // ITEM_ROWS * SEQ, width // parts), own.dtype)
    return pl.pallas_call(
        functools.partial(unspread_kernel, parts),
        out_shape=[out] * parts,
        scratch_shapes=[pltpu.VMEM((4, rows, width), own.dtype)],
        compiler_params=pltpu.CompilerParams(vmem_limit_bytes=40 * 2**20),
        name="unspread",
    )(own, core_tokens, y_tokens)


def natural(own_half, partner_half, width, axis):
    flip_y, flip_core = side(ACROSS_Y) == 1, side(CORE) == 1
    r0, r2 = jnp.split(own_half, 2, axis)
    r1, r3 = jnp.split(partner_half, 2, axis)
    a0, a2 = jnp.where(flip_y, r2, r0), jnp.where(flip_y, r0, r2)
    a1, a3 = jnp.where(flip_y, r3, r1), jnp.where(flip_y, r1, r3)
    b0, b1 = jnp.where(flip_core, a1, a0), jnp.where(flip_core, a0, a1)
    b2, b3 = jnp.where(flip_core, a3, a2), jnp.where(flip_core, a2, a3)
    return (b0, b1, b2, b3)


def dot(spec, left, right):
    return jnp.einsum(spec, left, right, preferred_element_type=jnp.float32)


def low(value):
    return value.astype(jnp.bfloat16)


def norm_rows(stream, gain, bias):
    mean = jnp.mean(stream, 1, keepdims=True)
    square = jnp.mean(stream * stream, 1, keepdims=True)
    rstd = lax.rsqrt(square - mean * mean + EPSILON)
    normed = (stream - mean) * rstd
    return normed, rstd, low(normed * gain + bias)


def norm_rows_back(d_out, normed, rstd, gain):
    g_gain = jnp.sum(d_out * normed, 0)
    g_bias = jnp.sum(d_out, 0)
    scaled = d_out * gain
    first = jnp.mean(scaled, 1, keepdims=True)
    second = jnp.mean(scaled * normed, 1, keepdims=True)
    return rstd * (scaled - first - normed * second), g_gain, g_bias


LAST = (((1,), (1,)), ((), ()))
LEAD = (((0,), (0,)), ((), ()))


def item_scores(key, query):
    scores = lax.dot_general(key, query, LAST, preferred_element_type=jnp.float32)
    present = lax.broadcasted_iota(jnp.int32, scores.shape, 0) < SEQ
    return jnp.where(present, scores * (1.0 / math.sqrt(HEAD)), -1e30)


def attend_kernel(*refs):
    def item(i, carry):
        attend_item(*(ref.at[i] for ref in refs))
        return carry

    lax.fori_loop(0, refs[0].shape[0], item, 0)


def attend_item(q_ref, k_ref, v_ref, out_ref, lse_ref):
    for h in range(q_ref.shape[1] // HEAD):
        at = slice(h * HEAD, (h + 1) * HEAD)
        scores = item_scores(k_ref[:, at], q_ref[:, at])
        peak = jnp.max(scores, axis=0, keepdims=True)
        weights = jnp.exp(scores - peak)
        total = jnp.sum(weights, axis=0, keepdims=True)
        probs = (weights * (1.0 / total)).astype(jnp.bfloat16)
        out = lax.dot_general(probs, v_ref[:, at], LEAD, preferred_element_type=jnp.float32)
        out_ref[:, at] = out.astype(jnp.bfloat16)
        lse_ref[h : h + 1, :] = peak + jnp.log(total)


def attend_back_kernel(*refs):
    def item(i, carry):
        attend_back_item(*(ref.at[i] for ref in refs))
        return carry

    lax.fori_loop(0, refs[0].shape[0], item, 0)


def attend_back_item(q_ref, k_ref, v_ref, lse_ref, d_ref, dq_ref, dk_ref, dv_ref, own_ref, partner_ref):
    scale = 1.0 / math.sqrt(HEAD)
    for h in range(q_ref.shape[1] // HEAD):
        at = slice(h * HEAD, (h + 1) * HEAD)
        query, key, d_out = q_ref[:, at], k_ref[:, at], d_ref[:, at]
        probs = jnp.exp(item_scores(key, query) - lse_ref[h : h + 1, :])
        d_probs = lax.dot_general(v_ref[:, at], d_out, LAST, preferred_element_type=jnp.float32)
        delta = jnp.sum(probs * d_probs, axis=0, keepdims=True)
        d_scores = (probs * (d_probs - delta)).astype(jnp.bfloat16)
        dq = lax.dot_general(d_scores, key, LEAD, preferred_element_type=jnp.float32)
        dk = jnp.dot(d_scores, query, preferred_element_type=jnp.float32)
        dv = jnp.dot(probs.astype(jnp.bfloat16), d_out, preferred_element_type=jnp.float32)
        cols = q_ref.shape[1] // 2
        side_ref, start = (own_ref, h * HEAD) if h * HEAD < cols else (partner_ref, h * HEAD - cols)
        for e, (ref, d) in enumerate(((dq_ref, dq * scale), (dk_ref, dk * scale), (dv_ref, dv))):
            d = d.astype(jnp.bfloat16)
            ref[:, at] = d
            side_ref[:, e * cols + start : e * cols + start + HEAD] = d


def by_item(value):
    return value.reshape(-1, ITEM_ROWS, value.shape[1])


def attention(query, key, value):
    rows, cols = query.shape
    heads, items = cols // HEAD, rows // ITEM_ROWS
    out, lse = pl.pallas_call(
        attend_kernel,
        out_shape=[
            jax.ShapeDtypeStruct((items, ITEM_ROWS, cols), jnp.bfloat16),
            jax.ShapeDtypeStruct((items, heads, ITEM_ROWS), jnp.float32),
        ],
        cost_estimate=pl.CostEstimate(
            flops=4 * rows * ITEM_ROWS * cols, bytes_accessed=8 * rows * cols, transcendentals=rows * ITEM_ROWS * heads
        ),
        compiler_params=pltpu.CompilerParams(vmem_limit_bytes=24 * 2**20),
        name="attend",
    )(by_item(query), by_item(key), by_item(value))
    return out.reshape(rows, cols), lse


def attention_back(query, key, value, lse, d_out):
    rows, cols = query.shape
    heads, items = cols // HEAD, rows // ITEM_ROWS
    shape = lambda width: jax.ShapeDtypeStruct((items, ITEM_ROWS, width), jnp.bfloat16)
    outs = pl.pallas_call(
        attend_back_kernel,
        out_shape=[shape(cols)] * 3 + [shape(3 * cols // 2)] * 2,
        cost_estimate=pl.CostEstimate(
            flops=10 * rows * ITEM_ROWS * cols, bytes_accessed=14 * rows * cols, transcendentals=rows * ITEM_ROWS * heads
        ),
        compiler_params=pltpu.CompilerParams(vmem_limit_bytes=32 * 2**20),
        name="attend_back",
    )(by_item(query), by_item(key), by_item(value), lse, by_item(d_out))
    return [o.reshape(rows, -1) for o in outs]


HIDDEN_BLOCK = 384


def feed_kernel(first, n_ref, g_ref, up_ref, bias_ref, down_ref, *refs):
    sums, (act_ref, d_up_ref, g_bias_ref, result_ref, d_n_ref) = refs[:-5], refs[-5:]
    wide = jnp.float32

    @pl.when(pl.program_id(0) == 0)
    def _():
        result_ref[...] = sums[0][...]
        d_n_ref[...] = jnp.zeros_like(d_n_ref) if first else sums[1][...]

    up = jnp.dot(n_ref[...], up_ref[...], preferred_element_type=wide) + bias_ref[...]
    d_act = lax.dot_general(g_ref[...], down_ref[...], LAST, preferred_element_type=wide)
    cumulative = 0.5 * (1.0 + lax.erf(up * ROOT_HALF))
    density = jnp.exp(-0.5 * up * up) * DENSITY_SCALE
    act = (up * cumulative).astype(jnp.bfloat16)
    d_up = (d_act * (cumulative + up * density)).astype(jnp.bfloat16)
    act_ref[...] = act
    d_up_ref[...] = d_up
    g_bias_ref[...] = jnp.sum(d_up.astype(wide), axis=0, keepdims=True)
    result_ref[...] += jnp.dot(act, down_ref[...], preferred_element_type=wide)
    d_n_ref[...] += lax.dot_general(d_up, up_ref[...], LAST, preferred_element_type=wide)


def feed(n, g, up, bias, down, result, d_n):
    rows, width = n.shape
    hidden = up.shape[1]
    whole = pl.BlockSpec((rows, width), lambda i: (0, 0))
    across = pl.BlockSpec((rows, HIDDEN_BLOCK), lambda i: (0, i))
    line = pl.BlockSpec((1, HIDDEN_BLOCK), lambda i: (0, i))
    sums = (result,) if d_n is None else (result, d_n)
    shape = jax.ShapeDtypeStruct
    return pl.pallas_call(
        functools.partial(feed_kernel, d_n is None),
        grid=(hidden // HIDDEN_BLOCK,),
        out_shape=[
            shape((rows, hidden), jnp.bfloat16),
            shape((rows, hidden), jnp.bfloat16),
            shape((1, hidden), jnp.float32),
            shape((rows, width), jnp.float32),
            shape((rows, width), jnp.float32),
        ],
        in_specs=[
            whole,
            whole,
            pl.BlockSpec((width, HIDDEN_BLOCK), lambda i: (0, i)),
            line,
            pl.BlockSpec((HIDDEN_BLOCK, width), lambda i: (i, 0)),
        ]
        + [whole] * len(sums),
        out_specs=[across, across, line, whole, whole],
        compiler_params=pltpu.CompilerParams(vmem_limit_bytes=40 * 2**20),
        cost_estimate=pl.CostEstimate(
            flops=10 * rows * width * hidden, bytes_accessed=4 * width * hidden, transcendentals=2 * rows * hidden
        ),
        name="feed",
    )(n, g, up, bias, down, *sums)


def body_items(
    main,
    long_skip,
    cotangent,
    timesteps,
    loss_codes,
    code_weights,
    item_counts,
    w_skip_main,
    w_skip_long,
    b_skip,
    ln1_gain,
    ln1_bias,
    w_qkv,
    w_proj,
    b_proj,
    ln2_gain,
    ln2_bias,
    w_up,
    b_up,
    w_down,
    b_down,
):
    local = main.shape[1]
    width = 4 * local
    rank = lax.axis_index("tp")

    vectors = jnp.concatenate(
        [jnp.stack([b_skip, ln1_gain, ln1_bias, b_proj, ln2_gain, ln2_bias, b_down]), b_up.reshape(4, local)]
    )
    y, core, x, z = side(ACROSS_Y), side(CORE), side(ACROSS_X), side(ACROSS_Z)
    cut = 2 * local
    tokens, cot_tokens = spread(main, long_skip, cotangent)
    tokens = tokens.reshape((2, 2) + tokens.shape[1:])
    cot_tokens = cot_tokens.reshape((2, 2) + cot_tokens.shape[1:])
    quarters = lambda w: w.reshape(2, 2, -1, width)
    qkv_rows = jnp.swapaxes(w_qkv, 1, 2).reshape(3, 2, 2, local // 4, width)
    one = (4, 2, 2, local // 4, width)
    far_tokens, core_near, core_far, far_vectors, core_vectors, wskip, wq, wk, wv, wp, *wu = gather_weights(
        tokens,
        vectors,
        [
            quarters(w_skip_main),
            quarters(w_skip_long),
            qkv_rows,
            quarters(w_proj),
            w_up.reshape(2, 2, 2, width // 8, width),
        ],
        [
            (0, (), 0, (0,)),
            (1, (), 0, (1,)),
            (2, (0,), 1, ()),
            (2, (1,), 2, ()),
            (2, (2,), 3, ()),
            (3, (), 4, ()),
            (4, (0,), (5, 6, 7, 8), (0,)),
            (4, (1,), (5, 6, 7, 8), (1,)),
        ],
        [(4, 2) + one[1:], one, one, one, one] + [(2, 2, 2, width // 8, width)] * 4,
    )
    own_vectors = jnp.concatenate([vectors, far_vectors], axis=1)
    partner_vectors = jnp.concatenate([core_vectors[0], core_vectors[1]], axis=1)
    joined = jnp.concatenate(natural(own_vectors[:7], partner_vectors[:7], local, 1), axis=1)
    b_skip_all, gain_one, bias_one, b_proj_all, gain_two, bias_two, b_down_all = (
        joined[k : k + 1] for k in range(7)
    )

    def up_vector(pair):
        near, far = jnp.split(pair[7:], 2, 1)
        return jnp.concatenate([near.reshape(1, -1), far.reshape(1, -1)], axis=1)

    b_up_all = jnp.concatenate([up_vector(own_vectors), up_vector(partner_vectors)], axis=1)

    wskip, wq, wk, wv, wp = (g.reshape(-1, width) for g in (wskip, wq, wk, wv, wp))
    wu = [w.reshape(width, width) for w in wu]
    near_tokens = pick(tokens, y)
    skip_rows = jnp.concatenate([pick(near_tokens, core), pick(far_tokens, core), core_near, core_far], axis=1)
    other = lambda value: swap(value, CORE)
    both = lambda mine, others: jnp.concatenate([mine, others], axis=0)
    shares = lambda value: both(value[:, : value.shape[1] // 2], other(value[:, value.shape[1] // 2 :]))

    def after(value, *events):
        return lax.optimization_barrier((value,) + events)[0]

    meet = lambda *values: lax.optimization_barrier(values)

    cot_near = pick(cot_tokens, y)
    cot_far = swap(after(pick(cot_tokens, 1 - y), wskip), ACROSS_Y)
    w_down_then = after(w_down, skip_rows)
    wd_core = other(w_down_then)
    wd_y = swap(w_down_then, ACROSS_Y)

    stream = dot("td,dc->tc", skip_rows, wskip) + b_skip_all
    normed_one, rstd_one, full_one = norm_rows(stream, gain_one, bias_one)
    skip_both = jnp.concatenate([pick(near_tokens, 1 - core), pick(far_tokens, 1 - core)], axis=1)
    skip_both = both(skip_rows[:, : 2 * cut], skip_both)
    n1_both = both(full_one, other(full_one))
    query, key, value = (low(dot("td,cd->tc", full_one, w)) for w in (wq, wk, wv))
    attended, logsum = attention(query, key, value)
    attended_both = shares(attended)
    stream_two = stream + dot("tc,cd->td", attended, wp) + b_proj_all
    cot_far, stream_two, skip_both, n1_both = meet(cot_far, stream_two, skip_both, n1_both)
    normed_two, rstd_two, full_two = norm_rows(stream_two, gain_two, bias_two)
    n2_both = both(full_two, other(full_two))
    cot_partner = other(jnp.stack([pick(cot_near, 1 - core), pick(cot_far, 1 - core)]))
    item_scale, valid = item_factors(timesteps, loss_codes, code_weights, item_counts[0])
    row_scale = jnp.repeat(pick(item_scale.reshape(4, -1), rank), ITEM_ROWS)[:, None]
    row_valid = jnp.repeat(pick(valid.reshape(4, -1), rank), ITEM_ROWS)[:, None]
    grad_low = arrange(pick(cot_near, core), pick(cot_far, core), cot_partner, row_scale)
    wd = [w_down, None, wd_core, None]
    grad_both = both(grad_low, other(grad_low))
    grad_wide = grad_low.astype(jnp.float32)
    g_b_down = jnp.sum(grad_wide, 0)

    def weight_grad(left, right):
        return low(dot("tf,tc->fc", left, right))

    def split(value, bit):
        halves = value.reshape(2, -1, width)
        return pick(halves, bit), pick(halves, 1 - bit)

    result, d_n2 = stream_two + b_down_all, None
    acts, d_up, g_b_up = [None] * 4, [None] * 4, [None] * 4
    for r in (0, 2, 1, 3):
        if r == 1:
            wd_y, d_n2 = meet(wd_y, d_n2)
            wd[1], wd[3] = wd_y, other(wd_y)
        bias = b_up_all[:, r * width : (r + 1) * width]
        acts[r], d_up[r], g_b_up[r], result, d_n2 = feed(full_two, grad_low, wu[r], bias, wd[r], result, d_n2)
    g_b_up = jnp.concatenate(g_b_up)
    down_theirs = weight_grad(both(acts[1], other(acts[3])), grad_both)
    down_come = swap(down_theirs, ACROSS_Y)
    up_theirs = weight_grad(n2_both, after(both(d_up[1], other(d_up[3])), down_theirs))
    up_come = swap(up_theirs, ACROSS_Y)
    d_n2, result, acts[0], d_up[0] = lax.optimization_barrier((d_n2, result, acts[0], d_up[0], up_theirs))[:4]
    down_mine = weight_grad(both(acts[0], other(acts[2])), grad_both)
    up_mine = weight_grad(n2_both, both(d_up[0], other(d_up[2])))

    outs = disperse(result, row_valid)
    out_core = other(outs[2:])
    out_y = swap(after(jnp.stack([outs[1], out_core[1]]), up_theirs), ACROSS_Y)
    back_two, g_ln2_gain, g_ln2_bias = norm_rows_back(d_n2, normed_two, rstd_two, gain_two)
    d_stream_two = low(back_two + grad_wide)
    d_stream_wide = d_stream_two.astype(jnp.float32)
    g_b_proj = jnp.sum(d_stream_wide, 0)
    chunked = lambda g, lead: g.reshape(lead + (-1, 2, 2, GRAD_ROWS, width))
    proj_part = chunked(weight_grad(attended_both, both(d_stream_two, other(d_stream_two))), (2,))
    d_attended = low(dot("tc,fc->tf", d_stream_two, wp))
    d_qkv = attention_back(query, key, value, logsum, d_attended)
    *d_qkv, d_own, d_partner = d_qkv
    qkv_part = chunked(weight_grad(both(d_own, other(d_partner)), n1_both), (3, 2))
    d_n1 = sum(dot("tc,cd->td", d, w) for d, w in zip(d_qkv, (wq, wk, wv)))
    back_one, g_ln1_gain, g_ln1_bias = norm_rows_back(d_n1, normed_one, rstd_one, gain_one)
    d_stream = low(back_one + d_stream_wide)
    down_come, d_stream = meet(down_come, d_stream)
    down_keep, down_send = split(add_low(down_mine, down_come), x)
    down_come = swap(down_send, ACROSS_X)
    d_stream_both = both(d_stream, other(d_stream))
    g_b_skip = jnp.sum(d_stream.astype(jnp.float32), 0)
    d_skip = low(dot("tc,fc->tf", d_stream, wskip))
    d_blocks = jnp.stack(jnp.split(d_skip, 4, 1))
    down_come, d_stream_both, d_blocks, proj_part, qkv_part = meet(
        down_come, d_stream_both, d_blocks, proj_part, qkv_part
    )
    down_keep, down_send = split(add_low(down_keep, down_come), z)
    down_come = swap(down_send, ACROSS_Z)
    skip_part = chunked(weight_grad(skip_both, d_stream_both), (2,))
    up_come, down_come, skip_part = meet(up_come, down_come, skip_part)
    down_quarter = add_low(down_keep, down_come)
    ready = chunked(add_low(up_mine, up_come), ())

    small = jnp.stack([g_b_skip, g_ln1_gain, g_ln1_bias, g_b_proj, g_ln2_gain, g_ln2_bias, g_b_down])
    arrived = other(jnp.concatenate([small, g_b_up[2:]]))
    small = jnp.moveaxis((small + arrived[:7]).reshape(7, 4, local), 1, 0)
    b_up_sums = g_b_up[:2] + arrived[7:]

    def vector_rows(shard, row):
        flat = jnp.concatenate([pick(small, shard).reshape(-1), b_up_sums[row]])
        return jnp.pad(flat, (0, 4 * GRAD_ROWS * width - flat.size)).reshape(1, 2, 2, GRAD_ROWS, width)

    vector_part = low(jnp.stack([vector_rows(rank, 0), vector_rows(peer(rank, 2), 1)]))
    g_w_up, *sums = reduce_grads(
        ready,
        [proj_part, qkv_part, vector_part, skip_part],
        [(0, (0,), (1,)), (1, (0, 0), (0, 1)), (1, (1, 0), (1, 1)), (1, (2, 0), (2, 1)), (2, (0,), (1,)), (3, (0,), (1,))],
        d_blocks,
        down_quarter,
    )
    *sums, from_core, y_blocks, down_quarter, z_quarter, x_quarters = sums
    out_y, y_blocks = meet(out_y, y_blocks)
    (out,) = unspread(outs[0], out_core[0], out_y, 1)
    wide = lambda value: value.reshape(-1, width).astype(jnp.float32)
    g_w_down = wide(in_order(x, in_order(z, down_quarter, z_quarter), in_order(z, x_quarters[0], x_quarters[1])))
    g_w_proj, g_q, g_k, g_v, vectors, g_skip = (wide(g) for g in sums)
    g_w_qkv = jnp.stack([g.T for g in (g_q, g_k, g_v)])
    vectors = vectors.reshape(-1)
    mine = vectors[: 7 * local].reshape(7, local)

    d_main, d_long = unspread(d_blocks[0], from_core[0], y_blocks, 2)
    return (
        out,
        d_main,
        d_long,
        g_skip[:local],
        g_skip[local:],
        mine[0],
        mine[1],
        mine[2],
        g_w_qkv,
        g_w_proj,
        mine[3],
        mine[4],
        mine[5],
        wide(g_w_up),
        vectors[7 * local : 7 * local + width],
        g_w_down,
        mine[6],
    )


def solution(mesh):
    by_items = mesh.shape["tp"] == 4 and mesh.shape["dp"] == 8
    return jax.shard_map(
        body_items if by_items else body_features,
        mesh=mesh,
        in_specs=(
            P("dp", "tp"),
            P("dp", "tp"),
            P("dp", "tp"),
            P("dp"),
            P("dp"),
            P(),
            P("dp"),
            P("tp", None),
            P("tp", None),
            P("tp"),
            P("tp"),
            P("tp"),
            P(None, None, "tp"),
            P("tp", None),
            P("tp"),
            P("tp"),
            P("tp"),
            P(None, "tp"),
            P("tp"),
            P("tp", None),
            P("tp"),
        ),
        out_specs=(
            P("dp", "tp"),
            P("dp", "tp"),
            P("dp", "tp"),
            P("tp", None),
            P("tp", None),
            P("tp"),
            P("tp"),
            P("tp"),
            P(None, None, "tp"),
            P("tp", None),
            P("tp"),
            P("tp"),
            P("tp"),
            P(None, "tp"),
            P("tp"),
            P("tp", None),
            P("tp"),
        ),
        check_vma=False,
    )
```

```python
import functools
import math

import jax
import jax.numpy as jnp
from jax import lax
from jax.experimental import pallas as pl
from jax.experimental.pallas import tpu as pltpu
from jax.sharding import PartitionSpec as P

HEAD = 72
SEQ = 258
TSTEPS = 1000


EPSILON = 1e-06
ROOT_HALF = 0.7071067811865476
DENSITY_SCALE = 0.3989422804014327


def item_factors(timesteps, loss_codes, code_weights, group_items):
    steps_float = timesteps.astype(jnp.float32)
    phase = (steps_float / TSTEPS + 0.008) / 1.008 * (math.pi / 2.0)
    cosine = jnp.cos(phase)
    signal = cosine * cosine
    weight = jnp.minimum(1.0, 5.0 * (1.0 - signal) / signal)
    picks = (
        loss_codes[:, None] == jnp.arange(code_weights.shape[0], dtype=jnp.int32)[None, :]
    ).astype(jnp.float32)
    coded = jnp.sum(picks * code_weights[None, :], axis=1)
    valid = (jnp.arange(timesteps.shape[0], dtype=jnp.int32) < group_items).astype(jnp.float32)
    return (weight * coded * valid, valid)


def layer_norm(stream, gain, bias, width):
    totals, squares = lax.psum((jnp.sum(stream, 0), jnp.sum(stream * stream, 0)), "tp")
    mean = totals / width
    rstd = lax.rsqrt(squares / width - mean * mean + EPSILON)
    normed = (stream - mean[None, :]) * rstd[None, :]
    rounded = (normed * gain[:, None] + bias[:, None]).astype(jnp.bfloat16)
    return (normed, rstd, lax.all_gather(rounded, "tp", axis=0, tiled=True))


def norm_back(d_normed, normed, rstd, gain, width):
    g_gain = jnp.sum(d_normed * normed, 1)
    g_bias = jnp.sum(d_normed, 1)
    scaled = d_normed * gain[:, None]
    first, second = lax.psum((jnp.sum(scaled, 0), jnp.sum(scaled * normed, 0)), "tp")
    back = rstd[None, :] * (scaled - first[None, :] / width - normed * second[None, :] / width)
    return (back, g_gain, g_bias)


def reduce_back(term, local_width):
    return lax.psum_scatter(
        term(jnp.int32(0), lax.axis_size("tp") * local_width).astype(jnp.bfloat16),
        "tp",
        scatter_dimension=0,
        tiled=True,
    ).astype(jnp.float32)


def fold_back(shard, pairs):
    piece = lax.all_gather(shard, "tp", axis=0, tiled=True)
    new_acts = tuple(
        (
            jnp.einsum("fc,ct->ft", weight, piece, preferred_element_type=jnp.float32)
            for weight, acts in pairs
        )
    )
    new_weights = tuple(
        (
            jnp.einsum("ft,ct->fc", acts, piece, preferred_element_type=jnp.float32)
            for weight, acts in pairs
        )
    )
    return (new_acts, new_weights)


def split_heads(flat, heads_here):
    pair_count = flat.shape[1] // (2 * SEQ)
    shaped = flat.reshape(heads_here, HEAD, pair_count, 2, SEQ)
    return jnp.moveaxis(shaped, 2, 0)


def join_heads(blocks):
    moved = jnp.moveaxis(blocks, 0, 2)
    return moved.reshape(moved.shape[0] * moved.shape[1], -1)


def attend(block):
    query_rows, key_rows, value_rows = block
    scale = 1.0 / math.sqrt(HEAD)
    scores = (
        jnp.einsum("hdbi,hdbj->hbij", query_rows, key_rows, preferred_element_type=jnp.float32)
        * scale
    )
    peak = jnp.max(scores, axis=-1, keepdims=True)
    logsum = peak + jnp.log(jnp.sum(jnp.exp(scores - peak), axis=-1, keepdims=True))
    probs = jnp.exp(scores - logsum).astype(jnp.bfloat16)
    attended = jnp.einsum("hbij,hdbj->hdbi", probs, value_rows, preferred_element_type=jnp.float32)
    return (attended.astype(jnp.bfloat16), logsum[..., 0])


def attend_back(block):
    query_rows, key_rows, value_rows, logsum, d_attended = block
    scale = 1.0 / math.sqrt(HEAD)
    scores = (
        jnp.einsum("hdbi,hdbj->hbij", query_rows, key_rows, preferred_element_type=jnp.float32)
        * scale
    )
    probs = jnp.exp(scores - logsum[..., None])
    probs_low = probs.astype(jnp.bfloat16)
    d_probs = jnp.einsum(
        "hdbi,hdbj->hbij", d_attended, value_rows, preferred_element_type=jnp.float32
    )
    delta = jnp.sum(probs * d_probs, axis=-1, keepdims=True)
    d_scores = (probs * (d_probs - delta)).astype(jnp.bfloat16)
    d_query = (
        jnp.einsum("hbij,hdbj->hdbi", d_scores, key_rows, preferred_element_type=jnp.float32)
        * scale
    )
    d_key = (
        jnp.einsum("hbij,hdbi->hdbj", d_scores, query_rows, preferred_element_type=jnp.float32)
        * scale
    )
    d_value = jnp.einsum(
        "hbij,hdbi->hdbj", probs_low, d_attended, preferred_element_type=jnp.float32
    )
    return (d_query.astype(jnp.bfloat16), d_key.astype(jnp.bfloat16), d_value.astype(jnp.bfloat16))


def body_features(
    main,
    long_skip,
    cotangent,
    timesteps,
    loss_codes,
    code_weights,
    item_counts,
    w_skip_main,
    w_skip_long,
    b_skip,
    ln1_gain,
    ln1_bias,
    w_qkv,
    w_proj,
    b_proj,
    ln2_gain,
    ln2_bias,
    w_up,
    b_up,
    w_down,
    b_down,
):
    local_width = main.shape[1]
    width = w_skip_main.shape[1]
    heads_here = local_width // HEAD
    item_scale, valid = item_factors(timesteps, loss_codes, code_weights, item_counts[0])
    row_scale = jnp.repeat(item_scale, SEQ)
    row_valid = jnp.repeat(valid, SEQ)
    main_cols = main.T
    long_cols = long_skip.T
    stream = (
        lax.psum_scatter(
            jnp.einsum("dc,dt->ct", w_skip_main, main_cols, preferred_element_type=jnp.float32)
            + jnp.einsum("dc,dt->ct", w_skip_long, long_cols, preferred_element_type=jnp.float32),
            "tp",
            scatter_dimension=0,
            tiled=True,
        )
        + b_skip[:, None]
    )
    normed_one, rstd_one, full_one = layer_norm(stream, ln1_gain, ln1_bias, width)
    qkv = jnp.einsum("edc,dt->ect", w_qkv, full_one, preferred_element_type=jnp.float32).astype(
        jnp.bfloat16
    )
    query_blocks = split_heads(qkv[0], heads_here)
    key_blocks = split_heads(qkv[1], heads_here)
    value_blocks = split_heads(qkv[2], heads_here)
    attended_blocks, logsums = lax.map(attend, (query_blocks, key_blocks, value_blocks))
    attended = join_heads(attended_blocks)
    cols_here = w_proj
    projected = lax.psum_scatter(
        jnp.einsum("rc,rt->ct", cols_here, attended, preferred_element_type=jnp.float32).astype(
            jnp.bfloat16
        ),
        "tp",
        scatter_dimension=0,
        tiled=True,
    ).astype(jnp.float32)
    stream_two = stream + projected + b_proj[:, None]
    normed_two, rstd_two, full_two = layer_norm(stream_two, ln2_gain, ln2_bias, width)
    upward = (
        jnp.einsum("dc,dt->ct", w_up, full_two, preferred_element_type=jnp.float32) + b_up[:, None]
    )
    activated = jax.nn.gelu(upward, approximate=False).astype(jnp.bfloat16)
    cols_here = w_down
    result = (
        stream_two
        + lax.psum_scatter(
            jnp.einsum(
                "fc,ft->ct", cols_here, activated, preferred_element_type=jnp.float32
            ).astype(jnp.bfloat16),
            "tp",
            scatter_dimension=0,
            tiled=True,
        ).astype(jnp.float32)
        + b_down[:, None]
    )
    out = (result * row_valid[None, :]).T.astype(jnp.bfloat16)
    grad_low = (cotangent.T.astype(jnp.float32) * row_scale[None, :]).astype(jnp.bfloat16)
    grad_wide = grad_low.astype(jnp.float32)
    g_b_down = jnp.sum(grad_wide, 1)
    (d_activated,), (g_w_down,) = fold_back(grad_low, ((w_down, activated),))
    cumulative = 0.5 * (1.0 + lax.erf(upward * ROOT_HALF))
    density = jnp.exp(-0.5 * upward * upward) * DENSITY_SCALE
    d_upward = (d_activated * (cumulative + upward * density)).astype(jnp.bfloat16)
    g_b_up = jnp.sum(d_upward.astype(jnp.float32), 1)
    g_w_up = jnp.einsum("dt,ft->df", full_two, d_upward, preferred_element_type=jnp.float32)

    def up_term(start, count_rows):
        return jnp.einsum("cf,ft->ct", w_up, d_upward, preferred_element_type=jnp.float32)

    d_normed_two = reduce_back(up_term, local_width)
    back_two, g_ln2_gain, g_ln2_bias = norm_back(
        d_normed_two, normed_two, rstd_two, ln2_gain, width
    )
    d_stream_two = (back_two + grad_wide).astype(jnp.bfloat16)
    d_stream_wide = d_stream_two.astype(jnp.float32)
    g_b_proj = jnp.sum(d_stream_wide, 1)
    (d_attended,), (g_w_proj,) = fold_back(d_stream_two, ((w_proj, attended),))
    d_attended_blocks = split_heads(d_attended.astype(jnp.bfloat16), heads_here)
    d_queries, d_keys, d_values = lax.map(
        attend_back, (query_blocks, key_blocks, value_blocks, logsums, d_attended_blocks)
    )
    d_qkv = jnp.stack([join_heads(d_queries), join_heads(d_keys), join_heads(d_values)], axis=0)
    g_w_qkv = jnp.einsum("dt,ect->edc", full_one, d_qkv, preferred_element_type=jnp.float32)

    def qkv_term(start, count_rows):
        return jnp.einsum("ecr,ert->ct", w_qkv, d_qkv, preferred_element_type=jnp.float32)

    d_normed_one = reduce_back(qkv_term, local_width)
    back_one, g_ln1_gain, g_ln1_bias = norm_back(
        d_normed_one, normed_one, rstd_one, ln1_gain, width
    )
    d_stream = (back_one + d_stream_wide).astype(jnp.bfloat16)
    g_b_skip = jnp.sum(d_stream.astype(jnp.float32), 1)
    (d_main_cols, d_long_cols), (g_w_main, g_w_long) = fold_back(
        d_stream, ((w_skip_main, main_cols), (w_skip_long, long_cols))
    )
    (
        g_w_main,
        g_w_long,
        g_b_skip,
        g_ln1_gain,
        g_ln1_bias,
        g_w_qkv,
        g_w_proj,
        g_b_proj,
        g_ln2_gain,
        g_ln2_bias,
        g_w_up,
        g_b_up,
        g_w_down,
        g_b_down,
    ) = (
        lax.psum(g_w_main.astype(jnp.bfloat16), "dp").astype(jnp.float32),
        lax.psum(g_w_long.astype(jnp.bfloat16), "dp").astype(jnp.float32),
        lax.psum(g_b_skip.astype(jnp.bfloat16), "dp").astype(jnp.float32),
        lax.psum(g_ln1_gain.astype(jnp.bfloat16), "dp").astype(jnp.float32),
        lax.psum(g_ln1_bias.astype(jnp.bfloat16), "dp").astype(jnp.float32),
        lax.psum(g_w_qkv.astype(jnp.bfloat16), "dp").astype(jnp.float32),
        lax.psum(g_w_proj.astype(jnp.bfloat16), "dp").astype(jnp.float32),
        lax.psum(g_b_proj.astype(jnp.bfloat16), "dp").astype(jnp.float32),
        lax.psum(g_ln2_gain.astype(jnp.bfloat16), "dp").astype(jnp.float32),
        lax.psum(g_ln2_bias.astype(jnp.bfloat16), "dp").astype(jnp.float32),
        lax.psum(g_w_up.astype(jnp.bfloat16), "dp").astype(jnp.float32),
        lax.psum(g_b_up.astype(jnp.bfloat16), "dp").astype(jnp.float32),
        lax.psum(g_w_down.astype(jnp.bfloat16), "dp").astype(jnp.float32),
        lax.psum(g_b_down.astype(jnp.bfloat16), "dp").astype(jnp.float32),
    )
    d_main = d_main_cols.T.astype(jnp.bfloat16)
    d_long = d_long_cols.T.astype(jnp.bfloat16)
    return (
        out,
        d_main,
        d_long,
        g_w_main,
        g_w_long,
        g_b_skip,
        g_ln1_gain,
        g_ln1_bias,
        g_w_qkv,
        g_w_proj,
        g_b_proj,
        g_ln2_gain,
        g_ln2_bias,
        g_w_up,
        g_b_up,
        g_w_down,
        g_b_down,
    )


ITEM_ROWS = 264
GRAD_ROWS = 24
CORE = ("tp", 1)
ACROSS_Y = ("tp", 2)
ACROSS_X = ("dp", 1)
ACROSS_Z = ("dp", 2)


def swap(value, link):
    axis, bit = link
    return lax.ppermute(value, axis, [(i, i ^ bit) for i in range(lax.axis_size(axis))])


def side(link):
    axis, bit = link
    return (lax.axis_index(axis) // bit) % 2


def in_order(bit, mine, theirs):
    flip = bit == 1
    return jnp.stack([jnp.where(flip, theirs, mine), jnp.where(flip, mine, theirs)])


def pick(value, index):
    return lax.dynamic_index_in_dim(value, index, 0, keepdims=False)


def peer(value, bit):
    return value + bit - 2 * bit * ((value // bit) % 2)


def greet(peers):
    barrier = pltpu.get_barrier_semaphore()
    for where in peers:
        pl.semaphore_signal(barrier, inc=1, device_id=where, device_id_type=pl.DeviceIdType.MESH)
    pl.semaphore_wait(barrier, len(peers))


def send(source, target, sems, index, where):
    return pltpu.make_async_remote_copy(
        src_ref=source,
        dst_ref=target,
        send_sem=sems.at[0, index],
        recv_sem=sems.at[1, index],
        device_id=where,
        device_id_type=pl.DeviceIdType.MESH,
    )


def gather_kernel(pieces, n_in, n_out, *refs):
    tokens, vectors, inputs = refs[0], refs[1], refs[2 : 2 + n_in]
    refs = refs[2 + n_in :]
    far_tokens, core_near, core_far, far_vectors, core_vectors = refs[:5]
    outs, held = refs[5 : 5 + n_out], refs[5 + n_out : 5 + n_out + n_in]
    y_sem, one_sem, two_sem, own_sem, far_sem, local_sem, token_sem = refs[5 + n_out + n_in :]
    n = len(pieces)
    shards = [inputs[a].at[lead] if lead else inputs[a] for a, lead, _, _ in pieces]
    stage = [held[a].at[lead] if lead else held[a] for a, lead, _, _ in pieces]
    fulls = [
        [outs[b[place]].at[tail] if isinstance(b, tuple) else outs[b].at[(place,) + tail] for place in range(4)]
        for _, _, b, tail in pieces
    ]
    dp, tp = lax.axis_index("dp"), lax.axis_index("tp")
    core, y = tp % 2, (tp // 2) % 2
    to_core, to_y = {"tp": peer(tp, 1)}, {"tp": peer(tp, 2)}
    links = ({"dp": peer(dp, 1)}, {"dp": peer(dp, 2)})
    bits = (dp % 2, (dp // 2) % 2)
    greet((to_core, to_y) + links)

    def places(k):
        return k % 2, 1 - k % 2, bits[k % 2], bits[1 - k % 2]

    def y_copy(k):
        _, _, f, s = places(k)
        return send(shards[k].at[s, f], fulls[k][1].at[s, f], y_sem, k, to_y)

    def one_copy(k):
        first, _, f, s = places(k)
        part = fulls[k][1].at[s, f]
        return send(part, part, one_sem, k, links[first])

    def two_copy(k):
        _, second, _, s = places(k)
        part = fulls[k][1].at[s]
        return send(part, part, two_sem, k, links[second])

    def own_copy(k):
        return send(shards[k], fulls[k][2], own_sem, k, to_core)

    def far_copy(k):
        return send(fulls[k][1], fulls[k][3], far_sem, k, to_core)

    def load(k):
        return pltpu.make_async_copy(shards[k], stage[k], local_sem.at[0, k])

    def store(k):
        return pltpu.make_async_copy(stage[k], fulls[k][0], local_sem.at[1, k])

    token_y = send(tokens.at[1 - y], far_tokens, token_sem, 0, to_y)
    token_near = send(tokens.at[y, 1 - core], core_near, token_sem, 1, to_core)
    token_far = send(far_tokens.at[1 - core], core_far, token_sem, 2, to_core)
    vectors_y = send(vectors, far_vectors, token_sem, 3, to_y)
    vectors_near = send(vectors, core_vectors.at[0], token_sem, 4, to_core)
    vectors_far = send(far_vectors, core_vectors.at[1], token_sem, 5, to_core)
    vectors_y.start()
    vectors_near.start()
    for k in range(n):
        y_copy(k).start()
    token_y.start()
    token_near.start()
    for k in range(n):
        load(k).start()
        own_copy(k).start()
    for step in range(n + 2):
        if step < n:
            y_copy(step).wait_recv()
            one_copy(step).start()
            load(step).wait()
            store(step).start()
        if 0 <= step - 1 < n:
            one_copy(step - 1).wait_recv()
            two_copy(step - 1).start()
        if 0 <= step - 2 < n:
            two_copy(step - 2).wait_recv()
            far_copy(step - 2).start()
    vectors_y.wait_recv()
    vectors_far.start()
    token_y.wait_recv()
    token_far.start()
    for copy in (token_near, token_far, vectors_near, vectors_far):
        copy.wait()
    token_y.wait_send()
    vectors_y.wait_send()
    for k in range(n):
        far_copy(k).wait()
        own_copy(k).wait()
        store(k).wait()
        for copy in (y_copy(k), one_copy(k), two_copy(k)):
            copy.wait_send()


def gather_weights(tokens, vectors, arrays, pieces, out_shapes):
    n = len(pieces)
    shape = lambda dims, like: jax.ShapeDtypeStruct(dims, like.dtype)
    rows = tokens.shape[2:]
    outs = [shape((2,) + rows, tokens), shape(rows, tokens), shape(rows, tokens)]
    outs += [shape(vectors.shape, vectors), shape((2,) + vectors.shape, vectors)]
    outs += [shape(dims, arrays[0]) for dims in out_shapes]
    sems = [pltpu.SemaphoreType.DMA((2, n))] * 6 + [pltpu.SemaphoreType.DMA((2, 6))]
    return pl.pallas_call(
        functools.partial(gather_kernel, pieces, len(arrays), len(out_shapes)),
        out_shape=outs,
        in_specs=[pl.BlockSpec(memory_space=pltpu.MemorySpace.HBM)] * (2 + len(arrays)),
        out_specs=[pl.BlockSpec(memory_space=pltpu.MemorySpace.HBM)] * len(outs),
        scratch_shapes=[pltpu.VMEM(a.shape, a.dtype) for a in arrays] + sems,
        compiler_params=pltpu.CompilerParams(
            collective_id=1, has_side_effects=True, vmem_limit_bytes=32 * 2**20
        ),
        name="gather_weights",
    )(tokens, vectors, *arrays)


def reduce_kernel(sizes, views, n_arrays, *refs):
    ready, arrays, blocks, quarter = refs[0], refs[1 : 1 + n_arrays], refs[1 + n_arrays], refs[2 + n_arrays]
    refs = refs[3 + n_arrays :]
    outs, refs = refs[: 1 + len(views)], refs[1 + len(views) :]
    from_core, y_blocks, own_quarter, z_quarter, x_quarters = refs[:5]
    total, from_y, from_one, half, from_two, from_far, final, part, far_part = refs[5:14]
    y_sem, one_sem, two_sem, far_sem, back_two, back_one, block_sem, load_sem, out_sem = refs[14:]
    chunks, n_ready = total.shape[0], sizes[0]
    dp, tp = lax.axis_index("dp"), lax.axis_index("tp")
    to_core, to_y, to_far = {"tp": peer(tp, 1)}, {"tp": peer(tp, 2)}, {"dp": peer(dp, 4)}
    to_x, to_z = {"dp": peer(dp, 1)}, {"dp": peer(dp, 2)}
    greet((to_core, to_y, to_x, to_z, to_far))

    def plan(s):
        z_first = (s % 4) // 3
        first, second = 1 + z_first, 2 - z_first
        places = (dp // first) % 2, (dp // second) % 2
        return ({"dp": peer(dp, first)}, {"dp": peer(dp, second)}) + places

    def y_copy(s, source):
        return send(source, from_y.at[s - n_ready], y_sem, s - n_ready, to_y)

    def one_copy(s):
        to_one, _, f, _ = plan(s)
        return send(total.at[s, 1 - f], from_one.at[s], one_sem, s, to_one)

    def two_copy(s):
        _, to_two, _, g = plan(s)
        return send(half.at[s, 1 - g], from_two.at[s], two_sem, s, to_two)

    def far_copy(s):
        _, _, _, g = plan(s)
        return send(half.at[s, g], from_far.at[s], far_sem, s, to_far)

    def back_two_copy(s):
        _, to_two, f, g = plan(s)
        part = final.at[s, f, g]
        return send(part, part, back_two, s, to_two)

    def back_one_copy(s):
        to_one, _, f, _ = plan(s)
        part = final.at[s, f]
        return send(part, part, back_one, s, to_one)

    def out_copies(s, act):
        at = 0
        for k, size in enumerate(sizes):

            @pl.when((s >= at) & (s < at + size))
            def _(k=k, at=at):
                act(pltpu.make_async_copy(final.at[s], outs[k].at[s - at], out_sem.at[s]))

            at += size

    quarter_load = pltpu.make_async_copy(quarter, part, load_sem.at[0])
    ready_load = pltpu.make_async_copy(ready, total.at[pl.ds(0, n_ready)], load_sem.at[1])
    ready_load.start()
    quarter_load.start()
    core_blocks = [send(blocks.at[2 + k], from_core.at[k], block_sem, k, to_core) for k in range(2)]
    own_block = send(blocks.at[1], y_blocks.at[0], block_sem, 2, to_y)
    core_block = send(from_core.at[1], y_blocks.at[1], block_sem, 3, to_y)
    quarter_far = send(quarter, far_part, block_sem, 4, to_far)
    quarter_z = send(own_quarter, z_quarter, block_sem, 5, to_z)
    quarter_x = send(own_quarter, x_quarters.at[0], block_sem, 6, to_x)
    quarter_zx = send(z_quarter, x_quarters.at[1], block_sem, 7, to_x)
    quarter_out = pltpu.make_async_copy(part, own_quarter, out_sem.at[chunks])
    loads, at = [], n_ready
    for k, (size, (a, mine, theirs)) in enumerate(zip(sizes[1:], views)):
        source = arrays[a].at[mine]
        loads.append(pltpu.make_async_copy(source, total.at[pl.ds(at, size)], load_sem.at[2 + k]))
        loads[-1].start()
        for r in range(size):
            y_copy(at + r, arrays[a].at[theirs + (r,)]).start()
        at += size
    for copy in core_blocks:
        copy.start()
    own_block.start()
    quarter_far.start()
    for copy in [ready_load, quarter_load] + loads:
        copy.wait()

    def plus(left, right):
        return (left.astype(jnp.float32) + right.astype(jnp.float32)).astype(jnp.bfloat16)

    def step(t, carry):
        @pl.when((t >= n_ready) & (t < chunks))
        def _():
            y_copy(t, total.at[t]).wait_recv()
            total[t] = plus(total[t], from_y[t - n_ready])

        @pl.when(t < chunks)
        def _():
            one_copy(t).start()

        @pl.when((t >= 2) & (t < chunks + 2))
        def _():
            s = t - 2
            _, _, f, _ = plan(s)
            one_copy(s).wait_recv()
            half[s] = plus(total[s, f], from_one[s])
            two_copy(s).start()

        @pl.when((t >= 3) & (t < chunks + 3))
        def _():
            s = t - 3
            _, _, _, g = plan(s)
            two_copy(s).wait_recv()
            half[s, g] = plus(half[s, g], from_two[s])
            far_copy(s).start()

        @pl.when((t >= 5) & (t < chunks + 5))
        def _():
            s = t - 5
            _, _, f, g = plan(s)
            far_copy(s).wait_recv()
            final[s, f, g] = plus(half[s, g], from_far[s])
            back_two_copy(s).start()

        @pl.when((t >= 6) & (t < chunks + 6))
        def _():
            back_two_copy(t - 6).wait_recv()
            back_one_copy(t - 6).start()

        @pl.when((t >= 7) & (t < chunks + 7))
        def _():
            back_one_copy(t - 7).wait_recv()
            out_copies(t - 7, lambda copy: copy.start())

        @pl.when(t == 2)
        def _():
            for copy in core_blocks:
                copy.wait_recv()
            core_block.start()

        @pl.when(t == 8)
        def _():
            quarter_far.wait()
            part[...] = plus(part[...], far_part[...])
            quarter_out.start()

        @pl.when(t == 9)
        def _():
            quarter_out.wait()
            quarter_z.start()
            quarter_x.start()

        @pl.when(t == 18)
        def _():
            quarter_z.wait_recv()
            quarter_zx.start()

        return carry

    lax.fori_loop(0, chunks + 7, step, 0)

    def finish_y(s, carry):
        y_copy(s, total.at[s]).wait_send()
        return carry

    lax.fori_loop(n_ready, chunks, finish_y, 0)

    def finish(s, carry):
        for copy in (one_copy(s), two_copy(s), far_copy(s), back_two_copy(s), back_one_copy(s)):
            copy.wait_send()
        out_copies(s, lambda copy: copy.wait())
        return carry

    lax.fori_loop(0, chunks, finish, 0)
    for copy in core_blocks:
        copy.wait_send()
    own_block.wait()
    core_block.wait()
    quarter_z.wait_send()
    quarter_x.wait()
    quarter_zx.wait()


def reduce_grads(ready, arrays, views, blocks, quarter):
    sizes = (ready.shape[0],) + tuple(arrays[a].shape[len(mine)] for a, mine, _ in views)
    chunks = sum(sizes)
    rows, width = ready.shape[-2:]
    kind = ready.dtype
    sem = lambda n: pltpu.SemaphoreType.DMA((2, n))
    two_blocks = jax.ShapeDtypeStruct((2,) + blocks.shape[1:], blocks.dtype)
    hbm = pl.BlockSpec(memory_space=pltpu.MemorySpace.HBM)
    vmem = lambda *lead: pltpu.VMEM(lead + (rows, width), kind)
    n_in, n_out = 3 + len(arrays), 6 + len(views)
    return pl.pallas_call(
        functools.partial(reduce_kernel, sizes, views, len(arrays)),
        out_shape=[jax.ShapeDtypeStruct((n, 2, 2, rows, width), kind) for n in sizes]
        + [two_blocks, two_blocks]
        + [jax.ShapeDtypeStruct(lead + quarter.shape, kind) for lead in ((), (), (2,))],
        in_specs=[hbm] * n_in,
        out_specs=[hbm] * n_out,
        scratch_shapes=[
            vmem(chunks, 2, 2),
            vmem(chunks - sizes[0], 2, 2),
            vmem(chunks, 2),
            vmem(chunks, 2),
            vmem(chunks),
            vmem(chunks),
            vmem(chunks, 2, 2),
            pltpu.VMEM(quarter.shape, kind),
            pltpu.VMEM(quarter.shape, kind),
            sem(chunks - sizes[0]),
            sem(chunks),
            sem(chunks),
            sem(chunks),
            sem(chunks),
            sem(chunks),
            sem(8),
            pltpu.SemaphoreType.DMA((2 + len(views),)),
            pltpu.SemaphoreType.DMA((chunks + 1,)),
        ],
        compiler_params=pltpu.CompilerParams(
            collective_id=2, has_side_effects=True, vmem_limit_bytes=56 * 2**20
        ),
        name="reduce_grads",
    )(ready, *arrays, blocks, quarter)


def add_low(mine, theirs):
    return (mine.astype(jnp.float32) + theirs.astype(jnp.float32)).astype(jnp.bfloat16)


def place_of(index):
    rank = lax.axis_index("tp")
    core, y = rank % 2, (rank // 2) % 2
    there_core, there_y = index % 2, index // 2
    apart = lambda a, b: a + b - 2 * a * b
    return apart(y, there_y) + 2 * apart(core, there_core)


def spread_kernel(main_ref, long_ref, cot_ref, tokens_ref, cot_tokens_ref):
    cols = main_ref.shape[1]
    items = tokens_ref.shape[1] // ITEM_ROWS
    for p in range(4):
        for i in range(items):
            source = slice((p * items + i) * SEQ, (p * items + i + 1) * SEQ)
            target = slice(i * ITEM_ROWS, i * ITEM_ROWS + SEQ)
            blank = slice(i * ITEM_ROWS + SEQ, (i + 1) * ITEM_ROWS)
            tokens_ref[p, target, :cols] = main_ref[source, :]
            tokens_ref[p, target, cols:] = long_ref[source, :]
            cot_tokens_ref[p, target, :] = cot_ref[source, :]
            tokens_ref[p, blank, :] = jnp.zeros((ITEM_ROWS - SEQ, 2 * cols), tokens_ref.dtype)
            cot_tokens_ref[p, blank, :] = jnp.zeros((ITEM_ROWS - SEQ, cols), tokens_ref.dtype)


def spread(main, long_skip, cotangent):
    rows, cols = main.shape
    padded = rows // SEQ // 4 * ITEM_ROWS
    return pl.pallas_call(
        spread_kernel,
        out_shape=[
            jax.ShapeDtypeStruct((4, padded, 2 * cols), main.dtype),
            jax.ShapeDtypeStruct((4, padded, cols), main.dtype),
        ],
        compiler_params=pltpu.CompilerParams(vmem_limit_bytes=40 * 2**20),
        name="spread",
    )(main, long_skip, cotangent)


def arrange_kernel(own_ref, y_ref, partner_ref, scale_ref, out_ref, held):
    cols = own_ref.shape[1]
    held[0] = own_ref[...]
    held[1] = y_ref[...]
    held[2] = partner_ref[0]
    held[3] = partner_ref[1]
    for j in range(4):
        block = held[place_of(j)].astype(jnp.float32) * scale_ref[...]
        out_ref[:, j * cols : (j + 1) * cols] = block.astype(out_ref.dtype)


def arrange(own, along_y, partner, scale):
    rows, cols = own.shape
    return pl.pallas_call(
        arrange_kernel,
        out_shape=jax.ShapeDtypeStruct((rows, 4 * cols), own.dtype),
        scratch_shapes=[pltpu.VMEM((4, rows, cols), own.dtype)],
        compiler_params=pltpu.CompilerParams(vmem_limit_bytes=24 * 2**20),
        name="arrange",
    )(own, along_y, partner, scale)


def disperse_kernel(rows_ref, valid_ref, out_ref):
    cols = out_ref.shape[2]
    for j in range(4):
        block = rows_ref[:, j * cols : (j + 1) * cols] * valid_ref[...]
        out_ref[place_of(j)] = block.astype(out_ref.dtype)


def disperse(rows, valid):
    count, width = rows.shape
    return pl.pallas_call(
        disperse_kernel,
        out_shape=jax.ShapeDtypeStruct((4, count, width // 4), jnp.bfloat16),
        compiler_params=pltpu.CompilerParams(vmem_limit_bytes=24 * 2**20),
        name="disperse",
    )(rows, valid)


def unspread_kernel(parts, own_ref, core_ref, y_ref, *refs):
    outs, held = refs[:parts], refs[parts]
    cols = outs[0].shape[1]
    items = own_ref.shape[0] // ITEM_ROWS
    held[0] = own_ref[...]
    held[1] = y_ref[0]
    held[2] = core_ref[...]
    held[3] = y_ref[1]
    for p in range(4):
        rows = held[place_of(p)]
        for i in range(items):
            target = slice((p * items + i) * SEQ, (p * items + i + 1) * SEQ)
            source = slice(i * ITEM_ROWS, i * ITEM_ROWS + SEQ)
            for k in range(parts):
                outs[k][target, :] = rows[source, k * cols : (k + 1) * cols]


def unspread(own, core_tokens, y_tokens, parts):
    rows, width = own.shape
    out = jax.ShapeDtypeStruct((4 * rows // ITEM_ROWS * SEQ, width // parts), own.dtype)
    return pl.pallas_call(
        functools.partial(unspread_kernel, parts),
        out_shape=[out] * parts,
        scratch_shapes=[pltpu.VMEM((4, rows, width), own.dtype)],
        compiler_params=pltpu.CompilerParams(vmem_limit_bytes=40 * 2**20),
        name="unspread",
    )(own, core_tokens, y_tokens)


def natural(own_half, partner_half, axis):
    flip_y, flip_core = side(ACROSS_Y) == 1, side(CORE) == 1
    r0, r2 = jnp.split(own_half, 2, axis)
    r1, r3 = jnp.split(partner_half, 2, axis)
    a0, a2 = jnp.where(flip_y, r2, r0), jnp.where(flip_y, r0, r2)
    a1, a3 = jnp.where(flip_y, r3, r1), jnp.where(flip_y, r1, r3)
    b0, b1 = jnp.where(flip_core, a1, a0), jnp.where(flip_core, a0, a1)
    b2, b3 = jnp.where(flip_core, a3, a2), jnp.where(flip_core, a2, a3)
    return (b0, b1, b2, b3)


def dot(spec, left, right):
    return jnp.einsum(spec, left, right, preferred_element_type=jnp.float32)


def low(value):
    return value.astype(jnp.bfloat16)


def norm_rows(stream, gain, bias):
    mean = jnp.mean(stream, 1, keepdims=True)
    square = jnp.mean(stream * stream, 1, keepdims=True)
    rstd = lax.rsqrt(square - mean * mean + EPSILON)
    normed = (stream - mean) * rstd
    return normed, rstd, low(normed * gain + bias)


def norm_rows_back(d_out, normed, rstd, gain):
    g_gain = jnp.sum(d_out * normed, 0)
    g_bias = jnp.sum(d_out, 0)
    scaled = d_out * gain
    first = jnp.mean(scaled, 1, keepdims=True)
    second = jnp.mean(scaled * normed, 1, keepdims=True)
    return rstd * (scaled - first - normed * second), g_gain, g_bias


LAST = (((1,), (1,)), ((), ()))
LEAD = (((0,), (0,)), ((), ()))


def item_scores(key, query):
    scores = lax.dot_general(key, query, LAST, preferred_element_type=jnp.float32)
    present = lax.broadcasted_iota(jnp.int32, scores.shape, 0) < SEQ
    return jnp.where(present, scores * (1.0 / math.sqrt(HEAD)), -1e30)


def attend_kernel(*refs):
    def item(i, carry):
        attend_item(*(ref.at[i] for ref in refs))
        return carry

    lax.fori_loop(0, refs[0].shape[0], item, 0)


def attend_item(q_ref, k_ref, v_ref, out_ref, lse_ref):
    for h in range(q_ref.shape[1] // HEAD):
        at = slice(h * HEAD, (h + 1) * HEAD)
        scores = item_scores(k_ref[:, at], q_ref[:, at])
        peak = jnp.max(scores, axis=0, keepdims=True)
        weights = jnp.exp(scores - peak)
        total = jnp.sum(weights, axis=0, keepdims=True)
        probs = (weights * (1.0 / total)).astype(jnp.bfloat16)
        out = lax.dot_general(probs, v_ref[:, at], LEAD, preferred_element_type=jnp.float32)
        out_ref[:, at] = out.astype(jnp.bfloat16)
        lse_ref[h : h + 1, :] = peak + jnp.log(total)


def attend_back_kernel(*refs):
    def item(i, carry):
        attend_back_item(*(ref.at[i] for ref in refs))
        return carry

    lax.fori_loop(0, refs[0].shape[0], item, 0)


def attend_back_item(q_ref, k_ref, v_ref, lse_ref, d_ref, dq_ref, dk_ref, dv_ref, own_ref, partner_ref):
    scale = 1.0 / math.sqrt(HEAD)
    for h in range(q_ref.shape[1] // HEAD):
        at = slice(h * HEAD, (h + 1) * HEAD)
        query, key, d_out = q_ref[:, at], k_ref[:, at], d_ref[:, at]
        probs = jnp.exp(item_scores(key, query) - lse_ref[h : h + 1, :])
        d_probs = lax.dot_general(v_ref[:, at], d_out, LAST, preferred_element_type=jnp.float32)
        delta = jnp.sum(probs * d_probs, axis=0, keepdims=True)
        d_scores = (probs * (d_probs - delta)).astype(jnp.bfloat16)
        dq = lax.dot_general(d_scores, key, LEAD, preferred_element_type=jnp.float32)
        dk = jnp.dot(d_scores, query, preferred_element_type=jnp.float32)
        dv = jnp.dot(probs.astype(jnp.bfloat16), d_out, preferred_element_type=jnp.float32)
        cols = q_ref.shape[1] // 2
        side_ref, start = (own_ref, h * HEAD) if h * HEAD < cols else (partner_ref, h * HEAD - cols)
        for e, (ref, d) in enumerate(((dq_ref, dq * scale), (dk_ref, dk * scale), (dv_ref, dv))):
            d = d.astype(jnp.bfloat16)
            ref[:, at] = d
            side_ref[:, e * cols + start : e * cols + start + HEAD] = d


def by_item(value):
    return value.reshape(-1, ITEM_ROWS, value.shape[1])


def attention(query, key, value):
    rows, cols = query.shape
    heads, items = cols // HEAD, rows // ITEM_ROWS
    out, lse = pl.pallas_call(
        attend_kernel,
        out_shape=[
            jax.ShapeDtypeStruct((items, ITEM_ROWS, cols), jnp.bfloat16),
            jax.ShapeDtypeStruct((items, heads, ITEM_ROWS), jnp.float32),
        ],
        cost_estimate=pl.CostEstimate(
            flops=4 * rows * ITEM_ROWS * cols, bytes_accessed=8 * rows * cols, transcendentals=rows * ITEM_ROWS * heads
        ),
        compiler_params=pltpu.CompilerParams(vmem_limit_bytes=24 * 2**20),
        name="attend",
    )(by_item(query), by_item(key), by_item(value))
    return out.reshape(rows, cols), lse


def attention_back(query, key, value, lse, d_out):
    rows, cols = query.shape
    heads, items = cols // HEAD, rows // ITEM_ROWS
    shape = lambda width: jax.ShapeDtypeStruct((items, ITEM_ROWS, width), jnp.bfloat16)
    outs = pl.pallas_call(
        attend_back_kernel,
        out_shape=[shape(cols)] * 3 + [shape(3 * cols // 2)] * 2,
        cost_estimate=pl.CostEstimate(
            flops=10 * rows * ITEM_ROWS * cols, bytes_accessed=14 * rows * cols, transcendentals=rows * ITEM_ROWS * heads
        ),
        compiler_params=pltpu.CompilerParams(vmem_limit_bytes=32 * 2**20),
        name="attend_back",
    )(by_item(query), by_item(key), by_item(value), lse, by_item(d_out))
    return [o.reshape(rows, -1) for o in outs]


HIDDEN_BLOCK = 384


def feed_kernel(first, n_ref, g_ref, up_ref, bias_ref, down_ref, *refs):
    sums, (act_ref, d_up_ref, g_bias_ref, result_ref, d_n_ref) = refs[:-5], refs[-5:]
    wide = jnp.float32

    @pl.when(pl.program_id(0) == 0)
    def _():
        result_ref[...] = sums[0][...]
        d_n_ref[...] = jnp.zeros_like(d_n_ref) if first else sums[1][...]

    up = jnp.dot(n_ref[...], up_ref[...], preferred_element_type=wide) + bias_ref[...]
    d_act = lax.dot_general(g_ref[...], down_ref[...], LAST, preferred_element_type=wide)
    cumulative = 0.5 * (1.0 + lax.erf(up * ROOT_HALF))
    density = jnp.exp(-0.5 * up * up) * DENSITY_SCALE
    act = (up * cumulative).astype(jnp.bfloat16)
    d_up = (d_act * (cumulative + up * density)).astype(jnp.bfloat16)
    act_ref[...] = act
    d_up_ref[...] = d_up
    g_bias_ref[...] = jnp.sum(d_up.astype(wide), axis=0, keepdims=True)
    result_ref[...] += jnp.dot(act, down_ref[...], preferred_element_type=wide)
    d_n_ref[...] += lax.dot_general(d_up, up_ref[...], LAST, preferred_element_type=wide)


def feed(n, g, up, bias, down, result, d_n):
    rows, width = n.shape
    hidden = up.shape[1]
    whole = pl.BlockSpec((rows, width), lambda i: (0, 0))
    across = pl.BlockSpec((rows, HIDDEN_BLOCK), lambda i: (0, i))
    line = pl.BlockSpec((1, HIDDEN_BLOCK), lambda i: (0, i))
    sums = (result,) if d_n is None else (result, d_n)
    shape = jax.ShapeDtypeStruct
    return pl.pallas_call(
        functools.partial(feed_kernel, d_n is None),
        grid=(hidden // HIDDEN_BLOCK,),
        out_shape=[
            shape((rows, hidden), jnp.bfloat16),
            shape((rows, hidden), jnp.bfloat16),
            shape((1, hidden), jnp.float32),
            shape((rows, width), jnp.float32),
            shape((rows, width), jnp.float32),
        ],
        in_specs=[
            whole,
            whole,
            pl.BlockSpec((width, HIDDEN_BLOCK), lambda i: (0, i)),
            line,
            pl.BlockSpec((HIDDEN_BLOCK, width), lambda i: (i, 0)),
        ]
        + [whole] * len(sums),
        out_specs=[across, across, line, whole, whole],
        compiler_params=pltpu.CompilerParams(vmem_limit_bytes=40 * 2**20),
        cost_estimate=pl.CostEstimate(
            flops=10 * rows * width * hidden, bytes_accessed=4 * width * hidden, transcendentals=2 * rows * hidden
        ),
        name="feed",
    )(n, g, up, bias, down, *sums)


def body_rows(
    main,
    long_skip,
    cotangent,
    timesteps,
    loss_codes,
    code_weights,
    item_counts,
    w_skip_main,
    w_skip_long,
    b_skip,
    ln1_gain,
    ln1_bias,
    w_qkv,
    w_proj,
    b_proj,
    ln2_gain,
    ln2_bias,
    w_up,
    b_up,
    w_down,
    b_down,
):
    local = main.shape[1]
    width = 4 * local
    rank = lax.axis_index("tp")

    vectors = jnp.concatenate(
        [jnp.stack([b_skip, ln1_gain, ln1_bias, b_proj, ln2_gain, ln2_bias, b_down]), b_up.reshape(4, local)]
    )
    y, core, x, z = side(ACROSS_Y), side(CORE), side(ACROSS_X), side(ACROSS_Z)
    cut = 2 * local
    tokens, cot_tokens = spread(main, long_skip, cotangent)
    tokens = tokens.reshape((2, 2) + tokens.shape[1:])
    cot_tokens = cot_tokens.reshape((2, 2) + cot_tokens.shape[1:])
    quarters = lambda w: w.reshape(2, 2, -1, width)
    qkv_rows = jnp.swapaxes(w_qkv, 1, 2).reshape(3, 2, 2, local // 4, width)
    one = (4, 2, 2, local // 4, width)
    far_tokens, core_near, core_far, far_vectors, core_vectors, wskip, wq, wk, wv, wp, *wu = gather_weights(
        tokens,
        vectors,
        [
            quarters(w_skip_main),
            quarters(w_skip_long),
            qkv_rows,
            quarters(w_proj),
            w_up.reshape(2, 2, 2, width // 8, width),
        ],
        [
            (0, (), 0, (0,)),
            (1, (), 0, (1,)),
            (2, (0,), 1, ()),
            (2, (1,), 2, ()),
            (2, (2,), 3, ()),
            (3, (), 4, ()),
            (4, (0,), (5, 6, 7, 8), (0,)),
            (4, (1,), (5, 6, 7, 8), (1,)),
        ],
        [(4, 2) + one[1:], one, one, one, one] + [(2, 2, 2, width // 8, width)] * 4,
    )
    own_vectors = jnp.concatenate([vectors, far_vectors], axis=1)
    partner_vectors = jnp.concatenate([core_vectors[0], core_vectors[1]], axis=1)
    joined = jnp.concatenate(natural(own_vectors[:7], partner_vectors[:7], 1), axis=1)
    b_skip_all, gain_one, bias_one, b_proj_all, gain_two, bias_two, b_down_all = (
        joined[k : k + 1] for k in range(7)
    )

    def up_vector(pair):
        near, far = jnp.split(pair[7:], 2, 1)
        return jnp.concatenate([near.reshape(1, -1), far.reshape(1, -1)], axis=1)

    b_up_all = jnp.concatenate([up_vector(own_vectors), up_vector(partner_vectors)], axis=1)

    wskip, wq, wk, wv, wp = (g.reshape(-1, width) for g in (wskip, wq, wk, wv, wp))
    wu = [w.reshape(width, width) for w in wu]
    near_tokens = pick(tokens, y)
    skip_rows = jnp.concatenate([pick(near_tokens, core), pick(far_tokens, core), core_near, core_far], axis=1)
    other = lambda value: swap(value, CORE)
    both = lambda mine, others: jnp.concatenate([mine, others], axis=0)
    shares = lambda value: both(value[:, : value.shape[1] // 2], other(value[:, value.shape[1] // 2 :]))

    def after(value, *events):
        return lax.optimization_barrier((value,) + events)[0]

    meet = lambda *values: lax.optimization_barrier(values)

    cot_near = pick(cot_tokens, y)
    cot_far = swap(after(pick(cot_tokens, 1 - y), wskip), ACROSS_Y)
    w_down_then = after(w_down, skip_rows)
    wd_core = other(w_down_then)
    wd_y = swap(w_down_then, ACROSS_Y)

    stream = dot("td,dc->tc", skip_rows, wskip) + b_skip_all
    cot_far, stream = meet(cot_far, stream)
    normed_one, rstd_one, full_one = norm_rows(stream, gain_one, bias_one)
    skip_both = jnp.concatenate([pick(near_tokens, 1 - core), pick(far_tokens, 1 - core)], axis=1)
    skip_both = both(skip_rows[:, : 2 * cut], skip_both)
    n1_both = both(full_one, other(full_one))
    query, key, value = (low(dot("td,cd->tc", full_one, w)) for w in (wq, wk, wv))
    attended, logsum = attention(query, key, value)
    attended_both = shares(attended)
    stream_two = stream + dot("tc,cd->td", attended, wp) + b_proj_all
    stream_two, skip_both, n1_both = meet(stream_two, skip_both, n1_both)
    normed_two, rstd_two, full_two = norm_rows(stream_two, gain_two, bias_two)
    n2_both = both(full_two, other(full_two))
    cot_partner = other(jnp.stack([pick(cot_near, 1 - core), pick(cot_far, 1 - core)]))
    item_scale, valid = item_factors(timesteps, loss_codes, code_weights, item_counts[0])
    row_scale = jnp.repeat(pick(item_scale.reshape(4, -1), rank), ITEM_ROWS)[:, None]
    row_valid = jnp.repeat(pick(valid.reshape(4, -1), rank), ITEM_ROWS)[:, None]
    grad_low = arrange(pick(cot_near, core), pick(cot_far, core), cot_partner, row_scale)
    grad_both = both(grad_low, other(grad_low))
    grad_wide = grad_low.astype(jnp.float32)
    g_b_down = jnp.sum(grad_wide, 0)

    def weight_grad(left, right):
        return low(dot("tf,tc->fc", left, right))

    def split(value, bit):
        halves = value.reshape(2, -1, width)
        return pick(halves, bit), pick(halves, 1 - bit)

    result, d_n2 = stream_two + b_down_all, None
    acts, d_up, g_b_up = [None] * 4, [None] * 4, [None] * 4
    wd_y, stream_two_then = meet(wd_y, result)
    result = stream_two_then
    wd = [w_down, wd_y, wd_core, other(wd_y)]

    def run_feed(r, result, d_n2):
        bias = b_up_all[:, r * width : (r + 1) * width]
        acts[r], d_up[r], g_b_up[r], result, d_n2 = feed(full_two, grad_low, wu[r], bias, wd[r], result, d_n2)
        return result, d_n2

    for r in (1, 3):
        result, d_n2 = run_feed(r, result, d_n2)
    down_theirs = weight_grad(both(acts[1], other(acts[3])), grad_both)
    down_come = swap(down_theirs, ACROSS_Y)
    up_theirs = weight_grad(n2_both, after(both(d_up[1], other(d_up[3])), down_theirs))
    up_come = swap(up_theirs, ACROSS_Y)
    d_n2, up_theirs = meet(d_n2, up_theirs)
    result, d_n2 = run_feed(0, result, d_n2)
    result, d_n2 = run_feed(2, result, d_n2)
    g_b_up = jnp.concatenate(g_b_up)
    down_mine = weight_grad(both(acts[0], other(acts[2])), grad_both)
    up_mine = weight_grad(n2_both, both(d_up[0], other(d_up[2])))
    down_mine, up_mine = meet(down_mine, up_mine)

    outs = disperse(result, row_valid)
    out_core = other(outs[2:])
    out_y = swap(after(jnp.stack([outs[1], out_core[1]]), up_theirs), ACROSS_Y)
    back_two, g_ln2_gain, g_ln2_bias = norm_rows_back(d_n2, normed_two, rstd_two, gain_two)
    d_stream_two = low(back_two + grad_wide)
    d_stream_wide = d_stream_two.astype(jnp.float32)
    g_b_proj = jnp.sum(d_stream_wide, 0)
    chunked = lambda g, lead: g.reshape(lead + (-1, 2, 2, GRAD_ROWS, width))
    proj_part = chunked(weight_grad(attended_both, both(d_stream_two, other(d_stream_two))), (2,))
    d_attended = low(dot("tc,fc->tf", d_stream_two, wp))
    d_qkv = attention_back(query, key, value, logsum, d_attended)
    down_come, *d_qkv = meet(down_come, *d_qkv)
    down_keep, down_send = split(add_low(down_mine, down_come), x)
    down_come = swap(down_send, ACROSS_X)
    *d_qkv, d_own, d_partner = d_qkv
    qkv_part = chunked(weight_grad(both(d_own, other(d_partner)), n1_both), (3, 2))
    d_n1 = sum(dot("tc,cd->td", d, w) for d, w in zip(d_qkv, (wq, wk, wv)))
    back_one, g_ln1_gain, g_ln1_bias = norm_rows_back(d_n1, normed_one, rstd_one, gain_one)
    d_stream = low(back_one + d_stream_wide)
    d_stream_both = both(d_stream, other(d_stream))
    g_b_skip = jnp.sum(d_stream.astype(jnp.float32), 0)
    d_skip = low(dot("tc,fc->tf", d_stream, wskip))
    d_blocks = jnp.stack(jnp.split(d_skip, 4, 1))
    down_come, d_stream_both, d_blocks, proj_part, qkv_part = meet(
        down_come, d_stream_both, d_blocks, proj_part, qkv_part
    )
    down_keep, down_send = split(add_low(down_keep, down_come), z)
    down_come = swap(down_send, ACROSS_Z)
    skip_part = chunked(weight_grad(skip_both, d_stream_both), (2,))
    up_come, down_come, skip_part = meet(up_come, down_come, skip_part)
    down_quarter = add_low(down_keep, down_come)
    ready = chunked(add_low(up_mine, up_come), ())

    small = jnp.stack([g_b_skip, g_ln1_gain, g_ln1_bias, g_b_proj, g_ln2_gain, g_ln2_bias, g_b_down])
    arrived = other(jnp.concatenate([small, g_b_up[2:]]))
    small = jnp.moveaxis((small + arrived[:7]).reshape(7, 4, local), 1, 0)
    b_up_sums = g_b_up[:2] + arrived[7:]

    def vector_rows(shard, row):
        flat = jnp.concatenate([pick(small, shard).reshape(-1), b_up_sums[row]])
        return jnp.pad(flat, (0, 4 * GRAD_ROWS * width - flat.size)).reshape(1, 2, 2, GRAD_ROWS, width)

    vector_part = low(jnp.stack([vector_rows(rank, 0), vector_rows(peer(rank, 2), 1)]))
    g_w_up, *sums = reduce_grads(
        ready,
        [proj_part, qkv_part, vector_part, skip_part],
        [(0, (0,), (1,)), (1, (0, 0), (0, 1)), (1, (1, 0), (1, 1)), (1, (2, 0), (2, 1)), (2, (0,), (1,)), (3, (0,), (1,))],
        d_blocks,
        down_quarter,
    )
    *sums, from_core, y_blocks, down_quarter, z_quarter, x_quarters = sums
    out_y, y_blocks = meet(out_y, y_blocks)
    (out,) = unspread(outs[0], out_core[0], out_y, 1)
    wide = lambda value: value.reshape(-1, width).astype(jnp.float32)
    g_w_down = wide(in_order(x, in_order(z, down_quarter, z_quarter), in_order(z, x_quarters[0], x_quarters[1])))
    g_w_proj, g_q, g_k, g_v, vectors, g_skip = (wide(g) for g in sums)
    g_w_qkv = jnp.stack([g.T for g in (g_q, g_k, g_v)])
    vectors = vectors.reshape(-1)
    mine = vectors[: 7 * local].reshape(7, local)

    d_main, d_long = unspread(d_blocks[0], from_core[0], y_blocks, 2)
    return (
        out,
        d_main,
        d_long,
        g_skip[:local],
        g_skip[local:],
        mine[0],
        mine[1],
        mine[2],
        g_w_qkv,
        g_w_proj,
        mine[3],
        mine[4],
        mine[5],
        wide(g_w_up),
        vectors[7 * local : 7 * local + width],
        g_w_down,
        mine[6],
    )


def body_items(*args):
    return body_rows(*args)


def solution(mesh):
    by_items = mesh.shape["tp"] == 4 and mesh.shape["dp"] == 8
    return jax.shard_map(
        body_items if by_items else body_features,
        mesh=mesh,
        in_specs=(
            P("dp", "tp"),
            P("dp", "tp"),
            P("dp", "tp"),
            P("dp"),
            P("dp"),
            P(),
            P("dp"),
            P("tp", None),
            P("tp", None),
            P("tp"),
            P("tp"),
            P("tp"),
            P(None, None, "tp"),
            P("tp", None),
            P("tp"),
            P("tp"),
            P("tp"),
            P(None, "tp"),
            P("tp"),
            P("tp", None),
            P("tp"),
        ),
        out_specs=(
            P("dp", "tp"),
            P("dp", "tp"),
            P("dp", "tp"),
            P("tp", None),
            P("tp", None),
            P("tp"),
            P("tp"),
            P("tp"),
            P(None, None, "tp"),
            P("tp", None),
            P("tp"),
            P("tp"),
            P("tp"),
            P(None, "tp"),
            P("tp"),
            P("tp", None),
            P("tp"),
        ),
        check_vma=False,
    )
```

```python
import functools
import math

import jax
import jax.numpy as jnp
from jax import lax
from jax.experimental import pallas as pl
from jax.experimental.pallas import tpu as pltpu
from jax.sharding import PartitionSpec as P

HEAD = 72
SEQ = 258
TSTEPS = 1000


EPSILON = 1e-06
ROOT_HALF = 0.7071067811865476
DENSITY_SCALE = 0.3989422804014327


def item_factors(timesteps, loss_codes, code_weights, group_items):
    steps_float = timesteps.astype(jnp.float32)
    phase = (steps_float / TSTEPS + 0.008) / 1.008 * (math.pi / 2.0)
    cosine = jnp.cos(phase)
    signal = cosine * cosine
    weight = jnp.minimum(1.0, 5.0 * (1.0 - signal) / signal)
    picks = (
        loss_codes[:, None] == jnp.arange(code_weights.shape[0], dtype=jnp.int32)[None, :]
    ).astype(jnp.float32)
    coded = jnp.sum(picks * code_weights[None, :], axis=1)
    valid = (jnp.arange(timesteps.shape[0], dtype=jnp.int32) < group_items).astype(jnp.float32)
    return (weight * coded * valid, valid)


def layer_norm(stream, gain, bias, width):
    totals, squares = lax.psum((jnp.sum(stream, 0), jnp.sum(stream * stream, 0)), "tp")
    mean = totals / width
    rstd = lax.rsqrt(squares / width - mean * mean + EPSILON)
    normed = (stream - mean[None, :]) * rstd[None, :]
    rounded = (normed * gain[:, None] + bias[:, None]).astype(jnp.bfloat16)
    return (normed, rstd, lax.all_gather(rounded, "tp", axis=0, tiled=True))


def norm_back(d_normed, normed, rstd, gain, width):
    g_gain = jnp.sum(d_normed * normed, 1)
    g_bias = jnp.sum(d_normed, 1)
    scaled = d_normed * gain[:, None]
    first, second = lax.psum((jnp.sum(scaled, 0), jnp.sum(scaled * normed, 0)), "tp")
    back = rstd[None, :] * (scaled - first[None, :] / width - normed * second[None, :] / width)
    return (back, g_gain, g_bias)


def reduce_back(term, local_width):
    return lax.psum_scatter(
        term(jnp.int32(0), lax.axis_size("tp") * local_width).astype(jnp.bfloat16),
        "tp",
        scatter_dimension=0,
        tiled=True,
    ).astype(jnp.float32)


def fold_back(shard, pairs):
    piece = lax.all_gather(shard, "tp", axis=0, tiled=True)
    new_acts = tuple(
        (
            jnp.einsum("fc,ct->ft", weight, piece, preferred_element_type=jnp.float32)
            for weight, acts in pairs
        )
    )
    new_weights = tuple(
        (
            jnp.einsum("ft,ct->fc", acts, piece, preferred_element_type=jnp.float32)
            for weight, acts in pairs
        )
    )
    return (new_acts, new_weights)


def split_heads(flat, heads_here):
    pair_count = flat.shape[1] // (2 * SEQ)
    shaped = flat.reshape(heads_here, HEAD, pair_count, 2, SEQ)
    return jnp.moveaxis(shaped, 2, 0)


def join_heads(blocks):
    moved = jnp.moveaxis(blocks, 0, 2)
    return moved.reshape(moved.shape[0] * moved.shape[1], -1)


def attend(block):
    query_rows, key_rows, value_rows = block
    scale = 1.0 / math.sqrt(HEAD)
    scores = (
        jnp.einsum("hdbi,hdbj->hbij", query_rows, key_rows, preferred_element_type=jnp.float32)
        * scale
    )
    peak = jnp.max(scores, axis=-1, keepdims=True)
    logsum = peak + jnp.log(jnp.sum(jnp.exp(scores - peak), axis=-1, keepdims=True))
    probs = jnp.exp(scores - logsum).astype(jnp.bfloat16)
    attended = jnp.einsum("hbij,hdbj->hdbi", probs, value_rows, preferred_element_type=jnp.float32)
    return (attended.astype(jnp.bfloat16), logsum[..., 0])


def attend_back(block):
    query_rows, key_rows, value_rows, logsum, d_attended = block
    scale = 1.0 / math.sqrt(HEAD)
    scores = (
        jnp.einsum("hdbi,hdbj->hbij", query_rows, key_rows, preferred_element_type=jnp.float32)
        * scale
    )
    probs = jnp.exp(scores - logsum[..., None])
    probs_low = probs.astype(jnp.bfloat16)
    d_probs = jnp.einsum(
        "hdbi,hdbj->hbij", d_attended, value_rows, preferred_element_type=jnp.float32
    )
    delta = jnp.sum(probs * d_probs, axis=-1, keepdims=True)
    d_scores = (probs * (d_probs - delta)).astype(jnp.bfloat16)
    d_query = (
        jnp.einsum("hbij,hdbj->hdbi", d_scores, key_rows, preferred_element_type=jnp.float32)
        * scale
    )
    d_key = (
        jnp.einsum("hbij,hdbi->hdbj", d_scores, query_rows, preferred_element_type=jnp.float32)
        * scale
    )
    d_value = jnp.einsum(
        "hbij,hdbi->hdbj", probs_low, d_attended, preferred_element_type=jnp.float32
    )
    return (d_query.astype(jnp.bfloat16), d_key.astype(jnp.bfloat16), d_value.astype(jnp.bfloat16))


def body_features(
    main,
    long_skip,
    cotangent,
    timesteps,
    loss_codes,
    code_weights,
    item_counts,
    w_skip_main,
    w_skip_long,
    b_skip,
    ln1_gain,
    ln1_bias,
    w_qkv,
    w_proj,
    b_proj,
    ln2_gain,
    ln2_bias,
    w_up,
    b_up,
    w_down,
    b_down,
):
    local_width = main.shape[1]
    width = w_skip_main.shape[1]
    heads_here = local_width // HEAD
    item_scale, valid = item_factors(timesteps, loss_codes, code_weights, item_counts[0])
    row_scale = jnp.repeat(item_scale, SEQ)
    row_valid = jnp.repeat(valid, SEQ)
    main_cols = main.T
    long_cols = long_skip.T
    stream = (
        lax.psum_scatter(
            jnp.einsum("dc,dt->ct", w_skip_main, main_cols, preferred_element_type=jnp.float32)
            + jnp.einsum("dc,dt->ct", w_skip_long, long_cols, preferred_element_type=jnp.float32),
            "tp",
            scatter_dimension=0,
            tiled=True,
        )
        + b_skip[:, None]
    )
    normed_one, rstd_one, full_one = layer_norm(stream, ln1_gain, ln1_bias, width)
    qkv = jnp.einsum("edc,dt->ect", w_qkv, full_one, preferred_element_type=jnp.float32).astype(
        jnp.bfloat16
    )
    query_blocks = split_heads(qkv[0], heads_here)
    key_blocks = split_heads(qkv[1], heads_here)
    value_blocks = split_heads(qkv[2], heads_here)
    attended_blocks, logsums = lax.map(attend, (query_blocks, key_blocks, value_blocks))
    attended = join_heads(attended_blocks)
    cols_here = w_proj
    projected = lax.psum_scatter(
        jnp.einsum("rc,rt->ct", cols_here, attended, preferred_element_type=jnp.float32).astype(
            jnp.bfloat16
        ),
        "tp",
        scatter_dimension=0,
        tiled=True,
    ).astype(jnp.float32)
    stream_two = stream + projected + b_proj[:, None]
    normed_two, rstd_two, full_two = layer_norm(stream_two, ln2_gain, ln2_bias, width)
    upward = (
        jnp.einsum("dc,dt->ct", w_up, full_two, preferred_element_type=jnp.float32) + b_up[:, None]
    )
    activated = jax.nn.gelu(upward, approximate=False).astype(jnp.bfloat16)
    cols_here = w_down
    result = (
        stream_two
        + lax.psum_scatter(
            jnp.einsum(
                "fc,ft->ct", cols_here, activated, preferred_element_type=jnp.float32
            ).astype(jnp.bfloat16),
            "tp",
            scatter_dimension=0,
            tiled=True,
        ).astype(jnp.float32)
        + b_down[:, None]
    )
    out = (result * row_valid[None, :]).T.astype(jnp.bfloat16)
    grad_low = (cotangent.T.astype(jnp.float32) * row_scale[None, :]).astype(jnp.bfloat16)
    grad_wide = grad_low.astype(jnp.float32)
    g_b_down = jnp.sum(grad_wide, 1)
    (d_activated,), (g_w_down,) = fold_back(grad_low, ((w_down, activated),))
    cumulative = 0.5 * (1.0 + lax.erf(upward * ROOT_HALF))
    density = jnp.exp(-0.5 * upward * upward) * DENSITY_SCALE
    d_upward = (d_activated * (cumulative + upward * density)).astype(jnp.bfloat16)
    g_b_up = jnp.sum(d_upward.astype(jnp.float32), 1)
    g_w_up = jnp.einsum("dt,ft->df", full_two, d_upward, preferred_element_type=jnp.float32)

    def up_term(start, count_rows):
        return jnp.einsum("cf,ft->ct", w_up, d_upward, preferred_element_type=jnp.float32)

    d_normed_two = reduce_back(up_term, local_width)
    back_two, g_ln2_gain, g_ln2_bias = norm_back(
        d_normed_two, normed_two, rstd_two, ln2_gain, width
    )
    d_stream_two = (back_two + grad_wide).astype(jnp.bfloat16)
    d_stream_wide = d_stream_two.astype(jnp.float32)
    g_b_proj = jnp.sum(d_stream_wide, 1)
    (d_attended,), (g_w_proj,) = fold_back(d_stream_two, ((w_proj, attended),))
    d_attended_blocks = split_heads(d_attended.astype(jnp.bfloat16), heads_here)
    d_queries, d_keys, d_values = lax.map(
        attend_back, (query_blocks, key_blocks, value_blocks, logsums, d_attended_blocks)
    )
    d_qkv = jnp.stack([join_heads(d_queries), join_heads(d_keys), join_heads(d_values)], axis=0)
    g_w_qkv = jnp.einsum("dt,ect->edc", full_one, d_qkv, preferred_element_type=jnp.float32)

    def qkv_term(start, count_rows):
        return jnp.einsum("ecr,ert->ct", w_qkv, d_qkv, preferred_element_type=jnp.float32)

    d_normed_one = reduce_back(qkv_term, local_width)
    back_one, g_ln1_gain, g_ln1_bias = norm_back(
        d_normed_one, normed_one, rstd_one, ln1_gain, width
    )
    d_stream = (back_one + d_stream_wide).astype(jnp.bfloat16)
    g_b_skip = jnp.sum(d_stream.astype(jnp.float32), 1)
    (d_main_cols, d_long_cols), (g_w_main, g_w_long) = fold_back(
        d_stream, ((w_skip_main, main_cols), (w_skip_long, long_cols))
    )
    (
        g_w_main,
        g_w_long,
        g_b_skip,
        g_ln1_gain,
        g_ln1_bias,
        g_w_qkv,
        g_w_proj,
        g_b_proj,
        g_ln2_gain,
        g_ln2_bias,
        g_w_up,
        g_b_up,
        g_w_down,
        g_b_down,
    ) = (
        lax.psum(g_w_main.astype(jnp.bfloat16), "dp").astype(jnp.float32),
        lax.psum(g_w_long.astype(jnp.bfloat16), "dp").astype(jnp.float32),
        lax.psum(g_b_skip.astype(jnp.bfloat16), "dp").astype(jnp.float32),
        lax.psum(g_ln1_gain.astype(jnp.bfloat16), "dp").astype(jnp.float32),
        lax.psum(g_ln1_bias.astype(jnp.bfloat16), "dp").astype(jnp.float32),
        lax.psum(g_w_qkv.astype(jnp.bfloat16), "dp").astype(jnp.float32),
        lax.psum(g_w_proj.astype(jnp.bfloat16), "dp").astype(jnp.float32),
        lax.psum(g_b_proj.astype(jnp.bfloat16), "dp").astype(jnp.float32),
        lax.psum(g_ln2_gain.astype(jnp.bfloat16), "dp").astype(jnp.float32),
        lax.psum(g_ln2_bias.astype(jnp.bfloat16), "dp").astype(jnp.float32),
        lax.psum(g_w_up.astype(jnp.bfloat16), "dp").astype(jnp.float32),
        lax.psum(g_b_up.astype(jnp.bfloat16), "dp").astype(jnp.float32),
        lax.psum(g_w_down.astype(jnp.bfloat16), "dp").astype(jnp.float32),
        lax.psum(g_b_down.astype(jnp.bfloat16), "dp").astype(jnp.float32),
    )
    d_main = d_main_cols.T.astype(jnp.bfloat16)
    d_long = d_long_cols.T.astype(jnp.bfloat16)
    return (
        out,
        d_main,
        d_long,
        g_w_main,
        g_w_long,
        g_b_skip,
        g_ln1_gain,
        g_ln1_bias,
        g_w_qkv,
        g_w_proj,
        g_b_proj,
        g_ln2_gain,
        g_ln2_bias,
        g_w_up,
        g_b_up,
        g_w_down,
        g_b_down,
    )


ITEM_ROWS = 264
GRAD_ROWS = 24
CORE = ("tp", 1)
ACROSS_Y = ("tp", 2)
ACROSS_X = ("dp", 1)
ACROSS_Z = ("dp", 2)


def swap(value, link):
    axis, bit = link
    return lax.ppermute(value, axis, [(i, i ^ bit) for i in range(lax.axis_size(axis))])


def side(link):
    axis, bit = link
    return (lax.axis_index(axis) // bit) % 2


def in_order(bit, mine, theirs):
    flip = bit == 1
    return jnp.stack([jnp.where(flip, theirs, mine), jnp.where(flip, mine, theirs)])


def pick(value, index):
    return lax.dynamic_index_in_dim(value, index, 0, keepdims=False)


def peer(value, bit):
    return value + bit - 2 * bit * ((value // bit) % 2)


def greet(peers):
    barrier = pltpu.get_barrier_semaphore()
    for where in peers:
        pl.semaphore_signal(barrier, inc=1, device_id=where, device_id_type=pl.DeviceIdType.MESH)
    pl.semaphore_wait(barrier, len(peers))


def send(source, target, sems, index, where):
    return pltpu.make_async_remote_copy(
        src_ref=source,
        dst_ref=target,
        send_sem=sems.at[0, index],
        recv_sem=sems.at[1, index],
        device_id=where,
        device_id_type=pl.DeviceIdType.MESH,
    )


def gather_kernel(pieces, n_in, n_out, *refs):
    tokens, vectors, inputs = refs[0], refs[1], refs[2 : 2 + n_in]
    refs = refs[2 + n_in :]
    far_tokens, core_near, core_far, far_vectors, core_vectors = refs[:5]
    outs, held = refs[5 : 5 + n_out], refs[5 + n_out : 5 + n_out + n_in]
    y_sem, one_sem, two_sem, own_sem, far_sem, local_sem, token_sem = refs[5 + n_out + n_in :]
    n = len(pieces)
    shards = [inputs[a].at[lead] if lead else inputs[a] for a, lead, _, _ in pieces]
    stage = [held[a].at[lead] if lead else held[a] for a, lead, _, _ in pieces]
    fulls = [
        [outs[b[place]].at[tail] if isinstance(b, tuple) else outs[b].at[(place,) + tail] for place in range(4)]
        for _, _, b, tail in pieces
    ]
    dp, tp = lax.axis_index("dp"), lax.axis_index("tp")
    core, y = tp % 2, (tp // 2) % 2
    to_core, to_y = {"tp": peer(tp, 1)}, {"tp": peer(tp, 2)}
    links = ({"dp": peer(dp, 1)}, {"dp": peer(dp, 2)})
    bits = (dp % 2, (dp // 2) % 2)
    greet((to_core, to_y) + links)

    def places(k):
        return k % 2, 1 - k % 2, bits[k % 2], bits[1 - k % 2]

    def y_copy(k):
        _, _, f, s = places(k)
        return send(shards[k].at[s, f], fulls[k][1].at[s, f], y_sem, k, to_y)

    def one_copy(k):
        first, _, f, s = places(k)
        part = fulls[k][1].at[s, f]
        return send(part, part, one_sem, k, links[first])

    def two_copy(k):
        _, second, _, s = places(k)
        part = fulls[k][1].at[s]
        return send(part, part, two_sem, k, links[second])

    def own_copy(k):
        return send(shards[k], fulls[k][2], own_sem, k, to_core)

    def far_copy(k):
        return send(fulls[k][1], fulls[k][3], far_sem, k, to_core)

    def load(k):
        return pltpu.make_async_copy(shards[k], stage[k], local_sem.at[0, k])

    def store(k):
        return pltpu.make_async_copy(stage[k], fulls[k][0], local_sem.at[1, k])

    token_y = send(tokens.at[1 - y], far_tokens, token_sem, 0, to_y)
    token_near = send(tokens.at[y, 1 - core], core_near, token_sem, 1, to_core)
    token_far = send(far_tokens.at[1 - core], core_far, token_sem, 2, to_core)
    vectors_y = send(vectors, far_vectors, token_sem, 3, to_y)
    vectors_near = send(vectors, core_vectors.at[0], token_sem, 4, to_core)
    vectors_far = send(far_vectors, core_vectors.at[1], token_sem, 5, to_core)
    vectors_y.start()
    vectors_near.start()
    for k in range(n):
        y_copy(k).start()
    token_y.start()
    token_near.start()
    for k in range(n):
        load(k).start()
        own_copy(k).start()
    for step in range(n + 2):
        if step < n:
            y_copy(step).wait_recv()
            one_copy(step).start()
            load(step).wait()
            store(step).start()
        if 0 <= step - 1 < n:
            one_copy(step - 1).wait_recv()
            two_copy(step - 1).start()
        if 0 <= step - 2 < n:
            two_copy(step - 2).wait_recv()
            far_copy(step - 2).start()
    vectors_y.wait_recv()
    vectors_far.start()
    token_y.wait_recv()
    token_far.start()
    for copy in (token_near, token_far, vectors_near, vectors_far):
        copy.wait()
    token_y.wait_send()
    vectors_y.wait_send()
    for k in range(n):
        far_copy(k).wait()
        own_copy(k).wait()
        store(k).wait()
        for copy in (y_copy(k), one_copy(k), two_copy(k)):
            copy.wait_send()


def gather_weights(tokens, vectors, arrays, pieces, out_shapes):
    n = len(pieces)
    shape = lambda dims, like: jax.ShapeDtypeStruct(dims, like.dtype)
    rows = tokens.shape[2:]
    outs = [shape((2,) + rows, tokens), shape(rows, tokens), shape(rows, tokens)]
    outs += [shape(vectors.shape, vectors), shape((2,) + vectors.shape, vectors)]
    outs += [shape(dims, arrays[0]) for dims in out_shapes]
    sems = [pltpu.SemaphoreType.DMA((2, n))] * 6 + [pltpu.SemaphoreType.DMA((2, 6))]
    return pl.pallas_call(
        functools.partial(gather_kernel, pieces, len(arrays), len(out_shapes)),
        out_shape=outs,
        in_specs=[pl.BlockSpec(memory_space=pltpu.MemorySpace.HBM)] * (2 + len(arrays)),
        out_specs=[pl.BlockSpec(memory_space=pltpu.MemorySpace.HBM)] * len(outs),
        scratch_shapes=[pltpu.VMEM(a.shape, a.dtype) for a in arrays] + sems,
        compiler_params=pltpu.CompilerParams(
            collective_id=1, has_side_effects=True, vmem_limit_bytes=32 * 2**20
        ),
        name="gather_weights",
    )(tokens, vectors, *arrays)


def reduce_kernel(sizes, views, n_arrays, *refs):
    ready, arrays, blocks, quarter = refs[0], refs[1 : 1 + n_arrays], refs[1 + n_arrays], refs[2 + n_arrays]
    refs = refs[3 + n_arrays :]
    outs, refs = refs[: 1 + len(views)], refs[1 + len(views) :]
    from_core, y_blocks, own_quarter, z_quarter, x_quarters = refs[:5]
    total, from_y, from_one, half, from_two, from_far, final, part, far_part = refs[5:14]
    y_sem, one_sem, two_sem, far_sem, back_two, back_one, block_sem, load_sem, out_sem = refs[14:]
    chunks, n_ready = total.shape[0], sizes[0]
    dp, tp = lax.axis_index("dp"), lax.axis_index("tp")
    to_core, to_y, to_far = {"tp": peer(tp, 1)}, {"tp": peer(tp, 2)}, {"dp": peer(dp, 4)}
    to_x, to_z = {"dp": peer(dp, 1)}, {"dp": peer(dp, 2)}
    greet((to_core, to_y, to_x, to_z, to_far))

    def plan(s):
        z_first = (s % 4) // 3
        first, second = 1 + z_first, 2 - z_first
        places = (dp // first) % 2, (dp // second) % 2
        return ({"dp": peer(dp, first)}, {"dp": peer(dp, second)}) + places

    def y_copy(s, source):
        return send(source, from_y.at[s - n_ready], y_sem, s - n_ready, to_y)

    def one_copy(s):
        to_one, _, f, _ = plan(s)
        return send(total.at[s, 1 - f], from_one.at[s], one_sem, s, to_one)

    def two_copy(s):
        _, to_two, _, g = plan(s)
        return send(half.at[s, 1 - g], from_two.at[s], two_sem, s, to_two)

    def far_copy(s):
        _, _, _, g = plan(s)
        return send(half.at[s, g], from_far.at[s], far_sem, s, to_far)

    def back_two_copy(s):
        _, to_two, f, g = plan(s)
        part = final.at[s, f, g]
        return send(part, part, back_two, s, to_two)

    def back_one_copy(s):
        to_one, _, f, _ = plan(s)
        part = final.at[s, f]
        return send(part, part, back_one, s, to_one)

    def out_copies(s, act):
        at = 0
        for k, size in enumerate(sizes):

            @pl.when((s >= at) & (s < at + size))
            def _(k=k, at=at):
                act(pltpu.make_async_copy(final.at[s], outs[k].at[s - at], out_sem.at[s]))

            at += size

    quarter_load = pltpu.make_async_copy(quarter, part, load_sem.at[0])
    ready_load = pltpu.make_async_copy(ready, total.at[pl.ds(0, n_ready)], load_sem.at[1])
    ready_load.start()
    quarter_load.start()
    core_blocks = [send(blocks.at[2 + k], from_core.at[k], block_sem, k, to_core) for k in range(2)]
    own_block = send(blocks.at[1], y_blocks.at[0], block_sem, 2, to_y)
    core_block = send(from_core.at[1], y_blocks.at[1], block_sem, 3, to_y)
    quarter_far = send(quarter, far_part, block_sem, 4, to_far)
    quarter_z = send(own_quarter, z_quarter, block_sem, 5, to_z)
    quarter_x = send(own_quarter, x_quarters.at[0], block_sem, 6, to_x)
    quarter_zx = send(z_quarter, x_quarters.at[1], block_sem, 7, to_x)
    quarter_out = pltpu.make_async_copy(part, own_quarter, out_sem.at[chunks])
    loads, at = [], n_ready
    for k, (size, (a, mine, theirs)) in enumerate(zip(sizes[1:], views)):
        source = arrays[a].at[mine]
        loads.append(pltpu.make_async_copy(source, total.at[pl.ds(at, size)], load_sem.at[2 + k]))
        loads[-1].start()
        for r in range(size):
            y_copy(at + r, arrays[a].at[theirs + (r,)]).start()
        at += size
    for copy in core_blocks:
        copy.start()
    own_block.start()
    quarter_far.start()
    for copy in [ready_load, quarter_load] + loads:
        copy.wait()

    def plus(left, right):
        return (left.astype(jnp.float32) + right.astype(jnp.float32)).astype(jnp.bfloat16)

    def step(t, carry):
        @pl.when((t >= n_ready) & (t < chunks))
        def _():
            y_copy(t, total.at[t]).wait_recv()
            total[t] = plus(total[t], from_y[t - n_ready])

        @pl.when(t < chunks)
        def _():
            one_copy(t).start()

        @pl.when((t >= 2) & (t < chunks + 2))
        def _():
            s = t - 2
            _, _, f, _ = plan(s)
            one_copy(s).wait_recv()
            half[s] = plus(total[s, f], from_one[s])
            two_copy(s).start()

        @pl.when((t >= 3) & (t < chunks + 3))
        def _():
            s = t - 3
            _, _, _, g = plan(s)
            two_copy(s).wait_recv()
            half[s, g] = plus(half[s, g], from_two[s])
            far_copy(s).start()

        @pl.when((t >= 5) & (t < chunks + 5))
        def _():
            s = t - 5
            _, _, f, g = plan(s)
            far_copy(s).wait_recv()
            final[s, f, g] = plus(half[s, g], from_far[s])
            back_two_copy(s).start()

        @pl.when((t >= 6) & (t < chunks + 6))
        def _():
            back_two_copy(t - 6).wait_recv()
            back_one_copy(t - 6).start()

        @pl.when((t >= 7) & (t < chunks + 7))
        def _():
            back_one_copy(t - 7).wait_recv()
            out_copies(t - 7, lambda copy: copy.start())

        @pl.when(t == 2)
        def _():
            for copy in core_blocks:
                copy.wait_recv()
            core_block.start()

        @pl.when(t == 8)
        def _():
            quarter_far.wait()
            part[...] = plus(part[...], far_part[...])
            quarter_out.start()

        @pl.when(t == 9)
        def _():
            quarter_out.wait()
            quarter_z.start()
            quarter_x.start()

        @pl.when(t == 18)
        def _():
            quarter_z.wait_recv()
            quarter_zx.start()

        return carry

    lax.fori_loop(0, chunks + 7, step, 0)

    def finish_y(s, carry):
        y_copy(s, total.at[s]).wait_send()
        return carry

    lax.fori_loop(n_ready, chunks, finish_y, 0)

    def finish(s, carry):
        for copy in (one_copy(s), two_copy(s), far_copy(s), back_two_copy(s), back_one_copy(s)):
            copy.wait_send()
        out_copies(s, lambda copy: copy.wait())
        return carry

    lax.fori_loop(0, chunks, finish, 0)
    for copy in core_blocks:
        copy.wait_send()
    own_block.wait()
    core_block.wait()
    quarter_z.wait_send()
    quarter_x.wait()
    quarter_zx.wait()


def reduce_grads(ready, arrays, views, blocks, quarter):
    sizes = (ready.shape[0],) + tuple(arrays[a].shape[len(mine)] for a, mine, _ in views)
    chunks = sum(sizes)
    rows, width = ready.shape[-2:]
    kind = ready.dtype
    sem = lambda n: pltpu.SemaphoreType.DMA((2, n))
    two_blocks = jax.ShapeDtypeStruct((2,) + blocks.shape[1:], blocks.dtype)
    hbm = pl.BlockSpec(memory_space=pltpu.MemorySpace.HBM)
    vmem = lambda *lead: pltpu.VMEM(lead + (rows, width), kind)
    n_in, n_out = 3 + len(arrays), 6 + len(views)
    return pl.pallas_call(
        functools.partial(reduce_kernel, sizes, views, len(arrays)),
        out_shape=[jax.ShapeDtypeStruct((n, 2, 2, rows, width), kind) for n in sizes]
        + [two_blocks, two_blocks]
        + [jax.ShapeDtypeStruct(lead + quarter.shape, kind) for lead in ((), (), (2,))],
        in_specs=[hbm] * n_in,
        out_specs=[hbm] * n_out,
        scratch_shapes=[
            vmem(chunks, 2, 2),
            vmem(chunks - sizes[0], 2, 2),
            vmem(chunks, 2),
            vmem(chunks, 2),
            vmem(chunks),
            vmem(chunks),
            vmem(chunks, 2, 2),
            pltpu.VMEM(quarter.shape, kind),
            pltpu.VMEM(quarter.shape, kind),
            sem(chunks - sizes[0]),
            sem(chunks),
            sem(chunks),
            sem(chunks),
            sem(chunks),
            sem(chunks),
            sem(8),
            pltpu.SemaphoreType.DMA((2 + len(views),)),
            pltpu.SemaphoreType.DMA((chunks + 1,)),
        ],
        compiler_params=pltpu.CompilerParams(
            collective_id=2, has_side_effects=True, vmem_limit_bytes=56 * 2**20
        ),
        name="reduce_grads",
    )(ready, *arrays, blocks, quarter)


def add_low(mine, theirs):
    return (mine.astype(jnp.float32) + theirs.astype(jnp.float32)).astype(jnp.bfloat16)


def place_of(index):
    rank = lax.axis_index("tp")
    core, y = rank % 2, (rank // 2) % 2
    there_core, there_y = index % 2, index // 2
    apart = lambda a, b: a + b - 2 * a * b
    return apart(y, there_y) + 2 * apart(core, there_core)


def spread_kernel(main_ref, long_ref, cot_ref, tokens_ref, cot_tokens_ref):
    cols = main_ref.shape[1]
    items = tokens_ref.shape[1] // ITEM_ROWS
    for p in range(4):
        for i in range(items):
            source = slice((p * items + i) * SEQ, (p * items + i + 1) * SEQ)
            target = slice(i * ITEM_ROWS, i * ITEM_ROWS + SEQ)
            blank = slice(i * ITEM_ROWS + SEQ, (i + 1) * ITEM_ROWS)
            tokens_ref[p, target, :cols] = main_ref[source, :]
            tokens_ref[p, target, cols:] = long_ref[source, :]
            cot_tokens_ref[p, target, :] = cot_ref[source, :]
            tokens_ref[p, blank, :] = jnp.zeros((ITEM_ROWS - SEQ, 2 * cols), tokens_ref.dtype)
            cot_tokens_ref[p, blank, :] = jnp.zeros((ITEM_ROWS - SEQ, cols), tokens_ref.dtype)


def spread(main, long_skip, cotangent):
    rows, cols = main.shape
    padded = rows // SEQ // 4 * ITEM_ROWS
    return pl.pallas_call(
        spread_kernel,
        out_shape=[
            jax.ShapeDtypeStruct((4, padded, 2 * cols), main.dtype),
            jax.ShapeDtypeStruct((4, padded, cols), main.dtype),
        ],
        compiler_params=pltpu.CompilerParams(vmem_limit_bytes=40 * 2**20),
        name="spread",
    )(main, long_skip, cotangent)


def arrange_kernel(own_ref, y_ref, partner_ref, scale_ref, out_ref, held):
    cols = own_ref.shape[1]
    held[0] = own_ref[...]
    held[1] = y_ref[...]
    held[2] = partner_ref[0]
    held[3] = partner_ref[1]
    for j in range(4):
        block = held[place_of(j)].astype(jnp.float32) * scale_ref[...]
        out_ref[:, j * cols : (j + 1) * cols] = block.astype(out_ref.dtype)


def arrange(own, along_y, partner, scale):
    rows, cols = own.shape
    return pl.pallas_call(
        arrange_kernel,
        out_shape=jax.ShapeDtypeStruct((rows, 4 * cols), own.dtype),
        scratch_shapes=[pltpu.VMEM((4, rows, cols), own.dtype)],
        compiler_params=pltpu.CompilerParams(vmem_limit_bytes=24 * 2**20),
        name="arrange",
    )(own, along_y, partner, scale)


def disperse_kernel(rows_ref, valid_ref, out_ref):
    cols = out_ref.shape[2]
    for j in range(4):
        block = rows_ref[:, j * cols : (j + 1) * cols] * valid_ref[...]
        out_ref[place_of(j)] = block.astype(out_ref.dtype)


def disperse(rows, valid):
    count, width = rows.shape
    return pl.pallas_call(
        disperse_kernel,
        out_shape=jax.ShapeDtypeStruct((4, count, width // 4), jnp.bfloat16),
        compiler_params=pltpu.CompilerParams(vmem_limit_bytes=24 * 2**20),
        name="disperse",
    )(rows, valid)


def unspread_kernel(parts, own_ref, core_ref, y_ref, *refs):
    outs, held = refs[:parts], refs[parts]
    cols = outs[0].shape[1]
    items = own_ref.shape[0] // ITEM_ROWS
    held[0] = own_ref[...]
    held[1] = y_ref[0]
    held[2] = core_ref[...]
    held[3] = y_ref[1]
    for p in range(4):
        rows = held[place_of(p)]
        for i in range(items):
            target = slice((p * items + i) * SEQ, (p * items + i + 1) * SEQ)
            source = slice(i * ITEM_ROWS, i * ITEM_ROWS + SEQ)
            for k in range(parts):
                outs[k][target, :] = rows[source, k * cols : (k + 1) * cols]


def unspread(own, core_tokens, y_tokens, parts):
    rows, width = own.shape
    out = jax.ShapeDtypeStruct((4 * rows // ITEM_ROWS * SEQ, width // parts), own.dtype)
    return pl.pallas_call(
        functools.partial(unspread_kernel, parts),
        out_shape=[out] * parts,
        scratch_shapes=[pltpu.VMEM((4, rows, width), own.dtype)],
        compiler_params=pltpu.CompilerParams(vmem_limit_bytes=40 * 2**20),
        name="unspread",
    )(own, core_tokens, y_tokens)


def natural(own_half, partner_half, axis):
    flip_y, flip_core = side(ACROSS_Y) == 1, side(CORE) == 1
    r0, r2 = jnp.split(own_half, 2, axis)
    r1, r3 = jnp.split(partner_half, 2, axis)
    a0, a2 = jnp.where(flip_y, r2, r0), jnp.where(flip_y, r0, r2)
    a1, a3 = jnp.where(flip_y, r3, r1), jnp.where(flip_y, r1, r3)
    b0, b1 = jnp.where(flip_core, a1, a0), jnp.where(flip_core, a0, a1)
    b2, b3 = jnp.where(flip_core, a3, a2), jnp.where(flip_core, a2, a3)
    return (b0, b1, b2, b3)


def dot(spec, left, right):
    return jnp.einsum(spec, left, right, preferred_element_type=jnp.float32)


def low(value):
    return value.astype(jnp.bfloat16)


def norm_rows(stream, gain, bias):
    mean = jnp.mean(stream, 1, keepdims=True)
    square = jnp.mean(stream * stream, 1, keepdims=True)
    rstd = lax.rsqrt(square - mean * mean + EPSILON)
    normed = (stream - mean) * rstd
    return normed, rstd, low(normed * gain + bias)


def norm_rows_back(d_out, normed, rstd, gain):
    g_gain = jnp.sum(d_out * normed, 0)
    g_bias = jnp.sum(d_out, 0)
    scaled = d_out * gain
    first = jnp.mean(scaled, 1, keepdims=True)
    second = jnp.mean(scaled * normed, 1, keepdims=True)
    return rstd * (scaled - first - normed * second), g_gain, g_bias


LAST = (((1,), (1,)), ((), ()))
LEAD = (((0,), (0,)), ((), ()))


def item_scores(key, query):
    scores = lax.dot_general(key, query, LAST, preferred_element_type=jnp.float32)
    present = lax.broadcasted_iota(jnp.int32, scores.shape, 0) < SEQ
    return jnp.where(present, scores * (1.0 / math.sqrt(HEAD)), -1e30)


def attend_kernel(*refs):
    def item(i, carry):
        attend_item(*(ref.at[i] for ref in refs))
        return carry

    lax.fori_loop(0, refs[0].shape[0], item, 0)


def attend_item(q_ref, k_ref, v_ref, out_ref, lse_ref):
    for h in range(q_ref.shape[1] // HEAD):
        at = slice(h * HEAD, (h + 1) * HEAD)
        scores = item_scores(k_ref[:, at], q_ref[:, at])
        peak = jnp.max(scores, axis=0, keepdims=True)
        weights = jnp.exp(scores - peak)
        total = jnp.sum(weights, axis=0, keepdims=True)
        probs = (weights * (1.0 / total)).astype(jnp.bfloat16)
        out = lax.dot_general(probs, v_ref[:, at], LEAD, preferred_element_type=jnp.float32)
        out_ref[:, at] = out.astype(jnp.bfloat16)
        lse_ref[h : h + 1, :] = peak + jnp.log(total)


def attend_back_kernel(*refs):
    def item(i, carry):
        attend_back_item(*(ref.at[i] for ref in refs))
        return carry

    lax.fori_loop(0, refs[0].shape[0], item, 0)


def attend_back_item(q_ref, k_ref, v_ref, lse_ref, d_ref, dq_ref, dk_ref, dv_ref, own_ref, partner_ref):
    scale = 1.0 / math.sqrt(HEAD)
    for h in range(q_ref.shape[1] // HEAD):
        at = slice(h * HEAD, (h + 1) * HEAD)
        query, key, d_out = q_ref[:, at], k_ref[:, at], d_ref[:, at]
        probs = jnp.exp(item_scores(key, query) - lse_ref[h : h + 1, :])
        d_probs = lax.dot_general(v_ref[:, at], d_out, LAST, preferred_element_type=jnp.float32)
        delta = jnp.sum(probs * d_probs, axis=0, keepdims=True)
        d_scores = (probs * (d_probs - delta)).astype(jnp.bfloat16)
        dq = lax.dot_general(d_scores, key, LEAD, preferred_element_type=jnp.float32)
        dk = jnp.dot(d_scores, query, preferred_element_type=jnp.float32)
        dv = jnp.dot(probs.astype(jnp.bfloat16), d_out, preferred_element_type=jnp.float32)
        cols = q_ref.shape[1] // 2
        side_ref, start = (own_ref, h * HEAD) if h * HEAD < cols else (partner_ref, h * HEAD - cols)
        for e, (ref, d) in enumerate(((dq_ref, dq * scale), (dk_ref, dk * scale), (dv_ref, dv))):
            d = d.astype(jnp.bfloat16)
            ref[:, at] = d
            side_ref[:, e * cols + start : e * cols + start + HEAD] = d


def by_item(value):
    return value.reshape(-1, ITEM_ROWS, value.shape[1])


def attention(query, key, value):
    rows, cols = query.shape
    heads, items = cols // HEAD, rows // ITEM_ROWS
    out, lse = pl.pallas_call(
        attend_kernel,
        out_shape=[
            jax.ShapeDtypeStruct((items, ITEM_ROWS, cols), jnp.bfloat16),
            jax.ShapeDtypeStruct((items, heads, ITEM_ROWS), jnp.float32),
        ],
        cost_estimate=pl.CostEstimate(
            flops=4 * rows * ITEM_ROWS * cols, bytes_accessed=8 * rows * cols, transcendentals=rows * ITEM_ROWS * heads
        ),
        compiler_params=pltpu.CompilerParams(vmem_limit_bytes=24 * 2**20),
        name="attend",
    )(by_item(query), by_item(key), by_item(value))
    return out.reshape(rows, cols), lse


def attention_back(query, key, value, lse, d_out):
    rows, cols = query.shape
    heads, items = cols // HEAD, rows // ITEM_ROWS
    shape = lambda width: jax.ShapeDtypeStruct((items, ITEM_ROWS, width), jnp.bfloat16)
    outs = pl.pallas_call(
        attend_back_kernel,
        out_shape=[shape(cols)] * 3 + [shape(3 * cols // 2)] * 2,
        cost_estimate=pl.CostEstimate(
            flops=10 * rows * ITEM_ROWS * cols, bytes_accessed=14 * rows * cols, transcendentals=rows * ITEM_ROWS * heads
        ),
        compiler_params=pltpu.CompilerParams(vmem_limit_bytes=32 * 2**20),
        name="attend_back",
    )(by_item(query), by_item(key), by_item(value), lse, by_item(d_out))
    return [o.reshape(rows, -1) for o in outs]


HIDDEN_BLOCK = 384


def feed_kernel(first, n_ref, g_ref, up_ref, bias_ref, down_ref, *refs):
    sums, (act_ref, d_up_ref, g_bias_ref, result_ref, d_n_ref) = refs[:-5], refs[-5:]
    wide = jnp.float32

    @pl.when(pl.program_id(0) == 0)
    def _():
        result_ref[...] = sums[0][...]
        d_n_ref[...] = jnp.zeros_like(d_n_ref) if first else sums[1][...]

    up = jnp.dot(n_ref[...], up_ref[...], preferred_element_type=wide) + bias_ref[...]
    d_act = lax.dot_general(g_ref[...], down_ref[...], LAST, preferred_element_type=wide)
    cumulative = 0.5 * (1.0 + lax.erf(up * ROOT_HALF))
    density = jnp.exp(-0.5 * up * up) * DENSITY_SCALE
    act = (up * cumulative).astype(jnp.bfloat16)
    d_up = (d_act * (cumulative + up * density)).astype(jnp.bfloat16)
    act_ref[...] = act
    d_up_ref[...] = d_up
    g_bias_ref[...] = jnp.sum(d_up.astype(wide), axis=0, keepdims=True)
    result_ref[...] += jnp.dot(act, down_ref[...], preferred_element_type=wide)
    d_n_ref[...] += lax.dot_general(d_up, up_ref[...], LAST, preferred_element_type=wide)


def feed(n, g, up, bias, down, result, d_n):
    rows, width = n.shape
    hidden = up.shape[1]
    whole = pl.BlockSpec((rows, width), lambda i: (0, 0))
    across = pl.BlockSpec((rows, HIDDEN_BLOCK), lambda i: (0, i))
    line = pl.BlockSpec((1, HIDDEN_BLOCK), lambda i: (0, i))
    sums = (result,) if d_n is None else (result, d_n)
    shape = jax.ShapeDtypeStruct
    return pl.pallas_call(
        functools.partial(feed_kernel, d_n is None),
        grid=(hidden // HIDDEN_BLOCK,),
        out_shape=[
            shape((rows, hidden), jnp.bfloat16),
            shape((rows, hidden), jnp.bfloat16),
            shape((1, hidden), jnp.float32),
            shape((rows, width), jnp.float32),
            shape((rows, width), jnp.float32),
        ],
        in_specs=[
            whole,
            whole,
            pl.BlockSpec((width, HIDDEN_BLOCK), lambda i: (0, i)),
            line,
            pl.BlockSpec((HIDDEN_BLOCK, width), lambda i: (i, 0)),
        ]
        + [whole] * len(sums),
        out_specs=[across, across, line, whole, whole],
        compiler_params=pltpu.CompilerParams(vmem_limit_bytes=40 * 2**20),
        cost_estimate=pl.CostEstimate(
            flops=10 * rows * width * hidden, bytes_accessed=4 * width * hidden, transcendentals=2 * rows * hidden
        ),
        name="feed",
    )(n, g, up, bias, down, *sums)


def body_rows(
    main,
    long_skip,
    cotangent,
    timesteps,
    loss_codes,
    code_weights,
    item_counts,
    w_skip_main,
    w_skip_long,
    b_skip,
    ln1_gain,
    ln1_bias,
    w_qkv,
    w_proj,
    b_proj,
    ln2_gain,
    ln2_bias,
    w_up,
    b_up,
    w_down,
    b_down,
):
    local = main.shape[1]
    width = 4 * local
    rank = lax.axis_index("tp")

    vectors = jnp.concatenate(
        [jnp.stack([b_skip, ln1_gain, ln1_bias, b_proj, ln2_gain, ln2_bias, b_down]), b_up.reshape(4, local)]
    )
    y, core, x, z = side(ACROSS_Y), side(CORE), side(ACROSS_X), side(ACROSS_Z)
    cut = 2 * local
    tokens, cot_tokens = spread(main, long_skip, cotangent)
    tokens = tokens.reshape((2, 2) + tokens.shape[1:])
    cot_tokens = cot_tokens.reshape((2, 2) + cot_tokens.shape[1:])
    quarters = lambda w: w.reshape(2, 2, -1, width)
    qkv_rows = jnp.swapaxes(w_qkv, 1, 2).reshape(3, 2, 2, local // 4, width)
    one = (4, 2, 2, local // 4, width)
    far_tokens, core_near, core_far, far_vectors, core_vectors, wskip, wq, wk, wv, wp, *wu = gather_weights(
        tokens,
        vectors,
        [
            quarters(w_skip_main),
            quarters(w_skip_long),
            qkv_rows,
            quarters(w_proj),
            w_up.reshape(2, 2, 2, width // 8, width),
        ],
        [
            (0, (), 0, (0,)),
            (1, (), 0, (1,)),
            (2, (0,), 1, ()),
            (2, (1,), 2, ()),
            (2, (2,), 3, ()),
            (3, (), 4, ()),
            (4, (0,), (5, 6, 7, 8), (0,)),
            (4, (1,), (5, 6, 7, 8), (1,)),
        ],
        [(4, 2) + one[1:], one, one, one, one] + [(2, 2, 2, width // 8, width)] * 4,
    )
    own_vectors = jnp.concatenate([vectors, far_vectors], axis=1)
    partner_vectors = jnp.concatenate([core_vectors[0], core_vectors[1]], axis=1)
    joined = jnp.concatenate(natural(own_vectors[:7], partner_vectors[:7], 1), axis=1)
    b_skip_all, gain_one, bias_one, b_proj_all, gain_two, bias_two, b_down_all = (
        joined[k : k + 1] for k in range(7)
    )

    def up_vector(pair):
        near, far = jnp.split(pair[7:], 2, 1)
        return jnp.concatenate([near.reshape(1, -1), far.reshape(1, -1)], axis=1)

    b_up_all = jnp.concatenate([up_vector(own_vectors), up_vector(partner_vectors)], axis=1)

    wskip, wq, wk, wv, wp = (g.reshape(-1, width) for g in (wskip, wq, wk, wv, wp))
    wu = [w.reshape(width, width) for w in wu]
    near_tokens = pick(tokens, y)
    skip_rows = jnp.concatenate([pick(near_tokens, core), pick(far_tokens, core), core_near, core_far], axis=1)
    other = lambda value: swap(value, CORE)
    both = lambda mine, others: jnp.concatenate([mine, others], axis=0)
    shares = lambda value: both(value[:, : value.shape[1] // 2], other(value[:, value.shape[1] // 2 :]))

    def after(value, *events):
        return lax.optimization_barrier((value,) + events)[0]

    meet = lambda *values: lax.optimization_barrier(values)

    cot_near = pick(cot_tokens, y)
    cot_far = swap(after(pick(cot_tokens, 1 - y), wskip), ACROSS_Y)
    w_down_then = after(w_down, skip_rows)
    wd_core = other(w_down_then)
    wd_y = swap(w_down_then, ACROSS_Y)

    stream = dot("td,dc->tc", skip_rows, wskip) + b_skip_all
    cot_far, stream = meet(cot_far, stream)
    normed_one, rstd_one, full_one = norm_rows(stream, gain_one, bias_one)
    skip_both = jnp.concatenate([pick(near_tokens, 1 - core), pick(far_tokens, 1 - core)], axis=1)
    skip_both = both(skip_rows[:, : 2 * cut], skip_both)
    n1_both = both(full_one, other(full_one))
    query, key, value = (low(dot("td,cd->tc", full_one, w)) for w in (wq, wk, wv))
    attended, logsum = attention(query, key, value)
    attended_both = shares(attended)
    stream_two = stream + dot("tc,cd->td", attended, wp) + b_proj_all
    stream_two, skip_both, n1_both = meet(stream_two, skip_both, n1_both)
    normed_two, rstd_two, full_two = norm_rows(stream_two, gain_two, bias_two)
    n2_both = both(full_two, other(full_two))
    cot_partner = other(jnp.stack([pick(cot_near, 1 - core), pick(cot_far, 1 - core)]))
    item_scale, valid = item_factors(timesteps, loss_codes, code_weights, item_counts[0])
    row_scale = jnp.repeat(pick(item_scale.reshape(4, -1), rank), ITEM_ROWS)[:, None]
    row_valid = jnp.repeat(pick(valid.reshape(4, -1), rank), ITEM_ROWS)[:, None]
    grad_low = arrange(pick(cot_near, core), pick(cot_far, core), cot_partner, row_scale)
    grad_both = both(grad_low, other(grad_low))
    grad_wide = grad_low.astype(jnp.float32)
    g_b_down = jnp.sum(grad_wide, 0)

    def weight_grad(left, right):
        return low(dot("tf,tc->fc", left, right))

    def split(value, bit):
        halves = value.reshape(2, -1, width)
        return pick(halves, bit), pick(halves, 1 - bit)

    result, d_n2 = stream_two + b_down_all, None
    acts, d_up, g_b_up = [None] * 4, [None] * 4, [None] * 4
    wd = [w_down, None, wd_core, None]

    def run_feed(r, result, d_n2):
        bias = b_up_all[:, r * width : (r + 1) * width]
        acts[r], d_up[r], g_b_up[r], result, d_n2 = feed(full_two, grad_low, wu[r], bias, wd[r], result, d_n2)
        return result, d_n2

    for r in (0, 2, 1, 3):
        if r == 1:
            wd_y, d_n2 = meet(wd_y, d_n2)
            wd[1], wd[3] = wd_y, other(wd_y)
        result, d_n2 = run_feed(r, result, d_n2)
    down_theirs = weight_grad(both(acts[1], other(acts[3])), grad_both)
    down_come = swap(down_theirs, ACROSS_Y)
    up_theirs = weight_grad(n2_both, after(both(d_up[1], other(d_up[3])), down_theirs))
    up_come = swap(up_theirs, ACROSS_Y)
    d_n2, result, acts[0], d_up[0], up_theirs = meet(d_n2, result, acts[0], d_up[0], up_theirs)
    g_b_up = jnp.concatenate(g_b_up)
    down_mine = weight_grad(both(acts[0], other(acts[2])), grad_both)
    up_mine = weight_grad(n2_both, both(d_up[0], other(d_up[2])))
    down_mine, up_mine = meet(down_mine, up_mine)

    outs = disperse(result, row_valid)
    d_n2 = after(d_n2, outs)
    out_core = other(outs[2:])
    out_y = swap(after(jnp.stack([outs[1], out_core[1]]), up_theirs), ACROSS_Y)
    back_two, g_ln2_gain, g_ln2_bias = norm_rows_back(d_n2, normed_two, rstd_two, gain_two)
    d_stream_two = low(back_two + grad_wide)
    d_stream_wide = d_stream_two.astype(jnp.float32)
    g_b_proj = jnp.sum(d_stream_wide, 0)
    chunked = lambda g, lead: g.reshape(lead + (-1, 2, 2, GRAD_ROWS, width))
    proj_part = chunked(weight_grad(attended_both, both(d_stream_two, other(d_stream_two))), (2,))
    d_attended = low(dot("tc,fc->tf", d_stream_two, wp))
    d_qkv = attention_back(query, key, value, logsum, d_attended)
    *d_qkv, d_own, d_partner = d_qkv
    d_n1 = sum(dot("tc,cd->td", d, w) for d, w in zip(d_qkv, (wq, wk, wv)))
    back_one, g_ln1_gain, g_ln1_bias = norm_rows_back(d_n1, normed_one, rstd_one, gain_one)
    d_stream = low(back_one + d_stream_wide)
    d_stream_both = both(d_stream, other(d_stream))
    g_b_skip = jnp.sum(d_stream.astype(jnp.float32), 0)
    d_skip = low(dot("tc,fc->tf", d_stream, wskip))
    d_blocks = jnp.stack(jnp.split(d_skip, 4, 1))
    down_come, d_blocks, proj_part, n1_both = meet(down_come, d_blocks, proj_part, n1_both)
    down_keep, down_send = split(add_low(down_mine, down_come), x)
    down_come = swap(down_send, ACROSS_X)
    qkv_part = chunked(weight_grad(both(d_own, other(d_partner)), n1_both), (3, 2))
    skip_part = chunked(weight_grad(skip_both, d_stream_both), (2,))
    down_come, skip_part, qkv_part = meet(down_come, skip_part, qkv_part)
    down_keep, down_send = split(add_low(down_keep, down_come), z)
    down_come = swap(down_send, ACROSS_Z)
    up_come, skip_part = meet(up_come, skip_part)
    down_quarter = add_low(down_keep, down_come)
    ready = chunked(add_low(up_mine, up_come), ())

    small = jnp.stack([g_b_skip, g_ln1_gain, g_ln1_bias, g_b_proj, g_ln2_gain, g_ln2_bias, g_b_down])
    arrived = other(jnp.concatenate([small, g_b_up[2:]]))
    small = jnp.moveaxis((small + arrived[:7]).reshape(7, 4, local), 1, 0)
    b_up_sums = g_b_up[:2] + arrived[7:]

    def vector_rows(shard, row):
        flat = jnp.concatenate([pick(small, shard).reshape(-1), b_up_sums[row]])
        return jnp.pad(flat, (0, 4 * GRAD_ROWS * width - flat.size)).reshape(1, 2, 2, GRAD_ROWS, width)

    vector_part = low(jnp.stack([vector_rows(rank, 0), vector_rows(peer(rank, 2), 1)]))
    g_w_up, *sums = reduce_grads(
        ready,
        [proj_part, qkv_part, vector_part, skip_part],
        [(0, (0,), (1,)), (1, (0, 0), (0, 1)), (1, (1, 0), (1, 1)), (1, (2, 0), (2, 1)), (2, (0,), (1,)), (3, (0,), (1,))],
        d_blocks,
        down_quarter,
    )
    *sums, from_core, y_blocks, down_quarter, z_quarter, x_quarters = sums
    out_y, y_blocks = meet(out_y, y_blocks)
    (out,) = unspread(outs[0], out_core[0], out_y, 1)
    wide = lambda value: value.reshape(-1, width).astype(jnp.float32)
    g_w_down = wide(in_order(x, in_order(z, down_quarter, z_quarter), in_order(z, x_quarters[0], x_quarters[1])))
    g_w_proj, g_q, g_k, g_v, vectors, g_skip = (wide(g) for g in sums)
    g_w_qkv = jnp.stack([g.T for g in (g_q, g_k, g_v)])
    vectors = vectors.reshape(-1)
    mine = vectors[: 7 * local].reshape(7, local)

    d_main, d_long = unspread(d_blocks[0], from_core[0], y_blocks, 2)
    return (
        out,
        d_main,
        d_long,
        g_skip[:local],
        g_skip[local:],
        mine[0],
        mine[1],
        mine[2],
        g_w_qkv,
        g_w_proj,
        mine[3],
        mine[4],
        mine[5],
        wide(g_w_up),
        vectors[7 * local : 7 * local + width],
        g_w_down,
        mine[6],
    )


def body_items(*args):
    return body_rows(*args)


def solution(mesh):
    by_items = mesh.shape["tp"] == 4 and mesh.shape["dp"] == 8
    return jax.shard_map(
        body_items if by_items else body_features,
        mesh=mesh,
        in_specs=(
            P("dp", "tp"),
            P("dp", "tp"),
            P("dp", "tp"),
            P("dp"),
            P("dp"),
            P(),
            P("dp"),
            P("tp", None),
            P("tp", None),
            P("tp"),
            P("tp"),
            P("tp"),
            P(None, None, "tp"),
            P("tp", None),
            P("tp"),
            P("tp"),
            P("tp"),
            P(None, "tp"),
            P("tp"),
            P("tp", None),
            P("tp"),
        ),
        out_specs=(
            P("dp", "tp"),
            P("dp", "tp"),
            P("dp", "tp"),
            P("tp", None),
            P("tp", None),
            P("tp"),
            P("tp"),
            P("tp"),
            P(None, None, "tp"),
            P("tp", None),
            P("tp"),
            P("tp"),
            P("tp"),
            P(None, "tp"),
            P("tp"),
            P("tp", None),
            P("tp"),
        ),
        check_vma=False,
    )
```

```python
import functools
import math

import jax
import jax.numpy as jnp
from jax import lax
from jax.experimental import pallas as pl
from jax.experimental.pallas import tpu as pltpu
from jax.sharding import PartitionSpec as P

HEAD = 72
SEQ = 258
TSTEPS = 1000


EPSILON = 1e-06
ROOT_HALF = 0.7071067811865476
DENSITY_SCALE = 0.3989422804014327


def item_factors(timesteps, loss_codes, code_weights, group_items):
    steps_float = timesteps.astype(jnp.float32)
    phase = (steps_float / TSTEPS + 0.008) / 1.008 * (math.pi / 2.0)
    cosine = jnp.cos(phase)
    signal = cosine * cosine
    weight = jnp.minimum(1.0, 5.0 * (1.0 - signal) / signal)
    picks = (
        loss_codes[:, None] == jnp.arange(code_weights.shape[0], dtype=jnp.int32)[None, :]
    ).astype(jnp.float32)
    coded = jnp.sum(picks * code_weights[None, :], axis=1)
    valid = (jnp.arange(timesteps.shape[0], dtype=jnp.int32) < group_items).astype(jnp.float32)
    return (weight * coded * valid, valid)


def layer_norm(stream, gain, bias, width):
    totals, squares = lax.psum((jnp.sum(stream, 0), jnp.sum(stream * stream, 0)), "tp")
    mean = totals / width
    rstd = lax.rsqrt(squares / width - mean * mean + EPSILON)
    normed = (stream - mean[None, :]) * rstd[None, :]
    rounded = (normed * gain[:, None] + bias[:, None]).astype(jnp.bfloat16)
    return (normed, rstd, lax.all_gather(rounded, "tp", axis=0, tiled=True))


def norm_back(d_normed, normed, rstd, gain, width):
    g_gain = jnp.sum(d_normed * normed, 1)
    g_bias = jnp.sum(d_normed, 1)
    scaled = d_normed * gain[:, None]
    first, second = lax.psum((jnp.sum(scaled, 0), jnp.sum(scaled * normed, 0)), "tp")
    back = rstd[None, :] * (scaled - first[None, :] / width - normed * second[None, :] / width)
    return (back, g_gain, g_bias)


def reduce_back(term, local_width):
    return lax.psum_scatter(
        term(jnp.int32(0), lax.axis_size("tp") * local_width).astype(jnp.bfloat16),
        "tp",
        scatter_dimension=0,
        tiled=True,
    ).astype(jnp.float32)


def fold_back(shard, pairs):
    piece = lax.all_gather(shard, "tp", axis=0, tiled=True)
    new_acts = tuple(
        (
            jnp.einsum("fc,ct->ft", weight, piece, preferred_element_type=jnp.float32)
            for weight, acts in pairs
        )
    )
    new_weights = tuple(
        (
            jnp.einsum("ft,ct->fc", acts, piece, preferred_element_type=jnp.float32)
            for weight, acts in pairs
        )
    )
    return (new_acts, new_weights)


def split_heads(flat, heads_here):
    pair_count = flat.shape[1] // (2 * SEQ)
    shaped = flat.reshape(heads_here, HEAD, pair_count, 2, SEQ)
    return jnp.moveaxis(shaped, 2, 0)


def join_heads(blocks):
    moved = jnp.moveaxis(blocks, 0, 2)
    return moved.reshape(moved.shape[0] * moved.shape[1], -1)


def attend(block):
    query_rows, key_rows, value_rows = block
    scale = 1.0 / math.sqrt(HEAD)
    scores = (
        jnp.einsum("hdbi,hdbj->hbij", query_rows, key_rows, preferred_element_type=jnp.float32)
        * scale
    )
    peak = jnp.max(scores, axis=-1, keepdims=True)
    logsum = peak + jnp.log(jnp.sum(jnp.exp(scores - peak), axis=-1, keepdims=True))
    probs = jnp.exp(scores - logsum).astype(jnp.bfloat16)
    attended = jnp.einsum("hbij,hdbj->hdbi", probs, value_rows, preferred_element_type=jnp.float32)
    return (attended.astype(jnp.bfloat16), logsum[..., 0])


def attend_back(block):
    query_rows, key_rows, value_rows, logsum, d_attended = block
    scale = 1.0 / math.sqrt(HEAD)
    scores = (
        jnp.einsum("hdbi,hdbj->hbij", query_rows, key_rows, preferred_element_type=jnp.float32)
        * scale
    )
    probs = jnp.exp(scores - logsum[..., None])
    probs_low = probs.astype(jnp.bfloat16)
    d_probs = jnp.einsum(
        "hdbi,hdbj->hbij", d_attended, value_rows, preferred_element_type=jnp.float32
    )
    delta = jnp.sum(probs * d_probs, axis=-1, keepdims=True)
    d_scores = (probs * (d_probs - delta)).astype(jnp.bfloat16)
    d_query = (
        jnp.einsum("hbij,hdbj->hdbi", d_scores, key_rows, preferred_element_type=jnp.float32)
        * scale
    )
    d_key = (
        jnp.einsum("hbij,hdbi->hdbj", d_scores, query_rows, preferred_element_type=jnp.float32)
        * scale
    )
    d_value = jnp.einsum(
        "hbij,hdbi->hdbj", probs_low, d_attended, preferred_element_type=jnp.float32
    )
    return (d_query.astype(jnp.bfloat16), d_key.astype(jnp.bfloat16), d_value.astype(jnp.bfloat16))


def body_features(
    main,
    long_skip,
    cotangent,
    timesteps,
    loss_codes,
    code_weights,
    item_counts,
    w_skip_main,
    w_skip_long,
    b_skip,
    ln1_gain,
    ln1_bias,
    w_qkv,
    w_proj,
    b_proj,
    ln2_gain,
    ln2_bias,
    w_up,
    b_up,
    w_down,
    b_down,
):
    local_width = main.shape[1]
    width = w_skip_main.shape[1]
    heads_here = local_width // HEAD
    item_scale, valid = item_factors(timesteps, loss_codes, code_weights, item_counts[0])
    row_scale = jnp.repeat(item_scale, SEQ)
    row_valid = jnp.repeat(valid, SEQ)
    main_cols = main.T
    long_cols = long_skip.T
    stream = (
        lax.psum_scatter(
            jnp.einsum("dc,dt->ct", w_skip_main, main_cols, preferred_element_type=jnp.float32)
            + jnp.einsum("dc,dt->ct", w_skip_long, long_cols, preferred_element_type=jnp.float32),
            "tp",
            scatter_dimension=0,
            tiled=True,
        )
        + b_skip[:, None]
    )
    normed_one, rstd_one, full_one = layer_norm(stream, ln1_gain, ln1_bias, width)
    qkv = jnp.einsum("edc,dt->ect", w_qkv, full_one, preferred_element_type=jnp.float32).astype(
        jnp.bfloat16
    )
    query_blocks = split_heads(qkv[0], heads_here)
    key_blocks = split_heads(qkv[1], heads_here)
    value_blocks = split_heads(qkv[2], heads_here)
    attended_blocks, logsums = lax.map(attend, (query_blocks, key_blocks, value_blocks))
    attended = join_heads(attended_blocks)
    cols_here = w_proj
    projected = lax.psum_scatter(
        jnp.einsum("rc,rt->ct", cols_here, attended, preferred_element_type=jnp.float32).astype(
            jnp.bfloat16
        ),
        "tp",
        scatter_dimension=0,
        tiled=True,
    ).astype(jnp.float32)
    stream_two = stream + projected + b_proj[:, None]
    normed_two, rstd_two, full_two = layer_norm(stream_two, ln2_gain, ln2_bias, width)
    upward = (
        jnp.einsum("dc,dt->ct", w_up, full_two, preferred_element_type=jnp.float32) + b_up[:, None]
    )
    activated = jax.nn.gelu(upward, approximate=False).astype(jnp.bfloat16)
    cols_here = w_down
    result = (
        stream_two
        + lax.psum_scatter(
            jnp.einsum(
                "fc,ft->ct", cols_here, activated, preferred_element_type=jnp.float32
            ).astype(jnp.bfloat16),
            "tp",
            scatter_dimension=0,
            tiled=True,
        ).astype(jnp.float32)
        + b_down[:, None]
    )
    out = (result * row_valid[None, :]).T.astype(jnp.bfloat16)
    grad_low = (cotangent.T.astype(jnp.float32) * row_scale[None, :]).astype(jnp.bfloat16)
    grad_wide = grad_low.astype(jnp.float32)
    g_b_down = jnp.sum(grad_wide, 1)
    (d_activated,), (g_w_down,) = fold_back(grad_low, ((w_down, activated),))
    cumulative = 0.5 * (1.0 + lax.erf(upward * ROOT_HALF))
    density = jnp.exp(-0.5 * upward * upward) * DENSITY_SCALE
    d_upward = (d_activated * (cumulative + upward * density)).astype(jnp.bfloat16)
    g_b_up = jnp.sum(d_upward.astype(jnp.float32), 1)
    g_w_up = jnp.einsum("dt,ft->df", full_two, d_upward, preferred_element_type=jnp.float32)

    def up_term(start, count_rows):
        return jnp.einsum("cf,ft->ct", w_up, d_upward, preferred_element_type=jnp.float32)

    d_normed_two = reduce_back(up_term, local_width)
    back_two, g_ln2_gain, g_ln2_bias = norm_back(
        d_normed_two, normed_two, rstd_two, ln2_gain, width
    )
    d_stream_two = (back_two + grad_wide).astype(jnp.bfloat16)
    d_stream_wide = d_stream_two.astype(jnp.float32)
    g_b_proj = jnp.sum(d_stream_wide, 1)
    (d_attended,), (g_w_proj,) = fold_back(d_stream_two, ((w_proj, attended),))
    d_attended_blocks = split_heads(d_attended.astype(jnp.bfloat16), heads_here)
    d_queries, d_keys, d_values = lax.map(
        attend_back, (query_blocks, key_blocks, value_blocks, logsums, d_attended_blocks)
    )
    d_qkv = jnp.stack([join_heads(d_queries), join_heads(d_keys), join_heads(d_values)], axis=0)
    g_w_qkv = jnp.einsum("dt,ect->edc", full_one, d_qkv, preferred_element_type=jnp.float32)

    def qkv_term(start, count_rows):
        return jnp.einsum("ecr,ert->ct", w_qkv, d_qkv, preferred_element_type=jnp.float32)

    d_normed_one = reduce_back(qkv_term, local_width)
    back_one, g_ln1_gain, g_ln1_bias = norm_back(
        d_normed_one, normed_one, rstd_one, ln1_gain, width
    )
    d_stream = (back_one + d_stream_wide).astype(jnp.bfloat16)
    g_b_skip = jnp.sum(d_stream.astype(jnp.float32), 1)
    (d_main_cols, d_long_cols), (g_w_main, g_w_long) = fold_back(
        d_stream, ((w_skip_main, main_cols), (w_skip_long, long_cols))
    )
    (
        g_w_main,
        g_w_long,
        g_b_skip,
        g_ln1_gain,
        g_ln1_bias,
        g_w_qkv,
        g_w_proj,
        g_b_proj,
        g_ln2_gain,
        g_ln2_bias,
        g_w_up,
        g_b_up,
        g_w_down,
        g_b_down,
    ) = (
        lax.psum(g_w_main.astype(jnp.bfloat16), "dp").astype(jnp.float32),
        lax.psum(g_w_long.astype(jnp.bfloat16), "dp").astype(jnp.float32),
        lax.psum(g_b_skip.astype(jnp.bfloat16), "dp").astype(jnp.float32),
        lax.psum(g_ln1_gain.astype(jnp.bfloat16), "dp").astype(jnp.float32),
        lax.psum(g_ln1_bias.astype(jnp.bfloat16), "dp").astype(jnp.float32),
        lax.psum(g_w_qkv.astype(jnp.bfloat16), "dp").astype(jnp.float32),
        lax.psum(g_w_proj.astype(jnp.bfloat16), "dp").astype(jnp.float32),
        lax.psum(g_b_proj.astype(jnp.bfloat16), "dp").astype(jnp.float32),
        lax.psum(g_ln2_gain.astype(jnp.bfloat16), "dp").astype(jnp.float32),
        lax.psum(g_ln2_bias.astype(jnp.bfloat16), "dp").astype(jnp.float32),
        lax.psum(g_w_up.astype(jnp.bfloat16), "dp").astype(jnp.float32),
        lax.psum(g_b_up.astype(jnp.bfloat16), "dp").astype(jnp.float32),
        lax.psum(g_w_down.astype(jnp.bfloat16), "dp").astype(jnp.float32),
        lax.psum(g_b_down.astype(jnp.bfloat16), "dp").astype(jnp.float32),
    )
    d_main = d_main_cols.T.astype(jnp.bfloat16)
    d_long = d_long_cols.T.astype(jnp.bfloat16)
    return (
        out,
        d_main,
        d_long,
        g_w_main,
        g_w_long,
        g_b_skip,
        g_ln1_gain,
        g_ln1_bias,
        g_w_qkv,
        g_w_proj,
        g_b_proj,
        g_ln2_gain,
        g_ln2_bias,
        g_w_up,
        g_b_up,
        g_w_down,
        g_b_down,
    )


ITEM_ROWS = 264
GRAD_ROWS = 24
CORE = ("tp", 1)
ACROSS_Y = ("tp", 2)


def swap(value, link):
    axis, bit = link
    return lax.ppermute(value, axis, [(i, i ^ bit) for i in range(lax.axis_size(axis))])


def side(link):
    axis, bit = link
    return (lax.axis_index(axis) // bit) % 2


def pick(value, index):
    return lax.dynamic_index_in_dim(value, index, 0, keepdims=False)


def peer(value, bit):
    return value + bit - 2 * bit * ((value // bit) % 2)


def greet(peers):
    barrier = pltpu.get_barrier_semaphore()
    for where in peers:
        pl.semaphore_signal(barrier, inc=1, device_id=where, device_id_type=pl.DeviceIdType.MESH)
    pl.semaphore_wait(barrier, len(peers))


def send(source, target, sems, index, where):
    return pltpu.make_async_remote_copy(
        src_ref=source,
        dst_ref=target,
        send_sem=sems.at[0, index],
        recv_sem=sems.at[1, index],
        device_id=where,
        device_id_type=pl.DeviceIdType.MESH,
    )


def gather_kernel(pieces, n_in, n_out, *refs):
    tokens, vectors, inputs = refs[0], refs[1], refs[2 : 2 + n_in]
    refs = refs[2 + n_in :]
    far_tokens, core_near, core_far, far_vectors, core_vectors = refs[:5]
    outs, held = refs[5 : 5 + n_out], refs[5 + n_out : 5 + n_out + n_in]
    y_sem, one_sem, two_sem, own_sem, far_sem, local_sem, token_sem = refs[5 + n_out + n_in :]
    n = len(pieces)
    shards = [inputs[a].at[lead] if lead else inputs[a] for a, lead, _, _ in pieces]
    stage = [held[a].at[lead] if lead else held[a] for a, lead, _, _ in pieces]
    fulls = [
        [outs[b[place]].at[tail] if isinstance(b, tuple) else outs[b].at[(place,) + tail] for place in range(4)]
        for _, _, b, tail in pieces
    ]
    dp, tp = lax.axis_index("dp"), lax.axis_index("tp")
    core, y = tp % 2, (tp // 2) % 2
    to_core, to_y = {"tp": peer(tp, 1)}, {"tp": peer(tp, 2)}
    links = ({"dp": peer(dp, 1)}, {"dp": peer(dp, 2)})
    bits = (dp % 2, (dp // 2) % 2)
    greet((to_core, to_y) + links)

    def places(k):
        return k % 2, 1 - k % 2, bits[k % 2], bits[1 - k % 2]

    def y_copy(k):
        _, _, f, s = places(k)
        return send(shards[k].at[s, f], fulls[k][1].at[s, f], y_sem, k, to_y)

    def one_copy(k):
        first, _, f, s = places(k)
        part = fulls[k][1].at[s, f]
        return send(part, part, one_sem, k, links[first])

    def two_copy(k):
        _, second, _, s = places(k)
        part = fulls[k][1].at[s]
        return send(part, part, two_sem, k, links[second])

    def own_copy(k):
        return send(shards[k], fulls[k][2], own_sem, k, to_core)

    def far_copy(k):
        return send(fulls[k][1], fulls[k][3], far_sem, k, to_core)

    def load(k):
        return pltpu.make_async_copy(shards[k], stage[k], local_sem.at[0, k])

    def store(k):
        return pltpu.make_async_copy(stage[k], fulls[k][0], local_sem.at[1, k])

    token_y = send(tokens.at[1 - y], far_tokens, token_sem, 0, to_y)
    token_near = send(tokens.at[y, 1 - core], core_near, token_sem, 1, to_core)
    token_far = send(far_tokens.at[1 - core], core_far, token_sem, 2, to_core)
    vectors_y = send(vectors, far_vectors, token_sem, 3, to_y)
    vectors_near = send(vectors, core_vectors.at[0], token_sem, 4, to_core)
    vectors_far = send(far_vectors, core_vectors.at[1], token_sem, 5, to_core)
    vectors_y.start()
    vectors_near.start()
    for k in range(n):
        y_copy(k).start()
    token_y.start()
    token_near.start()
    for k in range(n):
        load(k).start()
        own_copy(k).start()
    for step in range(n + 2):
        if step < n:
            y_copy(step).wait_recv()
            one_copy(step).start()
            load(step).wait()
            store(step).start()
        if 0 <= step - 1 < n:
            one_copy(step - 1).wait_recv()
            two_copy(step - 1).start()
        if 0 <= step - 2 < n:
            two_copy(step - 2).wait_recv()
            far_copy(step - 2).start()
    vectors_y.wait_recv()
    vectors_far.start()
    token_y.wait_recv()
    token_far.start()
    for copy in (token_near, token_far, vectors_near, vectors_far):
        copy.wait()
    token_y.wait_send()
    vectors_y.wait_send()
    for k in range(n):
        far_copy(k).wait()
        own_copy(k).wait()
        store(k).wait()
        for copy in (y_copy(k), one_copy(k), two_copy(k)):
            copy.wait_send()


def gather_weights(tokens, vectors, arrays, pieces, out_shapes):
    n = len(pieces)
    shape = lambda dims, like: jax.ShapeDtypeStruct(dims, like.dtype)
    rows = tokens.shape[2:]
    outs = [shape((2,) + rows, tokens), shape(rows, tokens), shape(rows, tokens)]
    outs += [shape(vectors.shape, vectors), shape((2,) + vectors.shape, vectors)]
    outs += [shape(dims, arrays[0]) for dims in out_shapes]
    sems = [pltpu.SemaphoreType.DMA((2, n))] * 6 + [pltpu.SemaphoreType.DMA((2, 6))]
    return pl.pallas_call(
        functools.partial(gather_kernel, pieces, len(arrays), len(out_shapes)),
        out_shape=outs,
        in_specs=[pl.BlockSpec(memory_space=pltpu.MemorySpace.HBM)] * (2 + len(arrays)),
        out_specs=[pl.BlockSpec(memory_space=pltpu.MemorySpace.HBM)] * len(outs),
        scratch_shapes=[pltpu.VMEM(a.shape, a.dtype) for a in arrays] + sems,
        compiler_params=pltpu.CompilerParams(
            collective_id=1, has_side_effects=True, vmem_limit_bytes=32 * 2**20
        ),
        name="gather_weights",
    )(tokens, vectors, *arrays)


def reduce_kernel(sizes, views, n_arrays, *refs):
    ready, arrays, blocks = refs[0], refs[1 : 1 + n_arrays], refs[1 + n_arrays]
    refs = refs[2 + n_arrays :]
    outs, refs = refs[: 1 + len(views)], refs[1 + len(views) :]
    from_core, y_blocks = refs[:2]
    total, from_y, from_one, half, from_two, from_far, final = refs[2:9]
    y_sem, one_sem, two_sem, far_sem, back_two, back_one, block_sem, load_sem, out_sem = refs[9:]
    chunks, n_ready = total.shape[0], sizes[0]
    dp, tp = lax.axis_index("dp"), lax.axis_index("tp")
    to_core, to_y, to_far = {"tp": peer(tp, 1)}, {"tp": peer(tp, 2)}, {"dp": peer(dp, 4)}
    greet((to_core, to_y, {"dp": peer(dp, 1)}, {"dp": peer(dp, 2)}, to_far))

    def plan(s):
        z_first = (s % 4) // 3
        first, second = 1 + z_first, 2 - z_first
        places = (dp // first) % 2, (dp // second) % 2
        return ({"dp": peer(dp, first)}, {"dp": peer(dp, second)}) + places

    def y_copy(s, source):
        return send(source, from_y.at[s - n_ready], y_sem, s - n_ready, to_y)

    def one_copy(s):
        to_one, _, f, _ = plan(s)
        return send(total.at[s, 1 - f], from_one.at[s], one_sem, s, to_one)

    def two_copy(s):
        _, to_two, _, g = plan(s)
        return send(half.at[s, 1 - g], from_two.at[s], two_sem, s, to_two)

    def far_copy(s):
        _, _, _, g = plan(s)
        return send(half.at[s, g], from_far.at[s], far_sem, s, to_far)

    def back_two_copy(s):
        _, to_two, f, g = plan(s)
        part = final.at[s, f, g]
        return send(part, part, back_two, s, to_two)

    def back_one_copy(s):
        to_one, _, f, _ = plan(s)
        part = final.at[s, f]
        return send(part, part, back_one, s, to_one)

    def out_copies(s, act):
        at = 0
        for k, size in enumerate(sizes):

            @pl.when((s >= at) & (s < at + size))
            def _(k=k, at=at):
                act(pltpu.make_async_copy(final.at[s], outs[k].at[s - at], out_sem.at[s]))

            at += size

    ready_load = pltpu.make_async_copy(ready, total.at[pl.ds(0, n_ready)], load_sem.at[0])
    ready_load.start()
    core_blocks = [send(blocks.at[2 + k], from_core.at[k], block_sem, k, to_core) for k in range(2)]
    own_block = send(blocks.at[1], y_blocks.at[0], block_sem, 2, to_y)
    core_block = send(from_core.at[1], y_blocks.at[1], block_sem, 3, to_y)
    loads, at = [], n_ready
    for k, (size, (a, mine, theirs)) in enumerate(zip(sizes[1:], views)):
        source = arrays[a].at[mine]
        loads.append(pltpu.make_async_copy(source, total.at[pl.ds(at, size)], load_sem.at[1 + k]))
        loads[-1].start()
        for r in range(size):
            y_copy(at + r, arrays[a].at[theirs + (r,)]).start()
        at += size
    for copy in core_blocks:
        copy.start()
    own_block.start()
    for copy in [ready_load] + loads:
        copy.wait()

    def plus(left, right):
        return (left.astype(jnp.float32) + right.astype(jnp.float32)).astype(jnp.bfloat16)

    def step(t, carry):
        @pl.when((t >= n_ready) & (t < chunks))
        def _():
            y_copy(t, total.at[t]).wait_recv()
            total[t] = plus(total[t], from_y[t - n_ready])

        @pl.when(t < chunks)
        def _():
            one_copy(t).start()

        @pl.when((t >= 2) & (t < chunks + 2))
        def _():
            s = t - 2
            _, _, f, _ = plan(s)
            one_copy(s).wait_recv()
            half[s] = plus(total[s, f], from_one[s])
            two_copy(s).start()

        @pl.when((t >= 3) & (t < chunks + 3))
        def _():
            s = t - 3
            _, _, _, g = plan(s)
            two_copy(s).wait_recv()
            half[s, g] = plus(half[s, g], from_two[s])
            far_copy(s).start()

        @pl.when((t >= 5) & (t < chunks + 5))
        def _():
            s = t - 5
            _, _, f, g = plan(s)
            far_copy(s).wait_recv()
            final[s, f, g] = plus(half[s, g], from_far[s])
            back_two_copy(s).start()

        @pl.when((t >= 6) & (t < chunks + 6))
        def _():
            back_two_copy(t - 6).wait_recv()
            back_one_copy(t - 6).start()

        @pl.when((t >= 7) & (t < chunks + 7))
        def _():
            back_one_copy(t - 7).wait_recv()
            out_copies(t - 7, lambda copy: copy.start())

        @pl.when(t == 2)
        def _():
            for copy in core_blocks:
                copy.wait_recv()
            core_block.start()

        return carry

    lax.fori_loop(0, chunks + 7, step, 0)

    def finish_y(s, carry):
        y_copy(s, total.at[s]).wait_send()
        return carry

    lax.fori_loop(n_ready, chunks, finish_y, 0)

    def finish(s, carry):
        for copy in (one_copy(s), two_copy(s), far_copy(s), back_two_copy(s), back_one_copy(s)):
            copy.wait_send()
        out_copies(s, lambda copy: copy.wait())
        return carry

    lax.fori_loop(0, chunks, finish, 0)
    for copy in core_blocks:
        copy.wait_send()
    own_block.wait()
    core_block.wait()


def reduce_grads(ready, arrays, views, blocks):
    sizes = (ready.shape[0],) + tuple(arrays[a].shape[len(mine)] for a, mine, _ in views)
    chunks = sum(sizes)
    rows, width = ready.shape[-2:]
    kind = ready.dtype
    sem = lambda n: pltpu.SemaphoreType.DMA((2, n))
    two_blocks = jax.ShapeDtypeStruct((2,) + blocks.shape[1:], blocks.dtype)
    hbm = pl.BlockSpec(memory_space=pltpu.MemorySpace.HBM)
    vmem = lambda *lead: pltpu.VMEM(lead + (rows, width), kind)
    n_in, n_out = 2 + len(arrays), 3 + len(views)
    return pl.pallas_call(
        functools.partial(reduce_kernel, sizes, views, len(arrays)),
        out_shape=[jax.ShapeDtypeStruct((n, 2, 2, rows, width), kind) for n in sizes]
        + [two_blocks, two_blocks],
        in_specs=[hbm] * n_in,
        out_specs=[hbm] * n_out,
        scratch_shapes=[
            vmem(chunks, 2, 2),
            vmem(chunks - sizes[0], 2, 2),
            vmem(chunks, 2),
            vmem(chunks, 2),
            vmem(chunks),
            vmem(chunks),
            vmem(chunks, 2, 2),
            sem(chunks - sizes[0]),
            sem(chunks),
            sem(chunks),
            sem(chunks),
            sem(chunks),
            sem(chunks),
            sem(4),
            pltpu.SemaphoreType.DMA((1 + len(views),)),
            pltpu.SemaphoreType.DMA((chunks,)),
        ],
        compiler_params=pltpu.CompilerParams(
            collective_id=2, has_side_effects=True, vmem_limit_bytes=56 * 2**20
        ),
        name="reduce_grads",
    )(ready, *arrays, blocks)


def add_low(mine, theirs):
    return (mine.astype(jnp.float32) + theirs.astype(jnp.float32)).astype(jnp.bfloat16)


def place_of(index):
    rank = lax.axis_index("tp")
    core, y = rank % 2, (rank // 2) % 2
    there_core, there_y = index % 2, index // 2
    apart = lambda a, b: a + b - 2 * a * b
    return apart(y, there_y) + 2 * apart(core, there_core)


def spread_kernel(main_ref, long_ref, cot_ref, tokens_ref, cot_tokens_ref):
    cols = main_ref.shape[1]
    items = tokens_ref.shape[1] // ITEM_ROWS
    for p in range(4):
        for i in range(items):
            source = slice((p * items + i) * SEQ, (p * items + i + 1) * SEQ)
            target = slice(i * ITEM_ROWS, i * ITEM_ROWS + SEQ)
            blank = slice(i * ITEM_ROWS + SEQ, (i + 1) * ITEM_ROWS)
            tokens_ref[p, target, :cols] = main_ref[source, :]
            tokens_ref[p, target, cols:] = long_ref[source, :]
            cot_tokens_ref[p, target, :] = cot_ref[source, :]
            tokens_ref[p, blank, :] = jnp.zeros((ITEM_ROWS - SEQ, 2 * cols), tokens_ref.dtype)
            cot_tokens_ref[p, blank, :] = jnp.zeros((ITEM_ROWS - SEQ, cols), tokens_ref.dtype)


def spread(main, long_skip, cotangent):
    rows, cols = main.shape
    padded = rows // SEQ // 4 * ITEM_ROWS
    return pl.pallas_call(
        spread_kernel,
        out_shape=[
            jax.ShapeDtypeStruct((4, padded, 2 * cols), main.dtype),
            jax.ShapeDtypeStruct((4, padded, cols), main.dtype),
        ],
        compiler_params=pltpu.CompilerParams(vmem_limit_bytes=40 * 2**20),
        name="spread",
    )(main, long_skip, cotangent)


def arrange_kernel(own_ref, y_ref, partner_ref, scale_ref, out_ref, held):
    cols = own_ref.shape[1]
    held[0] = own_ref[...]
    held[1] = y_ref[...]
    held[2] = partner_ref[0]
    held[3] = partner_ref[1]
    for j in range(4):
        block = held[place_of(j)].astype(jnp.float32) * scale_ref[...]
        out_ref[:, j * cols : (j + 1) * cols] = block.astype(out_ref.dtype)


def arrange(own, along_y, partner, scale):
    rows, cols = own.shape
    return pl.pallas_call(
        arrange_kernel,
        out_shape=jax.ShapeDtypeStruct((rows, 4 * cols), own.dtype),
        scratch_shapes=[pltpu.VMEM((4, rows, cols), own.dtype)],
        compiler_params=pltpu.CompilerParams(vmem_limit_bytes=24 * 2**20),
        name="arrange",
    )(own, along_y, partner, scale)


def disperse_kernel(rows_ref, valid_ref, out_ref):
    cols = out_ref.shape[2]
    for j in range(4):
        block = rows_ref[:, j * cols : (j + 1) * cols] * valid_ref[...]
        out_ref[place_of(j)] = block.astype(out_ref.dtype)


def disperse(rows, valid):
    count, width = rows.shape
    return pl.pallas_call(
        disperse_kernel,
        out_shape=jax.ShapeDtypeStruct((4, count, width // 4), jnp.bfloat16),
        compiler_params=pltpu.CompilerParams(vmem_limit_bytes=24 * 2**20),
        name="disperse",
    )(rows, valid)


def unspread_kernel(parts, own_ref, core_ref, y_ref, *refs):
    outs, held = refs[:parts], refs[parts]
    cols = outs[0].shape[1]
    items = own_ref.shape[0] // ITEM_ROWS
    held[0] = own_ref[...]
    held[1] = y_ref[0]
    held[2] = core_ref[...]
    held[3] = y_ref[1]
    for p in range(4):
        rows = held[place_of(p)]
        for i in range(items):
            target = slice((p * items + i) * SEQ, (p * items + i + 1) * SEQ)
            source = slice(i * ITEM_ROWS, i * ITEM_ROWS + SEQ)
            for k in range(parts):
                outs[k][target, :] = rows[source, k * cols : (k + 1) * cols]


def unspread(own, core_tokens, y_tokens, parts):
    rows, width = own.shape
    out = jax.ShapeDtypeStruct((4 * rows // ITEM_ROWS * SEQ, width // parts), own.dtype)
    return pl.pallas_call(
        functools.partial(unspread_kernel, parts),
        out_shape=[out] * parts,
        scratch_shapes=[pltpu.VMEM((4, rows, width), own.dtype)],
        compiler_params=pltpu.CompilerParams(vmem_limit_bytes=40 * 2**20),
        name="unspread",
    )(own, core_tokens, y_tokens)


def natural(own_half, partner_half, axis):
    flip_y, flip_core = side(ACROSS_Y) == 1, side(CORE) == 1
    r0, r2 = jnp.split(own_half, 2, axis)
    r1, r3 = jnp.split(partner_half, 2, axis)
    a0, a2 = jnp.where(flip_y, r2, r0), jnp.where(flip_y, r0, r2)
    a1, a3 = jnp.where(flip_y, r3, r1), jnp.where(flip_y, r1, r3)
    b0, b1 = jnp.where(flip_core, a1, a0), jnp.where(flip_core, a0, a1)
    b2, b3 = jnp.where(flip_core, a3, a2), jnp.where(flip_core, a2, a3)
    return (b0, b1, b2, b3)


def dot(spec, left, right):
    return jnp.einsum(spec, left, right, preferred_element_type=jnp.float32)


def low(value):
    return value.astype(jnp.bfloat16)


def norm_rows(stream, gain, bias):
    mean = jnp.mean(stream, 1, keepdims=True)
    square = jnp.mean(stream * stream, 1, keepdims=True)
    rstd = lax.rsqrt(square - mean * mean + EPSILON)
    normed = (stream - mean) * rstd
    return normed, rstd, low(normed * gain + bias)


def norm_rows_back(d_out, normed, rstd, gain):
    g_gain = jnp.sum(d_out * normed, 0)
    g_bias = jnp.sum(d_out, 0)
    scaled = d_out * gain
    first = jnp.mean(scaled, 1, keepdims=True)
    second = jnp.mean(scaled * normed, 1, keepdims=True)
    return rstd * (scaled - first - normed * second), g_gain, g_bias


LAST = (((1,), (1,)), ((), ()))
LEAD = (((0,), (0,)), ((), ()))


def item_scores(key, query):
    scores = lax.dot_general(key, query, LAST, preferred_element_type=jnp.float32)
    present = lax.broadcasted_iota(jnp.int32, scores.shape, 0) < SEQ
    return jnp.where(present, scores * (1.0 / math.sqrt(HEAD)), -1e30)


def attend_kernel(*refs):
    def item(i, carry):
        attend_item(*(ref.at[i] for ref in refs))
        return carry

    lax.fori_loop(0, refs[0].shape[0], item, 0)


def attend_item(q_ref, k_ref, v_ref, out_ref, lse_ref):
    for h in range(q_ref.shape[1] // HEAD):
        at = slice(h * HEAD, (h + 1) * HEAD)
        scores = item_scores(k_ref[:, at], q_ref[:, at])
        peak = jnp.max(scores, axis=0, keepdims=True)
        weights = jnp.exp(scores - peak)
        total = jnp.sum(weights, axis=0, keepdims=True)
        probs = (weights * (1.0 / total)).astype(jnp.bfloat16)
        out = lax.dot_general(probs, v_ref[:, at], LEAD, preferred_element_type=jnp.float32)
        out_ref[:, at] = out.astype(jnp.bfloat16)
        lse_ref[h : h + 1, :] = peak + jnp.log(total)


def attend_back_kernel(*refs):
    def item(i, carry):
        attend_back_item(*(ref.at[i] for ref in refs))
        return carry

    lax.fori_loop(0, refs[0].shape[0], item, 0)


def attend_back_item(q_ref, k_ref, v_ref, lse_ref, d_ref, dq_ref, dk_ref, dv_ref, own_ref, partner_ref):
    scale = 1.0 / math.sqrt(HEAD)
    for h in range(q_ref.shape[1] // HEAD):
        at = slice(h * HEAD, (h + 1) * HEAD)
        query, key, d_out = q_ref[:, at], k_ref[:, at], d_ref[:, at]
        probs = jnp.exp(item_scores(key, query) - lse_ref[h : h + 1, :])
        d_probs = lax.dot_general(v_ref[:, at], d_out, LAST, preferred_element_type=jnp.float32)
        delta = jnp.sum(probs * d_probs, axis=0, keepdims=True)
        d_scores = (probs * (d_probs - delta)).astype(jnp.bfloat16)
        dq = lax.dot_general(d_scores, key, LEAD, preferred_element_type=jnp.float32)
        dk = jnp.dot(d_scores, query, preferred_element_type=jnp.float32)
        dv = jnp.dot(probs.astype(jnp.bfloat16), d_out, preferred_element_type=jnp.float32)
        cols = q_ref.shape[1] // 2
        side_ref, start = (own_ref, h * HEAD) if h * HEAD < cols else (partner_ref, h * HEAD - cols)
        for e, (ref, d) in enumerate(((dq_ref, dq * scale), (dk_ref, dk * scale), (dv_ref, dv))):
            d = d.astype(jnp.bfloat16)
            ref[:, at] = d
            side_ref[:, e * cols + start : e * cols + start + HEAD] = d


def by_item(value):
    return value.reshape(-1, ITEM_ROWS, value.shape[1])


def attention(query, key, value):
    rows, cols = query.shape
    heads, items = cols // HEAD, rows // ITEM_ROWS
    out, lse = pl.pallas_call(
        attend_kernel,
        out_shape=[
            jax.ShapeDtypeStruct((items, ITEM_ROWS, cols), jnp.bfloat16),
            jax.ShapeDtypeStruct((items, heads, ITEM_ROWS), jnp.float32),
        ],
        cost_estimate=pl.CostEstimate(
            flops=4 * rows * ITEM_ROWS * cols, bytes_accessed=8 * rows * cols, transcendentals=rows * ITEM_ROWS * heads
        ),
        compiler_params=pltpu.CompilerParams(vmem_limit_bytes=24 * 2**20),
        name="attend",
    )(by_item(query), by_item(key), by_item(value))
    return out.reshape(rows, cols), lse


def attention_back(query, key, value, lse, d_out):
    rows, cols = query.shape
    heads, items = cols // HEAD, rows // ITEM_ROWS
    shape = lambda width: jax.ShapeDtypeStruct((items, ITEM_ROWS, width), jnp.bfloat16)
    outs = pl.pallas_call(
        attend_back_kernel,
        out_shape=[shape(cols)] * 3 + [shape(3 * cols // 2)] * 2,
        cost_estimate=pl.CostEstimate(
            flops=10 * rows * ITEM_ROWS * cols, bytes_accessed=14 * rows * cols, transcendentals=rows * ITEM_ROWS * heads
        ),
        compiler_params=pltpu.CompilerParams(vmem_limit_bytes=32 * 2**20),
        name="attend_back",
    )(by_item(query), by_item(key), by_item(value), lse, by_item(d_out))
    return [o.reshape(rows, -1) for o in outs]


HIDDEN_BLOCK = 384


def feed_kernel(first, n_ref, g_ref, up_ref, bias_ref, down_ref, *refs):
    sums, (act_ref, d_up_ref, g_bias_ref, result_ref, d_n_ref) = refs[:-5], refs[-5:]
    wide = jnp.float32

    @pl.when(pl.program_id(0) == 0)
    def _():
        result_ref[...] = sums[0][...]
        d_n_ref[...] = jnp.zeros_like(d_n_ref) if first else sums[1][...]

    up = jnp.dot(n_ref[...], up_ref[...], preferred_element_type=wide) + bias_ref[...]
    d_act = lax.dot_general(g_ref[...], down_ref[...], LAST, preferred_element_type=wide)
    cumulative = 0.5 * (1.0 + lax.erf(up * ROOT_HALF))
    density = jnp.exp(-0.5 * up * up) * DENSITY_SCALE
    act = (up * cumulative).astype(jnp.bfloat16)
    d_up = (d_act * (cumulative + up * density)).astype(jnp.bfloat16)
    act_ref[...] = act
    d_up_ref[...] = d_up
    g_bias_ref[...] = jnp.sum(d_up.astype(wide), axis=0, keepdims=True)
    result_ref[...] += jnp.dot(act, down_ref[...], preferred_element_type=wide)
    d_n_ref[...] += lax.dot_general(d_up, up_ref[...], LAST, preferred_element_type=wide)


def feed(n, g, up, bias, down, result, d_n):
    rows, width = n.shape
    hidden = up.shape[1]
    whole = pl.BlockSpec((rows, width), lambda i: (0, 0))
    across = pl.BlockSpec((rows, HIDDEN_BLOCK), lambda i: (0, i))
    line = pl.BlockSpec((1, HIDDEN_BLOCK), lambda i: (0, i))
    sums = (result,) if d_n is None else (result, d_n)
    shape = jax.ShapeDtypeStruct
    return pl.pallas_call(
        functools.partial(feed_kernel, d_n is None),
        grid=(hidden // HIDDEN_BLOCK,),
        out_shape=[
            shape((rows, hidden), jnp.bfloat16),
            shape((rows, hidden), jnp.bfloat16),
            shape((1, hidden), jnp.float32),
            shape((rows, width), jnp.float32),
            shape((rows, width), jnp.float32),
        ],
        in_specs=[
            whole,
            whole,
            pl.BlockSpec((width, HIDDEN_BLOCK), lambda i: (0, i)),
            line,
            pl.BlockSpec((HIDDEN_BLOCK, width), lambda i: (i, 0)),
        ]
        + [whole] * len(sums),
        out_specs=[across, across, line, whole, whole],
        compiler_params=pltpu.CompilerParams(vmem_limit_bytes=40 * 2**20),
        cost_estimate=pl.CostEstimate(
            flops=10 * rows * width * hidden, bytes_accessed=4 * width * hidden, transcendentals=2 * rows * hidden
        ),
        name="feed",
    )(n, g, up, bias, down, *sums)


def body_rows(
    main,
    long_skip,
    cotangent,
    timesteps,
    loss_codes,
    code_weights,
    item_counts,
    w_skip_main,
    w_skip_long,
    b_skip,
    ln1_gain,
    ln1_bias,
    w_qkv,
    w_proj,
    b_proj,
    ln2_gain,
    ln2_bias,
    w_up,
    b_up,
    w_down,
    b_down,
):
    local = main.shape[1]
    width = 4 * local
    rank = lax.axis_index("tp")

    vectors = jnp.concatenate(
        [jnp.stack([b_skip, ln1_gain, ln1_bias, b_proj, ln2_gain, ln2_bias, b_down]), b_up.reshape(4, local)]
    )
    y, core = side(ACROSS_Y), side(CORE)
    cut = 2 * local
    tokens, cot_tokens = spread(main, long_skip, cotangent)
    tokens = tokens.reshape((2, 2) + tokens.shape[1:])
    cot_tokens = cot_tokens.reshape((2, 2) + cot_tokens.shape[1:])
    quarters = lambda w: w.reshape(2, 2, -1, width)
    qkv_rows = jnp.swapaxes(w_qkv, 1, 2).reshape(3, 2, 2, local // 4, width)
    one = (4, 2, 2, local // 4, width)
    far_tokens, core_near, core_far, far_vectors, core_vectors, wskip, wq, wk, wv, wp, *wu = gather_weights(
        tokens,
        vectors,
        [
            quarters(w_skip_main),
            quarters(w_skip_long),
            qkv_rows,
            quarters(w_proj),
            w_up.reshape(2, 2, 2, width // 8, width),
        ],
        [
            (0, (), 0, (0,)),
            (1, (), 0, (1,)),
            (2, (0,), 1, ()),
            (2, (1,), 2, ()),
            (2, (2,), 3, ()),
            (3, (), 4, ()),
            (4, (0,), (5, 6, 7, 8), (0,)),
            (4, (1,), (5, 6, 7, 8), (1,)),
        ],
        [(4, 2) + one[1:], one, one, one, one] + [(2, 2, 2, width // 8, width)] * 4,
    )
    own_vectors = jnp.concatenate([vectors, far_vectors], axis=1)
    partner_vectors = jnp.concatenate([core_vectors[0], core_vectors[1]], axis=1)
    joined = jnp.concatenate(natural(own_vectors[:7], partner_vectors[:7], 1), axis=1)
    b_skip_all, gain_one, bias_one, b_proj_all, gain_two, bias_two, b_down_all = (
        joined[k : k + 1] for k in range(7)
    )

    def up_vector(pair):
        near, far = jnp.split(pair[7:], 2, 1)
        return jnp.concatenate([near.reshape(1, -1), far.reshape(1, -1)], axis=1)

    b_up_all = jnp.concatenate([up_vector(own_vectors), up_vector(partner_vectors)], axis=1)

    wskip, wq, wk, wv, wp = (g.reshape(-1, width) for g in (wskip, wq, wk, wv, wp))
    wu = [w.reshape(width, width) for w in wu]
    near_tokens = pick(tokens, y)
    skip_rows = jnp.concatenate([pick(near_tokens, core), pick(far_tokens, core), core_near, core_far], axis=1)
    other = lambda value: swap(value, CORE)
    both = lambda mine, others: jnp.concatenate([mine, others], axis=0)
    shares = lambda value: both(value[:, : value.shape[1] // 2], other(value[:, value.shape[1] // 2 :]))

    def after(value, *events):
        return lax.optimization_barrier((value,) + events)[0]

    meet = lambda *values: lax.optimization_barrier(values)

    cot_near = pick(cot_tokens, y)
    cot_far = swap(after(pick(cot_tokens, 1 - y), wskip), ACROSS_Y)
    w_down_then = after(w_down, skip_rows)
    wd_core = other(w_down_then)
    wd_y = swap(w_down_then, ACROSS_Y)

    stream = dot("td,dc->tc", skip_rows, wskip) + b_skip_all
    cot_far, stream = meet(cot_far, stream)
    normed_one, rstd_one, full_one = norm_rows(stream, gain_one, bias_one)
    skip_both = jnp.concatenate([pick(near_tokens, 1 - core), pick(far_tokens, 1 - core)], axis=1)
    skip_both = both(skip_rows[:, : 2 * cut], skip_both)
    n1_both = both(full_one, other(full_one))
    query, key, value = (low(dot("td,cd->tc", full_one, w)) for w in (wq, wk, wv))
    attended, logsum = attention(query, key, value)
    attended_both = shares(attended)
    stream_two = stream + dot("tc,cd->td", attended, wp) + b_proj_all
    stream_two, skip_both, n1_both = meet(stream_two, skip_both, n1_both)
    normed_two, rstd_two, full_two = norm_rows(stream_two, gain_two, bias_two)
    n2_both = both(full_two, other(full_two))
    cot_partner = other(jnp.stack([pick(cot_near, 1 - core), pick(cot_far, 1 - core)]))
    item_scale, valid = item_factors(timesteps, loss_codes, code_weights, item_counts[0])
    row_scale = jnp.repeat(pick(item_scale.reshape(4, -1), rank), ITEM_ROWS)[:, None]
    row_valid = jnp.repeat(pick(valid.reshape(4, -1), rank), ITEM_ROWS)[:, None]
    grad_low = arrange(pick(cot_near, core), pick(cot_far, core), cot_partner, row_scale)
    grad_both = both(grad_low, other(grad_low))
    grad_wide = grad_low.astype(jnp.float32)
    g_b_down = jnp.sum(grad_wide, 0)

    def weight_grad(left, right):
        return low(dot("tf,tc->fc", left, right))

    result, d_n2 = stream_two + b_down_all, None
    acts, d_up, g_b_up = [None] * 4, [None] * 4, [None] * 4
    wd = [w_down, None, wd_core, None]

    def run_feed(r, result, d_n2):
        bias = b_up_all[:, r * width : (r + 1) * width]
        acts[r], d_up[r], g_b_up[r], result, d_n2 = feed(full_two, grad_low, wu[r], bias, wd[r], result, d_n2)
        return result, d_n2

    for r in (0, 2, 1, 3):
        if r == 1:
            wd_y, d_n2 = meet(wd_y, d_n2)
            wd[1], wd[3] = wd_y, other(wd_y)
        result, d_n2 = run_feed(r, result, d_n2)
    down_theirs = weight_grad(both(acts[1], other(acts[3])), grad_both)
    down_come = swap(down_theirs, ACROSS_Y)
    up_theirs = weight_grad(n2_both, after(both(d_up[1], other(d_up[3])), down_theirs))
    up_come = swap(up_theirs[:cut], ACROSS_Y)
    d_n2, result, acts[0], d_up[0], up_theirs = meet(d_n2, result, acts[0], d_up[0], up_theirs)
    g_b_up = jnp.concatenate(g_b_up)
    down_mine = weight_grad(both(acts[0], other(acts[2])), grad_both)
    up_mine = weight_grad(n2_both, both(d_up[0], other(d_up[2])))
    down_mine, up_mine = meet(down_mine, up_mine)

    outs = disperse(result, row_valid)
    d_n2 = after(d_n2, outs)
    out_core = other(outs[2:])
    out_y = swap(after(jnp.stack([outs[1], out_core[1]]), up_theirs), ACROSS_Y)
    back_two, g_ln2_gain, g_ln2_bias = norm_rows_back(d_n2, normed_two, rstd_two, gain_two)
    d_stream_two = low(back_two + grad_wide)
    d_stream_wide = d_stream_two.astype(jnp.float32)
    g_b_proj = jnp.sum(d_stream_wide, 0)
    chunked = lambda g, lead: g.reshape(lead + (-1, 2, 2, GRAD_ROWS, width))
    proj_part = chunked(weight_grad(attended_both, both(d_stream_two, other(d_stream_two))), (2,))
    d_attended = low(dot("tc,fc->tf", d_stream_two, wp))
    d_qkv = attention_back(query, key, value, logsum, d_attended)
    *d_qkv, d_own, d_partner = d_qkv
    d_n1 = sum(dot("tc,cd->td", d, w) for d, w in zip(d_qkv, (wq, wk, wv)))
    back_one, g_ln1_gain, g_ln1_bias = norm_rows_back(d_n1, normed_one, rstd_one, gain_one)
    d_stream = low(back_one + d_stream_wide)
    d_stream_both = both(d_stream, other(d_stream))
    g_b_skip = jnp.sum(d_stream.astype(jnp.float32), 0)
    d_skip = low(dot("tc,fc->tf", d_stream, wskip))
    d_blocks = jnp.stack(jnp.split(d_skip, 4, 1))
    qkv_part = chunked(weight_grad(both(d_own, other(d_partner)), n1_both), (3, 2))
    skip_part = chunked(weight_grad(skip_both, d_stream_both), (2,))
    up_part = chunked(jnp.stack([up_mine[cut:], up_theirs[cut:]]), (2,))
    down_come, up_come, skip_part = meet(down_come, up_come, skip_part)
    ready = chunked(jnp.concatenate([add_low(down_mine, down_come), add_low(up_mine[:cut], up_come)]), ())

    small = jnp.stack([g_b_skip, g_ln1_gain, g_ln1_bias, g_b_proj, g_ln2_gain, g_ln2_bias, g_b_down])
    arrived = other(jnp.concatenate([small, g_b_up[2:]]))
    small = jnp.moveaxis((small + arrived[:7]).reshape(7, 4, local), 1, 0)
    b_up_sums = g_b_up[:2] + arrived[7:]

    def vector_rows(shard, row):
        flat = jnp.concatenate([pick(small, shard).reshape(-1), b_up_sums[row]])
        return jnp.pad(flat, (0, 4 * GRAD_ROWS * width - flat.size)).reshape(1, 2, 2, GRAD_ROWS, width)

    vector_part = low(jnp.stack([vector_rows(rank, 0), vector_rows(peer(rank, 2), 1)]))
    g_ready, *sums = reduce_grads(
        ready,
        [up_part, proj_part, qkv_part, vector_part, skip_part],
        [(0, (0,), (1,)), (1, (0,), (1,))]
        + [(2, (e, 0), (e, 1)) for e in range(3)]
        + [(3, (0,), (1,)), (4, (0,), (1,))],
        d_blocks,
    )
    *sums, from_core, y_blocks = sums
    out_y, y_blocks = meet(out_y, y_blocks)
    (out,) = unspread(outs[0], out_core[0], out_y, 1)
    wide = lambda value: value.reshape(-1, width).astype(jnp.float32)
    g_ready = g_ready.reshape(-1, width)
    g_w_down = wide(g_ready[:width])
    g_up_low, g_w_proj, g_q, g_k, g_v, vectors, g_skip = (wide(g) for g in sums)
    g_w_up = jnp.concatenate([wide(g_ready[width:]), g_up_low])
    g_w_qkv = jnp.stack([g.T for g in (g_q, g_k, g_v)])
    vectors = vectors.reshape(-1)
    mine = vectors[: 7 * local].reshape(7, local)

    d_main, d_long = unspread(d_blocks[0], from_core[0], y_blocks, 2)
    return (
        out,
        d_main,
        d_long,
        g_skip[:local],
        g_skip[local:],
        mine[0],
        mine[1],
        mine[2],
        g_w_qkv,
        g_w_proj,
        mine[3],
        mine[4],
        mine[5],
        g_w_up,
        vectors[7 * local : 7 * local + width],
        g_w_down,
        mine[6],
    )


def body_items(*args):
    return body_rows(*args)


def solution(mesh):
    by_items = mesh.shape["tp"] == 4 and mesh.shape["dp"] == 8
    return jax.shard_map(
        body_items if by_items else body_features,
        mesh=mesh,
        in_specs=(
            P("dp", "tp"),
            P("dp", "tp"),
            P("dp", "tp"),
            P("dp"),
            P("dp"),
            P(),
            P("dp"),
            P("tp", None),
            P("tp", None),
            P("tp"),
            P("tp"),
            P("tp"),
            P(None, None, "tp"),
            P("tp", None),
            P("tp"),
            P("tp"),
            P("tp"),
            P(None, "tp"),
            P("tp"),
            P("tp", None),
            P("tp"),
        ),
        out_specs=(
            P("dp", "tp"),
            P("dp", "tp"),
            P("dp", "tp"),
            P("tp", None),
            P("tp", None),
            P("tp"),
            P("tp"),
            P("tp"),
            P(None, None, "tp"),
            P("tp", None),
            P("tp"),
            P("tp"),
            P("tp"),
            P(None, "tp"),
            P("tp"),
            P("tp", None),
            P("tp"),
        ),
        check_vma=False,
    )
```
